32 devices in a mesh: dp: 4 (over z), col: 2 (over y), row: 4 (over x, core).
Axes of the slice: x: 2, y: 2, z: 4, core: 2. Of those that a mesh axis runs over, the one named last changes fastest.
Arguments:
- x_attn: bfloat16 [4096, 2048], P('dp', 'row')
- dy_attn: bfloat16 [4096, 2048], P('dp', 'col')
- x_mlp: bfloat16 [4096, 2048], P('dp', 'row')
- dy_gate: bfloat16 [4096, 16384], P('dp', 'col')
- dy_up: bfloat16 [4096, 16384], P('dp', 'col')
- h_mlp: bfloat16 [4096, 16384], P('dp', 'row')
- dy_out: bfloat16 [4096, 2048], P('dp', 'col')
- w_attn: float32 [2048, 2048], P('row', 'col')
- w_gate: float32 [2048, 16384], P('row', 'col')
- w_up: float32 [2048, 16384], P('row', 'col')
- w_down: float32 [16384, 2048], P('row', 'col')
- r_attn: float32 [2048], P('row')
- c_attn: float32 [2048], P('col')
- r_gate: float32 [2048], P('row')
- c_gate: float32 [16384], P('col')
- r_up: float32 [2048], P('row')
- c_up: float32 [16384], P('col')
- r_down: float32 [16384], P('row')
- c_down: float32 [2048], P('col')
- hyper_params: float32 [3], replicated
Outputs:
- output 1: float32 [2048, 2048], P('row', 'col')
- output 2: float32 [2048], P('row')
- output 3: float32 [2048], P('col')
- output 4: float32 [2048, 16384], P('row', 'col')
- output 5: float32 [2048], P('row')
- output 6: float32 [16384], P('col')
- output 7: float32 [2048, 16384], P('row', 'col')
- output 8: float32 [2048], P('row')
- output 9: float32 [16384], P('col')
- output 10: float32 [16384, 2048], P('row', 'col')
- output 11: float32 [16384], P('row')
- output 12: float32 [2048], P('col')
All inputs are finite; a program needn't handle non-finite values.
Results may differ from the reference program's by a relative error of at most 0.001.
Values are sent between devices in bfloat16 or wider.
A program may use at most 1 GiB of HBM per device.

```python
import jax
import jax.numpy as jnp

D_MODEL = 2048
D_FF = 16384
TOKENS = 4096

EPS_ONE = 1e-30
EPS_TWO = 1e-3


def draw_act(key, rows, cols, scale):
    k_val, k_slope, k_one, k_two = jax.random.split(key, 4)
    position = jnp.linspace(-1.0, 1.0, cols)
    slope_val = jax.random.uniform(k_slope, (), jnp.float32, 0.8, 1.2)
    up_scale = jnp.exp(0.5 * slope_val * position) * jax.random.uniform(k_one, (cols,), jnp.float32, 0.7, 1.3)
    down_scale = jnp.exp(-0.5 * slope_val * position) * jax.random.uniform(k_two, (cols,), jnp.float32, 0.7, 1.3)
    group_scale = jnp.stack([up_scale, down_scale])
    values = jax.random.normal(k_val, (2, rows // 2, cols), jnp.float32) * group_scale[:, None, :]
    return (values.reshape(rows, cols) * scale).astype(jnp.bfloat16)


def draw_weight(key, rows, cols):
    k_val, k_row, k_col = jax.random.split(key, 3)
    row_trend = jax.random.uniform(k_row, (), jnp.float32, 0.8, 1.2) * jnp.linspace(-0.5, 0.5, rows)
    col_trend = jax.random.uniform(k_col, (), jnp.float32, 0.8, 1.2) * jnp.linspace(-0.5, 0.5, cols)
    values = jax.random.normal(k_val, (rows, cols), jnp.float32) * jnp.exp(row_trend[:, None] + col_trend[None, :])
    return values * rows ** -0.5


def draw_stat(key, length):
    return jax.random.uniform(key, (length,), jnp.float32, 0.2, 0.8)


def setup_inputs(seed: int = 0) -> dict:
    key_list = jax.random.split(jax.random.key(seed), 20)
    dy_scale = TOKENS ** -0.5
    hyper_keys = jax.random.split(key_list[19], 3)
    hyper_params = jnp.stack([
        jax.random.uniform(hyper_keys[0], (), jnp.float32, 0.5, 0.9),
        jax.random.uniform(hyper_keys[1], (), jnp.float32, 0.5, 1.0),
        jax.random.uniform(hyper_keys[2], (), jnp.float32, 0.3, 0.6)])
    return {
        'x_attn': draw_act(key_list[0], TOKENS, D_MODEL, 1.0),
        'dy_attn': draw_act(key_list[1], TOKENS, D_MODEL, dy_scale),
        'x_mlp': draw_act(key_list[2], TOKENS, D_MODEL, 1.0),
        'dy_gate': draw_act(key_list[3], TOKENS, D_FF, dy_scale),
        'dy_up': draw_act(key_list[4], TOKENS, D_FF, dy_scale),
        'h_mlp': draw_act(key_list[5], TOKENS, D_FF, 1.0),
        'dy_out': draw_act(key_list[6], TOKENS, D_MODEL, dy_scale),
        'w_attn': draw_weight(key_list[7], D_MODEL, D_MODEL),
        'w_gate': draw_weight(key_list[8], D_MODEL, D_FF),
        'w_up': draw_weight(key_list[9], D_MODEL, D_FF),
        'w_down': draw_weight(key_list[10], D_FF, D_MODEL),
        'r_attn': draw_stat(key_list[11], D_MODEL),
        'c_attn': draw_stat(key_list[12], D_MODEL),
        'r_gate': draw_stat(key_list[13], D_MODEL),
        'c_gate': draw_stat(key_list[14], D_FF),
        'r_up': draw_stat(key_list[15], D_MODEL),
        'c_up': draw_stat(key_list[16], D_FF),
        'r_down': draw_stat(key_list[17], D_FF),
        'c_down': draw_stat(key_list[18], D_MODEL),
        'hyper_params': hyper_params,
    }


def adafactor_step(x_act, dy_act, weight, row_old, col_old, hyper_params):
    beta_two = hyper_params[0]
    rho_step = hyper_params[1]
    clip_thr = hyper_params[2]
    full_grad = jnp.dot(x_act.T, dy_act, preferred_element_type=jnp.float32)
    sq_grad = full_grad * full_grad + EPS_ONE
    new_row = beta_two * row_old + (1.0 - beta_two) * jnp.mean(sq_grad, axis=1)
    new_col = beta_two * col_old + (1.0 - beta_two) * jnp.mean(sq_grad, axis=0)
    row_total = jnp.sum(new_row)
    second_est = new_row[:, None] * new_col[None, :] / row_total
    update = full_grad / jnp.sqrt(second_est)
    upd_rms = jnp.sqrt(jnp.mean(update * update))
    update = update / jnp.maximum(1.0, upd_rms / clip_thr)
    w_rms = jnp.sqrt(jnp.mean(weight * weight))
    step_size = rho_step * jnp.maximum(EPS_TWO, w_rms)
    return (weight - step_size * update, new_row, new_col)


def reference(x_attn, dy_attn, x_mlp, dy_gate, dy_up, h_mlp, dy_out, w_attn, w_gate, w_up, w_down,
              r_attn, c_attn, r_gate, c_gate, r_up, c_up, r_down, c_down, hyper_params):
    attn_res = adafactor_step(x_attn, dy_attn, w_attn, r_attn, c_attn, hyper_params)
    gate_res = adafactor_step(x_mlp, dy_gate, w_gate, r_gate, c_gate, hyper_params)
    up_res = adafactor_step(x_mlp, dy_up, w_up, r_up, c_up, hyper_params)
    down_res = adafactor_step(h_mlp, dy_out, w_down, r_down, c_down, hyper_params)
    return (attn_res[0], attn_res[1], attn_res[2], gate_res[0], gate_res[1], gate_res[2],
            up_res[0], up_res[1], up_res[2], down_res[0], down_res[1], down_res[2])
```

```python
import functools
import jax
import jax.numpy as jnp
from jax import lax
from jax.experimental import pallas as pl
from jax.experimental.pallas import tpu as pltpu
from jax.sharding import PartitionSpec as P

EPS_ONE = 1e-30
EPS_TWO = 1e-3
MESH = pl.DeviceIdType.MESH
LANES = 128
F32 = jnp.float32
ATTN, GATE, UP, DOWN = range(4)


class Plan:
    def __init__(self, x_mlp, dy_gate, h_mlp, dy_out, mesh):
        self.dp, self.col, self.row = mesh.shape['dp'], mesh.shape['col'], mesh.shape['row']
        self.tok = x_mlp.shape[0]
        self.mc = x_mlp.shape[1]
        self.nc = dy_out.shape[1]
        self.ng = dy_gate.shape[1] // self.nc
        self.nh = h_mlp.shape[1] // self.mc
        self.tq = self.tok // self.row
        self.th = self.tok // self.col
        self.k_gate = 1
        self.k_up = 1 + self.ng
        self.k_out = 1 + 2 * self.ng
        self.k_h = self.k_out + 1
        self.k_xa = self.k_h + self.nh
        self.k_attn = self.k_xa + 1
        self.count = self.k_attn + 1
        self.n_dy = 2 * self.ng + 2
        self.n_x = self.nh + 2
        self.rows = {ATTN: self.mc, GATE: self.mc, UP: self.mc, DOWN: self.mc * self.nh}
        self.cols = {ATTN: self.nc, GATE: self.nc * self.ng, UP: self.nc * self.ng, DOWN: self.nc}

    def is_dy(self, k):
        return ((k >= self.k_gate) & (k <= self.k_out)) | (k == self.k_attn)

    def is_x(self, k):
        return (k == 0) | ((k >= self.k_h) & (k <= self.k_xa))

    def dy_at(self, k):
        return jnp.where(k == self.k_attn, self.n_dy - 1, k - 1)

    def x_at(self, k):
        return jnp.where(k == 0, 0, k - self.k_h + 1)


def kernel(plan, x_attn, dy_attn, x_mlp, dy_gate, dy_up, h_mlp, dy_out, w_attn, w_gate, w_up, w_down,
           r_attn, c_attn, r_gate, c_gate, r_up, c_up, r_down, c_down, hyper,
           g_attn, g_gate, g_up, g_down, nr_attn, nc_attn, nr_gate, nc_gate, nr_up, nc_up, nr_down, nc_down,
           al_attn, be_attn, al_gate, be_gate, al_up, be_up, al_down, be_down, buf_d, buf_x,
           lhs, tile_x, tile_d, grad, w_tile, r_lanes, r_row, c_sum, a_cols, w_sq, u_sq,
           rs_attn, rs_gate, rs_up, rs_down, cs_attn, cs_gate, cs_up, cs_down, st_all,
           z_send, z_recv, f_send, f_recv, c_send, c_recv, r1_send, r1_recv, r2_send, r2_recv, l_sem, g_sem, w_sem):
    p = plan
    z, y, r = lax.axis_index('dp'), lax.axis_index('col'), lax.axis_index('row')
    left, right = lax.rem(z + p.dp - 1, p.dp), lax.rem(z + 1, p.dp)
    w_refs = {ATTN: w_attn, GATE: w_gate, UP: w_up, DOWN: w_down}
    g_refs = {ATTN: g_attn, GATE: g_gate, UP: g_up, DOWN: g_down}
    old = {ATTN: (r_attn, c_attn), GATE: (r_gate, c_gate), UP: (r_up, c_up), DOWN: (r_down, c_down)}
    new = {ATTN: (nr_attn, nc_attn), GATE: (nr_gate, nc_gate), UP: (nr_up, nc_up), DOWN: (nr_down, nc_down)}
    fac = {ATTN: (al_attn, be_attn), GATE: (al_gate, be_gate), UP: (al_up, be_up), DOWN: (al_down, be_down)}
    rs = {ATTN: rs_attn, GATE: rs_gate, UP: rs_up, DOWN: rs_down}
    cs = {ATTN: cs_attn, GATE: cs_gate, UP: cs_up, DOWN: cs_down}

    def flip_row(v):
        bit0, bit1 = lax.rem(r, 2), lax.div(r, 2)
        if v & 1:
            bit0 = 1 - bit0
        if v & 2:
            bit1 = 1 - bit1
        return bit1 * 2 + bit0

    barrier = pltpu.get_barrier_semaphore()
    for to in (left, right):
        pl.semaphore_signal(barrier, inc=1, device_id=(to, y, r), device_id_type=MESH)
    for f in range(2):
        for v in range(4):
            if f or v:
                to_y = 1 - y if f else y
                pl.semaphore_signal(barrier, inc=1, device_id=(z, to_y, flip_row(v)), device_id_type=MESH)
    pl.semaphore_wait(barrier, 9)

    my_q = pl.ds(pl.multiple_of(r * p.tq, p.tq), p.tq)
    x_q = pl.ds(pl.multiple_of(flip_row(2) * p.tq, p.tq), p.tq)
    my_h = pl.ds(pl.multiple_of(y * p.th, p.th), p.th)

    def slot(k, s, dy):
        return buf_d.at[p.dy_at(k), s, my_q, :] if dy else buf_x.at[p.x_at(k), s, my_h, :]

    def ring(k, s, dy, src=None):
        return pltpu.make_async_remote_copy(
            src_ref=slot(k, s - 1, dy) if src is None else src, dst_ref=slot(k, s, dy),
            send_sem=z_send.at[k, s], recv_sem=z_recv.at[k, s],
            device_id=(left, y, r), device_id_type=MESH)

    def spread(k, s, dy):
        to = (z, y, flip_row(2)) if dy else (z, 1 - y, r)
        return pltpu.make_async_remote_copy(
            src_ref=slot(k, s, dy), dst_ref=slot(k, s, dy), send_sem=f_send.at[k, s], recv_sem=f_recv.at[k, s],
            device_id=to, device_id_type=MESH)

    def partner(k, which):
        part = buf_d.at[p.dy_at(k), :, x_q if which else my_q, :]
        return pltpu.make_async_remote_copy(
            src_ref=part, dst_ref=part, send_sem=c_send.at[p.dy_at(k), which], recv_sem=c_recv.at[p.dy_at(k), which],
            device_id=(z, y, flip_row(1)), device_id_type=MESH)

    def cut(ref, at, size):
        return ref.at[:, pl.ds(pl.multiple_of(at * size, size), size)]

    def send_own(k):
        def go(ref, at, size, dy):
            rows = my_q if dy else my_h
            ring(k, 0, dy, ref.at[rows, pl.ds(pl.multiple_of(at * size, size), size)]).start()

        pl.when(k == 0)(lambda: go(x_mlp, 0, p.mc, False))
        pl.when((k >= p.k_gate) & (k < p.k_up))(lambda: go(dy_gate, k - p.k_gate, p.nc, True))
        pl.when((k >= p.k_up) & (k < p.k_out))(lambda: go(dy_up, k - p.k_up, p.nc, True))
        pl.when(k == p.k_out)(lambda: go(dy_out, 0, p.nc, True))
        pl.when((k >= p.k_h) & (k < p.k_xa))(lambda: go(h_mlp, k - p.k_h, p.mc, False))
        pl.when(k == p.k_xa)(lambda: go(x_attn, 0, p.mc, False))
        pl.when(k == p.k_attn)(lambda: go(dy_attn, 0, p.nc, True))

    def arrive(k, s):
        def go(dy):
            ring(k, s, dy).wait_recv() if s else ring(k, 0, dy, slot(k, 0, dy)).wait_recv()
            if s < p.dp - 2:
                ring(k, s + 1, dy).start()
            spread(k, s, dy).start()
            if dy and s == p.dp - 2:
                partner(k, 0).start()

        pl.when(p.is_dy(k))(lambda: go(True))
        pl.when(p.is_x(k))(lambda: go(False))

    def spread_done(k):
        def go(dy):
            for s in range(p.dp - 1):
                spread(k, s, dy).wait_recv()
            if dy:
                partner(k, 1).start()

        pl.when(p.is_dy(k))(lambda: go(True))
        pl.when(p.is_x(k))(lambda: go(False))

    def load(src, at, size, buf, index, dst):
        copies = [pltpu.make_async_copy(cut(src, at, size), dst.at[z], l_sem.at[0])]
        for d in range(1, p.dp):
            copies.append(pltpu.make_async_copy(buf.at[index, d - 1], dst.at[lax.rem(z + d, p.dp)], l_sem.at[d]))
        for c in copies:
            c.start()
        for c in copies:
            c.wait()

    step_t = min(256, p.tok)

    def turn():
        @pl.loop(0, p.dp)
        def _(q):
            @pl.loop(0, p.tok // step_t)
            def _(t):
                at = pl.multiple_of(t * step_t, step_t)
                lhs[q, :, pl.ds(at, step_t)] = tile_x[q, pl.ds(at, step_t), :].T

    step_n = min(512, p.nc)

    def lane_sum(v):
        out = v[:, 0:LANES]
        for i in range(1, v.shape[1] // LANES):
            out = out + v[:, i * LANES:(i + 1) * LANES]
        return out

    def product(b, at):
        r_lanes[...] = jnp.zeros_like(r_lanes)

        @pl.loop(0, p.nc // step_n)
        def _(n):
            cols = pl.ds(pl.multiple_of(n * step_n, step_n), step_n)
            grad[at, :, cols] = jnp.dot(lhs[0], tile_d[b, 0, :, cols], preferred_element_type=F32)

            @pl.loop(1, p.dp)
            def _(q):
                grad[at, :, cols] += jnp.dot(lhs[q], tile_d[b, q, :, cols], preferred_element_type=F32)

            step_r = min(64, p.mc)

            def body(i, acc):
                rows = pl.ds(pl.multiple_of(i * step_r, step_r), step_r)
                block = grad[at, rows, cols]
                sq = block * block + EPS_ONE
                r_lanes[rows, :] += lane_sum(sq)
                return acc + jnp.sum(sq, axis=0, keepdims=True)

            c_sum[at, :, cols] = lax.fori_loop(0, p.mc // step_r, body, jnp.zeros((1, step_n), F32))

    def weigh(mat):
        block = w_tile[...]
        w_sq[mat] += jnp.sum(jnp.reshape(block * block, (p.mc * p.nc // (8 * LANES), 8, LANES)), axis=0)

    def to_row(block):
        return jnp.sum(block.T, axis=0, keepdims=True)

    def chunk(mat, i, b):
        last = mat == DOWN
        at_w = w_refs[mat].at[pl.ds(pl.multiple_of(i * p.mc, p.mc), p.mc), :] if last else cut(w_refs[mat], i, p.nc)
        get_w = pltpu.make_async_copy(at_w, w_tile, w_sem)
        get_w.start()
        product(b, i)
        at_g = g_refs[mat].at[pl.ds(pl.multiple_of(i * p.mc, p.mc), p.mc), :] if last else cut(g_refs[mat], i, p.nc)
        pltpu.make_async_copy(grad.at[i], at_g, g_sem.at[i]).start()
        if last:
            r_row[i] = to_row(r_lanes[...])
        else:
            row = to_row(r_lanes[...])
            r_row[0] = jnp.where(i == 0, row, r_row[0] + row)
        get_w.wait()
        weigh(mat)

    def total_first(mat):
        if mat == DOWN:
            for i in range(p.nh):
                rs[mat][y, :, i * p.mc:(i + 1) * p.mc] = r_row[i]
            block = c_sum[0]
            for i in range(1, p.nh):
                block = block + c_sum[i]
            cs[mat][r] = block
        else:
            rs[mat][y] = r_row[0]
            for i in range(p.cols[mat] // p.nc):
                cs[mat][r, :, i * p.nc:(i + 1) * p.nc] = c_sum[i]
        for c in first_copies(mat):
            c.start()

    def first_copies(mat):
        copies = [pltpu.make_async_remote_copy(
            src_ref=rs[mat].at[y], dst_ref=rs[mat].at[y], send_sem=r1_send.at[mat, 0], recv_sem=r1_recv.at[mat, 0],
            device_id=(z, 1 - y, r), device_id_type=MESH)]
        for v in range(1, 4):
            copies.append(pltpu.make_async_remote_copy(
                src_ref=cs[mat].at[r], dst_ref=cs[mat].at[r], send_sem=r1_send.at[mat, v],
                recv_sem=r1_recv.at[mat, v], device_id=(z, y, flip_row(v)), device_id_type=MESH))
        return copies

    def second_copies(mat):
        me = y * 4 + r
        copies = []
        for f in range(2):
            for v in range(4):
                if f or v:
                    copies.append(pltpu.make_async_remote_copy(
                        src_ref=st_all.at[mat, me], dst_ref=st_all.at[mat, me], send_sem=r2_send.at[mat, f * 4 + v],
                        recv_sem=r2_recv.at[mat, f * 4 + v],
                        device_id=(z, 1 - y if f else y, flip_row(v)), device_id_type=MESH))
        return copies

    def finish(mat):
        beta_two, rho_step, clip_thr = hyper[0], hyper[1], hyper[2]
        m_total, n_total = p.rows[mat] * p.row, p.cols[mat] * p.col
        total_first(mat)
        for c in first_copies(mat):
            c.wait_recv()
        r_new = beta_two * old[mat][0][...] + (1.0 - beta_two) * ((rs[mat][0] + rs[mat][1]) / n_total)
        c_all = ((cs[mat][0] + cs[mat][1]) + cs[mat][2]) + cs[mat][3]
        c_new = beta_two * old[mat][1][...] + (1.0 - beta_two) * (c_all / m_total)
        new[mat][0][...] = r_new
        new[mat][1][...] = c_new
        t_own = jnp.sum(r_new, axis=1, keepdims=True)
        a_row = jnp.sqrt(t_own) / jnp.sqrt(r_new)
        b_row = 1.0 / jnp.sqrt(c_new)
        fac[mat][1][...] = b_row
        parts = p.nh if mat == DOWN else 1
        for i in range(parts):
            a_cols[i] = jnp.broadcast_to(a_row[:, i * p.mc:(i + 1) * p.mc], (LANES, p.mc)).T
        u_sq[...] = jnp.zeros_like(u_sq)
        pieces = p.nh if mat == DOWN else p.cols[mat] // p.nc

        @pl.loop(0, pieces)
        def _(i):
            @pl.loop(0, p.nc // LANES)
            def _(n):
                cols = pl.ds(pl.multiple_of(n * LANES, LANES), LANES)
                if mat == DOWN:
                    a_block, b_block = a_cols[i], fac[mat][1][:, cols]
                else:
                    a_block = a_cols[0]
                    b_block = fac[mat][1][:, pl.ds(pl.multiple_of(i * p.nc + n * LANES, LANES), LANES)]
                upd = grad[i, :, cols] * a_block * b_block
                u_sq[...] += jnp.sum(jnp.reshape(upd * upd, (p.mc // 8, 8, LANES)), axis=0)

        def spot(v):
            return jnp.broadcast_to(jnp.sum(jnp.sum(v, axis=1, keepdims=True), axis=0, keepdims=True), (8, LANES))

        me = y * 4 + r
        st_all[mat, me, 0] = spot(u_sq[...])
        st_all[mat, me, 1] = spot(w_sq[mat])
        st_all[mat, me, 2] = jnp.broadcast_to(t_own, (8, LANES))
        for c in second_copies(mat):
            c.start()
        for c in second_copies(mat):
            c.wait_recv()
        t_all = st_all[mat, 0, 2]
        for i in range(1, p.row):
            t_all = t_all + st_all[mat, i, 2]
        u_all = st_all[mat, 0, 0] * (t_all / st_all[mat, 0, 2])
        w_all = st_all[mat, 0, 1]
        for i in range(1, p.row * p.col):
            u_all = u_all + st_all[mat, i, 0] * (t_all / st_all[mat, i, 2])
            w_all = w_all + st_all[mat, i, 1]
        upd_rms = jnp.sqrt(u_all / (m_total * n_total))
        w_rms = jnp.sqrt(w_all / (m_total * n_total))
        scale = rho_step * jnp.maximum(EPS_TWO, w_rms) / jnp.maximum(1.0, upd_rms / clip_thr)
        scale = scale * jnp.sqrt(t_all / st_all[mat, me, 2])
        fac[mat][0][...] = a_row * scale[0:1, 0:1]

        @pl.loop(0, pieces)
        def _(i):
            at_g = g_refs[mat].at[pl.ds(0, p.mc), pl.ds(0, p.nc)]
            pltpu.make_async_copy(grad.at[i], at_g, g_sem.at[i]).wait()

    def use_dy(k):
        @pl.when(p.is_dy(k))
        def _():
            partner(k, 0).wait_recv()
            partner(k, 1).wait_recv()
        b = jnp.where(k == p.k_out, 1, 0)

        @pl.when((k >= p.k_gate) & (k < p.k_up))
        def _():
            i = k - p.k_gate
            load(dy_gate, i, p.nc, buf_d, p.dy_at(k), tile_d.at[0])
            chunk(GATE, i, 0)
            pl.when(i == p.ng - 1)(lambda: finish(GATE))

        @pl.when((k >= p.k_up) & (k < p.k_out))
        def _():
            i = k - p.k_up
            load(dy_up, i, p.nc, buf_d, p.dy_at(k), tile_d.at[0])
            chunk(UP, i, 0)
            pl.when(i == p.ng - 1)(lambda: finish(UP))

        @pl.when(k == p.k_out)
        def _():
            load(dy_out, 0, p.nc, buf_d, p.dy_at(k), tile_d.at[1])

        @pl.when(k == p.k_attn)
        def _():
            load(dy_attn, 0, p.nc, buf_d, p.dy_at(k), tile_d.at[0])
            chunk(ATTN, 0, 0)
            finish(ATTN)

    def use_x(k):
        @pl.when(k == 0)
        def _():
            load(x_mlp, 0, p.mc, buf_x, 0, tile_x)
            turn()

        @pl.when((k >= p.k_h) & (k < p.k_xa))
        def _():
            i = k - p.k_h
            load(h_mlp, i, p.mc, buf_x, p.x_at(k), tile_x)
            turn()
            chunk(DOWN, i, 1)

        @pl.when(k == p.k_xa)
        def _():
            load(x_attn, 0, p.mc, buf_x, p.x_at(k), tile_x)
            turn()

    w_sq[...] = jnp.zeros_like(w_sq)
    send_own(0)
    send_own(1)

    @pl.loop(0, p.count + 4)
    def _(d):
        pl.when(d < p.count)(lambda: arrive(d, 0))
        pl.when((d >= 1) & (d - 1 < p.count))(lambda: arrive(d - 1, 1))
        pl.when((d >= 2) & (d - 2 < p.count))(lambda: arrive(d - 2, 2))
        pl.when(d + 2 < p.count)(lambda: send_own(d + 2))
        pl.when((d >= 3) & (d - 3 < p.count))(lambda: spread_done(d - 3))
        pl.when(d == p.count + 2)(lambda: finish(DOWN))
        pl.when(d >= 4)(lambda: use_dy(d - 4))
        pl.when((d >= 3) & (d - 3 < p.count))(lambda: use_x(d - 3))

    @pl.loop(0, p.count)
    def _(k):
        def go(dy):
            for s in range(p.dp - 1):
                ring(k, s, dy, slot(k, s, dy)).wait_send()
                spread(k, s, dy).wait_send()
            if dy:
                partner(k, 0).wait_send()
                partner(k, 1).wait_send()

        pl.when(p.is_dy(k))(lambda: go(True))
        pl.when(p.is_x(k))(lambda: go(False))

    for mat in range(4):
        for c in first_copies(mat) + second_copies(mat):
            c.wait_send()


def solution(mesh):
    act_spec = P('dp', 'row')
    grad_spec = P('dp', 'col')
    w_spec = P('row', 'col')
    row_spec = P('row')
    col_spec = P('col')
    in_specs = (act_spec, grad_spec, act_spec, grad_spec, grad_spec, act_spec, grad_spec,
                w_spec, w_spec, w_spec, w_spec,
                row_spec, col_spec, row_spec, col_spec, row_spec, col_spec, row_spec, col_spec, P())
    out_specs = (w_spec, row_spec, col_spec) * 4

    def per_device(x_attn, dy_attn, x_mlp, dy_gate, dy_up, h_mlp, dy_out, w_attn, w_gate, w_up, w_down,
                   r_attn, c_attn, r_gate, c_gate, r_up, c_up, r_down, c_down, hyper_params):
        p = Plan(x_mlp, dy_gate, h_mlp, dy_out, mesh)
        stats = [v.reshape(1, -1) for v in (r_attn, c_attn, r_gate, c_gate, r_up, c_up, r_down, c_down)]
        any_spec = pl.BlockSpec(memory_space=pl.ANY)
        vmem_spec = pl.BlockSpec(memory_space=pltpu.VMEM)
        row_shapes = []
        for mat in (ATTN, GATE, UP, DOWN):
            row_shapes += [jax.ShapeDtypeStruct((1, p.rows[mat]), F32), jax.ShapeDtypeStruct((1, p.cols[mat]), F32)]
        grads = [jax.ShapeDtypeStruct((p.rows[mat], p.cols[mat]), F32) for mat in (ATTN, GATE, UP, DOWN)]
        bf16 = jnp.bfloat16
        bufs = [jax.ShapeDtypeStruct((p.n_dy, p.dp - 1, p.tok, p.nc), bf16),
                jax.ShapeDtypeStruct((p.n_x, p.dp - 1, p.tok, p.mc), bf16)]
        pieces = max(p.ng, p.nh)
        dma = pltpu.SemaphoreType.DMA
        scratch = [
            pltpu.VMEM((p.dp, p.mc, p.tok), bf16),
            pltpu.VMEM((p.dp, p.tok, p.mc), bf16),
            pltpu.VMEM((2, p.dp, p.tok, p.nc), bf16),
            pltpu.VMEM((pieces, p.mc, p.nc), F32),
            pltpu.VMEM((p.mc, p.nc), F32),
            pltpu.VMEM((p.mc, LANES), F32),
            pltpu.VMEM((pieces, 1, p.mc), F32),
            pltpu.VMEM((pieces, 1, p.nc), F32),
            pltpu.VMEM((p.nh, p.mc, LANES), F32),
            pltpu.VMEM((4, 8, LANES), F32),
            pltpu.VMEM((8, LANES), F32),
        ]
        scratch += [pltpu.VMEM((2, 1, p.rows[mat]), F32) for mat in (ATTN, GATE, UP, DOWN)]
        scratch += [pltpu.VMEM((4, 1, p.cols[mat]), F32) for mat in (ATTN, GATE, UP, DOWN)]
        scratch += [
            pltpu.VMEM((4, 8, 3, 8, LANES), F32),
            dma((p.count, p.dp - 1)), dma((p.count, p.dp - 1)),
            dma((p.count, p.dp - 1)), dma((p.count, p.dp - 1)),
            dma((p.n_dy, 2)), dma((p.n_dy, 2)),
            dma((4, 4)), dma((4, 4)), dma((4, 8)), dma((4, 8)),
            dma((p.dp,)), dma((pieces,)), dma(()),
        ]
        out = pl.pallas_call(
            functools.partial(kernel, p),
            out_shape=grads + row_shapes + row_shapes + bufs,
            in_specs=[any_spec] * 11 + [vmem_spec] * 8 + [pl.BlockSpec(memory_space=pltpu.SMEM)],
            out_specs=[any_spec] * 4 + [vmem_spec] * 16 + [any_spec] * 2,
            scratch_shapes=scratch,
            compiler_params=pltpu.CompilerParams(collective_id=0, has_side_effects=True, vmem_limit_bytes=VMEM_LIMIT),
        )(x_attn, dy_attn, x_mlp, dy_gate, dy_up, h_mlp, dy_out, w_attn, w_gate, w_up, w_down, *stats, hyper_params)
        g_all, n_all, f_all = out[:4], out[4:12], out[12:20]
        result = []
        for mat, w_block in enumerate((w_attn, w_gate, w_up, w_down)):
            alpha, beta = f_all[2 * mat].reshape(-1), f_all[2 * mat + 1].reshape(-1)
            result.append(w_block - g_all[mat] * alpha[:, None] * beta[None, :])
            result.append(n_all[2 * mat].reshape(-1))
            result.append(n_all[2 * mat + 1].reshape(-1))
        return tuple(result)

    return jax.shard_map(per_device, mesh=mesh, in_specs=in_specs, out_specs=out_specs, check_vma=False)


VMEM_LIMIT = 66 * 1024 * 1024 // 1024 * 1024 - 3 * 1024 * 1024
```

```python
import functools
import jax
import jax.numpy as jnp
from jax import lax
from jax.experimental import pallas as pl
from jax.experimental.pallas import tpu as pltpu
from jax.sharding import PartitionSpec as P

EPS_ONE = 1e-30
EPS_TWO = 1e-3
MESH = pl.DeviceIdType.MESH
LANES = 128
F32 = jnp.float32
BF16 = jnp.bfloat16
ATTN, GATE, UP, DOWN = range(4)
MATS = (ATTN, GATE, UP, DOWN)
AHEAD = 2
VMEM_LIMIT = 40 * 1024 * 1024
STORE_LIMIT = 20 * 1024 * 1024
KEPT = (0, 3) + tuple(range(4, 12))


class Plan:
    def __init__(self, x_mlp, dy_gate, h_mlp, dy_out, mesh):
        self.dp, self.col, self.row = mesh.shape['dp'], mesh.shape['col'], mesh.shape['row']
        assert (self.dp, self.col, self.row) == (4, 2, 4)
        self.tok = x_mlp.shape[0]
        self.mc = x_mlp.shape[1]
        self.nc = dy_out.shape[1]
        self.ng = dy_gate.shape[1] // self.nc
        self.nh = h_mlp.shape[1] // self.mc
        self.tq = self.tok // self.row
        self.th = self.tok // self.col
        self.k_gate = 1
        self.k_xa = 1 + self.ng
        self.k_attn = self.k_xa + 1
        self.k_up = self.k_attn + 1
        self.k_out = self.k_up + self.ng
        self.k_h = self.k_out + 1
        self.count = self.k_h + self.nh
        self.n_dy = 2 * self.ng + 2
        self.n_x = self.nh + 2
        self.pieces = max(self.ng, self.nh)
        self.rows = {ATTN: self.mc, GATE: self.mc, UP: self.mc, DOWN: self.mc * self.nh}
        self.cols = {ATTN: self.nc, GATE: self.nc * self.ng, UP: self.nc * self.ng, DOWN: self.nc}
        self.parts = {ATTN: 1, GATE: self.ng, UP: self.ng, DOWN: self.nh}

    def is_dy(self, k):
        return ((k >= self.k_gate) & (k < self.k_xa)) | ((k >= self.k_attn) & (k <= self.k_out))

    def is_x(self, k):
        return (k == 0) | (k == self.k_xa) | (k >= self.k_h)

    def is_attn(self, k):
        return (k == self.k_xa) | (k == self.k_attn)

    def dy_at(self, k):
        return jnp.where(k < self.k_xa, k - 1, k - 2)

    def x_at(self, k):
        return jnp.where(k == 0, 0, jnp.where(k == self.k_xa, 1, k - self.k_h + 2))


def gather_kernel(plan, x_attn, dy_attn, x_mlp, dy_gate, dy_up, h_mlp, dy_out, w_attn, w_gate, w_up, w_down,
                  r_attn, c_attn, r_gate, c_gate, r_up, c_up, r_down, c_down, hyper,
                  o_attn, o_gate, o_up, grad, nr_attn, nc_attn, nr_gate, nc_gate, nr_up, nc_up, nr_down, nc_down,
                  buf_d, buf_x,
                  lhs, tile_x, tile_d, w_buf, r_lanes, r_row, c_sum, a_cols, w_sq, u_sq,
                  b_attn, b_gate, b_up, b_down,
                  rs_attn, rs_gate, rs_up, rs_down, cs_attn, cs_gate, cs_up, cs_down, st_all,
                  z_send, z_recv, f_send, f_recv, c_send, c_recv, r1_send, r1_recv, r2_send, r2_recv,
                  e_send, e_recv, l_sem, wi_sem, wo_sem):
    p = plan
    z, y, r = lax.axis_index('dp'), lax.axis_index('col'), lax.axis_index('row')
    low = z < 2
    mid = (z == 1) | (z == 2)
    end_z = jnp.where(low, 0, 3)
    mate_z = 3 - z
    w_refs = {ATTN: w_attn, GATE: w_gate, UP: w_up, DOWN: w_down}
    old = {ATTN: (r_attn, c_attn), GATE: (r_gate, c_gate), UP: (r_up, c_up), DOWN: (r_down, c_down)}
    new = {ATTN: (nr_attn, nc_attn), GATE: (nr_gate, nc_gate), UP: (nr_up, nc_up), DOWN: (nr_down, nc_down)}
    b_rows = {ATTN: b_attn, GATE: b_gate, UP: b_up, DOWN: b_down}
    rs = {ATTN: rs_attn, GATE: rs_gate, UP: rs_up, DOWN: rs_down}
    cs = {ATTN: cs_attn, GATE: cs_gate, UP: cs_up, DOWN: cs_down}

    def flip_row(v):
        bit0, bit1 = lax.rem(r, 2), lax.div(r, 2)
        if v & 1:
            bit0 = 1 - bit0
        if v & 2:
            bit1 = 1 - bit1
        return bit1 * 2 + bit0

    peers = [(f, v) for f in range(2) for v in range(4) if f or v]
    barrier = pltpu.get_barrier_semaphore()
    for f, v in peers:
        pl.semaphore_signal(barrier, inc=1, device_id=(z, 1 - y if f else y, flip_row(v)), device_id_type=MESH)

    @pl.when(mid)
    def _():
        pl.semaphore_signal(barrier, inc=1, device_id=(end_z, y, r), device_id_type=MESH)
        pl.semaphore_signal(barrier, inc=1, device_id=(mate_z, y, r), device_id_type=MESH)
        pl.semaphore_wait(barrier, len(peers) + 2)

    @pl.when(jnp.logical_not(mid))
    def _():
        pl.semaphore_signal(barrier, inc=1, device_id=(jnp.where(low, 1, 2), y, r), device_id_type=MESH)
        pl.semaphore_wait(barrier, len(peers) + 1)

    my_q = pl.ds(pl.multiple_of(r * p.tq, p.tq), p.tq)
    x_q = pl.ds(pl.multiple_of(flip_row(2) * p.tq, p.tq), p.tq)
    my_h = pl.ds(pl.multiple_of(y * p.th, p.th), p.th)

    def slot(k, s, dy):
        return buf_d.at[p.dy_at(k), s, my_q, :] if dy else buf_x.at[p.x_at(k), s, my_h, :]

    def pass_on(k, dy, src, to_z, to_slot, sem):
        return pltpu.make_async_remote_copy(
            src_ref=src, dst_ref=slot(k, to_slot, dy), send_sem=z_send.at[k, sem], recv_sem=z_recv.at[k, to_slot],
            device_id=(to_z, y, r), device_id_type=MESH)

    def spread(k, s, dy):
        to = (z, y, flip_row(2)) if dy else (z, 1 - y, r)
        return pltpu.make_async_remote_copy(
            src_ref=slot(k, s, dy), dst_ref=slot(k, s, dy), send_sem=f_send.at[k, s], recv_sem=f_recv.at[k, s],
            device_id=to, device_id_type=MESH)

    def partner(k, which):
        part = buf_d.at[p.dy_at(k), :, x_q if which else my_q, :]
        return pltpu.make_async_remote_copy(
            src_ref=part, dst_ref=part, send_sem=c_send.at[p.dy_at(k), which], recv_sem=c_recv.at[p.dy_at(k), which],
            device_id=(z, y, flip_row(1)), device_id_type=MESH)

    def typed(k, go):
        used = mid | jnp.logical_not(p.is_attn(k))
        pl.when(p.is_dy(k) & used)(lambda: go(True))
        pl.when(p.is_x(k) & used)(lambda: go(False))

    def cut(ref, at, size):
        return ref.at[:, pl.ds(pl.multiple_of(at * size, size), size)]

    def down_rows(ref, i):
        return ref.at[pl.ds(pl.multiple_of(i * p.mc, p.mc), p.mc), :]

    def own_to(k, dy, src):
        @pl.when(jnp.logical_not(mid))
        def _():
            pass_on(k, dy, src, jnp.where(low, 1, 2), jnp.where(low, 2, 0), 0).start()

        @pl.when(mid)
        def _():
            @pl.when(jnp.logical_not(p.is_attn(k)))
            def _():
                pass_on(k, dy, src, end_z, jnp.where(low, 0, 2), 0).start()
            pass_on(k, dy, src, mate_z, jnp.where(low, 2, 0), 1).start()

    def send_own(k):
        def go(ref, at, size, dy):
            own_to(k, dy, ref.at[my_q if dy else my_h, pl.ds(pl.multiple_of(at * size, size), size)])

        pl.when(k == 0)(lambda: go(x_mlp, 0, p.mc, False))
        pl.when((k >= p.k_gate) & (k < p.k_xa))(lambda: go(dy_gate, k - p.k_gate, p.nc, True))
        pl.when(k == p.k_xa)(lambda: go(x_attn, 0, p.mc, False))
        pl.when(k == p.k_attn)(lambda: go(dy_attn, 0, p.nc, True))
        pl.when((k >= p.k_up) & (k < p.k_out))(lambda: go(dy_up, k - p.k_up, p.nc, True))
        pl.when(k == p.k_out)(lambda: go(dy_out, 0, p.nc, True))
        pl.when(k >= p.k_h)(lambda: go(h_mlp, k - p.k_h, p.mc, False))

    def own_first_left(k):
        @pl.when(jnp.logical_not(mid & p.is_attn(k)))
        def _():
            pl.when(p.is_dy(k))(lambda: pass_on(k, True, slot(k, 0, True), z, 0, 0).wait_send())
            pl.when(p.is_x(k))(lambda: pass_on(k, False, slot(k, 0, False), z, 0, 0).wait_send())

    def arrive(k, turn_no):
        e = jnp.where(mid, lax.rem(turn_no + 2, 3), turn_no)
        s = jnp.where(low, e, 2 - e)

        def go(dy):
            pass_on(k, dy, slot(k, s, dy), z, s, 0).wait_recv()

            @pl.when(mid & (e == 2))
            def _():
                pass_on(k, dy, slot(k, s, dy), mate_z, 1, 4).start()

            @pl.when(mid & (e < 2) & jnp.logical_not(p.is_attn(k)))
            def _():
                pass_on(k, dy, slot(k, s, dy), end_z, jnp.where(low, s + 1, s - 1), 2 + e).start()

            spread(k, s, dy).start()
            if dy and turn_no == 2:
                partner(k, 0).start()

        typed(k, go)

    def spread_done(k):
        def go(dy):
            for s in range(p.dp - 1):
                spread(k, s, dy).wait_recv()
            if dy:
                partner(k, 1).start()

        typed(k, go)

    def load(src, at, size, buf, index, dst):
        copies = [pltpu.make_async_copy(cut(src, at, size), dst.at[z], l_sem.at[0])]
        for d in range(1, p.dp):
            copies.append(pltpu.make_async_copy(buf.at[index, d - 1], dst.at[lax.rem(z + d, p.dp)], l_sem.at[d]))
        for c in copies:
            c.start()
        for c in copies:
            c.wait()

    step_t = min(256, p.tok)

    def turn():
        @pl.loop(0, p.dp)
        def _(q):
            @pl.loop(0, p.tok // step_t)
            def _(t):
                at = pl.multiple_of(t * step_t, step_t)
                lhs[q, :, pl.ds(at, step_t)] = tile_x[q, pl.ds(at, step_t), :].T

    step_n = min(512, p.nc)
    step_r = min(64, p.mc)

    def lane_sum(v):
        out = v[:, 0:LANES]
        for i in range(1, v.shape[1] // LANES):
            out = out + v[:, i * LANES:(i + 1) * LANES]
        return out

    def product(at):
        r_lanes[...] = jnp.zeros_like(r_lanes)

        @pl.loop(0, p.nc // step_n)
        def _(n):
            cols = pl.ds(pl.multiple_of(n * step_n, step_n), step_n)
            grad[at, :, cols] = jnp.dot(lhs[0], tile_d[0, :, cols], preferred_element_type=F32)

            @pl.loop(1, p.dp)
            def _(q):
                grad[at, :, cols] += jnp.dot(lhs[q], tile_d[q, :, cols], preferred_element_type=F32)

            def body(i, acc):
                rows = pl.ds(pl.multiple_of(i * step_r, step_r), step_r)
                block = grad[at, rows, cols]
                sq = block * block + EPS_ONE
                r_lanes[rows, :] += lane_sum(sq)
                return acc + jnp.sum(sq, axis=0, keepdims=True)

            c_sum[at, :, cols] = lax.fori_loop(0, p.mc // step_r, body, jnp.zeros((1, step_n), F32))

    def to_row(block):
        return jnp.sum(block.T, axis=0, keepdims=True)

    def get_w(mat, i):
        src = down_rows(w_refs[mat], i) if mat == DOWN else cut(w_refs[mat], i, p.nc)
        return pltpu.make_async_copy(src, w_buf.at[lax.rem(i, 3)], wi_sem.at[lax.rem(i, 3)])

    def put_w(mat, i):
        dst = cut(o_gate if mat == GATE else o_up, i, p.nc)
        return pltpu.make_async_copy(w_buf.at[lax.rem(i, 3)], dst, wo_sem.at[lax.rem(i, 3)])

    def chunk(mat, i):
        get_w(mat, i).start()
        product(i)
        row = to_row(r_lanes[...])
        if mat == DOWN:
            r_row[i] = row
        else:
            r_row[0] = jnp.where(i == 0, row, r_row[0] + row)
        get_w(mat, i).wait()

        def body(n, acc):
            rows = pl.ds(pl.multiple_of(n * step_r, step_r), step_r)
            block = lane_sum(w_buf[lax.rem(i, 3), rows, :] * w_buf[lax.rem(i, 3), rows, :])
            return acc + jnp.sum(jnp.reshape(block, (step_r // 8, 8, LANES)), axis=0)

        w_sq[mat] += lax.fori_loop(0, p.mc // step_r, body, jnp.zeros((8, LANES), F32))

    def first_copies(mat):
        copies = [pltpu.make_async_remote_copy(
            src_ref=rs[mat].at[y], dst_ref=rs[mat].at[y], send_sem=r1_send.at[mat, 0], recv_sem=r1_recv.at[mat, 0],
            device_id=(z, 1 - y, r), device_id_type=MESH)]
        for v in range(1, 4):
            copies.append(pltpu.make_async_remote_copy(
                src_ref=cs[mat].at[r], dst_ref=cs[mat].at[r], send_sem=r1_send.at[mat, v],
                recv_sem=r1_recv.at[mat, v], device_id=(z, y, flip_row(v)), device_id_type=MESH))
        return copies

    def second_copies(mat):
        me = y * 4 + r
        return [pltpu.make_async_remote_copy(
            src_ref=st_all.at[mat, me], dst_ref=st_all.at[mat, me], send_sem=r2_send.at[mat, f * 4 + v],
            recv_sem=r2_recv.at[mat, f * 4 + v], device_id=(z, 1 - y if f else y, flip_row(v)), device_id_type=MESH)
            for f, v in peers]

    def finish(mat):
        beta_two, rho_step, clip_thr = hyper[0], hyper[1], hyper[2]
        m_total, n_total = p.rows[mat] * p.row, p.cols[mat] * p.col
        parts = p.parts[mat]
        for i in range(min(2, parts)):
            get_w(mat, jnp.int32(i)).start()
        if mat == DOWN:
            block = c_sum[0]
            for i in range(parts):
                rs[mat][y, :, i * p.mc:(i + 1) * p.mc] = r_row[i]
                if i:
                    block = block + c_sum[i]
            cs[mat][r] = block
        else:
            rs[mat][y] = r_row[0]
            for i in range(parts):
                cs[mat][r, :, i * p.nc:(i + 1) * p.nc] = c_sum[i]
        for c in first_copies(mat):
            c.start()
        for c in first_copies(mat):
            c.wait_recv()
        r_new = beta_two * old[mat][0][...] + (1.0 - beta_two) * ((rs[mat][0] + rs[mat][1]) / n_total)
        c_all = ((cs[mat][0] + cs[mat][1]) + cs[mat][2]) + cs[mat][3]
        c_new = beta_two * old[mat][1][...] + (1.0 - beta_two) * (c_all / m_total)
        new[mat][0][...] = r_new
        new[mat][1][...] = c_new
        t_own = jnp.sum(r_new, axis=1, keepdims=True)
        a_row = jnp.sqrt(t_own) / jnp.sqrt(r_new)
        b_rows[mat][...] = 1.0 / jnp.sqrt(c_new)
        for i in range(parts if mat == DOWN else 1):
            a_cols[i] = jnp.broadcast_to(a_row[:, i * p.mc:(i + 1) * p.mc], (LANES, p.mc)).T
        u_sq[...] = jnp.zeros_like(u_sq)
        groups = p.nc // LANES

        def factors(i, n):
            if mat == DOWN:
                return a_cols[i], b_rows[mat][:, pl.ds(pl.multiple_of(n * LANES, LANES), LANES)]
            return a_cols[0], b_rows[mat][:, pl.ds(pl.multiple_of(i * p.nc + n * LANES, LANES), LANES)]

        @pl.loop(0, parts * groups)
        def _(j):
            i, n = lax.div(j, groups), lax.rem(j, groups)
            a_block, b_block = factors(i, n)
            upd = grad[i, :, pl.ds(pl.multiple_of(n * LANES, LANES), LANES)] * a_block * b_block
            u_sq[...] += jnp.sum(jnp.reshape(upd * upd, (p.mc // 8, 8, LANES)), axis=0)

        def spot(v):
            return jnp.broadcast_to(jnp.sum(jnp.sum(v, axis=1, keepdims=True), axis=0, keepdims=True), (8, LANES))

        me = y * 4 + r
        st_all[mat, me, 0] = spot(u_sq[...])
        st_all[mat, me, 1] = spot(w_sq[mat])
        st_all[mat, me, 2] = jnp.broadcast_to(t_own, (8, LANES))
        for c in second_copies(mat):
            c.start()
        for c in second_copies(mat):
            c.wait_recv()
        t_all = st_all[mat, 0, 2]
        for i in range(1, p.row):
            t_all = t_all + st_all[mat, i, 2]
        u_all = st_all[mat, 0, 0] * (t_all / st_all[mat, 0, 2])
        w_all = st_all[mat, 0, 1]
        for i in range(1, p.row * p.col):
            u_all = u_all + st_all[mat, i, 0] * (t_all / st_all[mat, i, 2])
            w_all = w_all + st_all[mat, i, 1]
        upd_rms = jnp.sqrt(u_all / (m_total * n_total))
        w_rms = jnp.sqrt(w_all / (m_total * n_total))
        scale = rho_step * jnp.maximum(EPS_TWO, w_rms) / jnp.maximum(1.0, upd_rms / clip_thr)
        scale = scale * jnp.sqrt(t_all / st_all[mat, me, 2])
        b_rows[mat][...] = b_rows[mat][...] * scale[0:1, 0:1]

        @pl.loop(0, parts)
        def _(i):
            at = lax.rem(i, 3)
            get_w(mat, i).wait()

            @pl.loop(0, groups)
            def _(n):
                cols = pl.ds(pl.multiple_of(n * LANES, LANES), LANES)
                a_block, b_block = factors(i, n)
                fresh = w_buf[at, :, cols] - grad[i, :, cols] * a_block * b_block
                if mat == ATTN:
                    o_attn[:, cols] = fresh
                elif mat == DOWN:
                    grad[i, :, cols] = fresh
                else:
                    w_buf[at, :, cols] = fresh

            if mat in (GATE, UP):
                put_w(mat, i).start()
                pl.when(i >= 1)(lambda: put_w(mat, i - 1).wait())
            pl.when(i + 2 < parts)(lambda: get_w(mat, i + 2).start())

        if mat in (GATE, UP):
            put_w(mat, jnp.int32(parts - 1)).wait()

    def use_dy(k):
        @pl.when((k >= p.k_gate) & (k < p.k_xa))
        def _():
            i = k - p.k_gate
            load(dy_gate, i, p.nc, buf_d, p.dy_at(k), tile_d)
            chunk(GATE, i)
            pl.when(i == p.ng - 1)(lambda: finish(GATE))

        @pl.when((k == p.k_attn) & mid)
        def _():
            load(dy_attn, 0, p.nc, buf_d, p.dy_at(k), tile_d)
            chunk(ATTN, jnp.int32(0))
            finish(ATTN)

        @pl.when((k >= p.k_up) & (k < p.k_out))
        def _():
            i = k - p.k_up

            @pl.when(i == 0)
            def _():
                load(x_mlp, 0, p.mc, buf_x, 0, tile_x)
                turn()

            load(dy_up, i, p.nc, buf_d, p.dy_at(k), tile_d)
            chunk(UP, i)
            pl.when(i == p.ng - 1)(lambda: finish(UP))

        pl.when(k == p.k_out)(lambda: load(dy_out, 0, p.nc, buf_d, p.dy_at(k), tile_d))

    def got_partner(k):
        @pl.when(p.is_dy(k) & (mid | jnp.logical_not(p.is_attn(k))))
        def _():
            partner(k, 0).wait_recv()
            partner(k, 1).wait_recv()

    def use_x(k):
        @pl.when(k == 0)
        def _():
            load(x_mlp, 0, p.mc, buf_x, 0, tile_x)
            turn()

        @pl.when((k == p.k_xa) & mid)
        def _():
            load(x_attn, 0, p.mc, buf_x, p.x_at(k), tile_x)
            turn()

        @pl.when(k >= p.k_h)
        def _():
            i = k - p.k_h
            load(h_mlp, i, p.mc, buf_x, p.x_at(k), tile_x)
            turn()
            chunk(DOWN, i)
            pl.when(i == p.nh - 1)(lambda: finish(DOWN))

    def to_end():
        pairs = ((o_attn, o_attn), (nr_attn, nr_attn), (nc_attn, nc_attn))
        return [pltpu.make_async_remote_copy(
            src_ref=a, dst_ref=b, send_sem=e_send.at[i], recv_sem=e_recv.at[i],
            device_id=(end_z, y, r), device_id_type=MESH) for i, (a, b) in enumerate(pairs)]

    w_sq[...] = jnp.zeros_like(w_sq)
    for k in range(AHEAD):
        send_own(jnp.int32(k))

    @pl.loop(0, p.count + 1)
    def _(d):
        pl.when(d >= 1)(lambda: own_first_left(d - 1))

        @pl.when(d < p.count)
        def _():
            for i in range(3):
                arrive(d, i)

        pl.when(d + AHEAD < p.count)(lambda: send_own(d + AHEAD))

        @pl.when((d == p.count - 1) & mid)
        def _():
            for c in to_end():
                c.start()

        pl.when(d >= 1)(lambda: spread_done(d - 1))

        @pl.when(d >= 2)
        def _():
            got_partner(d - 2)
            use_dy(d - 2)

        pl.when(d >= 1)(lambda: use_x(d - 1))

    @pl.loop(0, p.count)
    def _(k):
        def go(dy):
            some = slot(k, 0, dy)

            @pl.when(mid)
            def _():
                pass_on(k, dy, some, z, 0, 1).wait_send()
                pass_on(k, dy, some, z, 0, 4).wait_send()

                @pl.when(jnp.logical_not(p.is_attn(k)))
                def _():
                    pass_on(k, dy, some, z, 0, 2).wait_send()
                    pass_on(k, dy, some, z, 0, 3).wait_send()

            for s in range(p.dp - 1):
                spread(k, s, dy).wait_send()
            if dy:
                partner(k, 0).wait_send()
                partner(k, 1).wait_send()

        typed(k, go)

    for mat in (GATE, UP, DOWN):
        for c in first_copies(mat) + second_copies(mat):
            c.wait_send()

    @pl.when(mid)
    def _():
        for c in first_copies(ATTN) + second_copies(ATTN):
            c.wait_send()
        for c in to_end():
            c.wait_send()

    @pl.when(jnp.logical_not(mid))
    def _():
        for c in to_end():
            c.wait_recv()


def store_kernel(plan, o_attn, o_gate, o_up, o_down, *refs):
    p = plan
    stats, (w_attn, w_gate, w_up, w_down), outs = refs[:8], refs[8:12], refs[12:20]
    bounce, in_sem, out_sem, s_sem = refs[20:]
    depth = bounce.shape[0]

    def cut(ref, i):
        return ref.at[:, i * p.nc:(i + 1) * p.nc]

    through = [(cut(o_gate, i), cut(w_gate, i)) for i in range(p.ng)] + [(cut(o_up, i), cut(w_up, i)) for i in range(p.ng)]
    loads = [pltpu.make_async_copy(a, bounce.at[i % depth], in_sem.at[i]) for i, (a, _) in enumerate(through)]
    puts = [pltpu.make_async_copy(bounce.at[i % depth], b, out_sem.at[i]) for i, (_, b) in enumerate(through)]
    for c in loads[:depth]:
        c.start()
    copies = [pltpu.make_async_copy(a, b, s_sem.at[i]) for i, (a, b) in enumerate(zip(stats, outs))]
    copies.append(pltpu.make_async_copy(o_attn, w_attn, s_sem.at[8]))
    for i in range(p.nh):
        copies.append(pltpu.make_async_copy(o_down.at[i], w_down.at[i * p.mc:(i + 1) * p.mc, :], s_sem.at[9 + i]))
    for c in copies:
        c.start()
    for i in range(len(through)):
        loads[i].wait()
        puts[i].start()
        again = i - depth // 2
        if 0 <= again and again + depth < len(through):
            puts[again].wait()
            loads[again + depth].start()
    for i in range(max(0, len(through) - depth), len(through)):
        puts[i].wait()
    for c in copies:
        c.wait()


def solution(mesh):
    act_spec = P('dp', 'row')
    grad_spec = P('dp', 'col')
    w_spec = P('row', 'col')
    row_spec = P('row')
    col_spec = P('col')
    in_specs = (act_spec, grad_spec, act_spec, grad_spec, grad_spec, act_spec, grad_spec,
                w_spec, w_spec, w_spec, w_spec,
                row_spec, col_spec, row_spec, col_spec, row_spec, col_spec, row_spec, col_spec, P())
    out_specs = (w_spec, row_spec, col_spec) * 4

    def per_device(x_attn, dy_attn, x_mlp, dy_gate, dy_up, h_mlp, dy_out, w_attn, w_gate, w_up, w_down,
                   r_attn, c_attn, r_gate, c_gate, r_up, c_up, r_down, c_down, hyper_params):
        p = Plan(x_mlp, dy_gate, h_mlp, dy_out, mesh)
        stats = [v.reshape(1, -1) for v in (r_attn, c_attn, r_gate, c_gate, r_up, c_up, r_down, c_down)]
        any_spec = pl.BlockSpec(memory_space=pl.ANY)
        vmem_spec = pl.BlockSpec(memory_space=pltpu.VMEM)
        row_shapes = []
        for mat in MATS:
            row_shapes += [jax.ShapeDtypeStruct((1, p.rows[mat]), F32), jax.ShapeDtypeStruct((1, p.cols[mat]), F32)]
        w_shapes = [jax.ShapeDtypeStruct((p.rows[mat], p.cols[mat]), F32) for mat in MATS]
        o_shapes = [pltpu.VMEM((p.mc, p.nc), F32), w_shapes[GATE], w_shapes[UP],
                    pltpu.VMEM((p.pieces, p.mc, p.nc), F32)]
        bufs = [jax.ShapeDtypeStruct((p.n_dy, p.dp - 1, p.tok, p.nc), BF16),
                jax.ShapeDtypeStruct((p.n_x, p.dp - 1, p.tok, p.mc), BF16)]
        dma = pltpu.SemaphoreType.DMA
        scratch = [
            pltpu.VMEM((p.dp, p.mc, p.tok), BF16),
            pltpu.VMEM((p.dp, p.tok, p.mc), BF16),
            pltpu.VMEM((p.dp, p.tok, p.nc), BF16),
            pltpu.VMEM((3, p.mc, p.nc), F32),
            pltpu.VMEM((p.mc, LANES), F32),
            pltpu.VMEM((p.pieces, 1, p.mc), F32),
            pltpu.VMEM((p.pieces, 1, p.nc), F32),
            pltpu.VMEM((p.nh, p.mc, LANES), F32),
            pltpu.VMEM((4, 8, LANES), F32),
            pltpu.VMEM((8, LANES), F32),
        ]
        scratch += [pltpu.VMEM((1, p.cols[mat]), F32) for mat in MATS]
        scratch += [pltpu.VMEM((2, 1, p.rows[mat]), F32) for mat in MATS]
        scratch += [pltpu.VMEM((4, 1, p.cols[mat]), F32) for mat in MATS]
        scratch += [
            pltpu.VMEM((4, 8, 3, 8, LANES), F32),
            dma((p.count, 5)), dma((p.count, p.dp - 1)),
            dma((p.count, p.dp - 1)), dma((p.count, p.dp - 1)),
            dma((p.n_dy, 2)), dma((p.n_dy, 2)),
            dma((4, 4)), dma((4, 4)), dma((4, 8)), dma((4, 8)),
            dma((3,)), dma((3,)),
            dma((p.dp,)), dma((3,)), dma((3,)),
        ]
        out = pl.pallas_call(
            functools.partial(gather_kernel, p),
            out_shape=o_shapes + [pltpu.VMEM(v.shape, F32) for v in row_shapes] + bufs,
            in_specs=[any_spec] * 11 + [vmem_spec] * 8 + [pl.BlockSpec(memory_space=pltpu.SMEM)],
            out_specs=[vmem_spec, any_spec, any_spec, vmem_spec] + [vmem_spec] * 8 + [any_spec] * 2,
            scratch_shapes=scratch,
            compiler_params=pltpu.CompilerParams(collective_id=0, has_side_effects=True, vmem_limit_bytes=VMEM_LIMIT),
        )(x_attn, dy_attn, x_mlp, dy_gate, dy_up, h_mlp, dy_out, w_attn, w_gate, w_up, w_down, *stats, hyper_params)
        res = pl.pallas_call(
            functools.partial(store_kernel, p),
            out_shape=w_shapes + row_shapes,
            in_specs=[vmem_spec, any_spec, any_spec, vmem_spec] + [vmem_spec] * 8,
            out_specs=[any_spec] * 12,
            scratch_shapes=[pltpu.VMEM((8, p.mc, p.nc), F32), dma((2 * p.ng,)), dma((2 * p.ng,)), dma((9 + p.nh,))],
            compiler_params=pltpu.CompilerParams(vmem_limit_bytes=STORE_LIMIT),
        )(*[pltpu.with_memory_space_constraint(v, pltpu.VMEM) if i in KEPT else v for i, v in enumerate(out[:12])])
        result = []
        for mat in MATS:
            result += [res[mat], res[4 + 2 * mat].reshape(-1), res[5 + 2 * mat].reshape(-1)]
        return tuple(result)

    return jax.shard_map(per_device, mesh=mesh, in_specs=in_specs, out_specs=out_specs, check_vma=False)
```

```python
import functools
import jax
import jax.numpy as jnp
from jax import lax
from jax.experimental import pallas as pl
from jax.experimental.pallas import tpu as pltpu
from jax.sharding import PartitionSpec as P

EPS_ONE = 1e-30
EPS_TWO = 1e-3
MESH = pl.DeviceIdType.MESH
LANES = 128
F32 = jnp.float32
BF16 = jnp.bfloat16
ATTN, GATE, UP, DOWN = range(4)
MATS = (ATTN, GATE, UP, DOWN)
AHEAD = 3
LATE = 3
VMEM_LIMIT = 40 * 1024 * 1024
STORE_LIMIT = 20 * 1024 * 1024
KEPT = (0, 3) + tuple(range(4, 12))


class Plan:
    def __init__(self, x_mlp, dy_gate, h_mlp, dy_out, mesh):
        self.dp, self.col, self.row = mesh.shape['dp'], mesh.shape['col'], mesh.shape['row']
        assert (self.dp, self.col, self.row) == (4, 2, 4)
        self.tok = x_mlp.shape[0]
        self.mc = x_mlp.shape[1]
        self.nc = dy_out.shape[1]
        self.ng = dy_gate.shape[1] // self.nc
        self.nh = h_mlp.shape[1] // self.mc
        self.tq = self.tok // self.row
        self.th = self.tok // self.col
        self.k_gate = 1
        self.k_xa = 1 + self.ng
        self.k_attn = self.k_xa + 1
        self.k_up = self.k_attn + 1
        self.k_out = self.k_up + self.ng
        self.k_h = self.k_out + 1
        self.count = self.k_h + self.nh
        self.n_dy = 2 * self.ng + 2
        self.n_x = self.nh + 2
        self.pieces = max(self.ng, self.nh)
        self.rows = {ATTN: self.mc, GATE: self.mc, UP: self.mc, DOWN: self.mc * self.nh}
        self.cols = {ATTN: self.nc, GATE: self.nc * self.ng, UP: self.nc * self.ng, DOWN: self.nc}
        self.parts = {ATTN: 1, GATE: self.ng, UP: self.ng, DOWN: self.nh}

    def is_dy(self, k):
        return ((k >= self.k_gate) & (k < self.k_xa)) | ((k >= self.k_attn) & (k <= self.k_out))

    def is_x(self, k):
        return (k == 0) | (k == self.k_xa) | (k >= self.k_h)

    def is_attn(self, k):
        return (k == self.k_xa) | (k == self.k_attn)

    def dy_at(self, k):
        return jnp.where(k < self.k_xa, k - 1, k - 2)

    def x_at(self, k):
        return jnp.where(k == 0, 0, jnp.where(k == self.k_xa, 1, k - self.k_h + 2))


def gather_kernel(plan, x_attn, dy_attn, x_mlp, dy_gate, dy_up, h_mlp, dy_out, w_attn, w_gate, w_up, w_down,
                  r_attn, c_attn, r_gate, c_gate, r_up, c_up, r_down, c_down, hyper,
                  o_attn, o_gate, o_up, grad, nr_attn, nc_attn, nr_gate, nc_gate, nr_up, nc_up, nr_down, nc_down,
                  buf_d, buf_x,
                  lhs, tile_x, tile_d, w_buf, r_lanes, r_row, c_sum, a_cols, w_sq,
                  b_attn, b_gate, b_up, b_down,
                  rs_attn, rs_gate, rs_up, rs_down, cs_attn, cs_gate, cs_up, cs_down, st_all,
                  z_send, z_recv, f_send, f_recv, c_send, c_recv, r1_send, r1_recv, r2_send, r2_recv,
                  e_send, e_recv, l_sem, wi_sem, wo_sem):
    p = plan
    z, y, r = lax.axis_index('dp'), lax.axis_index('col'), lax.axis_index('row')
    low = z < 2
    mid = (z == 1) | (z == 2)
    end_z = jnp.where(low, 0, 3)
    mate_z = 3 - z
    w_refs = {ATTN: w_attn, GATE: w_gate, UP: w_up, DOWN: w_down}
    old = {ATTN: (r_attn, c_attn), GATE: (r_gate, c_gate), UP: (r_up, c_up), DOWN: (r_down, c_down)}
    new = {ATTN: (nr_attn, nc_attn), GATE: (nr_gate, nc_gate), UP: (nr_up, nc_up), DOWN: (nr_down, nc_down)}
    b_rows = {ATTN: b_attn, GATE: b_gate, UP: b_up, DOWN: b_down}
    rs = {ATTN: rs_attn, GATE: rs_gate, UP: rs_up, DOWN: rs_down}
    cs = {ATTN: cs_attn, GATE: cs_gate, UP: cs_up, DOWN: cs_down}

    def flip_row(v):
        bit0, bit1 = lax.rem(r, 2), lax.div(r, 2)
        if v & 1:
            bit0 = 1 - bit0
        if v & 2:
            bit1 = 1 - bit1
        return bit1 * 2 + bit0

    peers = [(f, v) for f in range(2) for v in range(4) if f or v]
    barrier = pltpu.get_barrier_semaphore()
    for f, v in peers:
        pl.semaphore_signal(barrier, inc=1, device_id=(z, 1 - y if f else y, flip_row(v)), device_id_type=MESH)

    @pl.when(mid)
    def _():
        pl.semaphore_signal(barrier, inc=1, device_id=(end_z, y, r), device_id_type=MESH)
        pl.semaphore_signal(barrier, inc=1, device_id=(mate_z, y, r), device_id_type=MESH)
        pl.semaphore_wait(barrier, len(peers) + 2)

    @pl.when(jnp.logical_not(mid))
    def _():
        pl.semaphore_signal(barrier, inc=1, device_id=(jnp.where(low, 1, 2), y, r), device_id_type=MESH)
        pl.semaphore_wait(barrier, len(peers) + 1)

    my_q = pl.ds(pl.multiple_of(r * p.tq, p.tq), p.tq)
    x_q = pl.ds(pl.multiple_of(flip_row(2) * p.tq, p.tq), p.tq)
    my_h = pl.ds(pl.multiple_of(y * p.th, p.th), p.th)

    def slot(k, s, dy):
        return buf_d.at[p.dy_at(k), s, my_q, :] if dy else buf_x.at[p.x_at(k), s, my_h, :]

    def pass_on(k, dy, src, to_z, to_slot, sem):
        return pltpu.make_async_remote_copy(
            src_ref=src, dst_ref=slot(k, to_slot, dy), send_sem=z_send.at[k, sem], recv_sem=z_recv.at[k, to_slot],
            device_id=(to_z, y, r), device_id_type=MESH)

    def spread(k, s, dy):
        to = (z, y, flip_row(2)) if dy else (z, 1 - y, r)
        return pltpu.make_async_remote_copy(
            src_ref=slot(k, s, dy), dst_ref=slot(k, s, dy), send_sem=f_send.at[k, s], recv_sem=f_recv.at[k, s],
            device_id=to, device_id_type=MESH)

    def partner(k, which):
        part = buf_d.at[p.dy_at(k), :, x_q if which else my_q, :]
        return pltpu.make_async_remote_copy(
            src_ref=part, dst_ref=part, send_sem=c_send.at[p.dy_at(k), which], recv_sem=c_recv.at[p.dy_at(k), which],
            device_id=(z, y, flip_row(1)), device_id_type=MESH)

    def typed(k, go):
        used = mid | jnp.logical_not(p.is_attn(k))
        pl.when(p.is_dy(k) & used)(lambda: go(True))
        pl.when(p.is_x(k) & used)(lambda: go(False))

    def cut(ref, at, size):
        return ref.at[:, pl.ds(pl.multiple_of(at * size, size), size)]

    def down_rows(ref, i):
        return ref.at[pl.ds(pl.multiple_of(i * p.mc, p.mc), p.mc), :]

    def own_to(k, dy, src):
        @pl.when(jnp.logical_not(mid))
        def _():
            pass_on(k, dy, src, jnp.where(low, 1, 2), jnp.where(low, 2, 0), 0).start()

        @pl.when(mid)
        def _():
            @pl.when(jnp.logical_not(p.is_attn(k)))
            def _():
                pass_on(k, dy, src, end_z, jnp.where(low, 0, 2), 0).start()
            pass_on(k, dy, src, mate_z, jnp.where(low, 2, 0), 1).start()

    def send_own(k):
        def go(ref, at, size, dy):
            own_to(k, dy, ref.at[my_q if dy else my_h, pl.ds(pl.multiple_of(at * size, size), size)])

        pl.when(k == 0)(lambda: go(x_mlp, 0, p.mc, False))
        pl.when((k >= p.k_gate) & (k < p.k_xa))(lambda: go(dy_gate, k - p.k_gate, p.nc, True))
        pl.when(k == p.k_xa)(lambda: go(x_attn, 0, p.mc, False))
        pl.when(k == p.k_attn)(lambda: go(dy_attn, 0, p.nc, True))
        pl.when((k >= p.k_up) & (k < p.k_out))(lambda: go(dy_up, k - p.k_up, p.nc, True))
        pl.when(k == p.k_out)(lambda: go(dy_out, 0, p.nc, True))
        pl.when(k >= p.k_h)(lambda: go(h_mlp, k - p.k_h, p.mc, False))

    def own_first_left(k):
        @pl.when(jnp.logical_not(mid & p.is_attn(k)))
        def _():
            pl.when(p.is_dy(k))(lambda: pass_on(k, True, slot(k, 0, True), z, 0, 0).wait_send())
            pl.when(p.is_x(k))(lambda: pass_on(k, False, slot(k, 0, False), z, 0, 0).wait_send())

    def arrive(k, turn_no):
        e = jnp.where(mid, lax.rem(turn_no + 2, 3), turn_no)
        s = jnp.where(low, e, 2 - e)

        def go(dy):
            pass_on(k, dy, slot(k, s, dy), z, s, 0).wait_recv()

            @pl.when(mid & (e == 2))
            def _():
                pass_on(k, dy, slot(k, s, dy), mate_z, 1, 4).start()

            @pl.when(mid & (e < 2) & jnp.logical_not(p.is_attn(k)))
            def _():
                pass_on(k, dy, slot(k, s, dy), end_z, jnp.where(low, s + 1, s - 1), 2 + e).start()

            spread(k, s, dy).start()
            if dy and turn_no == 2:
                partner(k, 0).start()

        typed(k, go)

    def spread_done(k, dy):
        for s in range(p.dp - 1):
            spread(k, s, dy).wait_recv()

    def load(src, at, size, buf, index, dst):
        copies = [pltpu.make_async_copy(cut(src, at, size), dst.at[z], l_sem.at[0])]
        for d in range(1, p.dp):
            copies.append(pltpu.make_async_copy(buf.at[index, d - 1], dst.at[lax.rem(z + d, p.dp)], l_sem.at[d]))
        for c in copies:
            c.start()
        for c in copies:
            c.wait()

    step_t = min(256, p.tok)

    def turn():
        @pl.loop(0, p.dp)
        def _(q):
            @pl.loop(0, p.tok // step_t)
            def _(t):
                at = pl.multiple_of(t * step_t, step_t)
                lhs[q, :, pl.ds(at, step_t)] = tile_x[q, pl.ds(at, step_t), :].T

    step_n = min(512, p.nc)
    step_r = min(64, p.mc)

    def lane_sum(v):
        out = v[:, 0:LANES]
        for i in range(1, v.shape[1] // LANES):
            out = out + v[:, i * LANES:(i + 1) * LANES]
        return out

    def product(at):
        r_lanes[...] = jnp.zeros_like(r_lanes)

        @pl.loop(0, p.nc // step_n)
        def _(n):
            cols = pl.ds(pl.multiple_of(n * step_n, step_n), step_n)
            grad[at, :, cols] = jnp.dot(lhs[0], tile_d[0, :, cols], preferred_element_type=F32)

            @pl.loop(1, p.dp)
            def _(q):
                grad[at, :, cols] += jnp.dot(lhs[q], tile_d[q, :, cols], preferred_element_type=F32)

            def body(i, acc):
                rows = pl.ds(pl.multiple_of(i * step_r, step_r), step_r)
                block = grad[at, rows, cols]
                sq = block * block + EPS_ONE
                r_lanes[rows, :] += lane_sum(sq)
                return acc + jnp.sum(sq, axis=0, keepdims=True)

            c_sum[at, :, cols] = lax.fori_loop(0, p.mc // step_r, body, jnp.zeros((1, step_n), F32))

    def fold(v):
        v = jnp.reshape(v, (v.shape[0] // 8, 8, LANES))
        while v.shape[0] > 1:
            v = v[:v.shape[0] // 2] + v[v.shape[0] // 2:]
        return v[0]

    def to_row(block):
        return jnp.sum(block.T, axis=0, keepdims=True)

    def get_w(mat, i):
        src = down_rows(w_refs[mat], i) if mat == DOWN else cut(w_refs[mat], i, p.nc)
        return pltpu.make_async_copy(src, w_buf.at[lax.rem(i, 3)], wi_sem.at[lax.rem(i, 3)])

    def put_w(mat, i):
        dst = cut(o_gate if mat == GATE else o_up, i, p.nc)
        return pltpu.make_async_copy(w_buf.at[lax.rem(i, 3)], dst, wo_sem.at[lax.rem(i, 3)])

    def chunk(mat, i):
        get_w(mat, i).start()
        product(i)
        row = to_row(r_lanes[...])
        if mat == DOWN:
            r_row[i] = row
        else:
            r_row[0] = jnp.where(i == 0, row, r_row[0] + row)
        get_w(mat, i).wait()

        def body(n, acc):
            rows = pl.ds(pl.multiple_of(n * step_r, step_r), step_r)
            block = lane_sum(w_buf[lax.rem(i, 3), rows, :] * w_buf[lax.rem(i, 3), rows, :])
            return acc + fold(block)

        w_sq[mat] += lax.fori_loop(0, p.mc // step_r, body, jnp.zeros((8, LANES), F32))

    def first_copies(mat):
        copies = [pltpu.make_async_remote_copy(
            src_ref=rs[mat].at[y], dst_ref=rs[mat].at[y], send_sem=r1_send.at[mat, 0], recv_sem=r1_recv.at[mat, 0],
            device_id=(z, 1 - y, r), device_id_type=MESH)]
        for v in range(1, 4):
            copies.append(pltpu.make_async_remote_copy(
                src_ref=cs[mat].at[r], dst_ref=cs[mat].at[r], send_sem=r1_send.at[mat, v],
                recv_sem=r1_recv.at[mat, v], device_id=(z, y, flip_row(v)), device_id_type=MESH))
        return copies

    def second_copies(mat):
        me = y * 4 + r
        return [pltpu.make_async_remote_copy(
            src_ref=st_all.at[mat, me], dst_ref=st_all.at[mat, me], send_sem=r2_send.at[mat, f * 4 + v],
            recv_sem=r2_recv.at[mat, f * 4 + v], device_id=(z, 1 - y if f else y, flip_row(v)), device_id_type=MESH)
            for f, v in peers]

    def finish(mat):
        beta_two, rho_step, clip_thr = hyper[0], hyper[1], hyper[2]
        m_total, n_total = p.rows[mat] * p.row, p.cols[mat] * p.col
        parts = p.parts[mat]
        for i in range(min(2, parts)):
            get_w(mat, jnp.int32(i)).start()
        if mat == DOWN:
            block = c_sum[0]
            for i in range(parts):
                rs[mat][y, :, i * p.mc:(i + 1) * p.mc] = r_row[i]
                if i:
                    block = block + c_sum[i]
            cs[mat][r] = block
        else:
            rs[mat][y] = r_row[0]
            for i in range(parts):
                cs[mat][r, :, i * p.nc:(i + 1) * p.nc] = c_sum[i]
        for c in first_copies(mat):
            c.start()
        for c in first_copies(mat):
            c.wait_recv()
        r_new = beta_two * old[mat][0][...] + (1.0 - beta_two) * ((rs[mat][0] + rs[mat][1]) / n_total)
        c_all = ((cs[mat][0] + cs[mat][1]) + cs[mat][2]) + cs[mat][3]
        c_new = beta_two * old[mat][1][...] + (1.0 - beta_two) * (c_all / m_total)
        new[mat][0][...] = r_new
        new[mat][1][...] = c_new
        t_own = jnp.sum(r_new, axis=1, keepdims=True)
        a_row = jnp.sqrt(t_own) / jnp.sqrt(r_new)
        b_rows[mat][...] = 1.0 / jnp.sqrt(c_new)
        for i in range(parts if mat == DOWN else 1):
            a_cols[i] = jnp.broadcast_to(a_row[:, i * p.mc:(i + 1) * p.mc], (LANES, p.mc)).T
        blocks = p.mc // step_r

        def factors(i, n):
            rows = pl.ds(pl.multiple_of(n * step_r, step_r), step_r)
            if mat == DOWN:
                return rows, a_cols[i, rows, :], b_rows[mat].at[:, :]
            return rows, a_cols[0, rows, :], b_rows[mat].at[:, pl.ds(pl.multiple_of(i * p.nc, p.nc), p.nc)]

        def add_up(j, acc):
            i, n = lax.div(j, blocks), lax.rem(j, blocks)
            rows, a_block, b_ref = factors(i, n)
            for c in range(0, p.nc, LANES):
                upd = grad[i, rows, c:c + LANES] * a_block * b_ref[:, c:c + LANES]
                acc = acc + fold(upd * upd)
            return acc

        u_part = lax.fori_loop(0, parts * blocks, add_up, jnp.zeros((8, LANES), F32))

        def spot(v):
            return jnp.broadcast_to(jnp.sum(jnp.sum(v, axis=1, keepdims=True), axis=0, keepdims=True), (8, LANES))

        me = y * 4 + r
        st_all[mat, me, 0] = spot(u_part)
        st_all[mat, me, 1] = spot(w_sq[mat])
        st_all[mat, me, 2] = jnp.broadcast_to(t_own, (8, LANES))
        for c in second_copies(mat):
            c.start()
        for c in second_copies(mat):
            c.wait_recv()
        t_all = st_all[mat, 0, 2]
        for i in range(1, p.row):
            t_all = t_all + st_all[mat, i, 2]
        u_all = st_all[mat, 0, 0] * (t_all / st_all[mat, 0, 2])
        w_all = st_all[mat, 0, 1]
        for i in range(1, p.row * p.col):
            u_all = u_all + st_all[mat, i, 0] * (t_all / st_all[mat, i, 2])
            w_all = w_all + st_all[mat, i, 1]
        upd_rms = jnp.sqrt(u_all / (m_total * n_total))
        w_rms = jnp.sqrt(w_all / (m_total * n_total))
        scale = rho_step * jnp.maximum(EPS_TWO, w_rms) / jnp.maximum(1.0, upd_rms / clip_thr)
        scale = scale * jnp.sqrt(t_all / st_all[mat, me, 2])
        b_rows[mat][...] = b_rows[mat][...] * scale[0:1, 0:1]

        @pl.loop(0, parts)
        def _(i):
            at = lax.rem(i, 3)
            get_w(mat, i).wait()

            @pl.loop(0, blocks)
            def _(n):
                rows, a_block, b_ref = factors(i, n)
                for c in range(0, p.nc, LANES):
                    cols = slice(c, c + LANES)
                    fresh = w_buf[at, rows, cols] - grad[i, rows, cols] * a_block * b_ref[:, cols]
                    if mat == ATTN:
                        o_attn[rows, cols] = fresh
                    elif mat == DOWN:
                        grad[i, rows, cols] = fresh
                    else:
                        w_buf[at, rows, cols] = fresh

            if mat in (GATE, UP):
                put_w(mat, i).start()
                pl.when(i >= 1)(lambda: put_w(mat, i - 1).wait())
            pl.when(i + 2 < parts)(lambda: get_w(mat, i + 2).start())

        if mat in (GATE, UP):
            put_w(mat, jnp.int32(parts - 1)).wait()

    def take_x(src, at, k):
        spread_done(k, False)
        load(src, at, p.mc, buf_x, p.x_at(k), tile_x)
        turn()

    def again_x():
        load(x_mlp, 0, p.mc, buf_x, 0, tile_x)
        turn()

    def use_dy(k):
        @pl.when(p.is_dy(k) & (mid | jnp.logical_not(p.is_attn(k))))
        def _():
            partner(k, 0).wait_recv()
            partner(k, 1).wait_recv()

        @pl.when((k >= p.k_gate) & (k < p.k_xa))
        def _():
            i = k - p.k_gate
            pl.when(i == 0)(lambda: take_x(x_mlp, 0, jnp.int32(0)))
            load(dy_gate, i, p.nc, buf_d, p.dy_at(k), tile_d)
            chunk(GATE, i)
            pl.when(i == p.ng - 1)(lambda: finish(GATE))

        @pl.when((k == p.k_attn) & mid)
        def _():
            take_x(x_attn, 0, jnp.int32(p.k_xa))
            load(dy_attn, 0, p.nc, buf_d, p.dy_at(k), tile_d)
            chunk(ATTN, jnp.int32(0))
            finish(ATTN)

        @pl.when((k >= p.k_up) & (k < p.k_out))
        def _():
            i = k - p.k_up
            pl.when(i == 0)(again_x)
            load(dy_up, i, p.nc, buf_d, p.dy_at(k), tile_d)
            chunk(UP, i)
            pl.when(i == p.ng - 1)(lambda: finish(UP))

        pl.when(k == p.k_out)(lambda: load(dy_out, 0, p.nc, buf_d, p.dy_at(k), tile_d))

    def h_until(d):
        late = jnp.where(mid, LATE, 1)
        return jnp.clip(jnp.minimum(2 * (d - p.k_out - LATE), d - p.k_out - late), 0, p.nh)

    def use_h(i):
        take_x(h_mlp, i, p.k_h + i)
        chunk(DOWN, i)
        pl.when(i == p.nh - 1)(lambda: finish(DOWN))

    def to_end():
        pairs = ((o_attn, o_attn), (nr_attn, nr_attn), (nc_attn, nc_attn))
        return [pltpu.make_async_remote_copy(
            src_ref=a, dst_ref=b, send_sem=e_send.at[i], recv_sem=e_recv.at[i],
            device_id=(end_z, y, r), device_id_type=MESH) for i, (a, b) in enumerate(pairs)]

    w_sq[...] = jnp.zeros_like(w_sq)
    for k in range(AHEAD):
        send_own(jnp.int32(k))

    @pl.loop(0, p.count + LATE)
    def _(d):
        pl.when((d >= 1) & (d <= p.count))(lambda: own_first_left(d - 1))

        @pl.when(d < p.count)
        def _():
            for i in range(3):
                arrive(d, i)

        pl.when(d + AHEAD < p.count)(lambda: send_own(d + AHEAD))

        @pl.when((d == p.count - 1) & mid)
        def _():
            for c in to_end():
                c.start()

        k = d - LATE

        @pl.when((k >= 0) & p.is_dy(k) & (mid | jnp.logical_not(p.is_attn(k))))
        def _():
            spread_done(k, True)
            partner(k, 1).start()

        pl.when(d > LATE)(lambda: use_dy(d - LATE - 1))

        @pl.loop(0, 2)
        def _(j):
            i = h_until(d - 1) + j
            pl.when(i < h_until(d))(lambda: use_h(i))

    @pl.loop(0, p.count)
    def _(k):
        def go(dy):
            some = slot(k, 0, dy)

            @pl.when(mid)
            def _():
                pass_on(k, dy, some, z, 0, 1).wait_send()
                pass_on(k, dy, some, z, 0, 4).wait_send()

                @pl.when(jnp.logical_not(p.is_attn(k)))
                def _():
                    pass_on(k, dy, some, z, 0, 2).wait_send()
                    pass_on(k, dy, some, z, 0, 3).wait_send()

            for s in range(p.dp - 1):
                spread(k, s, dy).wait_send()
            if dy:
                partner(k, 0).wait_send()
                partner(k, 1).wait_send()

        typed(k, go)

    for mat in (GATE, UP, DOWN):
        for c in first_copies(mat) + second_copies(mat):
            c.wait_send()

    @pl.when(mid)
    def _():
        for c in first_copies(ATTN) + second_copies(ATTN):
            c.wait_send()
        for c in to_end():
            c.wait_send()

    @pl.when(jnp.logical_not(mid))
    def _():
        for c in to_end():
            c.wait_recv()


def store_kernel(plan, o_attn, o_gate, o_up, o_down, *refs):
    p = plan
    stats, (w_attn, w_gate, w_up, w_down), outs = refs[:8], refs[8:12], refs[12:20]
    bounce, in_sem, out_sem, s_sem = refs[20:]
    depth = bounce.shape[0]

    def cut(ref, i):
        return ref.at[:, i * p.nc:(i + 1) * p.nc]

    through = [(cut(o_gate, i), cut(w_gate, i)) for i in range(p.ng)] + [(cut(o_up, i), cut(w_up, i)) for i in range(p.ng)]
    loads = [pltpu.make_async_copy(a, bounce.at[i % depth], in_sem.at[i]) for i, (a, _) in enumerate(through)]
    puts = [pltpu.make_async_copy(bounce.at[i % depth], b, out_sem.at[i]) for i, (_, b) in enumerate(through)]
    for c in loads[:depth]:
        c.start()
    copies = [pltpu.make_async_copy(a, b, s_sem.at[i]) for i, (a, b) in enumerate(zip(stats, outs))]
    copies.append(pltpu.make_async_copy(o_attn, w_attn, s_sem.at[8]))
    for i in range(p.nh):
        copies.append(pltpu.make_async_copy(o_down.at[i], w_down.at[i * p.mc:(i + 1) * p.mc, :], s_sem.at[9 + i]))
    for c in copies:
        c.start()
    for i in range(len(through)):
        loads[i].wait()
        puts[i].start()
        again = i - depth // 2
        if 0 <= again and again + depth < len(through):
            puts[again].wait()
            loads[again + depth].start()
    for i in range(max(0, len(through) - depth), len(through)):
        puts[i].wait()
    for c in copies:
        c.wait()


def solution(mesh):
    act_spec = P('dp', 'row')
    grad_spec = P('dp', 'col')
    w_spec = P('row', 'col')
    row_spec = P('row')
    col_spec = P('col')
    in_specs = (act_spec, grad_spec, act_spec, grad_spec, grad_spec, act_spec, grad_spec,
                w_spec, w_spec, w_spec, w_spec,
                row_spec, col_spec, row_spec, col_spec, row_spec, col_spec, row_spec, col_spec, P())
    out_specs = (w_spec, row_spec, col_spec) * 4

    def per_device(x_attn, dy_attn, x_mlp, dy_gate, dy_up, h_mlp, dy_out, w_attn, w_gate, w_up, w_down,
                   r_attn, c_attn, r_gate, c_gate, r_up, c_up, r_down, c_down, hyper_params):
        p = Plan(x_mlp, dy_gate, h_mlp, dy_out, mesh)
        stats = [v.reshape(1, -1) for v in (r_attn, c_attn, r_gate, c_gate, r_up, c_up, r_down, c_down)]
        any_spec = pl.BlockSpec(memory_space=pl.ANY)
        vmem_spec = pl.BlockSpec(memory_space=pltpu.VMEM)
        row_shapes = []
        for mat in MATS:
            row_shapes += [jax.ShapeDtypeStruct((1, p.rows[mat]), F32), jax.ShapeDtypeStruct((1, p.cols[mat]), F32)]
        w_shapes = [jax.ShapeDtypeStruct((p.rows[mat], p.cols[mat]), F32) for mat in MATS]
        o_shapes = [pltpu.VMEM((p.mc, p.nc), F32), w_shapes[GATE], w_shapes[UP],
                    pltpu.VMEM((p.pieces, p.mc, p.nc), F32)]
        bufs = [jax.ShapeDtypeStruct((p.n_dy, p.dp - 1, p.tok, p.nc), BF16),
                jax.ShapeDtypeStruct((p.n_x, p.dp - 1, p.tok, p.mc), BF16)]
        dma = pltpu.SemaphoreType.DMA
        scratch = [
            pltpu.VMEM((p.dp, p.mc, p.tok), BF16),
            pltpu.VMEM((p.dp, p.tok, p.mc), BF16),
            pltpu.VMEM((p.dp, p.tok, p.nc), BF16),
            pltpu.VMEM((3, p.mc, p.nc), F32),
            pltpu.VMEM((p.mc, LANES), F32),
            pltpu.VMEM((p.pieces, 1, p.mc), F32),
            pltpu.VMEM((p.pieces, 1, p.nc), F32),
            pltpu.VMEM((p.nh, p.mc, LANES), F32),
            pltpu.VMEM((4, 8, LANES), F32),
        ]
        scratch += [pltpu.VMEM((1, p.cols[mat]), F32) for mat in MATS]
        scratch += [pltpu.VMEM((2, 1, p.rows[mat]), F32) for mat in MATS]
        scratch += [pltpu.VMEM((4, 1, p.cols[mat]), F32) for mat in MATS]
        scratch += [
            pltpu.VMEM((4, 8, 3, 8, LANES), F32),
            dma((p.count, 5)), dma((p.count, p.dp - 1)),
            dma((p.count, p.dp - 1)), dma((p.count, p.dp - 1)),
            dma((p.n_dy, 2)), dma((p.n_dy, 2)),
            dma((4, 4)), dma((4, 4)), dma((4, 8)), dma((4, 8)),
            dma((3,)), dma((3,)),
            dma((p.dp,)), dma((3,)), dma((3,)),
        ]
        out = pl.pallas_call(
            functools.partial(gather_kernel, p),
            out_shape=o_shapes + [pltpu.VMEM(v.shape, F32) for v in row_shapes] + bufs,
            in_specs=[any_spec] * 11 + [vmem_spec] * 8 + [pl.BlockSpec(memory_space=pltpu.SMEM)],
            out_specs=[vmem_spec, any_spec, any_spec, vmem_spec] + [vmem_spec] * 8 + [any_spec] * 2,
            scratch_shapes=scratch,
            compiler_params=pltpu.CompilerParams(collective_id=0, has_side_effects=True, vmem_limit_bytes=VMEM_LIMIT),
        )(x_attn, dy_attn, x_mlp, dy_gate, dy_up, h_mlp, dy_out, w_attn, w_gate, w_up, w_down, *stats, hyper_params)
        res = pl.pallas_call(
            functools.partial(store_kernel, p),
            out_shape=w_shapes + row_shapes,
            in_specs=[vmem_spec, any_spec, any_spec, vmem_spec] + [vmem_spec] * 8,
            out_specs=[any_spec] * 12,
            scratch_shapes=[pltpu.VMEM((8, p.mc, p.nc), F32), dma((2 * p.ng,)), dma((2 * p.ng,)), dma((9 + p.nh,))],
            compiler_params=pltpu.CompilerParams(vmem_limit_bytes=STORE_LIMIT),
        )(*[pltpu.with_memory_space_constraint(v, pltpu.VMEM) if i in KEPT else v for i, v in enumerate(out[:12])])
        result = []
        for mat in MATS:
            result += [res[mat], res[4 + 2 * mat].reshape(-1), res[5 + 2 * mat].reshape(-1)]
        return tuple(result)

    return jax.shard_map(per_device, mesh=mesh, in_specs=in_specs, out_specs=out_specs, check_vma=False)
```

```python
import functools
import jax
import jax.numpy as jnp
from jax import lax
from jax.experimental import pallas as pl
from jax.experimental.pallas import tpu as pltpu
from jax.sharding import PartitionSpec as P

EPS_ONE = 1e-30
EPS_TWO = 1e-3
MESH = pl.DeviceIdType.MESH
LANES = 128
F32 = jnp.float32
BF16 = jnp.bfloat16
ATTN, GATE, UP, DOWN = range(4)
MATS = (ATTN, GATE, UP, DOWN)
AHEAD_MID, AHEAD_END = 2, 6
LATE = 3
VMEM_LIMIT = 40 * 1024 * 1024
STORE_LIMIT = 20 * 1024 * 1024
KEPT = (0, 3) + tuple(range(4, 12))


def look(k, table):
    out = jnp.int32(0)
    for i, v in enumerate(table):
        if v:
            out = jnp.where(k == i, v, out)
    return out


class Plan:
    def __init__(self, x_mlp, dy_gate, h_mlp, dy_out, mesh):
        self.dp, self.col, self.row = mesh.shape['dp'], mesh.shape['col'], mesh.shape['row']
        assert (self.dp, self.col, self.row) == (4, 2, 4)
        self.tok = x_mlp.shape[0]
        self.mc = x_mlp.shape[1]
        self.nc = dy_out.shape[1]
        self.ng = dy_gate.shape[1] // self.nc
        self.nh = h_mlp.shape[1] // self.mc
        self.tq = self.tok // self.row
        self.th = self.tok // self.col
        g = [('gate', i) for i in range(self.ng)]
        u = [('up', i) for i in range(self.ng)]
        h = [('h', i) for i in range(self.nh)]
        one, two = max(1, self.ng // 4), max(2, 3 * self.ng // 4)
        self.order = ([('x_mlp', 0)] + g[:one] + h[:1] + g[one:two] + h[1:2] + g[two:] + [('x_attn', 0), ('attn', 0)]
                      + u + [('out', 0)] + h[2:])
        self.count = len(self.order)
        self.place = {v: k for k, v in enumerate(self.order)}
        self.n_dy = 2 * self.ng + 2
        self.n_x = self.nh + 2
        self.pieces = max(self.ng, self.nh)
        self.rows = {ATTN: self.mc, GATE: self.mc, UP: self.mc, DOWN: self.mc * self.nh}
        self.cols = {ATTN: self.nc, GATE: self.nc * self.ng, UP: self.nc * self.ng, DOWN: self.nc}
        self.parts = {ATTN: 1, GATE: self.ng, UP: self.ng, DOWN: self.nh}
        base = {'gate': 0, 'up': self.ng, 'out': 2 * self.ng, 'attn': 2 * self.ng + 1, 'x_mlp': 0, 'x_attn': 1, 'h': 2}
        self.dy_table = [1 if n in ('gate', 'up', 'out', 'attn') else 0 for n, _ in self.order]
        self.at_table = [base[n] + i for n, i in self.order]
        self.attn_table = [1 if n in ('x_attn', 'attn') else 0 for n, _ in self.order]
        self.steps = {m: self.schedule(m) for m in (True, False)}
        last = max(max(v.values()) for v in self.steps.values())
        self.turns = max(last + 1, 3 * (self.count + LATE + 1))

    def schedule(self, mid):
        tasks = []
        for name, mat in (('gate', GATE), ('attn', ATTN), ('up', UP), ('out', None), ('h', DOWN)):
            if name == 'attn' and not mid:
                continue
            for i in range(sum(1 for n, _ in self.order if n == name)):
                need = [(self.place[name, i], 1 if name == 'h' and not mid else LATE + (name != 'h'))]
                if i == 0 and name in ('gate', 'attn'):
                    need.append((self.place['x_mlp' if name == 'gate' else 'x_attn', 0], LATE))
                tasks.append(((name, i), max(k + late for k, late in need)))
            if mat is not None:
                tasks += [(('finish', mat, stage), 0) for stage in range(4 if self.parts[mat] > 1 else 3)]
        out, t = {}, 0
        for task, first in tasks:
            t = max(t, 3 * first)
            out[task] = t
            t += 1
        return out

    def is_dy(self, k):
        return look(k, self.dy_table) == 1

    def is_attn(self, k):
        return look(k, self.attn_table) == 1

    def at(self, k):
        return look(k, self.at_table)


def gather_kernel(plan, x_attn, dy_attn, x_mlp, dy_gate, dy_up, h_mlp, dy_out, w_attn, w_gate, w_up, w_down,
                  r_attn, c_attn, r_gate, c_gate, r_up, c_up, r_down, c_down, hyper,
                  o_attn, o_gate, o_up, grad, nr_attn, nc_attn, nr_gate, nc_gate, nr_up, nc_up, nr_down, nc_down,
                  buf_d, buf_x,
                  lhs, tile_x, tile_d, w_buf, r_lanes, r_row, c_sum, a_cols, w_sq,
                  b_attn, b_gate, b_up, b_down,
                  rs_attn, rs_gate, rs_up, rs_down, cs_attn, cs_gate, cs_up, cs_down, st_all,
                  z_send, z_recv, f_send, f_recv, c_send, c_recv, r1_send, r1_recv, r2_send, r2_recv,
                  e_send, e_recv, l_sem, wi_sem, wo_sem):
    p = plan
    z, y, r = lax.axis_index('dp'), lax.axis_index('col'), lax.axis_index('row')
    low = z < 2
    mid = (z == 1) | (z == 2)
    end_z = jnp.where(low, 0, 3)
    mate_z = 3 - z
    w_refs = {ATTN: w_attn, GATE: w_gate, UP: w_up, DOWN: w_down}
    old = {ATTN: (r_attn, c_attn), GATE: (r_gate, c_gate), UP: (r_up, c_up), DOWN: (r_down, c_down)}
    new = {ATTN: (nr_attn, nc_attn), GATE: (nr_gate, nc_gate), UP: (nr_up, nc_up), DOWN: (nr_down, nc_down)}
    b_rows = {ATTN: b_attn, GATE: b_gate, UP: b_up, DOWN: b_down}
    rs = {ATTN: rs_attn, GATE: rs_gate, UP: rs_up, DOWN: rs_down}
    cs = {ATTN: cs_attn, GATE: cs_gate, UP: cs_up, DOWN: cs_down}

    def flip_row(v):
        bit0, bit1 = lax.rem(r, 2), lax.div(r, 2)
        if v & 1:
            bit0 = 1 - bit0
        if v & 2:
            bit1 = 1 - bit1
        return bit1 * 2 + bit0

    peers = [(f, v) for f in range(2) for v in range(4) if f or v]
    barrier = pltpu.get_barrier_semaphore()
    for f, v in peers:
        pl.semaphore_signal(barrier, inc=1, device_id=(z, 1 - y if f else y, flip_row(v)), device_id_type=MESH)

    @pl.when(mid)
    def _():
        pl.semaphore_signal(barrier, inc=1, device_id=(end_z, y, r), device_id_type=MESH)
        pl.semaphore_signal(barrier, inc=1, device_id=(mate_z, y, r), device_id_type=MESH)
        pl.semaphore_wait(barrier, len(peers) + 2)

    @pl.when(jnp.logical_not(mid))
    def _():
        pl.semaphore_signal(barrier, inc=1, device_id=(jnp.where(low, 1, 2), y, r), device_id_type=MESH)
        pl.semaphore_wait(barrier, len(peers) + 1)

    my_q = pl.ds(pl.multiple_of(r * p.tq, p.tq), p.tq)
    x_q = pl.ds(pl.multiple_of(flip_row(2) * p.tq, p.tq), p.tq)
    my_h = pl.ds(pl.multiple_of(y * p.th, p.th), p.th)

    def slot(k, s, dy):
        return buf_d.at[p.at(k), s, my_q, :] if dy else buf_x.at[p.at(k), s, my_h, :]

    def pass_on(k, dy, src, to_z, to_slot, sem):
        return pltpu.make_async_remote_copy(
            src_ref=src, dst_ref=slot(k, to_slot, dy), send_sem=z_send.at[k, sem], recv_sem=z_recv.at[k, to_slot],
            device_id=(to_z, y, r), device_id_type=MESH)

    def spread(k, s, dy):
        to = (z, y, flip_row(2)) if dy else (z, 1 - y, r)
        return pltpu.make_async_remote_copy(
            src_ref=slot(k, s, dy), dst_ref=slot(k, s, dy), send_sem=f_send.at[k, s], recv_sem=f_recv.at[k, s],
            device_id=to, device_id_type=MESH)

    def partner(k, which):
        part = buf_d.at[p.at(k), :, x_q if which else my_q, :]
        return pltpu.make_async_remote_copy(
            src_ref=part, dst_ref=part, send_sem=c_send.at[p.at(k), which], recv_sem=c_recv.at[p.at(k), which],
            device_id=(z, y, flip_row(1)), device_id_type=MESH)

    def typed(k, go):
        used = mid | jnp.logical_not(p.is_attn(k))
        pl.when(p.is_dy(k) & used)(lambda: go(True))
        pl.when(jnp.logical_not(p.is_dy(k)) & used)(lambda: go(False))

    def cut(ref, at, size):
        return ref.at[:, pl.ds(pl.multiple_of(at * size, size), size)]

    def down_rows(ref, i):
        return ref.at[pl.ds(pl.multiple_of(i * p.mc, p.mc), p.mc), :]

    def own_to(k, dy, src):
        @pl.when(jnp.logical_not(mid))
        def _():
            pass_on(k, dy, src, jnp.where(low, 1, 2), jnp.where(low, 2, 0), 0).start()

        @pl.when(mid)
        def _():
            @pl.when(jnp.logical_not(p.is_attn(k)))
            def _():
                pass_on(k, dy, src, end_z, jnp.where(low, 0, 2), 0).start()
            pass_on(k, dy, src, mate_z, jnp.where(low, 2, 0), 1).start()

    def send_own(k):
        def go(ref, at, size, dy):
            own_to(k, dy, ref.at[my_q if dy else my_h, pl.ds(pl.multiple_of(at * size, size), size)])

        for name, ref, dy in (('x_mlp', x_mlp, False), ('gate', dy_gate, True), ('x_attn', x_attn, False),
                              ('attn', dy_attn, True), ('up', dy_up, True), ('out', dy_out, True), ('h', h_mlp, False)):
            at = look(k, [i + 1 if n == name else 0 for n, i in p.order])
            size = p.nc if dy else p.mc
            pl.when(at > 0)(functools.partial(go, ref, at - 1, size, dy))

    def own_first_left(k):
        @pl.when(jnp.logical_not(mid & p.is_attn(k)))
        def _():
            pl.when(p.is_dy(k))(lambda: pass_on(k, True, slot(k, 0, True), z, 0, 0).wait_send())
            pl.when(jnp.logical_not(p.is_dy(k)))(lambda: pass_on(k, False, slot(k, 0, False), z, 0, 0).wait_send())

    def arrive(k, e, whole):
        s = jnp.where(low, e, 2 - e)

        def go(dy):
            pass_on(k, dy, slot(k, s, dy), z, s, 0).wait_recv()

            @pl.when(mid & (e == 2))
            def _():
                pass_on(k, dy, slot(k, s, dy), mate_z, 1, 4).start()

            @pl.when(mid & (e < 2) & jnp.logical_not(p.is_attn(k)))
            def _():
                pass_on(k, dy, slot(k, s, dy), end_z, jnp.where(low, s + 1, s - 1), 2 + e).start()

            spread(k, s, dy).start()
            if dy:
                pl.when(whole)(lambda: partner(k, 0).start())

        typed(k, go)

    def spread_done(k, dy):
        for s in range(p.dp - 1):
            spread(k, s, dy).wait_recv()

    def load(src, at, size, buf, index, dst):
        copies = [pltpu.make_async_copy(cut(src, at, size), dst.at[z], l_sem.at[0])]
        for d in range(1, p.dp):
            copies.append(pltpu.make_async_copy(buf.at[index, d - 1], dst.at[lax.rem(z + d, p.dp)], l_sem.at[d]))
        for c in copies:
            c.start()
        for c in copies:
            c.wait()

    step_t = min(256, p.tok)

    def turn():
        @pl.loop(0, p.dp)
        def _(q):
            @pl.loop(0, p.tok // step_t)
            def _(t):
                at = pl.multiple_of(t * step_t, step_t)
                lhs[q, :, pl.ds(at, step_t)] = tile_x[q, pl.ds(at, step_t), :].T

    step_n = min(512, p.nc)
    step_r = min(64, p.mc)

    def lane_sum(v):
        out = v[:, 0:LANES]
        for i in range(1, v.shape[1] // LANES):
            out = out + v[:, i * LANES:(i + 1) * LANES]
        return out

    def product(at):
        r_lanes[...] = jnp.zeros_like(r_lanes)

        @pl.loop(0, p.nc // step_n)
        def _(n):
            cols = pl.ds(pl.multiple_of(n * step_n, step_n), step_n)
            grad[at, :, cols] = jnp.dot(lhs[0], tile_d[0, :, cols], preferred_element_type=F32)

            @pl.loop(1, p.dp)
            def _(q):
                grad[at, :, cols] += jnp.dot(lhs[q], tile_d[q, :, cols], preferred_element_type=F32)

            def body(i, acc):
                rows = pl.ds(pl.multiple_of(i * step_r, step_r), step_r)
                block = grad[at, rows, cols]
                sq = block * block + EPS_ONE
                r_lanes[rows, :] += lane_sum(sq)
                return acc + jnp.sum(sq, axis=0, keepdims=True)

            c_sum[at, :, cols] = lax.fori_loop(0, p.mc // step_r, body, jnp.zeros((1, step_n), F32))

    def fold(v):
        v = jnp.reshape(v, (v.shape[0] // 8, 8, LANES))
        while v.shape[0] > 1:
            v = v[:v.shape[0] // 2] + v[v.shape[0] // 2:]
        return v[0]

    def to_row(block):
        return jnp.sum(block.T, axis=0, keepdims=True)

    def get_w(mat, i):
        src = down_rows(w_refs[mat], i) if mat == DOWN else cut(w_refs[mat], i, p.nc)
        return pltpu.make_async_copy(src, w_buf.at[lax.rem(i, 3)], wi_sem.at[lax.rem(i, 3)])

    def put_w(mat, i):
        dst = cut(o_gate if mat == GATE else o_up, i, p.nc)
        return pltpu.make_async_copy(w_buf.at[lax.rem(i, 3)], dst, wo_sem.at[lax.rem(i, 3)])

    def chunk(mat, i):
        get_w(mat, i).start()
        product(i)
        row = to_row(r_lanes[...])
        if mat == DOWN:
            r_row[i] = row
        else:
            r_row[0] = jnp.where(i == 0, row, r_row[0] + row)
        get_w(mat, i).wait()

        def body(n, acc):
            rows = pl.ds(pl.multiple_of(n * step_r, step_r), step_r)
            block = lane_sum(w_buf[lax.rem(i, 3), rows, :] * w_buf[lax.rem(i, 3), rows, :])
            return acc + fold(block)

        w_sq[mat] += lax.fori_loop(0, p.mc // step_r, body, jnp.zeros((8, LANES), F32))

    def first_copies(mat):
        copies = [pltpu.make_async_remote_copy(
            src_ref=rs[mat].at[y], dst_ref=rs[mat].at[y], send_sem=r1_send.at[mat, 0], recv_sem=r1_recv.at[mat, 0],
            device_id=(z, 1 - y, r), device_id_type=MESH)]
        for v in range(1, 4):
            copies.append(pltpu.make_async_remote_copy(
                src_ref=cs[mat].at[r], dst_ref=cs[mat].at[r], send_sem=r1_send.at[mat, v],
                recv_sem=r1_recv.at[mat, v], device_id=(z, y, flip_row(v)), device_id_type=MESH))
        return copies

    def second_copies(mat):
        me = y * 4 + r
        return [pltpu.make_async_remote_copy(
            src_ref=st_all.at[mat, me], dst_ref=st_all.at[mat, me], send_sem=r2_send.at[mat, f * 4 + v],
            recv_sem=r2_recv.at[mat, f * 4 + v], device_id=(z, 1 - y if f else y, flip_row(v)), device_id_type=MESH)
            for f, v in peers]

    def scale_rows(mat):
        return p.rows[mat] * p.row, p.cols[mat] * p.col

    blocks = p.mc // step_r

    def factors(mat, i, n):
        rows = pl.ds(pl.multiple_of(n * step_r, step_r), step_r)
        if mat == DOWN:
            return rows, a_cols[i, rows, :], b_rows[mat].at[:, :]
        return rows, a_cols[0, rows, :], b_rows[mat].at[:, pl.ds(pl.multiple_of(i * p.nc, p.nc), p.nc)]

    def finish_first(mat):
        parts = p.parts[mat]
        for i in range(min(2, parts)):
            get_w(mat, jnp.int32(i)).start()
        if mat == DOWN:
            block = c_sum[0]
            for i in range(parts):
                rs[mat][y, :, i * p.mc:(i + 1) * p.mc] = r_row[i]
                if i:
                    block = block + c_sum[i]
            cs[mat][r] = block
        else:
            rs[mat][y] = r_row[0]
            for i in range(parts):
                cs[mat][r, :, i * p.nc:(i + 1) * p.nc] = c_sum[i]
        for c in first_copies(mat):
            c.start()

    def finish_second(mat):
        beta_two = hyper[0]
        m_total, n_total = scale_rows(mat)
        parts = p.parts[mat]
        for c in first_copies(mat):
            c.wait_recv()
        r_new = beta_two * old[mat][0][...] + (1.0 - beta_two) * ((rs[mat][0] + rs[mat][1]) / n_total)
        c_all = ((cs[mat][0] + cs[mat][1]) + cs[mat][2]) + cs[mat][3]
        c_new = beta_two * old[mat][1][...] + (1.0 - beta_two) * (c_all / m_total)
        new[mat][0][...] = r_new
        new[mat][1][...] = c_new
        t_own = jnp.sum(r_new, axis=1, keepdims=True)
        a_row = jnp.sqrt(t_own) / jnp.sqrt(r_new)
        b_rows[mat][...] = 1.0 / jnp.sqrt(c_new)
        for i in range(parts if mat == DOWN else 1):
            a_cols[i] = jnp.broadcast_to(a_row[:, i * p.mc:(i + 1) * p.mc], (LANES, p.mc)).T

        def add_up(j, acc):
            i, n = lax.div(j, blocks), lax.rem(j, blocks)
            rows, a_block, b_ref = factors(mat, i, n)
            for c in range(0, p.nc, LANES):
                upd = grad[i, rows, c:c + LANES] * a_block * b_ref[:, c:c + LANES]
                acc = acc + fold(upd * upd)
            return acc

        u_part = lax.fori_loop(0, parts * blocks, add_up, jnp.zeros((8, LANES), F32))

        def spot(v):
            return jnp.broadcast_to(jnp.sum(jnp.sum(v, axis=1, keepdims=True), axis=0, keepdims=True), (8, LANES))

        me = y * 4 + r
        st_all[mat, me, 0] = spot(u_part)
        st_all[mat, me, 1] = spot(w_sq[mat])
        st_all[mat, me, 2] = jnp.broadcast_to(t_own, (8, LANES))
        for c in second_copies(mat):
            c.start()

    def finish_third(mat):
        rho_step, clip_thr = hyper[1], hyper[2]
        m_total, n_total = scale_rows(mat)
        me = y * 4 + r
        for c in second_copies(mat):
            c.wait_recv()
        t_all = st_all[mat, 0, 2]
        for i in range(1, p.row):
            t_all = t_all + st_all[mat, i, 2]
        u_all = st_all[mat, 0, 0] * (t_all / st_all[mat, 0, 2])
        w_all = st_all[mat, 0, 1]
        for i in range(1, p.row * p.col):
            u_all = u_all + st_all[mat, i, 0] * (t_all / st_all[mat, i, 2])
            w_all = w_all + st_all[mat, i, 1]
        upd_rms = jnp.sqrt(u_all / (m_total * n_total))
        w_rms = jnp.sqrt(w_all / (m_total * n_total))
        scale = rho_step * jnp.maximum(EPS_TWO, w_rms) / jnp.maximum(1.0, upd_rms / clip_thr)
        scale = scale * jnp.sqrt(t_all / st_all[mat, me, 2])
        b_rows[mat][...] = b_rows[mat][...] * scale[0:1, 0:1]

    def renew(mat, low_i, high_i):
        parts = p.parts[mat]

        @pl.loop(low_i, high_i)
        def _(i):
            at = lax.rem(i, 3)
            get_w(mat, i).wait()

            @pl.loop(0, blocks)
            def _(n):
                rows, a_block, b_ref = factors(mat, i, n)
                for c in range(0, p.nc, LANES):
                    cols = slice(c, c + LANES)
                    fresh = w_buf[at, rows, cols] - grad[i, rows, cols] * a_block * b_ref[:, cols]
                    if mat == ATTN:
                        o_attn[rows, cols] = fresh
                    elif mat == DOWN:
                        grad[i, rows, cols] = fresh
                    else:
                        w_buf[at, rows, cols] = fresh

            if mat in (GATE, UP):
                put_w(mat, i).start()
                pl.when(i >= 1)(lambda: put_w(mat, i - 1).wait())
            pl.when(i + 2 < parts)(lambda: get_w(mat, i + 2).start())

        if mat in (GATE, UP) and high_i == parts:
            put_w(mat, jnp.int32(parts - 1)).wait()

    def finish(mat, stage):
        parts = p.parts[mat]
        half = parts // 2 if parts > 1 else parts
        if stage == 0:
            finish_first(mat)
        elif stage == 1:
            finish_second(mat)
        elif stage == 2:
            finish_third(mat)
            renew(mat, 0, half)
        else:
            renew(mat, half, parts)

    def take_x(src, at, k):
        spread_done(k, False)
        load(src, at, p.mc, buf_x, p.at(k), tile_x)
        turn()

    def again_x():
        load(x_mlp, 0, p.mc, buf_x, 0, tile_x)
        turn()

    def got(name, i):
        k = look(i, [p.place[name, j] for j in range(sum(1 for n, _ in p.order if n == name))])
        partner(k, 0).wait_recv()
        partner(k, 1).wait_recv()
        return k

    def use_gate(i):
        pl.when(i == 0)(lambda: take_x(x_mlp, 0, jnp.int32(p.place['x_mlp', 0])))
        k = got('gate', i)
        load(dy_gate, i, p.nc, buf_d, p.at(k), tile_d)
        chunk(GATE, i)

    def use_attn(i):
        take_x(x_attn, 0, jnp.int32(p.place['x_attn', 0]))
        k = got('attn', i)
        load(dy_attn, 0, p.nc, buf_d, p.at(k), tile_d)
        chunk(ATTN, i)

    def use_up(i):
        pl.when(i == 0)(again_x)
        k = got('up', i)
        load(dy_up, i, p.nc, buf_d, p.at(k), tile_d)
        chunk(UP, i)

    def use_out(i):
        k = got('out', i)
        load(dy_out, 0, p.nc, buf_d, p.at(k), tile_d)

    def use_h(i):
        take_x(h_mlp, i, look(i, [p.place['h', j] for j in range(p.nh)]))
        chunk(DOWN, i)

    def work(t):
        for name, use in (('gate', use_gate), ('attn', use_attn), ('up', use_up), ('out', use_out), ('h', use_h)):
            at = jnp.int32(0)
            for i in range(sum(1 for n, _ in p.order if n == name)):
                when_mid = p.steps[True].get((name, i), -1)
                when_end = p.steps[False].get((name, i), -1)
                at = jnp.where(t == jnp.where(mid, when_mid, when_end), i + 1, at)
            pl.when(at > 0)(functools.partial(use, at - 1))
        for mat in MATS:
            for stage in range(4):
                when_mid = p.steps[True].get(('finish', mat, stage), -1)
                when_end = p.steps[False].get(('finish', mat, stage), -1)
                if when_mid >= 0:
                    pl.when(t == jnp.where(mid, when_mid, when_end))(functools.partial(finish, mat, stage))

    def to_end():
        pairs = ((o_attn, o_attn), (nr_attn, nr_attn), (nc_attn, nc_attn))
        return [pltpu.make_async_remote_copy(
            src_ref=a, dst_ref=b, send_sem=e_send.at[i], recv_sem=e_recv.at[i],
            device_id=(end_z, y, r), device_id_type=MESH) for i, (a, b) in enumerate(pairs)]

    w_sq[...] = jnp.zeros_like(w_sq)
    ahead = jnp.where(mid, AHEAD_MID, AHEAD_END)

    @pl.loop(0, AHEAD_END)
    def _(k):
        pl.when(k < ahead)(lambda: send_own(k))

    @pl.when(mid)
    def _():
        arrive(jnp.int32(0), jnp.int32(2), jnp.bool_(False))

    @pl.loop(0, p.turns)
    def _(t):
        d, turn_no = lax.div(t, 3), lax.rem(t, 3)
        pl.when((turn_no == 0) & (d >= 1) & (d <= p.count))(lambda: own_first_left(d - 1))
        early = mid & (turn_no == 0)
        k = jnp.where(early, d + 1, d)
        e = jnp.where(mid, lax.rem(turn_no + 2, 3), turn_no)
        pl.when(k < p.count)(lambda: arrive(k, e, turn_no == 2))

        @pl.when(turn_no == 2)
        def _():
            pl.when(d + ahead < p.count)(lambda: send_own(d + ahead))

            @pl.when((d == p.count - 1) & mid)
            def _():
                for c in to_end():
                    c.start()

            k = d - LATE

            @pl.when((k >= 0) & (k < p.count) & p.is_dy(k) & (mid | jnp.logical_not(p.is_attn(k))))
            def _():
                spread_done(k, True)
                partner(k, 1).start()

        work(t)

    @pl.loop(0, p.count)
    def _(k):
        def go(dy):
            some = slot(k, 0, dy)

            @pl.when(mid)
            def _():
                pass_on(k, dy, some, z, 0, 1).wait_send()
                pass_on(k, dy, some, z, 0, 4).wait_send()

                @pl.when(jnp.logical_not(p.is_attn(k)))
                def _():
                    pass_on(k, dy, some, z, 0, 2).wait_send()
                    pass_on(k, dy, some, z, 0, 3).wait_send()

            for s in range(p.dp - 1):
                spread(k, s, dy).wait_send()
            if dy:
                partner(k, 0).wait_send()
                partner(k, 1).wait_send()

        typed(k, go)

    for mat in (GATE, UP, DOWN):
        for c in first_copies(mat) + second_copies(mat):
            c.wait_send()

    @pl.when(mid)
    def _():
        for c in first_copies(ATTN) + second_copies(ATTN):
            c.wait_send()
        for c in to_end():
            c.wait_send()

    @pl.when(jnp.logical_not(mid))
    def _():
        for c in to_end():
            c.wait_recv()


def store_kernel(plan, o_attn, o_gate, o_up, o_down, *refs):
    p = plan
    stats, (w_attn, w_gate, w_up, w_down), outs = refs[:8], refs[8:12], refs[12:20]
    bounce, in_sem, out_sem, s_sem = refs[20:]
    depth = bounce.shape[0]

    def cut(ref, i):
        return ref.at[:, i * p.nc:(i + 1) * p.nc]

    through = [(cut(o_gate, i), cut(w_gate, i)) for i in range(p.ng)] + [(cut(o_up, i), cut(w_up, i)) for i in range(p.ng)]
    loads = [pltpu.make_async_copy(a, bounce.at[i % depth], in_sem.at[i]) for i, (a, _) in enumerate(through)]
    puts = [pltpu.make_async_copy(bounce.at[i % depth], b, out_sem.at[i]) for i, (_, b) in enumerate(through)]
    for c in loads[:depth]:
        c.start()
    copies = [pltpu.make_async_copy(a, b, s_sem.at[i]) for i, (a, b) in enumerate(zip(stats, outs))]
    copies.append(pltpu.make_async_copy(o_attn, w_attn, s_sem.at[8]))
    for i in range(p.nh):
        copies.append(pltpu.make_async_copy(o_down.at[i], w_down.at[i * p.mc:(i + 1) * p.mc, :], s_sem.at[9 + i]))
    for c in copies:
        c.start()
    for i in range(len(through)):
        loads[i].wait()
        puts[i].start()
        again = i - depth // 2
        if 0 <= again and again + depth < len(through):
            puts[again].wait()
            loads[again + depth].start()
    for i in range(max(0, len(through) - depth), len(through)):
        puts[i].wait()
    for c in copies:
        c.wait()


def solution(mesh):
    act_spec = P('dp', 'row')
    grad_spec = P('dp', 'col')
    w_spec = P('row', 'col')
    row_spec = P('row')
    col_spec = P('col')
    in_specs = (act_spec, grad_spec, act_spec, grad_spec, grad_spec, act_spec, grad_spec,
                w_spec, w_spec, w_spec, w_spec,
                row_spec, col_spec, row_spec, col_spec, row_spec, col_spec, row_spec, col_spec, P())
    out_specs = (w_spec, row_spec, col_spec) * 4

    def per_device(x_attn, dy_attn, x_mlp, dy_gate, dy_up, h_mlp, dy_out, w_attn, w_gate, w_up, w_down,
                   r_attn, c_attn, r_gate, c_gate, r_up, c_up, r_down, c_down, hyper_params):
        p = Plan(x_mlp, dy_gate, h_mlp, dy_out, mesh)
        stats = [v.reshape(1, -1) for v in (r_attn, c_attn, r_gate, c_gate, r_up, c_up, r_down, c_down)]
        any_spec = pl.BlockSpec(memory_space=pl.ANY)
        vmem_spec = pl.BlockSpec(memory_space=pltpu.VMEM)
        row_shapes = []
        for mat in MATS:
            row_shapes += [jax.ShapeDtypeStruct((1, p.rows[mat]), F32), jax.ShapeDtypeStruct((1, p.cols[mat]), F32)]
        w_shapes = [jax.ShapeDtypeStruct((p.rows[mat], p.cols[mat]), F32) for mat in MATS]
        o_shapes = [pltpu.VMEM((p.mc, p.nc), F32), w_shapes[GATE], w_shapes[UP],
                    pltpu.VMEM((p.pieces, p.mc, p.nc), F32)]
        bufs = [jax.ShapeDtypeStruct((p.n_dy, p.dp - 1, p.tok, p.nc), BF16),
                jax.ShapeDtypeStruct((p.n_x, p.dp - 1, p.tok, p.mc), BF16)]
        dma = pltpu.SemaphoreType.DMA
        scratch = [
            pltpu.VMEM((p.dp, p.mc, p.tok), BF16),
            pltpu.VMEM((p.dp, p.tok, p.mc), BF16),
            pltpu.VMEM((p.dp, p.tok, p.nc), BF16),
            pltpu.VMEM((3, p.mc, p.nc), F32),
            pltpu.VMEM((p.mc, LANES), F32),
            pltpu.VMEM((p.pieces, 1, p.mc), F32),
            pltpu.VMEM((p.pieces, 1, p.nc), F32),
            pltpu.VMEM((p.nh, p.mc, LANES), F32),
            pltpu.VMEM((4, 8, LANES), F32),
        ]
        scratch += [pltpu.VMEM((1, p.cols[mat]), F32) for mat in MATS]
        scratch += [pltpu.VMEM((2, 1, p.rows[mat]), F32) for mat in MATS]
        scratch += [pltpu.VMEM((4, 1, p.cols[mat]), F32) for mat in MATS]
        scratch += [
            pltpu.VMEM((4, 8, 3, 8, LANES), F32),
            dma((p.count, 5)), dma((p.count, p.dp - 1)),
            dma((p.count, p.dp - 1)), dma((p.count, p.dp - 1)),
            dma((p.n_dy, 2)), dma((p.n_dy, 2)),
            dma((4, 4)), dma((4, 4)), dma((4, 8)), dma((4, 8)),
            dma((3,)), dma((3,)),
            dma((p.dp,)), dma((3,)), dma((3,)),
        ]
        out = pl.pallas_call(
            functools.partial(gather_kernel, p),
            out_shape=o_shapes + [pltpu.VMEM(v.shape, F32) for v in row_shapes] + bufs,
            in_specs=[any_spec] * 11 + [vmem_spec] * 8 + [pl.BlockSpec(memory_space=pltpu.SMEM)],
            out_specs=[vmem_spec, any_spec, any_spec, vmem_spec] + [vmem_spec] * 8 + [any_spec] * 2,
            scratch_shapes=scratch,
            compiler_params=pltpu.CompilerParams(collective_id=0, has_side_effects=True, vmem_limit_bytes=VMEM_LIMIT),
        )(x_attn, dy_attn, x_mlp, dy_gate, dy_up, h_mlp, dy_out, w_attn, w_gate, w_up, w_down, *stats, hyper_params)
        res = pl.pallas_call(
            functools.partial(store_kernel, p),
            out_shape=w_shapes + row_shapes,
            in_specs=[vmem_spec, any_spec, any_spec, vmem_spec] + [vmem_spec] * 8,
            out_specs=[any_spec] * 12,
            scratch_shapes=[pltpu.VMEM((8, p.mc, p.nc), F32), dma((2 * p.ng,)), dma((2 * p.ng,)), dma((9 + p.nh,))],
            compiler_params=pltpu.CompilerParams(vmem_limit_bytes=STORE_LIMIT),
        )(*[pltpu.with_memory_space_constraint(v, pltpu.VMEM) if i in KEPT else v for i, v in enumerate(out[:12])])
        result = []
        for mat in MATS:
            result += [res[mat], res[4 + 2 * mat].reshape(-1), res[5 + 2 * mat].reshape(-1)]
        return tuple(result)

    return jax.shard_map(per_device, mesh=mesh, in_specs=in_specs, out_specs=out_specs, check_vma=False)
```

```python
import functools
import jax
import jax.numpy as jnp
from jax import lax
from jax.experimental import pallas as pl
from jax.experimental.pallas import tpu as pltpu
from jax.sharding import PartitionSpec as P

EPS_ONE = 1e-30
EPS_TWO = 1e-3
MESH = pl.DeviceIdType.MESH
LANES = 128
F32 = jnp.float32
BF16 = jnp.bfloat16
ATTN, GATE, UP, DOWN = range(4)
MATS = (ATTN, GATE, UP, DOWN)
FIRST = {'gate': ('x_mlp', 0), 'attn': ('x_attn', 0), 'up': ('x_mlp', 0), 'h': ('out', 0)}
AHEAD_MID, AHEAD_END = 2, 6
LATE = 3
VMEM_LIMIT = 28 * 1024 * 1024
STORE_LIMIT = 28 * 1024 * 1024
UP_KEPT = True
HBM_KEPT = (1,) if UP_KEPT else (1, 2)
DEPTH, WIDE = 4, 4


def look(k, table):
    out = jnp.int32(0)
    for i, v in enumerate(table):
        if v:
            out = jnp.where(k == i, v, out)
    return out


class Plan:
    def __init__(self, x_mlp, dy_gate, h_mlp, dy_out, mesh):
        self.dp, self.col, self.row = mesh.shape['dp'], mesh.shape['col'], mesh.shape['row']
        assert (self.dp, self.col, self.row) == (4, 2, 4)
        self.tok = x_mlp.shape[0]
        self.mc = x_mlp.shape[1]
        self.nc = dy_out.shape[1]
        self.ng = dy_gate.shape[1] // self.nc
        self.nh = h_mlp.shape[1] // self.mc
        self.tq = self.tok // self.row
        self.th = self.tok // self.col
        g = [('gate', i) for i in range(self.ng)]
        u = [('up', i) for i in range(self.ng)]
        h = [('h', i) for i in range(self.nh)]
        self.order = [('x_mlp', 0)] + g + [('x_attn', 0), ('attn', 0)] + u + [('out', 0)] + h
        self.count = len(self.order)
        self.place = {v: k for k, v in enumerate(self.order)}
        self.n_dy = 2 * self.ng + 2
        self.n_x = self.nh + 2
        self.pieces = max(self.ng, self.nh)
        self.rows = {ATTN: self.mc, GATE: self.mc, UP: self.mc, DOWN: self.mc * self.nh}
        self.cols = {ATTN: self.nc, GATE: self.nc * self.ng, UP: self.nc * self.ng, DOWN: self.nc}
        self.parts = {ATTN: 1, GATE: self.ng, UP: self.ng, DOWN: self.nh}
        base = {'gate': 0, 'up': self.ng, 'out': 2 * self.ng, 'attn': 2 * self.ng + 1, 'x_mlp': 0, 'x_attn': 1, 'h': 2}
        self.dy_table = [1 if n in ('gate', 'up', 'out', 'attn') else 0 for n, _ in self.order]
        self.at_table = [base[n] + i for n, i in self.order]
        self.attn_table = [1 if n in ('x_attn', 'attn') else 0 for n, _ in self.order]
        self.steps = {m: self.schedule(m) for m in (True, False)}
        last = max(max(v.values()) for v in self.steps.values())
        self.turns = max(last + 1, 3 * (self.count + LATE + 1))

    def schedule(self, mid):
        tasks = []
        for name, mat in (('gate', GATE), ('attn', ATTN), ('up', UP), ('h', DOWN)):
            if name == 'attn' and not mid:
                continue
            for i in range(self.parts[mat]):
                k = self.place[name, i]
                need = [3 * (k + LATE + 1)] if name != 'h' else [3 * (k + LATE) if mid else 3 * k + 5]
                if i == 0:
                    need.append(3 * (self.place[FIRST[name]] + LATE + (name == 'h')))
                tasks.append(((name, i), max(need)))
            stages = {ATTN: (1, 2), DOWN: (1, 2)}.get(mat, (1, 2, 3))
            tasks += [(('finish', mat, stage), 0) for stage in stages]
        out, t = {}, 0
        for task, first in tasks:
            t = max(t, first)
            out[task] = t
            t += 1
        return out

    def is_dy(self, k):
        return look(k, self.dy_table) == 1

    def is_attn(self, k):
        return look(k, self.attn_table) == 1

    def at(self, k):
        return look(k, self.at_table)


def gather_kernel(plan, x_attn, dy_attn, x_mlp, dy_gate, dy_up, h_mlp, dy_out, w_attn, w_gate, w_up, w_down,
                  r_attn, c_attn, r_gate, c_gate, r_up, c_up, r_down, c_down, hyper,
                  o_attn, o_gate, o_up, grad, nr_attn, nc_attn, nr_gate, nc_gate, nr_up, nc_up, nr_down, nc_down,
                  al_down, be_down, buf_d, buf_x,
                  lhs, tile_x, tile_d, w_buf, r_lanes, r_row, c_sum, a_cols, a_rows, w_sq,
                  b_attn, b_gate, b_up, b_down,
                  rs_attn, rs_gate, rs_up, rs_down, cs_attn, cs_gate, cs_up, cs_down, st_all,
                  z_send, z_recv, f_send, f_recv, c_send, c_recv, r1_send, r1_recv, r2_send, r2_recv,
                  e_send, e_recv, l_sem, wi_sem, wo_sem):
    p = plan
    z, y, r = lax.axis_index('dp'), lax.axis_index('col'), lax.axis_index('row')
    low = z < 2
    mid = (z == 1) | (z == 2)
    end_z = jnp.where(low, 0, 3)
    mate_z = 3 - z
    w_refs = {ATTN: w_attn, GATE: w_gate, UP: w_up, DOWN: w_down}
    old = {ATTN: (r_attn, c_attn), GATE: (r_gate, c_gate), UP: (r_up, c_up), DOWN: (r_down, c_down)}
    new = {ATTN: (nr_attn, nc_attn), GATE: (nr_gate, nc_gate), UP: (nr_up, nc_up), DOWN: (nr_down, nc_down)}
    b_rows = {ATTN: b_attn, GATE: b_gate, UP: b_up, DOWN: b_down}
    rs = {ATTN: rs_attn, GATE: rs_gate, UP: rs_up, DOWN: rs_down}
    cs = {ATTN: cs_attn, GATE: cs_gate, UP: cs_up, DOWN: cs_down}

    def flip_row(v):
        bit0, bit1 = lax.rem(r, 2), lax.div(r, 2)
        if v & 1:
            bit0 = 1 - bit0
        if v & 2:
            bit1 = 1 - bit1
        return bit1 * 2 + bit0

    peers = [(f, v) for f in range(2) for v in range(4) if f or v]
    barrier = pltpu.get_barrier_semaphore()
    for f, v in peers:
        pl.semaphore_signal(barrier, inc=1, device_id=(z, 1 - y if f else y, flip_row(v)), device_id_type=MESH)

    @pl.when(mid)
    def _():
        pl.semaphore_signal(barrier, inc=1, device_id=(end_z, y, r), device_id_type=MESH)
        pl.semaphore_signal(barrier, inc=1, device_id=(mate_z, y, r), device_id_type=MESH)
        pl.semaphore_wait(barrier, len(peers) + 2)

    @pl.when(jnp.logical_not(mid))
    def _():
        pl.semaphore_signal(barrier, inc=1, device_id=(jnp.where(low, 1, 2), y, r), device_id_type=MESH)
        pl.semaphore_wait(barrier, len(peers) + 1)

    my_q = pl.ds(pl.multiple_of(r * p.tq, p.tq), p.tq)
    x_q = pl.ds(pl.multiple_of(flip_row(2) * p.tq, p.tq), p.tq)
    my_h = pl.ds(pl.multiple_of(y * p.th, p.th), p.th)

    def slot(k, s, dy):
        return buf_d.at[p.at(k), s, my_q, :] if dy else buf_x.at[p.at(k), s, my_h, :]

    def pass_on(k, dy, src, to_z, to_slot, sem):
        return pltpu.make_async_remote_copy(
            src_ref=src, dst_ref=slot(k, to_slot, dy), send_sem=z_send.at[k, sem], recv_sem=z_recv.at[k, to_slot],
            device_id=(to_z, y, r), device_id_type=MESH)

    def spread(k, s, dy):
        to = (z, y, flip_row(2)) if dy else (z, 1 - y, r)
        return pltpu.make_async_remote_copy(
            src_ref=slot(k, s, dy), dst_ref=slot(k, s, dy), send_sem=f_send.at[k, s], recv_sem=f_recv.at[k, s],
            device_id=to, device_id_type=MESH)

    def partner(k, which):
        part = buf_d.at[p.at(k), :, x_q if which else my_q, :]
        return pltpu.make_async_remote_copy(
            src_ref=part, dst_ref=part, send_sem=c_send.at[p.at(k), which], recv_sem=c_recv.at[p.at(k), which],
            device_id=(z, y, flip_row(1)), device_id_type=MESH)

    def typed(k, go):
        used = mid | jnp.logical_not(p.is_attn(k))
        pl.when(p.is_dy(k) & used)(lambda: go(True))
        pl.when(jnp.logical_not(p.is_dy(k)) & used)(lambda: go(False))

    def cut(ref, at, size):
        return ref.at[:, pl.ds(pl.multiple_of(at * size, size), size)]

    def down_rows(ref, i):
        return ref.at[pl.ds(pl.multiple_of(i * p.mc, p.mc), p.mc), :]

    def own_to(k, dy, src):
        @pl.when(jnp.logical_not(mid))
        def _():
            pass_on(k, dy, src, jnp.where(low, 1, 2), jnp.where(low, 2, 0), 0).start()

        @pl.when(mid)
        def _():
            @pl.when(jnp.logical_not(p.is_attn(k)))
            def _():
                pass_on(k, dy, src, end_z, jnp.where(low, 0, 2), 0).start()
            pass_on(k, dy, src, mate_z, jnp.where(low, 2, 0), 1).start()

    def send_own(k):
        def go(ref, at, size, dy):
            own_to(k, dy, ref.at[my_q if dy else my_h, pl.ds(pl.multiple_of(at * size, size), size)])

        for name, ref, dy in (('x_mlp', x_mlp, False), ('gate', dy_gate, True), ('x_attn', x_attn, False),
                              ('attn', dy_attn, True), ('up', dy_up, True), ('out', dy_out, True), ('h', h_mlp, False)):
            at = look(k, [i + 1 if n == name else 0 for n, i in p.order])
            size = p.nc if dy else p.mc
            pl.when(at > 0)(functools.partial(go, ref, at - 1, size, dy))

    def own_first_left(k):
        @pl.when(jnp.logical_not(mid & p.is_attn(k)))
        def _():
            pl.when(p.is_dy(k))(lambda: pass_on(k, True, slot(k, 0, True), z, 0, 0).wait_send())
            pl.when(jnp.logical_not(p.is_dy(k)))(lambda: pass_on(k, False, slot(k, 0, False), z, 0, 0).wait_send())

    def arrive(k, e, whole):
        s = jnp.where(low, e, 2 - e)

        def go(dy):
            pass_on(k, dy, slot(k, s, dy), z, s, 0).wait_recv()

            @pl.when(mid & (e == 2))
            def _():
                pass_on(k, dy, slot(k, s, dy), mate_z, 1, 4).start()

            @pl.when(mid & (e < 2) & jnp.logical_not(p.is_attn(k)))
            def _():
                pass_on(k, dy, slot(k, s, dy), end_z, jnp.where(low, s + 1, s - 1), 2 + e).start()

            spread(k, s, dy).start()
            if dy and whole:
                pl.when(e == jnp.where(mid, 1, 2))(lambda: partner(k, 0).start())

        typed(k, go)

    def spread_done(k, dy):
        for s in range(p.dp - 1):
            spread(k, s, dy).wait_recv()

    def load(src, at, size, buf, index, dst):
        copies = [pltpu.make_async_copy(cut(src, at, size), dst.at[z], l_sem.at[0])]
        for d in range(1, p.dp):
            copies.append(pltpu.make_async_copy(buf.at[index, d - 1], dst.at[lax.rem(z + d, p.dp)], l_sem.at[d]))
        for c in copies:
            c.start()
        for c in copies:
            c.wait()

    step_t = min(256, p.tok)

    def turn():
        @pl.loop(0, p.dp)
        def _(q):
            @pl.loop(0, p.tok // step_t)
            def _(t):
                at = pl.multiple_of(t * step_t, step_t)
                lhs[q, :, pl.ds(at, step_t)] = tile_x[q, pl.ds(at, step_t), :].T

    step_n = min(512, p.nc)
    step_r = min(64, p.mc)

    def lane_sum(v):
        out = v[:, 0:LANES]
        for i in range(1, v.shape[1] // LANES):
            out = out + v[:, i * LANES:(i + 1) * LANES]
        return out

    def product(at):
        r_lanes[...] = jnp.zeros_like(r_lanes)

        @pl.loop(0, p.nc // step_n)
        def _(n):
            cols = pl.ds(pl.multiple_of(n * step_n, step_n), step_n)
            grad[at, :, cols] = jnp.dot(lhs[0], tile_d[0, :, cols], preferred_element_type=F32)

            @pl.loop(1, p.dp)
            def _(q):
                grad[at, :, cols] += jnp.dot(lhs[q], tile_d[q, :, cols], preferred_element_type=F32)

            def body(i, acc):
                rows = pl.ds(pl.multiple_of(i * step_r, step_r), step_r)
                block = grad[at, rows, cols]
                sq = block * block + EPS_ONE
                r_lanes[rows, :] += lane_sum(sq)
                return acc + jnp.sum(sq, axis=0, keepdims=True)

            c_sum[at, :, cols] = lax.fori_loop(0, p.mc // step_r, body, jnp.zeros((1, step_n), F32))

    def fold(v):
        v = jnp.reshape(v, (v.shape[0] // 8, 8, LANES))
        while v.shape[0] > 1:
            v = v[:v.shape[0] // 2] + v[v.shape[0] // 2:]
        return v[0]

    def to_row(block):
        return jnp.sum(block.T, axis=0, keepdims=True)

    def get_w(mat, i):
        src = down_rows(w_refs[mat], i) if mat == DOWN else cut(w_refs[mat], i, p.nc)
        return pltpu.make_async_copy(src, w_buf.at[lax.rem(i, 3)], wi_sem.at[lax.rem(i, 3)])

    def put_w(mat, i):
        dst = cut(o_gate if mat == GATE else o_up, i, p.nc)
        return pltpu.make_async_copy(w_buf.at[lax.rem(i, 3)], dst, wo_sem.at[lax.rem(i, 3)])

    def chunk(mat, i):
        get_w(mat, i).start()
        product(i)
        row = to_row(r_lanes[...])
        if mat == DOWN:
            r_row[i] = row
        else:
            r_row[0] = jnp.where(i == 0, row, r_row[0] + row)
        get_w(mat, i).wait()

        def body(n, acc):
            rows = pl.ds(pl.multiple_of(n * step_r, step_r), step_r)
            block = lane_sum(w_buf[lax.rem(i, 3), rows, :] * w_buf[lax.rem(i, 3), rows, :])
            return acc + fold(block)

        w_sq[mat] += lax.fori_loop(0, p.mc // step_r, body, jnp.zeros((8, LANES), F32))

    def first_copies(mat):
        copies = [pltpu.make_async_remote_copy(
            src_ref=rs[mat].at[y], dst_ref=rs[mat].at[y], send_sem=r1_send.at[mat, 0], recv_sem=r1_recv.at[mat, 0],
            device_id=(z, 1 - y, r), device_id_type=MESH)]
        for v in range(1, 4):
            copies.append(pltpu.make_async_remote_copy(
                src_ref=cs[mat].at[r], dst_ref=cs[mat].at[r], send_sem=r1_send.at[mat, v],
                recv_sem=r1_recv.at[mat, v], device_id=(z, y, flip_row(v)), device_id_type=MESH))
        return copies

    def second_copies(mat):
        me = y * 4 + r
        return [pltpu.make_async_remote_copy(
            src_ref=st_all.at[mat, me], dst_ref=st_all.at[mat, me], send_sem=r2_send.at[mat, f * 4 + v],
            recv_sem=r2_recv.at[mat, f * 4 + v], device_id=(z, 1 - y if f else y, flip_row(v)), device_id_type=MESH)
            for f, v in peers]

    def scale_rows(mat):
        return p.rows[mat] * p.row, p.cols[mat] * p.col

    blocks = p.mc // step_r

    def factors(mat, i, n):
        rows = pl.ds(pl.multiple_of(n * step_r, step_r), step_r)
        if mat == DOWN:
            return rows, a_cols[i, rows, :], b_rows[mat].at[:, :]
        return rows, a_cols[0, rows, :], b_rows[mat].at[:, pl.ds(pl.multiple_of(i * p.nc, p.nc), p.nc)]

    def finish_first(mat):
        parts = p.parts[mat]
        if mat != DOWN:
            for i in range(min(2, parts)):
                get_w(mat, jnp.int32(i)).start()
        if mat == DOWN:
            block = c_sum[0]
            for i in range(parts):
                rs[mat][y, :, i * p.mc:(i + 1) * p.mc] = r_row[i]
                if i:
                    block = block + c_sum[i]
            cs[mat][r] = block
        else:
            rs[mat][y] = r_row[0]
            for i in range(parts):
                cs[mat][r, :, i * p.nc:(i + 1) * p.nc] = c_sum[i]
        for c in first_copies(mat):
            c.start()

    def finish_second(mat):
        beta_two = hyper[0]
        m_total, n_total = scale_rows(mat)
        parts = p.parts[mat]
        for c in first_copies(mat):
            c.wait_recv()
        r_new = beta_two * old[mat][0][...] + (1.0 - beta_two) * ((rs[mat][0] + rs[mat][1]) / n_total)
        c_all = ((cs[mat][0] + cs[mat][1]) + cs[mat][2]) + cs[mat][3]
        c_new = beta_two * old[mat][1][...] + (1.0 - beta_two) * (c_all / m_total)
        new[mat][0][...] = r_new
        new[mat][1][...] = c_new
        t_own = jnp.sum(r_new, axis=1, keepdims=True)
        a_row = jnp.sqrt(t_own) / jnp.sqrt(r_new)
        b_rows[mat][...] = 1.0 / jnp.sqrt(c_new)
        if mat == DOWN:
            a_rows[...] = a_row
        for i in range(parts if mat == DOWN else 1):
            a_cols[i] = jnp.broadcast_to(a_row[:, i * p.mc:(i + 1) * p.mc], (LANES, p.mc)).T

        def add_up(j, acc):
            i, n = lax.div(j, blocks), lax.rem(j, blocks)
            rows, a_block, b_ref = factors(mat, i, n)
            for c in range(0, p.nc, LANES):
                upd = grad[i, rows, c:c + LANES] * a_block * b_ref[:, c:c + LANES]
                acc = acc + fold(upd * upd)
            return acc

        u_part = lax.fori_loop(0, parts * blocks, add_up, jnp.zeros((8, LANES), F32))

        def spot(v):
            return jnp.broadcast_to(jnp.sum(jnp.sum(v, axis=1, keepdims=True), axis=0, keepdims=True), (8, LANES))

        me = y * 4 + r
        st_all[mat, me, 0] = spot(u_part)
        st_all[mat, me, 1] = spot(w_sq[mat])
        st_all[mat, me, 2] = jnp.broadcast_to(t_own, (8, LANES))
        for c in second_copies(mat):
            c.start()

    def finish_third(mat):
        rho_step, clip_thr = hyper[1], hyper[2]
        m_total, n_total = scale_rows(mat)
        me = y * 4 + r
        for c in second_copies(mat):
            c.wait_recv()
        t_all = st_all[mat, 0, 2]
        for i in range(1, p.row):
            t_all = t_all + st_all[mat, i, 2]
        u_all = st_all[mat, 0, 0] * (t_all / st_all[mat, 0, 2])
        w_all = st_all[mat, 0, 1]
        for i in range(1, p.row * p.col):
            u_all = u_all + st_all[mat, i, 0] * (t_all / st_all[mat, i, 2])
            w_all = w_all + st_all[mat, i, 1]
        upd_rms = jnp.sqrt(u_all / (m_total * n_total))
        w_rms = jnp.sqrt(w_all / (m_total * n_total))
        scale = rho_step * jnp.maximum(EPS_TWO, w_rms) / jnp.maximum(1.0, upd_rms / clip_thr)
        scale = scale * jnp.sqrt(t_all / st_all[mat, me, 2])
        b_rows[mat][...] = b_rows[mat][...] * scale[0:1, 0:1]

    def renew(mat, low_i, high_i):
        parts = p.parts[mat]

        @pl.loop(low_i, high_i)
        def _(i):
            at = lax.rem(i, 3)
            get_w(mat, i).wait()

            @pl.loop(0, blocks)
            def _(n):
                rows, a_block, b_ref = factors(mat, i, n)
                for c in range(0, p.nc, LANES):
                    cols = slice(c, c + LANES)
                    fresh = w_buf[at, rows, cols] - grad[i, rows, cols] * a_block * b_ref[:, cols]
                    if mat == ATTN:
                        o_attn[rows, cols] = fresh
                    elif mat == UP and UP_KEPT:
                        o_up[i, rows, cols] = fresh
                    else:
                        w_buf[at, rows, cols] = fresh

            if mat == GATE or (mat == UP and not UP_KEPT):
                put_w(mat, i).start()
                pl.when(i >= 1)(lambda: put_w(mat, i - 1).wait())
            pl.when(i + 2 < parts)(lambda: get_w(mat, i + 2).start())

        if (mat == GATE or (mat == UP and not UP_KEPT)) and high_i == parts:
            put_w(mat, jnp.int32(parts - 1)).wait()

    def finish(mat, stage):
        parts = p.parts[mat]
        half = parts // 2 if parts > 1 else parts
        if stage == 1:
            finish_second(mat)
        elif stage == 2:
            finish_third(mat)
            if mat == DOWN:
                al_down[...] = a_rows[...]
                be_down[...] = b_rows[mat][...]
            else:
                renew(mat, 0, half)
        else:
            renew(mat, half, parts)

    def take_x(src, at, k):
        spread_done(k, False)
        load(src, at, p.mc, buf_x, p.at(k), tile_x)
        turn()

    def again_x():
        load(x_mlp, 0, p.mc, buf_x, 0, tile_x)
        turn()

    def got(name, i):
        k = look(i, [p.place[name, j] for j in range(sum(1 for n, _ in p.order if n == name))])
        partner(k, 0).wait_recv()
        partner(k, 1).wait_recv()
        return k

    def use_gate(i):
        pl.when(i == 0)(lambda: take_x(x_mlp, 0, jnp.int32(p.place['x_mlp', 0])))
        k = got('gate', i)
        load(dy_gate, i, p.nc, buf_d, p.at(k), tile_d)
        chunk(GATE, i)
        pl.when(i == p.parts[GATE] - 1)(lambda: finish_first(GATE))

    def use_attn(i):
        take_x(x_attn, 0, jnp.int32(p.place['x_attn', 0]))
        k = got('attn', i)
        load(dy_attn, 0, p.nc, buf_d, p.at(k), tile_d)
        chunk(ATTN, i)
        finish_first(ATTN)

    def use_up(i):
        pl.when(i == 0)(again_x)
        k = got('up', i)
        load(dy_up, i, p.nc, buf_d, p.at(k), tile_d)
        chunk(UP, i)
        pl.when(i == p.parts[UP] - 1)(lambda: finish_first(UP))

    def use_out():
        k = got('out', jnp.int32(0))
        load(dy_out, 0, p.nc, buf_d, p.at(k), tile_d)

    def use_h(i):
        pl.when(i == 0)(use_out)
        take_x(h_mlp, i, look(i, [p.place['h', j] for j in range(p.nh)]))
        chunk(DOWN, i)
        pl.when(i == p.parts[DOWN] - 1)(lambda: finish_first(DOWN))

    def work(t):
        for name, use in (('gate', use_gate), ('attn', use_attn), ('up', use_up), ('h', use_h)):
            at = jnp.int32(0)
            for i in range(sum(1 for n, _ in p.order if n == name)):
                when_mid = p.steps[True].get((name, i), -1)
                when_end = p.steps[False].get((name, i), -1)
                at = jnp.where(t == jnp.where(mid, when_mid, when_end), i + 1, at)
            pl.when(at > 0)(functools.partial(use, at - 1))
        for mat in MATS:
            for stage in (1, 2, 3):
                when_mid = p.steps[True].get(('finish', mat, stage), -1)
                when_end = p.steps[False].get(('finish', mat, stage), -1)
                if when_mid >= 0:
                    pl.when(t == jnp.where(mid, when_mid, when_end))(functools.partial(finish, mat, stage))

    def to_end():
        pairs = ((o_attn, o_attn), (nr_attn, nr_attn), (nc_attn, nc_attn))
        return [pltpu.make_async_remote_copy(
            src_ref=a, dst_ref=b, send_sem=e_send.at[i], recv_sem=e_recv.at[i],
            device_id=(end_z, y, r), device_id_type=MESH) for i, (a, b) in enumerate(pairs)]

    w_sq[...] = jnp.zeros_like(w_sq)
    ahead = jnp.where(mid, AHEAD_MID, AHEAD_END)

    @pl.loop(0, AHEAD_END)
    def _(k):
        pl.when(k < ahead)(lambda: send_own(k))

    @pl.when(mid)
    def _():
        arrive(jnp.int32(0), jnp.int32(2), False)

    @pl.when(jnp.logical_not(mid))
    def _():
        for k in range(AHEAD_MID):
            arrive(jnp.int32(k), jnp.int32(0), False)

    @pl.loop(0, p.turns)
    def _(t):
        d, turn_no = lax.div(t, 3), lax.rem(t, 3)
        pl.when((turn_no == 0) & (d >= 1) & (d <= p.count))(lambda: own_first_left(d - 1))
        early = jnp.where(mid, jnp.where(turn_no == 0, 1, 0), jnp.where(turn_no == 2, AHEAD_MID, 0))
        e = lax.rem(turn_no + jnp.where(mid, 2, 1), 3)
        k = d + early
        pl.when(k < p.count)(lambda: arrive(k, e, True))

        @pl.when(turn_no == 2)
        def _():
            pl.when(d + ahead < p.count)(lambda: send_own(d + ahead))

            @pl.when((d == p.count - 1) & mid)
            def _():
                for c in to_end():
                    c.start()

            k = d - LATE

            @pl.when((k >= 0) & (k < p.count) & p.is_dy(k) & (mid | jnp.logical_not(p.is_attn(k))))
            def _():
                spread_done(k, True)
                partner(k, 1).start()

        work(t)

    @pl.loop(0, p.count)
    def _(k):
        def go(dy):
            some = slot(k, 0, dy)

            @pl.when(mid)
            def _():
                pass_on(k, dy, some, z, 0, 1).wait_send()
                pass_on(k, dy, some, z, 0, 4).wait_send()

                @pl.when(jnp.logical_not(p.is_attn(k)))
                def _():
                    pass_on(k, dy, some, z, 0, 2).wait_send()
                    pass_on(k, dy, some, z, 0, 3).wait_send()

            for s in range(p.dp - 1):
                spread(k, s, dy).wait_send()
            if dy:
                partner(k, 0).wait_send()
                partner(k, 1).wait_send()

        typed(k, go)

    for mat in (GATE, UP, DOWN):
        for c in first_copies(mat) + second_copies(mat):
            c.wait_send()

    @pl.when(mid)
    def _():
        for c in first_copies(ATTN) + second_copies(ATTN):
            c.wait_send()
        for c in to_end():
            c.wait_send()

    @pl.when(jnp.logical_not(mid))
    def _():
        for c in to_end():
            c.wait_recv()


def store_kernel(plan, o_attn, o_gate, o_up, grad, *refs):
    p = plan
    stats, al_down, be_down, w_old, (w_attn, w_gate, w_up, w_down), outs = (
        refs[:8], refs[8], refs[9], refs[10], refs[11:15], refs[15:23])
    bounce, w_buf, a_col, in_sem, out_sem, s_sem, wi_sem, wo_sem = refs[23:]
    depth, wide = bounce.shape[0], w_buf.shape[0]

    def cut(ref, i):
        return ref.at[:, i * p.nc:(i + 1) * p.nc]

    def rows(ref, i):
        return ref.at[i * p.mc:(i + 1) * p.mc, :]

    through = [(cut(o_gate, i), cut(w_gate, i)) for i in range(p.ng)]
    if not UP_KEPT:
        through += [(cut(o_up, i), cut(w_up, i)) for i in range(p.ng)]
    loads = [pltpu.make_async_copy(a, bounce.at[i % depth], in_sem.at[i]) for i, (a, _) in enumerate(through)]
    puts = [pltpu.make_async_copy(bounce.at[i % depth], b, out_sem.at[i]) for i, (_, b) in enumerate(through)]
    w_in = [pltpu.make_async_copy(rows(w_old, i), w_buf.at[i % wide], wi_sem.at[i]) for i in range(p.nh)]
    w_out = [pltpu.make_async_copy(w_buf.at[i % wide], rows(w_down, i), wo_sem.at[i]) for i in range(p.nh)]
    for i in range(wide // 2):
        w_in[i].start()
    for c in loads[:depth]:
        c.start()
    copies = [pltpu.make_async_copy(a, b, s_sem.at[i]) for i, (a, b) in enumerate(zip(stats, outs))]
    copies.append(pltpu.make_async_copy(o_attn, w_attn, s_sem.at[8]))
    if UP_KEPT:
        copies += [pltpu.make_async_copy(o_up.at[i], cut(w_up, i), s_sem.at[9 + i]) for i in range(p.ng)]
    for c in copies:
        c.start()
    step_r = min(64, p.mc)
    per = -(-len(through) // p.nh)
    done = 0
    for i in range(p.nh):
        a_col[...] = jnp.broadcast_to(al_down[:, i * p.mc:(i + 1) * p.mc], (LANES, p.mc)).T
        w_in[i].wait()

        @pl.loop(0, p.mc // step_r)
        def _(n):
            at = pl.ds(pl.multiple_of(n * step_r, step_r), step_r)
            a_block = a_col[at, :]
            for c in range(0, p.nc, LANES):
                cols = slice(c, c + LANES)
                w_buf[i % wide, at, cols] = w_buf[i % wide, at, cols] - grad[i, at, cols] * a_block * be_down[:, cols]

        w_out[i].start()
        again = i + wide // 2
        if again < p.nh:
            if again >= wide:
                w_out[again - wide].wait()
            w_in[again].start()
        for j in range(done, min(len(through), done + per)):
            loads[j].wait()
            puts[j].start()
            again = j + depth // 2
            if depth <= again < len(through):
                puts[again - depth].wait()
                loads[again].start()
        done += per
    for i in range(max(0, p.nh - wide), p.nh):
        if i + wide >= p.nh:
            w_out[i].wait()
    for i in range(max(0, len(through) - depth), len(through)):
        puts[i].wait()
    for c in copies:
        c.wait()


def solution(mesh):
    act_spec = P('dp', 'row')
    grad_spec = P('dp', 'col')
    w_spec = P('row', 'col')
    row_spec = P('row')
    col_spec = P('col')
    in_specs = (act_spec, grad_spec, act_spec, grad_spec, grad_spec, act_spec, grad_spec,
                w_spec, w_spec, w_spec, w_spec,
                row_spec, col_spec, row_spec, col_spec, row_spec, col_spec, row_spec, col_spec, P())
    out_specs = (w_spec, row_spec, col_spec) * 4

    def per_device(x_attn, dy_attn, x_mlp, dy_gate, dy_up, h_mlp, dy_out, w_attn, w_gate, w_up, w_down,
                   r_attn, c_attn, r_gate, c_gate, r_up, c_up, r_down, c_down, hyper_params):
        p = Plan(x_mlp, dy_gate, h_mlp, dy_out, mesh)
        stats = [v.reshape(1, -1) for v in (r_attn, c_attn, r_gate, c_gate, r_up, c_up, r_down, c_down)]
        any_spec = pl.BlockSpec(memory_space=pl.ANY)
        vmem_spec = pl.BlockSpec(memory_space=pltpu.VMEM)
        up_spec = vmem_spec if UP_KEPT else any_spec
        row_shapes = []
        for mat in MATS:
            row_shapes += [jax.ShapeDtypeStruct((1, p.rows[mat]), F32), jax.ShapeDtypeStruct((1, p.cols[mat]), F32)]
        w_shapes = [jax.ShapeDtypeStruct((p.rows[mat], p.cols[mat]), F32) for mat in MATS]
        o_shapes = [pltpu.VMEM((p.mc, p.nc), F32), w_shapes[GATE],
                    pltpu.VMEM((p.ng, p.mc, p.nc), F32) if UP_KEPT else w_shapes[UP],
                    pltpu.VMEM((p.pieces, p.mc, p.nc), F32)]
        bufs = [jax.ShapeDtypeStruct((p.n_dy, p.dp - 1, p.tok, p.nc), BF16),
                jax.ShapeDtypeStruct((p.n_x, p.dp - 1, p.tok, p.mc), BF16)]
        dma = pltpu.SemaphoreType.DMA
        scratch = [
            pltpu.VMEM((p.dp, p.mc, p.tok), BF16),
            pltpu.VMEM((p.dp, p.tok, p.mc), BF16),
            pltpu.VMEM((p.dp, p.tok, p.nc), BF16),
            pltpu.VMEM((3, p.mc, p.nc), F32),
            pltpu.VMEM((p.mc, LANES), F32),
            pltpu.VMEM((p.pieces, 1, p.mc), F32),
            pltpu.VMEM((p.pieces, 1, p.nc), F32),
            pltpu.VMEM((p.nh, p.mc, LANES), F32),
            pltpu.VMEM((1, p.rows[DOWN]), F32),
            pltpu.VMEM((4, 8, LANES), F32),
        ]
        scratch += [pltpu.VMEM((1, p.cols[mat]), F32) for mat in MATS]
        scratch += [pltpu.VMEM((2, 1, p.rows[mat]), F32) for mat in MATS]
        scratch += [pltpu.VMEM((4, 1, p.cols[mat]), F32) for mat in MATS]
        scratch += [
            pltpu.VMEM((4, 8, 3, 8, LANES), F32),
            dma((p.count, 5)), dma((p.count, p.dp - 1)),
            dma((p.count, p.dp - 1)), dma((p.count, p.dp - 1)),
            dma((p.n_dy, 2)), dma((p.n_dy, 2)),
            dma((4, 4)), dma((4, 4)), dma((4, 8)), dma((4, 8)),
            dma((3,)), dma((3,)),
            dma((p.dp,)), dma((3,)), dma((3,)),
        ]
        out = pl.pallas_call(
            functools.partial(gather_kernel, p),
            out_shape=o_shapes + [pltpu.VMEM(v.shape, F32) for v in row_shapes + row_shapes[-2:]] + bufs,
            in_specs=[any_spec] * 11 + [vmem_spec] * 8 + [pl.BlockSpec(memory_space=pltpu.SMEM)],
            out_specs=[vmem_spec, any_spec, up_spec, vmem_spec] + [vmem_spec] * 10 + [any_spec] * 2,
            scratch_shapes=scratch,
            compiler_params=pltpu.CompilerParams(collective_id=0, has_side_effects=True, vmem_limit_bytes=VMEM_LIMIT),
        )(x_attn, dy_attn, x_mlp, dy_gate, dy_up, h_mlp, dy_out, w_attn, w_gate, w_up, w_down, *stats, hyper_params)
        res = pl.pallas_call(
            functools.partial(store_kernel, p),
            out_shape=w_shapes + row_shapes,
            in_specs=[vmem_spec, any_spec, up_spec, vmem_spec] + [vmem_spec] * 10 + [any_spec],
            out_specs=[any_spec] * 12,
            scratch_shapes=[pltpu.VMEM((DEPTH, p.mc, p.nc), F32), pltpu.VMEM((WIDE, p.mc, p.nc), F32),
                            pltpu.VMEM((p.mc, LANES), F32), dma((2 * p.ng,)), dma((2 * p.ng,)), dma((9 + p.ng,)),
                            dma((p.nh,)), dma((p.nh,))],
            compiler_params=pltpu.CompilerParams(vmem_limit_bytes=STORE_LIMIT),
        )(*[pltpu.with_memory_space_constraint(v, pltpu.VMEM) if i not in HBM_KEPT else v for i, v in enumerate(out[:14])],
          w_down)
        result = []
        for mat in MATS:
            result += [res[mat], res[4 + 2 * mat].reshape(-1), res[5 + 2 * mat].reshape(-1)]
        return tuple(result)

    return jax.shard_map(per_device, mesh=mesh, in_specs=in_specs, out_specs=out_specs, check_vma=False)
```

```python
import functools
import jax
import jax.numpy as jnp
from jax import lax
from jax.experimental import pallas as pl
from jax.experimental.pallas import tpu as pltpu
from jax.sharding import PartitionSpec as P

EPS_ONE = 1e-30
EPS_TWO = 1e-3
MESH = pl.DeviceIdType.MESH
LANES = 128
F32 = jnp.float32
BF16 = jnp.bfloat16
ATTN, GATE, UP, DOWN = range(4)
MATS = (ATTN, GATE, UP, DOWN)
FIRST = {'gate': ('x_mlp', 0), 'attn': ('x_attn', 0), 'up': ('x_mlp', 0), 'h': ('out', 0)}
AHEAD_MID, AHEAD_END = 2, 6
LATE_MID, LATE_END = 3, 2
VMEM_LIMIT = 28 * 1024 * 1024
STORE_LIMIT = 28 * 1024 * 1024
UP_KEPT = True
HBM_KEPT = (1,) if UP_KEPT else (1, 2)
DEPTH, WIDE = 4, 4


def look(k, table):
    out = jnp.int32(0)
    for i, v in enumerate(table):
        if v:
            out = jnp.where(k == i, v, out)
    return out


class Plan:
    def __init__(self, x_mlp, dy_gate, h_mlp, dy_out, mesh):
        self.dp, self.col, self.row = mesh.shape['dp'], mesh.shape['col'], mesh.shape['row']
        assert (self.dp, self.col, self.row) == (4, 2, 4)
        self.tok = x_mlp.shape[0]
        self.mc = x_mlp.shape[1]
        self.nc = dy_out.shape[1]
        self.ng = dy_gate.shape[1] // self.nc
        self.nh = h_mlp.shape[1] // self.mc
        self.tq = self.tok // self.row
        self.th = self.tok // self.col
        g = [('gate', i) for i in range(self.ng)]
        u = [('up', i) for i in range(self.ng)]
        h = [('h', i) for i in range(self.nh)]
        one, two = max(1, self.ng // 4), max(2, 3 * self.ng // 4)
        self.order = ([('x_mlp', 0)] + g[:one] + h[:1] + g[one:two] + h[1:2] + g[two:] + [('x_attn', 0), ('attn', 0)]
                      + u + [('out', 0)] + h[2:])
        self.count = len(self.order)
        self.place = {v: k for k, v in enumerate(self.order)}
        self.n_dy = 2 * self.ng + 2
        self.n_x = self.nh + 2
        self.pieces = max(self.ng, self.nh)
        self.rows = {ATTN: self.mc, GATE: self.mc, UP: self.mc, DOWN: self.mc * self.nh}
        self.cols = {ATTN: self.nc, GATE: self.nc * self.ng, UP: self.nc * self.ng, DOWN: self.nc}
        self.parts = {ATTN: 1, GATE: self.ng, UP: self.ng, DOWN: self.nh}
        base = {'gate': 0, 'up': self.ng, 'out': 2 * self.ng, 'attn': 2 * self.ng + 1, 'x_mlp': 0, 'x_attn': 1, 'h': 2}
        self.dy_table = [1 if n in ('gate', 'up', 'out', 'attn') else 0 for n, _ in self.order]
        self.at_table = [base[n] + i for n, i in self.order]
        self.attn_table = [1 if n in ('x_attn', 'attn') else 0 for n, _ in self.order]
        self.steps = {m: self.schedule(m) for m in (True, False)}
        last = max(max(v.values()) for v in self.steps.values())
        self.turns = max(last + 1, 3 * (self.count + LATE_MID + 1))

    def schedule(self, mid):
        late = LATE_MID if mid else LATE_END
        tasks = []
        for name, mat in (('gate', GATE), ('attn', ATTN), ('up', UP), ('h', DOWN)):
            if name == 'attn' and not mid:
                continue
            for i in range(self.parts[mat]):
                k = self.place[name, i]
                need = [3 * (k + late + 1)] if name != 'h' else [3 * (k + late) if mid else 3 * k + 5]
                if i == 0:
                    need.append(3 * (self.place[FIRST[name]] + late + (name == 'h')))
                tasks.append(((name, i), max(need)))
            stages = {ATTN: (1, 2), DOWN: (1, 2)}.get(mat, (1, 2, 3))
            tasks += [(('finish', mat, stage), 0) for stage in stages]
        out, t = {}, 0
        for task, first in tasks:
            t = max(t, first)
            out[task] = t
            t += 1
        return out

    def is_dy(self, k):
        return look(k, self.dy_table) == 1

    def is_attn(self, k):
        return look(k, self.attn_table) == 1

    def at(self, k):
        return look(k, self.at_table)


def gather_kernel(plan, x_attn, dy_attn, x_mlp, dy_gate, dy_up, h_mlp, dy_out, w_attn, w_gate, w_up, w_down,
                  r_attn, c_attn, r_gate, c_gate, r_up, c_up, r_down, c_down, hyper,
                  o_attn, o_gate, o_up, grad, nr_attn, nc_attn, nr_gate, nc_gate, nr_up, nc_up, nr_down, nc_down,
                  al_down, be_down, buf_d, buf_x,
                  lhs, tile_x, tile_d, w_buf, r_lanes, r_row, c_sum, a_cols, a_rows, w_sq,
                  b_attn, b_gate, b_up, b_down,
                  rs_attn, rs_gate, rs_up, rs_down, cs_attn, cs_gate, cs_up, cs_down, st_all,
                  z_send, z_recv, f_send, f_recv, c_send, c_recv, r1_send, r1_recv, r2_send, r2_recv,
                  e_send, e_recv, l_sem, wi_sem, wo_sem):
    p = plan
    z, y, r = lax.axis_index('dp'), lax.axis_index('col'), lax.axis_index('row')
    low = z < 2
    mid = (z == 1) | (z == 2)
    end_z = jnp.where(low, 0, 3)
    mate_z = 3 - z
    w_refs = {ATTN: w_attn, GATE: w_gate, UP: w_up, DOWN: w_down}
    old = {ATTN: (r_attn, c_attn), GATE: (r_gate, c_gate), UP: (r_up, c_up), DOWN: (r_down, c_down)}
    new = {ATTN: (nr_attn, nc_attn), GATE: (nr_gate, nc_gate), UP: (nr_up, nc_up), DOWN: (nr_down, nc_down)}
    b_rows = {ATTN: b_attn, GATE: b_gate, UP: b_up, DOWN: b_down}
    rs = {ATTN: rs_attn, GATE: rs_gate, UP: rs_up, DOWN: rs_down}
    cs = {ATTN: cs_attn, GATE: cs_gate, UP: cs_up, DOWN: cs_down}

    def flip_row(v):
        bit0, bit1 = lax.rem(r, 2), lax.div(r, 2)
        if v & 1:
            bit0 = 1 - bit0
        if v & 2:
            bit1 = 1 - bit1
        return bit1 * 2 + bit0

    peers = [(f, v) for f in range(2) for v in range(4) if f or v]
    barrier = pltpu.get_barrier_semaphore()
    for f, v in peers:
        pl.semaphore_signal(barrier, inc=1, device_id=(z, 1 - y if f else y, flip_row(v)), device_id_type=MESH)

    @pl.when(mid)
    def _():
        pl.semaphore_signal(barrier, inc=1, device_id=(end_z, y, r), device_id_type=MESH)
        pl.semaphore_signal(barrier, inc=1, device_id=(mate_z, y, r), device_id_type=MESH)
        pl.semaphore_wait(barrier, len(peers) + 2)

    @pl.when(jnp.logical_not(mid))
    def _():
        pl.semaphore_signal(barrier, inc=1, device_id=(jnp.where(low, 1, 2), y, r), device_id_type=MESH)
        pl.semaphore_wait(barrier, len(peers) + 1)

    my_q = pl.ds(pl.multiple_of(r * p.tq, p.tq), p.tq)
    x_q = pl.ds(pl.multiple_of(flip_row(2) * p.tq, p.tq), p.tq)
    my_h = pl.ds(pl.multiple_of(y * p.th, p.th), p.th)

    def slot(k, s, dy):
        return buf_d.at[p.at(k), s, my_q, :] if dy else buf_x.at[p.at(k), s, my_h, :]

    def pass_on(k, dy, src, to_z, to_slot, sem):
        return pltpu.make_async_remote_copy(
            src_ref=src, dst_ref=slot(k, to_slot, dy), send_sem=z_send.at[k, sem], recv_sem=z_recv.at[k, to_slot],
            device_id=(to_z, y, r), device_id_type=MESH)

    def spread(k, s, dy):
        to = (z, y, flip_row(2)) if dy else (z, 1 - y, r)
        return pltpu.make_async_remote_copy(
            src_ref=slot(k, s, dy), dst_ref=slot(k, s, dy), send_sem=f_send.at[k, s], recv_sem=f_recv.at[k, s],
            device_id=to, device_id_type=MESH)

    def partner(k, which):
        part = buf_d.at[p.at(k), :, x_q if which else my_q, :]
        return pltpu.make_async_remote_copy(
            src_ref=part, dst_ref=part, send_sem=c_send.at[p.at(k), which], recv_sem=c_recv.at[p.at(k), which],
            device_id=(z, y, flip_row(1)), device_id_type=MESH)

    def typed(k, go):
        used = mid | jnp.logical_not(p.is_attn(k))
        pl.when(p.is_dy(k) & used)(lambda: go(True))
        pl.when(jnp.logical_not(p.is_dy(k)) & used)(lambda: go(False))

    def cut(ref, at, size):
        return ref.at[:, pl.ds(pl.multiple_of(at * size, size), size)]

    def down_rows(ref, i):
        return ref.at[pl.ds(pl.multiple_of(i * p.mc, p.mc), p.mc), :]

    def own_to(k, dy, src):
        @pl.when(jnp.logical_not(mid))
        def _():
            pass_on(k, dy, src, jnp.where(low, 1, 2), jnp.where(low, 2, 0), 0).start()

        @pl.when(mid)
        def _():
            @pl.when(jnp.logical_not(p.is_attn(k)))
            def _():
                pass_on(k, dy, src, end_z, jnp.where(low, 0, 2), 0).start()
            pass_on(k, dy, src, mate_z, jnp.where(low, 2, 0), 1).start()

    def send_own(k):
        def go(ref, at, size, dy):
            own_to(k, dy, ref.at[my_q if dy else my_h, pl.ds(pl.multiple_of(at * size, size), size)])

        for name, ref, dy in (('x_mlp', x_mlp, False), ('gate', dy_gate, True), ('x_attn', x_attn, False),
                              ('attn', dy_attn, True), ('up', dy_up, True), ('out', dy_out, True), ('h', h_mlp, False)):
            at = look(k, [i + 1 if n == name else 0 for n, i in p.order])
            size = p.nc if dy else p.mc
            pl.when(at > 0)(functools.partial(go, ref, at - 1, size, dy))

    def own_first_left(k):
        @pl.when(jnp.logical_not(mid & p.is_attn(k)))
        def _():
            pl.when(p.is_dy(k))(lambda: pass_on(k, True, slot(k, 0, True), z, 0, 0).wait_send())
            pl.when(jnp.logical_not(p.is_dy(k)))(lambda: pass_on(k, False, slot(k, 0, False), z, 0, 0).wait_send())

    def arrive(k, e, whole):
        s = jnp.where(low, e, 2 - e)

        def go(dy):
            pass_on(k, dy, slot(k, s, dy), z, s, 0).wait_recv()

            @pl.when(mid & (e == 2))
            def _():
                pass_on(k, dy, slot(k, s, dy), mate_z, 1, 4).start()

            @pl.when(mid & (e < 2) & jnp.logical_not(p.is_attn(k)))
            def _():
                pass_on(k, dy, slot(k, s, dy), end_z, jnp.where(low, s + 1, s - 1), 2 + e).start()

            spread(k, s, dy).start()
            if dy and whole:
                pl.when(e == jnp.where(mid, 1, 2))(lambda: partner(k, 0).start())

        typed(k, go)

    def spread_done(k, dy):
        for s in range(p.dp - 1):
            spread(k, s, dy).wait_recv()

    def load(src, at, size, buf, index, dst):
        copies = [pltpu.make_async_copy(cut(src, at, size), dst.at[z], l_sem.at[0])]
        for d in range(1, p.dp):
            copies.append(pltpu.make_async_copy(buf.at[index, d - 1], dst.at[lax.rem(z + d, p.dp)], l_sem.at[d]))
        for c in copies:
            c.start()
        for c in copies:
            c.wait()

    step_t = min(256, p.tok)

    def turn():
        @pl.loop(0, p.dp)
        def _(q):
            @pl.loop(0, p.tok // step_t)
            def _(t):
                at = pl.multiple_of(t * step_t, step_t)
                lhs[q, :, pl.ds(at, step_t)] = tile_x[q, pl.ds(at, step_t), :].T

    step_n = min(512, p.nc)
    step_r = min(64, p.mc)

    def lane_sum(v):
        out = v[:, 0:LANES]
        for i in range(1, v.shape[1] // LANES):
            out = out + v[:, i * LANES:(i + 1) * LANES]
        return out

    def product(at):
        r_lanes[...] = jnp.zeros_like(r_lanes)

        @pl.loop(0, p.nc // step_n)
        def _(n):
            cols = pl.ds(pl.multiple_of(n * step_n, step_n), step_n)
            grad[at, :, cols] = jnp.dot(lhs[0], tile_d[0, :, cols], preferred_element_type=F32)

            @pl.loop(1, p.dp)
            def _(q):
                grad[at, :, cols] += jnp.dot(lhs[q], tile_d[q, :, cols], preferred_element_type=F32)

            def body(i, acc):
                rows = pl.ds(pl.multiple_of(i * step_r, step_r), step_r)
                block = grad[at, rows, cols]
                sq = block * block + EPS_ONE
                r_lanes[rows, :] += lane_sum(sq)
                return acc + jnp.sum(sq, axis=0, keepdims=True)

            c_sum[at, :, cols] = lax.fori_loop(0, p.mc // step_r, body, jnp.zeros((1, step_n), F32))

    def fold(v):
        v = jnp.reshape(v, (v.shape[0] // 8, 8, LANES))
        while v.shape[0] > 1:
            v = v[:v.shape[0] // 2] + v[v.shape[0] // 2:]
        return v[0]

    def to_row(block):
        return jnp.sum(block.T, axis=0, keepdims=True)

    def get_w(mat, i):
        src = down_rows(w_refs[mat], i) if mat == DOWN else cut(w_refs[mat], i, p.nc)
        return pltpu.make_async_copy(src, w_buf.at[lax.rem(i, 3)], wi_sem.at[lax.rem(i, 3)])

    def put_w(mat, i):
        dst = cut(o_gate if mat == GATE else o_up, i, p.nc)
        return pltpu.make_async_copy(w_buf.at[lax.rem(i, 3)], dst, wo_sem.at[lax.rem(i, 3)])

    def chunk(mat, i):
        get_w(mat, i).start()
        product(i)
        row = to_row(r_lanes[...])
        if mat == DOWN:
            r_row[i] = row
        else:
            r_row[0] = jnp.where(i == 0, row, r_row[0] + row)
        get_w(mat, i).wait()

        def body(n, acc):
            rows = pl.ds(pl.multiple_of(n * step_r, step_r), step_r)
            block = lane_sum(w_buf[lax.rem(i, 3), rows, :] * w_buf[lax.rem(i, 3), rows, :])
            return acc + fold(block)

        w_sq[mat] += lax.fori_loop(0, p.mc // step_r, body, jnp.zeros((8, LANES), F32))

    def first_copies(mat):
        copies = [pltpu.make_async_remote_copy(
            src_ref=rs[mat].at[y], dst_ref=rs[mat].at[y], send_sem=r1_send.at[mat, 0], recv_sem=r1_recv.at[mat, 0],
            device_id=(z, 1 - y, r), device_id_type=MESH)]
        for v in range(1, 4):
            copies.append(pltpu.make_async_remote_copy(
                src_ref=cs[mat].at[r], dst_ref=cs[mat].at[r], send_sem=r1_send.at[mat, v],
                recv_sem=r1_recv.at[mat, v], device_id=(z, y, flip_row(v)), device_id_type=MESH))
        return copies

    def second_copies(mat):
        me = y * 4 + r
        return [pltpu.make_async_remote_copy(
            src_ref=st_all.at[mat, me], dst_ref=st_all.at[mat, me], send_sem=r2_send.at[mat, f * 4 + v],
            recv_sem=r2_recv.at[mat, f * 4 + v], device_id=(z, 1 - y if f else y, flip_row(v)), device_id_type=MESH)
            for f, v in peers]

    def scale_rows(mat):
        return p.rows[mat] * p.row, p.cols[mat] * p.col

    blocks = p.mc // step_r

    def factors(mat, i, n):
        rows = pl.ds(pl.multiple_of(n * step_r, step_r), step_r)
        if mat == DOWN:
            return rows, a_cols[i, rows, :], b_rows[mat].at[:, :]
        return rows, a_cols[0, rows, :], b_rows[mat].at[:, pl.ds(pl.multiple_of(i * p.nc, p.nc), p.nc)]

    def finish_first(mat):
        parts = p.parts[mat]
        if mat != DOWN:
            for i in range(min(2, parts)):
                get_w(mat, jnp.int32(i)).start()
        if mat == DOWN:
            block = c_sum[0]
            for i in range(parts):
                rs[mat][y, :, i * p.mc:(i + 1) * p.mc] = r_row[i]
                if i:
                    block = block + c_sum[i]
            cs[mat][r] = block
        else:
            rs[mat][y] = r_row[0]
            for i in range(parts):
                cs[mat][r, :, i * p.nc:(i + 1) * p.nc] = c_sum[i]
        for c in first_copies(mat):
            c.start()

    def finish_second(mat):
        beta_two = hyper[0]
        m_total, n_total = scale_rows(mat)
        parts = p.parts[mat]
        for c in first_copies(mat):
            c.wait_recv()
        r_new = beta_two * old[mat][0][...] + (1.0 - beta_two) * ((rs[mat][0] + rs[mat][1]) / n_total)
        c_all = ((cs[mat][0] + cs[mat][1]) + cs[mat][2]) + cs[mat][3]
        c_new = beta_two * old[mat][1][...] + (1.0 - beta_two) * (c_all / m_total)
        new[mat][0][...] = r_new
        new[mat][1][...] = c_new
        t_own = jnp.sum(r_new, axis=1, keepdims=True)
        a_row = jnp.sqrt(t_own) / jnp.sqrt(r_new)
        b_rows[mat][...] = 1.0 / jnp.sqrt(c_new)
        if mat == DOWN:
            a_rows[...] = a_row
        for i in range(parts if mat == DOWN else 1):
            a_cols[i] = jnp.broadcast_to(a_row[:, i * p.mc:(i + 1) * p.mc], (LANES, p.mc)).T

        def add_up(j, acc):
            i, n = lax.div(j, blocks), lax.rem(j, blocks)
            rows, a_block, b_ref = factors(mat, i, n)
            for c in range(0, p.nc, LANES):
                upd = grad[i, rows, c:c + LANES] * a_block * b_ref[:, c:c + LANES]
                acc = acc + fold(upd * upd)
            return acc

        u_part = lax.fori_loop(0, parts * blocks, add_up, jnp.zeros((8, LANES), F32))

        def spot(v):
            return jnp.broadcast_to(jnp.sum(jnp.sum(v, axis=1, keepdims=True), axis=0, keepdims=True), (8, LANES))

        me = y * 4 + r
        st_all[mat, me, 0] = spot(u_part)
        st_all[mat, me, 1] = spot(w_sq[mat])
        st_all[mat, me, 2] = jnp.broadcast_to(t_own, (8, LANES))
        for c in second_copies(mat):
            c.start()

    def finish_third(mat):
        rho_step, clip_thr = hyper[1], hyper[2]
        m_total, n_total = scale_rows(mat)
        me = y * 4 + r
        for c in second_copies(mat):
            c.wait_recv()
        t_all = st_all[mat, 0, 2]
        for i in range(1, p.row):
            t_all = t_all + st_all[mat, i, 2]
        u_all = st_all[mat, 0, 0] * (t_all / st_all[mat, 0, 2])
        w_all = st_all[mat, 0, 1]
        for i in range(1, p.row * p.col):
            u_all = u_all + st_all[mat, i, 0] * (t_all / st_all[mat, i, 2])
            w_all = w_all + st_all[mat, i, 1]
        upd_rms = jnp.sqrt(u_all / (m_total * n_total))
        w_rms = jnp.sqrt(w_all / (m_total * n_total))
        scale = rho_step * jnp.maximum(EPS_TWO, w_rms) / jnp.maximum(1.0, upd_rms / clip_thr)
        scale = scale * jnp.sqrt(t_all / st_all[mat, me, 2])
        b_rows[mat][...] = b_rows[mat][...] * scale[0:1, 0:1]

    def renew(mat, low_i, high_i):
        parts = p.parts[mat]

        @pl.loop(low_i, high_i)
        def _(i):
            at = lax.rem(i, 3)
            get_w(mat, i).wait()

            @pl.loop(0, blocks)
            def _(n):
                rows, a_block, b_ref = factors(mat, i, n)
                for c in range(0, p.nc, LANES):
                    cols = slice(c, c + LANES)
                    fresh = w_buf[at, rows, cols] - grad[i, rows, cols] * a_block * b_ref[:, cols]
                    if mat == ATTN:
                        o_attn[rows, cols] = fresh
                    elif mat == UP and UP_KEPT:
                        o_up[i, rows, cols] = fresh
                    else:
                        w_buf[at, rows, cols] = fresh

            if mat == GATE or (mat == UP and not UP_KEPT):
                put_w(mat, i).start()
                pl.when(i >= 1)(lambda: put_w(mat, i - 1).wait())
            pl.when(i + 2 < parts)(lambda: get_w(mat, i + 2).start())

        if (mat == GATE or (mat == UP and not UP_KEPT)) and high_i == parts:
            put_w(mat, jnp.int32(parts - 1)).wait()

    def finish(mat, stage):
        parts = p.parts[mat]
        half = parts // 2 if parts > 1 else parts
        if stage == 1:
            finish_second(mat)
        elif stage == 2:
            finish_third(mat)
            if mat == DOWN:
                al_down[...] = a_rows[...]
                be_down[...] = b_rows[mat][...]
            else:
                renew(mat, 0, half)
        else:
            renew(mat, half, parts)

    def take_x(src, at, k):
        spread_done(k, False)
        load(src, at, p.mc, buf_x, p.at(k), tile_x)
        turn()

    def again_x():
        load(x_mlp, 0, p.mc, buf_x, 0, tile_x)
        turn()

    def got(name, i):
        k = look(i, [p.place[name, j] for j in range(sum(1 for n, _ in p.order if n == name))])
        partner(k, 0).wait_recv()
        partner(k, 1).wait_recv()
        return k

    def use_gate(i):
        pl.when(i == 0)(lambda: take_x(x_mlp, 0, jnp.int32(p.place['x_mlp', 0])))
        k = got('gate', i)
        load(dy_gate, i, p.nc, buf_d, p.at(k), tile_d)
        chunk(GATE, i)
        pl.when(i == p.parts[GATE] - 1)(lambda: finish_first(GATE))

    def use_attn(i):
        take_x(x_attn, 0, jnp.int32(p.place['x_attn', 0]))
        k = got('attn', i)
        load(dy_attn, 0, p.nc, buf_d, p.at(k), tile_d)
        chunk(ATTN, i)
        finish_first(ATTN)

    def use_up(i):
        pl.when(i == 0)(again_x)
        k = got('up', i)
        load(dy_up, i, p.nc, buf_d, p.at(k), tile_d)
        chunk(UP, i)
        pl.when(i == p.parts[UP] - 1)(lambda: finish_first(UP))

    def use_out():
        k = got('out', jnp.int32(0))
        load(dy_out, 0, p.nc, buf_d, p.at(k), tile_d)

    def use_h(i):
        pl.when(i == 0)(use_out)
        take_x(h_mlp, i, look(i, [p.place['h', j] for j in range(p.nh)]))
        chunk(DOWN, i)
        pl.when(i == p.parts[DOWN] - 1)(lambda: finish_first(DOWN))

    def work(t):
        for name, use in (('gate', use_gate), ('attn', use_attn), ('up', use_up), ('h', use_h)):
            at = jnp.int32(0)
            for i in range(sum(1 for n, _ in p.order if n == name)):
                when_mid = p.steps[True].get((name, i), -1)
                when_end = p.steps[False].get((name, i), -1)
                at = jnp.where(t == jnp.where(mid, when_mid, when_end), i + 1, at)
            pl.when(at > 0)(functools.partial(use, at - 1))
        for mat in MATS:
            for stage in (1, 2, 3):
                when_mid = p.steps[True].get(('finish', mat, stage), -1)
                when_end = p.steps[False].get(('finish', mat, stage), -1)
                if when_mid >= 0:
                    pl.when(t == jnp.where(mid, when_mid, when_end))(functools.partial(finish, mat, stage))

    def to_end():
        pairs = ((o_attn, o_attn), (nr_attn, nr_attn), (nc_attn, nc_attn))
        return [pltpu.make_async_remote_copy(
            src_ref=a, dst_ref=b, send_sem=e_send.at[i], recv_sem=e_recv.at[i],
            device_id=(end_z, y, r), device_id_type=MESH) for i, (a, b) in enumerate(pairs)]

    w_sq[...] = jnp.zeros_like(w_sq)
    ahead = jnp.where(mid, AHEAD_MID, AHEAD_END)

    @pl.loop(0, AHEAD_END)
    def _(k):
        pl.when(k < ahead)(lambda: send_own(k))

    @pl.when(mid)
    def _():
        arrive(jnp.int32(0), jnp.int32(2), False)

    @pl.when(jnp.logical_not(mid))
    def _():
        for k in range(AHEAD_MID):
            arrive(jnp.int32(k), jnp.int32(0), False)

    @pl.loop(0, p.turns)
    def _(t):
        d, turn_no = lax.div(t, 3), lax.rem(t, 3)
        pl.when((turn_no == 0) & (d >= 1) & (d <= p.count))(lambda: own_first_left(d - 1))
        early = jnp.where(mid, jnp.where(turn_no == 0, 1, 0), jnp.where(turn_no == 2, AHEAD_MID, 0))
        e = lax.rem(turn_no + jnp.where(mid, 2, 1), 3)
        k = d + early
        pl.when(k < p.count)(lambda: arrive(k, e, True))

        @pl.when(turn_no == 2)
        def _():
            pl.when(d + ahead < p.count)(lambda: send_own(d + ahead))

            @pl.when((d == p.count - 1) & mid)
            def _():
                for c in to_end():
                    c.start()

            k = d - jnp.where(mid, LATE_MID, LATE_END)

            @pl.when((k >= 0) & (k < p.count) & p.is_dy(k) & (mid | jnp.logical_not(p.is_attn(k))))
            def _():
                spread_done(k, True)
                partner(k, 1).start()

        work(t)

    @pl.loop(0, p.count)
    def _(k):
        def go(dy):
            some = slot(k, 0, dy)

            @pl.when(mid)
            def _():
                pass_on(k, dy, some, z, 0, 1).wait_send()
                pass_on(k, dy, some, z, 0, 4).wait_send()

                @pl.when(jnp.logical_not(p.is_attn(k)))
                def _():
                    pass_on(k, dy, some, z, 0, 2).wait_send()
                    pass_on(k, dy, some, z, 0, 3).wait_send()

            for s in range(p.dp - 1):
                spread(k, s, dy).wait_send()
            if dy:
                partner(k, 0).wait_send()
                partner(k, 1).wait_send()

        typed(k, go)

    for mat in (GATE, UP, DOWN):
        for c in first_copies(mat) + second_copies(mat):
            c.wait_send()

    @pl.when(mid)
    def _():
        for c in first_copies(ATTN) + second_copies(ATTN):
            c.wait_send()
        for c in to_end():
            c.wait_send()

    @pl.when(jnp.logical_not(mid))
    def _():
        for c in to_end():
            c.wait_recv()


def store_kernel(plan, o_attn, o_gate, o_up, grad, *refs):
    p = plan
    stats, al_down, be_down, w_old, (w_attn, w_gate, w_up, w_down), outs = (
        refs[:8], refs[8], refs[9], refs[10], refs[11:15], refs[15:23])
    bounce, w_buf, a_col, in_sem, out_sem, s_sem, wi_sem, wo_sem = refs[23:]
    depth, wide = bounce.shape[0], w_buf.shape[0]

    def cut(ref, i):
        return ref.at[:, i * p.nc:(i + 1) * p.nc]

    def rows(ref, i):
        return ref.at[i * p.mc:(i + 1) * p.mc, :]

    through = [(cut(o_gate, i), cut(w_gate, i)) for i in range(p.ng)]
    if not UP_KEPT:
        through += [(cut(o_up, i), cut(w_up, i)) for i in range(p.ng)]
    loads = [pltpu.make_async_copy(a, bounce.at[i % depth], in_sem.at[i]) for i, (a, _) in enumerate(through)]
    puts = [pltpu.make_async_copy(bounce.at[i % depth], b, out_sem.at[i]) for i, (_, b) in enumerate(through)]
    w_in = [pltpu.make_async_copy(rows(w_old, i), w_buf.at[i % wide], wi_sem.at[i]) for i in range(p.nh)]
    w_out = [pltpu.make_async_copy(w_buf.at[i % wide], rows(w_down, i), wo_sem.at[i]) for i in range(p.nh)]
    for i in range(wide // 2):
        w_in[i].start()
    for c in loads[:depth]:
        c.start()
    copies = [pltpu.make_async_copy(a, b, s_sem.at[i]) for i, (a, b) in enumerate(zip(stats, outs))]
    copies.append(pltpu.make_async_copy(o_attn, w_attn, s_sem.at[8]))
    if UP_KEPT:
        copies += [pltpu.make_async_copy(o_up.at[i], cut(w_up, i), s_sem.at[9 + i]) for i in range(p.ng)]
    for c in copies:
        c.start()
    step_r = min(64, p.mc)
    per = -(-len(through) // p.nh)
    done = 0
    for i in range(p.nh):
        a_col[...] = jnp.broadcast_to(al_down[:, i * p.mc:(i + 1) * p.mc], (LANES, p.mc)).T
        w_in[i].wait()

        @pl.loop(0, p.mc // step_r)
        def _(n):
            at = pl.ds(pl.multiple_of(n * step_r, step_r), step_r)
            a_block = a_col[at, :]
            for c in range(0, p.nc, LANES):
                cols = slice(c, c + LANES)
                w_buf[i % wide, at, cols] = w_buf[i % wide, at, cols] - grad[i, at, cols] * a_block * be_down[:, cols]

        w_out[i].start()
        again = i + wide // 2
        if again < p.nh:
            if again >= wide:
                w_out[again - wide].wait()
            w_in[again].start()
        for j in range(done, min(len(through), done + per)):
            loads[j].wait()
            puts[j].start()
            again = j + depth // 2
            if depth <= again < len(through):
                puts[again - depth].wait()
                loads[again].start()
        done += per
    for i in range(max(0, p.nh - wide), p.nh):
        if i + wide >= p.nh:
            w_out[i].wait()
    for i in range(max(0, len(through) - depth), len(through)):
        puts[i].wait()
    for c in copies:
        c.wait()


def solution(mesh):
    act_spec = P('dp', 'row')
    grad_spec = P('dp', 'col')
    w_spec = P('row', 'col')
    row_spec = P('row')
    col_spec = P('col')
    in_specs = (act_spec, grad_spec, act_spec, grad_spec, grad_spec, act_spec, grad_spec,
                w_spec, w_spec, w_spec, w_spec,
                row_spec, col_spec, row_spec, col_spec, row_spec, col_spec, row_spec, col_spec, P())
    out_specs = (w_spec, row_spec, col_spec) * 4

    def per_device(x_attn, dy_attn, x_mlp, dy_gate, dy_up, h_mlp, dy_out, w_attn, w_gate, w_up, w_down,
                   r_attn, c_attn, r_gate, c_gate, r_up, c_up, r_down, c_down, hyper_params):
        p = Plan(x_mlp, dy_gate, h_mlp, dy_out, mesh)
        stats = [v.reshape(1, -1) for v in (r_attn, c_attn, r_gate, c_gate, r_up, c_up, r_down, c_down)]
        any_spec = pl.BlockSpec(memory_space=pl.ANY)
        vmem_spec = pl.BlockSpec(memory_space=pltpu.VMEM)
        up_spec = vmem_spec if UP_KEPT else any_spec
        row_shapes = []
        for mat in MATS:
            row_shapes += [jax.ShapeDtypeStruct((1, p.rows[mat]), F32), jax.ShapeDtypeStruct((1, p.cols[mat]), F32)]
        w_shapes = [jax.ShapeDtypeStruct((p.rows[mat], p.cols[mat]), F32) for mat in MATS]
        o_shapes = [pltpu.VMEM((p.mc, p.nc), F32), w_shapes[GATE],
                    pltpu.VMEM((p.ng, p.mc, p.nc), F32) if UP_KEPT else w_shapes[UP],
                    pltpu.VMEM((p.pieces, p.mc, p.nc), F32)]
        bufs = [jax.ShapeDtypeStruct((p.n_dy, p.dp - 1, p.tok, p.nc), BF16),
                jax.ShapeDtypeStruct((p.n_x, p.dp - 1, p.tok, p.mc), BF16)]
        dma = pltpu.SemaphoreType.DMA
        scratch = [
            pltpu.VMEM((p.dp, p.mc, p.tok), BF16),
            pltpu.VMEM((p.dp, p.tok, p.mc), BF16),
            pltpu.VMEM((p.dp, p.tok, p.nc), BF16),
            pltpu.VMEM((3, p.mc, p.nc), F32),
            pltpu.VMEM((p.mc, LANES), F32),
            pltpu.VMEM((p.pieces, 1, p.mc), F32),
            pltpu.VMEM((p.pieces, 1, p.nc), F32),
            pltpu.VMEM((p.nh, p.mc, LANES), F32),
            pltpu.VMEM((1, p.rows[DOWN]), F32),
            pltpu.VMEM((4, 8, LANES), F32),
        ]
        scratch += [pltpu.VMEM((1, p.cols[mat]), F32) for mat in MATS]
        scratch += [pltpu.VMEM((2, 1, p.rows[mat]), F32) for mat in MATS]
        scratch += [pltpu.VMEM((4, 1, p.cols[mat]), F32) for mat in MATS]
        scratch += [
            pltpu.VMEM((4, 8, 3, 8, LANES), F32),
            dma((p.count, 5)), dma((p.count, p.dp - 1)),
            dma((p.count, p.dp - 1)), dma((p.count, p.dp - 1)),
            dma((p.n_dy, 2)), dma((p.n_dy, 2)),
            dma((4, 4)), dma((4, 4)), dma((4, 8)), dma((4, 8)),
            dma((3,)), dma((3,)),
            dma((p.dp,)), dma((3,)), dma((3,)),
        ]
        out = pl.pallas_call(
            functools.partial(gather_kernel, p),
            out_shape=o_shapes + [pltpu.VMEM(v.shape, F32) for v in row_shapes + row_shapes[-2:]] + bufs,
            in_specs=[any_spec] * 11 + [vmem_spec] * 8 + [pl.BlockSpec(memory_space=pltpu.SMEM)],
            out_specs=[vmem_spec, any_spec, up_spec, vmem_spec] + [vmem_spec] * 10 + [any_spec] * 2,
            scratch_shapes=scratch,
            compiler_params=pltpu.CompilerParams(collective_id=0, has_side_effects=True, vmem_limit_bytes=VMEM_LIMIT),
        )(x_attn, dy_attn, x_mlp, dy_gate, dy_up, h_mlp, dy_out, w_attn, w_gate, w_up, w_down, *stats, hyper_params)
        res = pl.pallas_call(
            functools.partial(store_kernel, p),
            out_shape=w_shapes + row_shapes,
            in_specs=[vmem_spec, any_spec, up_spec, vmem_spec] + [vmem_spec] * 10 + [any_spec],
            out_specs=[any_spec] * 12,
            scratch_shapes=[pltpu.VMEM((DEPTH, p.mc, p.nc), F32), pltpu.VMEM((WIDE, p.mc, p.nc), F32),
                            pltpu.VMEM((p.mc, LANES), F32), dma((2 * p.ng,)), dma((2 * p.ng,)), dma((9 + p.ng,)),
                            dma((p.nh,)), dma((p.nh,))],
            compiler_params=pltpu.CompilerParams(vmem_limit_bytes=STORE_LIMIT),
        )(*[pltpu.with_memory_space_constraint(v, pltpu.VMEM) if i not in HBM_KEPT else v for i, v in enumerate(out[:14])],
          w_down)
        result = []
        for mat in MATS:
            result += [res[mat], res[4 + 2 * mat].reshape(-1), res[5 + 2 * mat].reshape(-1)]
        return tuple(result)

    return jax.shard_map(per_device, mesh=mesh, in_specs=in_specs, out_specs=out_specs, check_vma=False)
```

```python
import functools
import jax
import jax.numpy as jnp
from jax import lax
from jax.experimental import pallas as pl
from jax.experimental.pallas import tpu as pltpu
from jax.sharding import PartitionSpec as P

EPS_ONE = 1e-30
EPS_TWO = 1e-3
MESH = pl.DeviceIdType.MESH
LANES = 128
F32 = jnp.float32
BF16 = jnp.bfloat16
ATTN, GATE, UP, DOWN = range(4)
MATS = (ATTN, GATE, UP, DOWN)
FIRST = {'gate': ('x_mlp', 0), 'attn': ('x_attn', 0), 'up': ('x_mlp', 0), 'h': ('out', 0)}
AHEAD_MID, AHEAD_END = 2, 6
LATE_MID, LATE_END = 3, 2
VMEM_LIMIT = 29 * 1024 * 1024
STORE_LIMIT = 29 * 1024 * 1024
UP_KEPT = True
HBM_KEPT = (1,) if UP_KEPT else (1, 2)
DEPTH, WIDE = 4, 4


def look(k, table):
    out = jnp.int32(0)
    for i, v in enumerate(table):
        if v:
            out = jnp.where(k == i, v, out)
    return out


class Plan:
    def __init__(self, x_mlp, dy_gate, h_mlp, dy_out, mesh):
        self.dp, self.col, self.row = mesh.shape['dp'], mesh.shape['col'], mesh.shape['row']
        assert (self.dp, self.col, self.row) == (4, 2, 4)
        self.tok = x_mlp.shape[0]
        self.mc = x_mlp.shape[1]
        self.nc = dy_out.shape[1]
        self.ng = dy_gate.shape[1] // self.nc
        self.nh = h_mlp.shape[1] // self.mc
        self.tq = self.tok // self.row
        self.th = self.tok // self.col
        g = [('gate', i) for i in range(self.ng)]
        u = [('up', i) for i in range(self.ng)]
        h = [('h', i) for i in range(self.nh)]
        one, two = max(1, self.ng // 4), max(2, 3 * self.ng // 4)
        self.order = ([('x_mlp', 0)] + g[:one] + h[:1] + g[one:two] + h[1:2] + g[two:] + [('x_attn', 0), ('attn', 0)]
                      + u + [('out', 0)] + h[2:])
        self.count = len(self.order)
        self.place = {v: k for k, v in enumerate(self.order)}
        self.first_rows = self.mc // 2
        self.n_dy = 2 * self.ng + 2
        self.n_x = self.nh + 2
        self.pieces = max(self.ng, self.nh)
        self.rows = {ATTN: self.mc, GATE: self.mc, UP: self.mc, DOWN: self.mc * self.nh}
        self.cols = {ATTN: self.nc, GATE: self.nc * self.ng, UP: self.nc * self.ng, DOWN: self.nc}
        self.parts = {ATTN: 1, GATE: self.ng, UP: self.ng, DOWN: self.nh}
        base = {'gate': 0, 'up': self.ng, 'out': 2 * self.ng, 'attn': 2 * self.ng + 1, 'x_mlp': 0, 'x_attn': 1, 'h': 2}
        self.dy_table = [1 if n in ('gate', 'up', 'out', 'attn') else 0 for n, _ in self.order]
        self.at_table = [base[n] + i for n, i in self.order]
        self.attn_table = [1 if n in ('x_attn', 'attn') else 0 for n, _ in self.order]
        self.steps = {m: self.schedule(m) for m in (True, False)}
        last = max(max(v.values()) for v in self.steps.values())
        self.turns = max(last + 1, 3 * (self.count + LATE_MID + 1))

    def schedule(self, mid):
        late = LATE_MID if mid else LATE_END
        tasks = []
        for name, mat in (('gate', GATE), ('attn', ATTN), ('up', UP), ('h', DOWN)):
            if name == 'attn' and not mid:
                continue
            for i in range(self.parts[mat]):
                k = self.place[name, i]
                need = [3 * (k + late + 1)] if name != 'h' else [3 * (k + late) if mid else 3 * k + 5]
                if i == 0:
                    need.append(3 * (self.place[FIRST[name]] + late + (name == 'h')))
                tasks.append(((name, i), max(need)))
            stages = {ATTN: (1, 2), DOWN: (1, 2)}.get(mat, (1, 2, 3))
            if mid or mat != DOWN:
                tasks += [(('finish', mat, stage), 0) for stage in stages]
        out, t = {}, 0
        for task, first in tasks:
            t = max(t, first)
            out[task] = t
            t += 1
        return out

    def is_dy(self, k):
        return look(k, self.dy_table) == 1

    def is_attn(self, k):
        return look(k, self.attn_table) == 1

    def at(self, k):
        return look(k, self.at_table)


def gather_kernel(plan, x_attn, dy_attn, x_mlp, dy_gate, dy_up, h_mlp, dy_out, w_attn, w_gate, w_up, w_down,
                  r_attn, c_attn, r_gate, c_gate, r_up, c_up, r_down, c_down, hyper,
                  o_attn, o_gate, o_up, grad, nr_attn, nc_attn, nr_gate, nc_gate, nr_up, nc_up, nr_down, nc_down,
                  al_down, be_down, o_rest, buf_d, buf_x,
                  lhs, tile_x, tile_d, w_buf, r_lanes, r_row, c_sum, a_cols, a_rows, w_sq,
                  b_attn, b_gate, b_up, b_down,
                  rs_attn, rs_gate, rs_up, rs_down, cs_attn, cs_gate, cs_up, cs_down, st_all,
                  z_send, z_recv, f_send, f_recv, c_send, c_recv, r1_send, r1_recv, r2_send, r2_recv,
                  e_send, e_recv, l_sem, wi_sem, wo_sem):
    p = plan
    z, y, r = lax.axis_index('dp'), lax.axis_index('col'), lax.axis_index('row')
    low = z < 2
    mid = (z == 1) | (z == 2)
    end_z = jnp.where(low, 0, 3)
    mate_z = 3 - z
    w_refs = {ATTN: w_attn, GATE: w_gate, UP: w_up, DOWN: w_down}
    old = {ATTN: (r_attn, c_attn), GATE: (r_gate, c_gate), UP: (r_up, c_up), DOWN: (r_down, c_down)}
    new = {ATTN: (nr_attn, nc_attn), GATE: (nr_gate, nc_gate), UP: (nr_up, nc_up), DOWN: (nr_down, nc_down)}
    b_rows = {ATTN: b_attn, GATE: b_gate, UP: b_up, DOWN: b_down}
    rs = {ATTN: rs_attn, GATE: rs_gate, UP: rs_up, DOWN: rs_down}
    cs = {ATTN: cs_attn, GATE: cs_gate, UP: cs_up, DOWN: cs_down}

    def flip_row(v):
        bit0, bit1 = lax.rem(r, 2), lax.div(r, 2)
        if v & 1:
            bit0 = 1 - bit0
        if v & 2:
            bit1 = 1 - bit1
        return bit1 * 2 + bit0

    peers = [(f, v) for f in range(2) for v in range(4) if f or v]
    barrier = pltpu.get_barrier_semaphore()
    for f, v in peers:
        pl.semaphore_signal(barrier, inc=1, device_id=(z, 1 - y if f else y, flip_row(v)), device_id_type=MESH)

    @pl.when(mid)
    def _():
        pl.semaphore_signal(barrier, inc=1, device_id=(end_z, y, r), device_id_type=MESH)
        pl.semaphore_signal(barrier, inc=1, device_id=(mate_z, y, r), device_id_type=MESH)
        pl.semaphore_wait(barrier, len(peers) + 2)

    @pl.when(jnp.logical_not(mid))
    def _():
        pl.semaphore_signal(barrier, inc=1, device_id=(jnp.where(low, 1, 2), y, r), device_id_type=MESH)
        pl.semaphore_wait(barrier, len(peers) + 1)

    my_q = pl.ds(pl.multiple_of(r * p.tq, p.tq), p.tq)
    x_q = pl.ds(pl.multiple_of(flip_row(2) * p.tq, p.tq), p.tq)
    my_h = pl.ds(pl.multiple_of(y * p.th, p.th), p.th)

    def slot(k, s, dy):
        return buf_d.at[p.at(k), s, my_q, :] if dy else buf_x.at[p.at(k), s, my_h, :]

    def pass_on(k, dy, src, to_z, to_slot, sem):
        return pltpu.make_async_remote_copy(
            src_ref=src, dst_ref=slot(k, to_slot, dy), send_sem=z_send.at[k, sem], recv_sem=z_recv.at[k, to_slot],
            device_id=(to_z, y, r), device_id_type=MESH)

    def spread(k, s, dy):
        to = (z, y, flip_row(2)) if dy else (z, 1 - y, r)
        return pltpu.make_async_remote_copy(
            src_ref=slot(k, s, dy), dst_ref=slot(k, s, dy), send_sem=f_send.at[k, s], recv_sem=f_recv.at[k, s],
            device_id=to, device_id_type=MESH)

    def partner(k, which):
        part = buf_d.at[p.at(k), :, x_q if which else my_q, :]
        return pltpu.make_async_remote_copy(
            src_ref=part, dst_ref=part, send_sem=c_send.at[p.at(k), which], recv_sem=c_recv.at[p.at(k), which],
            device_id=(z, y, flip_row(1)), device_id_type=MESH)

    def typed(k, go):
        used = mid | jnp.logical_not(p.is_attn(k))
        pl.when(p.is_dy(k) & used)(lambda: go(True))
        pl.when(jnp.logical_not(p.is_dy(k)) & used)(lambda: go(False))

    def cut(ref, at, size):
        return ref.at[:, pl.ds(pl.multiple_of(at * size, size), size)]

    def down_rows(ref, i):
        return ref.at[pl.ds(pl.multiple_of(i * p.mc, p.mc), p.mc), :]

    def own_to(k, dy, src):
        @pl.when(jnp.logical_not(mid))
        def _():
            pass_on(k, dy, src, jnp.where(low, 1, 2), jnp.where(low, 2, 0), 0).start()

        @pl.when(mid)
        def _():
            @pl.when(jnp.logical_not(p.is_attn(k)))
            def _():
                pass_on(k, dy, src, end_z, jnp.where(low, 0, 2), 0).start()
            pass_on(k, dy, src, mate_z, jnp.where(low, 2, 0), 1).start()

    def send_own(k):
        def go(ref, at, size, dy):
            own_to(k, dy, ref.at[my_q if dy else my_h, pl.ds(pl.multiple_of(at * size, size), size)])

        for name, ref, dy in (('x_mlp', x_mlp, False), ('gate', dy_gate, True), ('x_attn', x_attn, False),
                              ('attn', dy_attn, True), ('up', dy_up, True), ('out', dy_out, True), ('h', h_mlp, False)):
            at = look(k, [i + 1 if n == name else 0 for n, i in p.order])
            size = p.nc if dy else p.mc
            pl.when(at > 0)(functools.partial(go, ref, at - 1, size, dy))

    def own_first_left(k):
        @pl.when(jnp.logical_not(mid & p.is_attn(k)))
        def _():
            pl.when(p.is_dy(k))(lambda: pass_on(k, True, slot(k, 0, True), z, 0, 0).wait_send())
            pl.when(jnp.logical_not(p.is_dy(k)))(lambda: pass_on(k, False, slot(k, 0, False), z, 0, 0).wait_send())

    def arrive(k, e, whole):
        s = jnp.where(low, e, 2 - e)

        def go(dy):
            pass_on(k, dy, slot(k, s, dy), z, s, 0).wait_recv()

            @pl.when(mid & (e == 2))
            def _():
                pass_on(k, dy, slot(k, s, dy), mate_z, 1, 4).start()

            @pl.when(mid & (e < 2) & jnp.logical_not(p.is_attn(k)))
            def _():
                pass_on(k, dy, slot(k, s, dy), end_z, jnp.where(low, s + 1, s - 1), 2 + e).start()

            spread(k, s, dy).start()
            if dy and whole:
                pl.when(e == jnp.where(mid, 1, 2))(lambda: partner(k, 0).start())

        typed(k, go)

    def spread_done(k, dy):
        for s in range(p.dp - 1):
            spread(k, s, dy).wait_recv()

    def load(src, at, size, buf, index, dst):
        copies = [pltpu.make_async_copy(cut(src, at, size), dst.at[z], l_sem.at[0])]
        for d in range(1, p.dp):
            copies.append(pltpu.make_async_copy(buf.at[index, d - 1], dst.at[lax.rem(z + d, p.dp)], l_sem.at[d]))
        for c in copies:
            c.start()
        for c in copies:
            c.wait()

    step_t = min(256, p.tok)

    def turn():
        @pl.loop(0, p.dp)
        def _(q):
            @pl.loop(0, p.tok // step_t)
            def _(t):
                at = pl.multiple_of(t * step_t, step_t)
                lhs[q, :, pl.ds(at, step_t)] = tile_x[q, pl.ds(at, step_t), :].T

    step_n = min(512, p.nc)
    step_r = min(64, p.mc)

    def lane_sum(v):
        out = v[:, 0:LANES]
        for i in range(1, v.shape[1] // LANES):
            out = out + v[:, i * LANES:(i + 1) * LANES]
        return out

    def product(at, count):
        r_lanes[...] = jnp.zeros_like(r_lanes)

        @pl.loop(0, p.nc // step_n)
        def _(n):
            cols = pl.ds(pl.multiple_of(n * step_n, step_n), step_n)
            grad[at, :, cols] = jnp.dot(lhs[0], tile_d[0, :, cols], preferred_element_type=F32)

            @pl.loop(1, p.dp)
            def _(q):
                grad[at, :, cols] += jnp.dot(lhs[q], tile_d[q, :, cols], preferred_element_type=F32)

            def body(i, acc):
                rows = pl.ds(pl.multiple_of(i * step_r, step_r), step_r)
                block = grad[at, rows, cols]
                sq = block * block + EPS_ONE
                r_lanes[rows, :] += lane_sum(sq)
                return acc + jnp.sum(sq, axis=0, keepdims=True)

            @pl.when(count)
            def _():
                c_sum[at, :, cols] = lax.fori_loop(0, p.mc // step_r, body, jnp.zeros((1, step_n), F32))

    def fold(v):
        v = jnp.reshape(v, (v.shape[0] // 8, 8, LANES))
        while v.shape[0] > 1:
            v = v[:v.shape[0] // 2] + v[v.shape[0] // 2:]
        return v[0]

    def to_row(block):
        return jnp.sum(block.T, axis=0, keepdims=True)

    def get_w(mat, i):
        src = down_rows(w_refs[mat], i) if mat == DOWN else cut(w_refs[mat], i, p.nc)
        return pltpu.make_async_copy(src, w_buf.at[lax.rem(i, 3)], wi_sem.at[lax.rem(i, 3)])

    def put_w(mat, i):
        dst = cut(o_gate if mat == GATE else o_up, i, p.nc)
        return pltpu.make_async_copy(w_buf.at[lax.rem(i, 3)], dst, wo_sem.at[lax.rem(i, 3)])

    def chunk(mat, i):
        count = mid if mat == DOWN else jnp.bool_(True)
        pl.when(count)(lambda: get_w(mat, i).start())
        product(i, count)

        @pl.when(count)
        def _():
            row = to_row(r_lanes[...])
            if mat == DOWN:
                r_row[i] = row
            else:
                r_row[0] = jnp.where(i == 0, row, r_row[0] + row)
            get_w(mat, i).wait()

            def body(n, acc):
                rows = pl.ds(pl.multiple_of(n * step_r, step_r), step_r)
                block = lane_sum(w_buf[lax.rem(i, 3), rows, :] * w_buf[lax.rem(i, 3), rows, :])
                return acc + fold(block)

            w_sq[mat] += lax.fori_loop(0, p.mc // step_r, body, jnp.zeros((8, LANES), F32))

    def first_copies(mat):
        copies = [pltpu.make_async_remote_copy(
            src_ref=rs[mat].at[y], dst_ref=rs[mat].at[y], send_sem=r1_send.at[mat, 0], recv_sem=r1_recv.at[mat, 0],
            device_id=(z, 1 - y, r), device_id_type=MESH)]
        for v in range(1, 4):
            copies.append(pltpu.make_async_remote_copy(
                src_ref=cs[mat].at[r], dst_ref=cs[mat].at[r], send_sem=r1_send.at[mat, v],
                recv_sem=r1_recv.at[mat, v], device_id=(z, y, flip_row(v)), device_id_type=MESH))
        return copies

    def second_copies(mat):
        me = y * 4 + r
        return [pltpu.make_async_remote_copy(
            src_ref=st_all.at[mat, me], dst_ref=st_all.at[mat, me], send_sem=r2_send.at[mat, f * 4 + v],
            recv_sem=r2_recv.at[mat, f * 4 + v], device_id=(z, 1 - y if f else y, flip_row(v)), device_id_type=MESH)
            for f, v in peers]

    def scale_rows(mat):
        return p.rows[mat] * p.row, p.cols[mat] * p.col

    blocks = p.mc // step_r

    def factors(mat, i, n):
        rows = pl.ds(pl.multiple_of(n * step_r, step_r), step_r)
        if mat == DOWN:
            return rows, a_cols[i, rows, :], b_rows[mat].at[:, :]
        return rows, a_cols[0, rows, :], b_rows[mat].at[:, pl.ds(pl.multiple_of(i * p.nc, p.nc), p.nc)]

    def finish_first(mat):
        parts = p.parts[mat]
        if mat != DOWN:
            for i in range(min(2, parts)):
                get_w(mat, jnp.int32(i)).start()
        if mat == DOWN:
            block = c_sum[0]
            for i in range(parts):
                rs[mat][y, :, i * p.mc:(i + 1) * p.mc] = r_row[i]
                if i:
                    block = block + c_sum[i]
            cs[mat][r] = block
        else:
            rs[mat][y] = r_row[0]
            for i in range(parts):
                cs[mat][r, :, i * p.nc:(i + 1) * p.nc] = c_sum[i]
        for c in first_copies(mat):
            c.start()

    def finish_second(mat):
        beta_two = hyper[0]
        m_total, n_total = scale_rows(mat)
        parts = p.parts[mat]
        for c in first_copies(mat):
            c.wait_recv()
        r_new = beta_two * old[mat][0][...] + (1.0 - beta_two) * ((rs[mat][0] + rs[mat][1]) / n_total)
        c_all = ((cs[mat][0] + cs[mat][1]) + cs[mat][2]) + cs[mat][3]
        c_new = beta_two * old[mat][1][...] + (1.0 - beta_two) * (c_all / m_total)
        new[mat][0][...] = r_new
        new[mat][1][...] = c_new
        t_own = jnp.sum(r_new, axis=1, keepdims=True)
        a_row = jnp.sqrt(t_own) / jnp.sqrt(r_new)
        b_rows[mat][...] = 1.0 / jnp.sqrt(c_new)
        if mat == DOWN:
            a_rows[...] = a_row
        for i in range(parts if mat == DOWN else 1):
            a_cols[i] = jnp.broadcast_to(a_row[:, i * p.mc:(i + 1) * p.mc], (LANES, p.mc)).T

        def add_up(j, acc):
            i, n = lax.div(j, blocks), lax.rem(j, blocks)
            rows, a_block, b_ref = factors(mat, i, n)
            for c in range(0, p.nc, LANES):
                upd = grad[i, rows, c:c + LANES] * a_block * b_ref[:, c:c + LANES]
                acc = acc + fold(upd * upd)
            return acc

        u_part = lax.fori_loop(0, parts * blocks, add_up, jnp.zeros((8, LANES), F32))

        def spot(v):
            return jnp.broadcast_to(jnp.sum(jnp.sum(v, axis=1, keepdims=True), axis=0, keepdims=True), (8, LANES))

        me = y * 4 + r
        st_all[mat, me, 0] = spot(u_part)
        st_all[mat, me, 1] = spot(w_sq[mat])
        st_all[mat, me, 2] = jnp.broadcast_to(t_own, (8, LANES))
        for c in second_copies(mat):
            c.start()

    def finish_third(mat):
        rho_step, clip_thr = hyper[1], hyper[2]
        m_total, n_total = scale_rows(mat)
        me = y * 4 + r
        for c in second_copies(mat):
            c.wait_recv()
        t_all = st_all[mat, 0, 2]
        for i in range(1, p.row):
            t_all = t_all + st_all[mat, i, 2]
        u_all = st_all[mat, 0, 0] * (t_all / st_all[mat, 0, 2])
        w_all = st_all[mat, 0, 1]
        for i in range(1, p.row * p.col):
            u_all = u_all + st_all[mat, i, 0] * (t_all / st_all[mat, i, 2])
            w_all = w_all + st_all[mat, i, 1]
        upd_rms = jnp.sqrt(u_all / (m_total * n_total))
        w_rms = jnp.sqrt(w_all / (m_total * n_total))
        scale = rho_step * jnp.maximum(EPS_TWO, w_rms) / jnp.maximum(1.0, upd_rms / clip_thr)
        scale = scale * jnp.sqrt(t_all / st_all[mat, me, 2])
        b_rows[mat][...] = b_rows[mat][...] * scale[0:1, 0:1]

    def renew(mat, low_i, high_i):
        parts = p.parts[mat]

        @pl.loop(low_i, high_i)
        def _(i):
            at = lax.rem(i, 3)
            get_w(mat, i).wait()

            @pl.loop(0, blocks)
            def _(n):
                rows, a_block, b_ref = factors(mat, i, n)
                for c in range(0, p.nc, LANES):
                    cols = slice(c, c + LANES)
                    fresh = w_buf[at, rows, cols] - grad[i, rows, cols] * a_block * b_ref[:, cols]
                    if mat == ATTN:
                        o_attn[rows, cols] = fresh
                    elif mat == UP and UP_KEPT:
                        o_up[i, rows, cols] = fresh
                    else:
                        w_buf[at, rows, cols] = fresh

            if mat == ATTN:
                put_rest().start()
                put_rest().wait()
            if mat == GATE or (mat == UP and not UP_KEPT):
                put_w(mat, i).start()
                pl.when(i >= 1)(lambda: put_w(mat, i - 1).wait())
            pl.when(i + 2 < parts)(lambda: get_w(mat, i + 2).start())

        if (mat == GATE or (mat == UP and not UP_KEPT)) and high_i == parts:
            put_w(mat, jnp.int32(parts - 1)).wait()

    def put_rest():
        return pltpu.make_async_copy(o_attn.at[pl.ds(p.first_rows, p.mc - p.first_rows), :], o_rest, wo_sem.at[0])

    def finish(mat, stage):
        parts = p.parts[mat]
        half = parts // 2 if parts > 1 else parts
        if stage == 1:
            finish_second(mat)
        elif stage == 2:
            finish_third(mat)
            if mat == DOWN:
                al_down[...] = a_rows[...]
                be_down[...] = b_rows[mat][...]
                for c in to_end_down():
                    c.start()
            else:
                renew(mat, 0, half)
        else:
            renew(mat, half, parts)

    def take_x(src, at, k):
        spread_done(k, False)
        load(src, at, p.mc, buf_x, p.at(k), tile_x)
        turn()

    def again_x():
        load(x_mlp, 0, p.mc, buf_x, 0, tile_x)
        turn()

    def got(name, i):
        k = look(i, [p.place[name, j] for j in range(sum(1 for n, _ in p.order if n == name))])
        partner(k, 0).wait_recv()
        partner(k, 1).wait_recv()
        return k

    def use_gate(i):
        pl.when(i == 0)(lambda: take_x(x_mlp, 0, jnp.int32(p.place['x_mlp', 0])))
        k = got('gate', i)
        load(dy_gate, i, p.nc, buf_d, p.at(k), tile_d)
        chunk(GATE, i)
        pl.when(i == p.parts[GATE] - 1)(lambda: finish_first(GATE))

    def use_attn(i):
        take_x(x_attn, 0, jnp.int32(p.place['x_attn', 0]))
        k = got('attn', i)
        load(dy_attn, 0, p.nc, buf_d, p.at(k), tile_d)
        chunk(ATTN, i)
        finish_first(ATTN)

    def use_up(i):
        pl.when(i == 0)(again_x)
        k = got('up', i)
        load(dy_up, i, p.nc, buf_d, p.at(k), tile_d)
        chunk(UP, i)
        pl.when(i == p.parts[UP] - 1)(lambda: finish_first(UP))

    def use_out():
        k = got('out', jnp.int32(0))
        load(dy_out, 0, p.nc, buf_d, p.at(k), tile_d)

    def use_h(i):
        pl.when(i == 0)(use_out)
        take_x(h_mlp, i, look(i, [p.place['h', j] for j in range(p.nh)]))
        chunk(DOWN, i)
        pl.when((i == p.parts[DOWN] - 1) & mid)(lambda: finish_first(DOWN))

    def work(t):
        for name, use in (('gate', use_gate), ('attn', use_attn), ('up', use_up), ('h', use_h)):
            at = jnp.int32(0)
            for i in range(sum(1 for n, _ in p.order if n == name)):
                when_mid = p.steps[True].get((name, i), -1)
                when_end = p.steps[False].get((name, i), -1)
                at = jnp.where(t == jnp.where(mid, when_mid, when_end), i + 1, at)
            pl.when(at > 0)(functools.partial(use, at - 1))
        for mat in MATS:
            for stage in (1, 2, 3):
                when_mid = p.steps[True].get(('finish', mat, stage), -1)
                when_end = p.steps[False].get(('finish', mat, stage), -1)
                if when_mid >= 0:
                    pl.when(t == jnp.where(mid, when_mid, when_end))(functools.partial(finish, mat, stage))

    def sent_to_end(refs, first):
        return [pltpu.make_async_remote_copy(
            src_ref=ref, dst_ref=ref, send_sem=e_send.at[first + i], recv_sem=e_recv.at[first + i],
            device_id=(end_z, y, r), device_id_type=MESH) for i, ref in enumerate(refs)]

    def to_end():
        return sent_to_end((nr_attn, nc_attn, o_attn.at[pl.ds(0, p.first_rows), :]), 0)

    def to_end_down():
        return sent_to_end((nr_down, nc_down, al_down, be_down), 3)

    w_sq[...] = jnp.zeros_like(w_sq)
    ahead = jnp.where(mid, AHEAD_MID, AHEAD_END)

    @pl.loop(0, AHEAD_END)
    def _(k):
        pl.when(k < ahead)(lambda: send_own(k))

    @pl.when(mid)
    def _():
        arrive(jnp.int32(0), jnp.int32(2), False)

    @pl.when(jnp.logical_not(mid))
    def _():
        for k in range(AHEAD_MID):
            arrive(jnp.int32(k), jnp.int32(0), False)

    @pl.loop(0, p.turns)
    def _(t):
        d, turn_no = lax.div(t, 3), lax.rem(t, 3)
        pl.when((turn_no == 0) & (d >= 1) & (d < p.count))(lambda: own_first_left(d - 1))
        early = jnp.where(mid, jnp.where(turn_no == 0, 1, 0), jnp.where(turn_no == 2, AHEAD_MID, 0))
        e = lax.rem(turn_no + jnp.where(mid, 2, 1), 3)
        k = d + early
        pl.when(k < p.count)(lambda: arrive(k, e, True))

        @pl.when(turn_no == 2)
        def _():
            pl.when(d + ahead < p.count)(lambda: send_own(d + ahead))

            @pl.when((d == p.count - 1) & mid)
            def _():
                for c in to_end():
                    c.start()

            k = d - jnp.where(mid, LATE_MID, LATE_END)

            @pl.when((k >= 0) & (k < p.count) & p.is_dy(k) & (mid | jnp.logical_not(p.is_attn(k))))
            def _():
                spread_done(k, True)
                partner(k, 1).start()

        work(t)

    @pl.loop(0, p.count)
    def _(k):
        def go(dy):
            some = slot(k, 0, dy)

            @pl.when(mid)
            def _():
                pass_on(k, dy, some, z, 0, 1).wait_send()
                pass_on(k, dy, some, z, 0, 4).wait_send()

                @pl.when(jnp.logical_not(p.is_attn(k)))
                def _():
                    pass_on(k, dy, some, z, 0, 2).wait_send()
                    pass_on(k, dy, some, z, 0, 3).wait_send()

            for s in range(p.dp - 1):
                spread(k, s, dy).wait_send()
            if dy:
                partner(k, 0).wait_send()
                partner(k, 1).wait_send()

        typed(k, go)

    own_first_left(jnp.int32(p.count - 1))
    for mat in (GATE, UP):
        for c in first_copies(mat) + second_copies(mat):
            c.wait_send()

    @pl.when(mid)
    def _():
        for mat in (ATTN, DOWN):
            for c in first_copies(mat) + second_copies(mat):
                c.wait_send()
        for c in to_end() + to_end_down():
            c.wait_send()

    @pl.when(jnp.logical_not(mid))
    def _():
        for c in to_end() + to_end_down():
            c.wait_recv()


def store_kernel(plan, o_attn, o_gate, o_up, grad, *refs):
    p = plan
    stats, al_down, be_down, w_old, (w_attn, w_gate, w_up, w_down), outs = (
        refs[:8], refs[8], refs[9], refs[10], refs[11:15], refs[15:23])
    bounce, w_buf, a_col, in_sem, out_sem, s_sem, wi_sem, wo_sem = refs[23:]
    depth, wide = bounce.shape[0], w_buf.shape[0]

    def cut(ref, i):
        return ref.at[:, i * p.nc:(i + 1) * p.nc]

    def rows(ref, i):
        return ref.at[i * p.mc:(i + 1) * p.mc, :]

    through = [(cut(o_gate, i), cut(w_gate, i)) for i in range(p.ng)]
    if not UP_KEPT:
        through += [(cut(o_up, i), cut(w_up, i)) for i in range(p.ng)]
    loads = [pltpu.make_async_copy(a, bounce.at[i % depth], in_sem.at[i]) for i, (a, _) in enumerate(through)]
    puts = [pltpu.make_async_copy(bounce.at[i % depth], b, out_sem.at[i]) for i, (_, b) in enumerate(through)]
    w_in = [pltpu.make_async_copy(rows(w_old, i), w_buf.at[i % wide], wi_sem.at[i]) for i in range(p.nh)]
    w_out = [pltpu.make_async_copy(w_buf.at[i % wide], rows(w_down, i), wo_sem.at[i]) for i in range(p.nh)]
    for i in range(wide // 2):
        w_in[i].start()
    for c in loads[:depth]:
        c.start()
    copies = [pltpu.make_async_copy(a, b, s_sem.at[i]) for i, (a, b) in enumerate(zip(stats, outs))]
    copies.append(pltpu.make_async_copy(o_attn, w_attn, s_sem.at[8]))
    if UP_KEPT:
        copies += [pltpu.make_async_copy(o_up.at[i], cut(w_up, i), s_sem.at[9 + i]) for i in range(p.ng)]
    for c in copies:
        c.start()
    step_r = min(64, p.mc)
    per = -(-len(through) // p.nh)
    done = 0
    for i in range(p.nh):
        a_col[...] = jnp.broadcast_to(al_down[:, i * p.mc:(i + 1) * p.mc], (LANES, p.mc)).T
        w_in[i].wait()

        @pl.loop(0, p.mc // step_r)
        def _(n):
            at = pl.ds(pl.multiple_of(n * step_r, step_r), step_r)
            a_block = a_col[at, :]
            for c in range(0, p.nc, LANES):
                cols = slice(c, c + LANES)
                w_buf[i % wide, at, cols] = w_buf[i % wide, at, cols] - grad[i, at, cols] * a_block * be_down[:, cols]

        w_out[i].start()
        again = i + wide // 2
        if again < p.nh:
            if again >= wide:
                w_out[again - wide].wait()
            w_in[again].start()
        for j in range(done, min(len(through), done + per)):
            loads[j].wait()
            puts[j].start()
            again = j + depth // 2
            if depth <= again < len(through):
                puts[again - depth].wait()
                loads[again].start()
        done += per
    for i in range(max(0, p.nh - wide), p.nh):
        if i + wide >= p.nh:
            w_out[i].wait()
    for i in range(max(0, len(through) - depth), len(through)):
        puts[i].wait()
    for c in copies:
        c.wait()


def solution(mesh):
    act_spec = P('dp', 'row')
    grad_spec = P('dp', 'col')
    w_spec = P('row', 'col')
    row_spec = P('row')
    col_spec = P('col')
    in_specs = (act_spec, grad_spec, act_spec, grad_spec, grad_spec, act_spec, grad_spec,
                w_spec, w_spec, w_spec, w_spec,
                row_spec, col_spec, row_spec, col_spec, row_spec, col_spec, row_spec, col_spec, P())
    out_specs = (w_spec, row_spec, col_spec) * 4

    def per_device(x_attn, dy_attn, x_mlp, dy_gate, dy_up, h_mlp, dy_out, w_attn, w_gate, w_up, w_down,
                   r_attn, c_attn, r_gate, c_gate, r_up, c_up, r_down, c_down, hyper_params):
        p = Plan(x_mlp, dy_gate, h_mlp, dy_out, mesh)
        stats = [v.reshape(1, -1) for v in (r_attn, c_attn, r_gate, c_gate, r_up, c_up, r_down, c_down)]
        any_spec = pl.BlockSpec(memory_space=pl.ANY)
        vmem_spec = pl.BlockSpec(memory_space=pltpu.VMEM)
        up_spec = vmem_spec if UP_KEPT else any_spec
        row_shapes = []
        for mat in MATS:
            row_shapes += [jax.ShapeDtypeStruct((1, p.rows[mat]), F32), jax.ShapeDtypeStruct((1, p.cols[mat]), F32)]
        w_shapes = [jax.ShapeDtypeStruct((p.rows[mat], p.cols[mat]), F32) for mat in MATS]
        o_shapes = [pltpu.VMEM((p.mc, p.nc), F32), w_shapes[GATE],
                    pltpu.VMEM((p.ng, p.mc, p.nc), F32) if UP_KEPT else w_shapes[UP],
                    pltpu.VMEM((p.pieces, p.mc, p.nc), F32)]
        bufs = [jax.ShapeDtypeStruct((p.n_dy, p.dp - 1, p.tok, p.nc), BF16),
                jax.ShapeDtypeStruct((p.n_x, p.dp - 1, p.tok, p.mc), BF16)]
        rest = jax.ShapeDtypeStruct((p.mc - p.first_rows, p.nc), F32)
        dma = pltpu.SemaphoreType.DMA
        scratch = [
            pltpu.VMEM((p.dp, p.mc, p.tok), BF16),
            pltpu.VMEM((p.dp, p.tok, p.mc), BF16),
            pltpu.VMEM((p.dp, p.tok, p.nc), BF16),
            pltpu.VMEM((3, p.mc, p.nc), F32),
            pltpu.VMEM((p.mc, LANES), F32),
            pltpu.VMEM((p.pieces, 1, p.mc), F32),
            pltpu.VMEM((p.pieces, 1, p.nc), F32),
            pltpu.VMEM((p.nh, p.mc, LANES), F32),
            pltpu.VMEM((1, p.rows[DOWN]), F32),
            pltpu.VMEM((4, 8, LANES), F32),
        ]
        scratch += [pltpu.VMEM((1, p.cols[mat]), F32) for mat in MATS]
        scratch += [pltpu.VMEM((2, 1, p.rows[mat]), F32) for mat in MATS]
        scratch += [pltpu.VMEM((4, 1, p.cols[mat]), F32) for mat in MATS]
        scratch += [
            pltpu.VMEM((4, 8, 3, 8, LANES), F32),
            dma((p.count, 5)), dma((p.count, p.dp - 1)),
            dma((p.count, p.dp - 1)), dma((p.count, p.dp - 1)),
            dma((p.n_dy, 2)), dma((p.n_dy, 2)),
            dma((4, 4)), dma((4, 4)), dma((4, 8)), dma((4, 8)),
            dma((7,)), dma((7,)),
            dma((p.dp,)), dma((3,)), dma((3,)),
        ]
        out = pl.pallas_call(
            functools.partial(gather_kernel, p),
            out_shape=o_shapes + [pltpu.VMEM(v.shape, F32) for v in row_shapes + row_shapes[-2:]] + [rest] + bufs,
            in_specs=[any_spec] * 11 + [vmem_spec] * 8 + [pl.BlockSpec(memory_space=pltpu.SMEM)],
            out_specs=[vmem_spec, any_spec, up_spec, vmem_spec] + [vmem_spec] * 10 + [any_spec] * 3,
            scratch_shapes=scratch,
            compiler_params=pltpu.CompilerParams(collective_id=0, has_side_effects=True, vmem_limit_bytes=VMEM_LIMIT),
        )(x_attn, dy_attn, x_mlp, dy_gate, dy_up, h_mlp, dy_out, w_attn, w_gate, w_up, w_down, *stats, hyper_params)
        res = pl.pallas_call(
            functools.partial(store_kernel, p),
            out_shape=w_shapes + row_shapes,
            in_specs=[vmem_spec, any_spec, up_spec, vmem_spec] + [vmem_spec] * 10 + [any_spec],
            out_specs=[any_spec] * 12,
            scratch_shapes=[pltpu.VMEM((DEPTH, p.mc, p.nc), F32), pltpu.VMEM((WIDE, p.mc, p.nc), F32),
                            pltpu.VMEM((p.mc, LANES), F32), dma((2 * p.ng,)), dma((2 * p.ng,)), dma((9 + p.ng,)),
                            dma((p.nh,)), dma((p.nh,))],
            compiler_params=pltpu.CompilerParams(vmem_limit_bytes=STORE_LIMIT),
            cost_estimate=pl.CostEstimate(flops=60_000_000_000, bytes_accessed=90_000_000, transcendentals=0),
        )(*[pltpu.with_memory_space_constraint(v, pltpu.VMEM) if i not in HBM_KEPT else v for i, v in enumerate(out[:14])],
          w_down)
        z = lax.axis_index('dp')
        got = lax.ppermute(out[14], 'dp', [(1, 0), (2, 3)])
        rows = jnp.where((z == 1) | (z == 2), out[14], got)
        res = [lax.dynamic_update_slice(res[0], rows, (p.first_rows, 0))] + list(res[1:])
        result = []
        for mat in MATS:
            result += [res[mat], res[4 + 2 * mat].reshape(-1), res[5 + 2 * mat].reshape(-1)]
        return tuple(result)

    return jax.shard_map(per_device, mesh=mesh, in_specs=in_specs, out_specs=out_specs, check_vma=False)
```

```python
import functools
import jax
import jax.numpy as jnp
from jax import lax
from jax.experimental import pallas as pl
from jax.experimental.pallas import tpu as pltpu
from jax.sharding import PartitionSpec as P

EPS_ONE = 1e-30
EPS_TWO = 1e-3
MESH = pl.DeviceIdType.MESH
LANES = 128
F32 = jnp.float32
BF16 = jnp.bfloat16
ATTN, GATE, UP, DOWN = range(4)
MATS = (ATTN, GATE, UP, DOWN)
FIRST = {'gate': ('x_mlp', 0), 'attn': ('x_attn', 0), 'up': ('x_mlp', 0), 'h': ('out', 0)}
AHEAD_MID, AHEAD_END = 2, 6
PARTS = 4
LATE_MID, LATE_END = 3, 2
VMEM_LIMIT = 29 * 1024 * 1024
STORE_LIMIT = 29 * 1024 * 1024
UP_KEPT = True
HBM_KEPT = (1,) if UP_KEPT else (1, 2)
DEPTH, WIDE = 4, 4


def look(k, table):
    out = jnp.int32(0)
    for i, v in enumerate(table):
        if v:
            out = jnp.where(k == i, v, out)
    return out


class Plan:
    def __init__(self, x_mlp, dy_gate, h_mlp, dy_out, mesh):
        self.dp, self.col, self.row = mesh.shape['dp'], mesh.shape['col'], mesh.shape['row']
        assert (self.dp, self.col, self.row) == (4, 2, 4)
        self.tok = x_mlp.shape[0]
        self.mc = x_mlp.shape[1]
        self.nc = dy_out.shape[1]
        self.ng = dy_gate.shape[1] // self.nc
        self.nh = h_mlp.shape[1] // self.mc
        self.tq = self.tok // self.row
        self.th = self.tok // self.col
        g = [('gate', i) for i in range(self.ng)]
        u = [('up', i) for i in range(self.ng)]
        h = [('h', i) for i in range(self.nh)]
        one, two = max(1, self.ng // 4), max(2, 3 * self.ng // 4)
        self.order = ([('x_mlp', 0)] + g[:one] + h[:1] + g[one:two] + h[1:2] + g[two:] + [('x_attn', 0), ('attn', 0)]
                      + u + [('out', 0)] + h[2:])
        self.count = len(self.order)
        self.place = {v: k for k, v in enumerate(self.order)}
        self.first_rows = self.mc * 5 // 16
        self.n_dy = 2 * self.ng + 2
        self.n_x = self.nh + 2
        self.pieces = max(self.ng, self.nh)
        self.rows = {ATTN: self.mc, GATE: self.mc, UP: self.mc, DOWN: self.mc * self.nh}
        self.cols = {ATTN: self.nc, GATE: self.nc * self.ng, UP: self.nc * self.ng, DOWN: self.nc}
        self.parts = {ATTN: 1, GATE: self.ng, UP: self.ng, DOWN: self.nh}
        base = {'gate': 0, 'up': self.ng, 'out': 2 * self.ng, 'attn': 2 * self.ng + 1, 'x_mlp': 0, 'x_attn': 1, 'h': 2}
        self.dy_table = [1 if n in ('gate', 'up', 'out', 'attn') else 0 for n, _ in self.order]
        self.at_table = [base[n] + i for n, i in self.order]
        self.attn_table = [1 if n in ('x_attn', 'attn') else 0 for n, _ in self.order]
        self.steps = {m: self.schedule(m) for m in (True, False)}
        last = max(max(v.values()) for v in self.steps.values())
        self.turns = max(last + 1, 3 * (self.count + LATE_MID + 1))

    def schedule(self, mid):
        late = LATE_MID if mid else LATE_END
        tasks = []
        for name, mat in (('gate', GATE), ('attn', ATTN), ('up', UP), ('h', DOWN)):
            if name == 'attn' and not mid:
                continue
            for i in range(self.parts[mat]):
                k = self.place[name, i]
                need = [3 * (k + late + 1)] if name != 'h' else [3 * (k + late) if mid else 3 * k + 5]
                if i == 0:
                    need.append(3 * (self.place[FIRST[name]] + late + (name == 'h')))
                tasks.append(((name, i), max(need)))
            stages = {ATTN: (1, 2), DOWN: (1, 2)}.get(mat, (1, 2, 3))
            if mid or mat != DOWN:
                tasks += [(('finish', mat, stage), 0) for stage in stages]
        out, t = {}, 0
        for task, first in tasks:
            t = max(t, first)
            out[task] = t
            t += 1
        return out

    def is_dy(self, k):
        return look(k, self.dy_table) == 1

    def is_attn(self, k):
        return look(k, self.attn_table) == 1

    def at(self, k):
        return look(k, self.at_table)


def gather_kernel(plan, x_attn, dy_attn, x_mlp, dy_gate, dy_up, h_mlp, dy_out, w_attn, w_gate, w_up, w_down,
                  r_attn, c_attn, r_gate, c_gate, r_up, c_up, r_down, c_down, hyper,
                  o_attn, o_gate, o_up, grad, nr_attn, nc_attn, nr_gate, nc_gate, nr_up, nc_up, nr_down, nc_down,
                  al_down, be_down, o_rest, buf_d, buf_x,
                  lhs, tile_x, tile_d, w_buf, r_lanes, r_row, c_sum, a_cols, a_rows, w_sq,
                  b_attn, b_gate, b_up, b_down,
                  rs_attn, rs_gate, rs_up, rs_down, cs_attn, cs_gate, cs_up, cs_down, st_all,
                  z_send, z_recv, f_send, f_recv, c_send, c_recv, r1_send, r1_recv, r2_send, r2_recv,
                  e_send, e_recv, l_sem, wi_sem, wo_sem):
    p = plan
    z, y, r = lax.axis_index('dp'), lax.axis_index('col'), lax.axis_index('row')
    low = z < 2
    mid = (z == 1) | (z == 2)
    end_z = jnp.where(low, 0, 3)
    mate_z = 3 - z
    w_refs = {ATTN: w_attn, GATE: w_gate, UP: w_up, DOWN: w_down}
    old = {ATTN: (r_attn, c_attn), GATE: (r_gate, c_gate), UP: (r_up, c_up), DOWN: (r_down, c_down)}
    new = {ATTN: (nr_attn, nc_attn), GATE: (nr_gate, nc_gate), UP: (nr_up, nc_up), DOWN: (nr_down, nc_down)}
    b_rows = {ATTN: b_attn, GATE: b_gate, UP: b_up, DOWN: b_down}
    rs = {ATTN: rs_attn, GATE: rs_gate, UP: rs_up, DOWN: rs_down}
    cs = {ATTN: cs_attn, GATE: cs_gate, UP: cs_up, DOWN: cs_down}

    def flip_row(v):
        bit0, bit1 = lax.rem(r, 2), lax.div(r, 2)
        if v & 1:
            bit0 = 1 - bit0
        if v & 2:
            bit1 = 1 - bit1
        return bit1 * 2 + bit0

    peers = [(f, v) for f in range(2) for v in range(4) if f or v]
    barrier = pltpu.get_barrier_semaphore()
    for f, v in peers:
        pl.semaphore_signal(barrier, inc=1, device_id=(z, 1 - y if f else y, flip_row(v)), device_id_type=MESH)

    @pl.when(mid)
    def _():
        pl.semaphore_signal(barrier, inc=1, device_id=(end_z, y, r), device_id_type=MESH)
        pl.semaphore_signal(barrier, inc=1, device_id=(mate_z, y, r), device_id_type=MESH)
        pl.semaphore_wait(barrier, len(peers) + 2)

    @pl.when(jnp.logical_not(mid))
    def _():
        pl.semaphore_signal(barrier, inc=1, device_id=(jnp.where(low, 1, 2), y, r), device_id_type=MESH)
        pl.semaphore_wait(barrier, len(peers) + 1)

    my_q = pl.ds(pl.multiple_of(r * p.tq, p.tq), p.tq)
    x_q = pl.ds(pl.multiple_of(flip_row(2) * p.tq, p.tq), p.tq)
    my_h = pl.ds(pl.multiple_of(y * p.th, p.th), p.th)

    def rows_of(dy, part):
        if dy:
            return my_q
        if part is None:
            return my_h
        size = p.th // PARTS
        return pl.ds(pl.multiple_of(y * p.th + part * size, size), size)

    def line_of(k, part):
        return k if part is None else k + part

    def slot(k, s, dy, part):
        return (buf_d if dy else buf_x).at[p.at(k), s, rows_of(dy, part), :]

    def pass_on(k, dy, part, src, to_z, to_slot, sem):
        line = line_of(k, part)
        return pltpu.make_async_remote_copy(
            src_ref=src, dst_ref=slot(k, to_slot, dy, part), send_sem=z_send.at[line, sem],
            recv_sem=z_recv.at[line, to_slot], device_id=(to_z, y, r), device_id_type=MESH)

    def spread(k, s, dy, part):
        to = (z, y, flip_row(2)) if dy else (z, 1 - y, r)
        line = line_of(k, part)
        return pltpu.make_async_remote_copy(
            src_ref=slot(k, s, dy, part), dst_ref=slot(k, s, dy, part), send_sem=f_send.at[line, s],
            recv_sem=f_recv.at[line, s], device_id=to, device_id_type=MESH)

    def partner(k, which):
        part = buf_d.at[p.at(k), :, x_q if which else my_q, :]
        return pltpu.make_async_remote_copy(
            src_ref=part, dst_ref=part, send_sem=c_send.at[p.at(k), which], recv_sem=c_recv.at[p.at(k), which],
            device_id=(z, y, flip_row(1)), device_id_type=MESH)

    def in_parts(k, go):
        pl.when(k != p.count - 1)(lambda: go(None))

        @pl.when(k == p.count - 1)
        def _():
            pl.loop(0, PARTS)(go)

    def typed(k, go):
        used = mid | jnp.logical_not(p.is_attn(k))
        pl.when(p.is_dy(k) & used)(lambda: go(True, None))
        pl.when(jnp.logical_not(p.is_dy(k)) & used)(lambda: in_parts(k, lambda part: go(False, part)))

    def cut(ref, at, size):
        return ref.at[:, pl.ds(pl.multiple_of(at * size, size), size)]

    def down_rows(ref, i):
        return ref.at[pl.ds(pl.multiple_of(i * p.mc, p.mc), p.mc), :]

    def own_to(k, dy, part, src):
        @pl.when(jnp.logical_not(mid))
        def _():
            pass_on(k, dy, part, src, jnp.where(low, 1, 2), jnp.where(low, 2, 0), 0).start()

        @pl.when(mid)
        def _():
            @pl.when(jnp.logical_not(p.is_attn(k)))
            def _():
                pass_on(k, dy, part, src, end_z, jnp.where(low, 0, 2), 0).start()
            pass_on(k, dy, part, src, mate_z, jnp.where(low, 2, 0), 1).start()

    def send_own(k):
        def go(ref, at, size, dy):
            def send(part):
                own_to(k, dy, part, ref.at[rows_of(dy, part), pl.ds(pl.multiple_of(at * size, size), size)])

            if ref is h_mlp:
                in_parts(k, send)
            else:
                send(None)

        for name, ref, dy in (('x_mlp', x_mlp, False), ('gate', dy_gate, True), ('x_attn', x_attn, False),
                              ('attn', dy_attn, True), ('up', dy_up, True), ('out', dy_out, True), ('h', h_mlp, False)):
            at = look(k, [i + 1 if n == name else 0 for n, i in p.order])
            size = p.nc if dy else p.mc
            pl.when(at > 0)(functools.partial(go, ref, at - 1, size, dy))

    def own_first_left(k):
        @pl.when(jnp.logical_not(mid & p.is_attn(k)))
        def _():
            def go(dy, part):
                pass_on(k, dy, part, slot(k, 0, dy, part), z, 0, 0).wait_send()

            pl.when(p.is_dy(k))(lambda: go(True, None))
            pl.when(jnp.logical_not(p.is_dy(k)))(lambda: in_parts(k, lambda part: go(False, part)))

    def arrive(k, e, whole):
        s = jnp.where(low, e, 2 - e)

        def go(dy, part):
            here = slot(k, s, dy, part)
            pass_on(k, dy, part, here, z, s, 0).wait_recv()

            @pl.when(mid & (e == 2))
            def _():
                pass_on(k, dy, part, here, mate_z, 1, 4).start()

            @pl.when(mid & (e < 2) & jnp.logical_not(p.is_attn(k)))
            def _():
                pass_on(k, dy, part, here, end_z, jnp.where(low, s + 1, s - 1), 2 + e).start()

            spread(k, s, dy, part).start()
            if dy and whole:
                pl.when(e == jnp.where(mid, 1, 2))(lambda: partner(k, 0).start())

        typed(k, go)

    def spread_done(k, dy):
        for s in range(p.dp - 1):
            spread(k, s, dy, None).wait_recv()

    def load(src, at, size, buf, index, dst):
        copies = [pltpu.make_async_copy(cut(src, at, size), dst.at[z], l_sem.at[0])]
        for d in range(1, p.dp):
            copies.append(pltpu.make_async_copy(buf.at[index, d - 1], dst.at[lax.rem(z + d, p.dp)], l_sem.at[d]))
        for c in copies:
            c.start()
        for c in copies:
            c.wait()

    step_t = min(256, p.tok)

    def turn(q):
        @pl.loop(0, p.tok // step_t)
        def _(t):
            at = pl.multiple_of(t * step_t, step_t)
            lhs[q, :, pl.ds(at, step_t)] = tile_x[q, pl.ds(at, step_t), :].T

    step_n = min(512, p.nc)
    step_r = min(64, p.mc)

    def lane_sum(v):
        out = v[:, 0:LANES]
        for i in range(1, v.shape[1] // LANES):
            out = out + v[:, i * LANES:(i + 1) * LANES]
        return out

    def product(at, count):
        r_lanes[...] = jnp.zeros_like(r_lanes)

        @pl.loop(0, p.nc // step_n)
        def _(n):
            cols = pl.ds(pl.multiple_of(n * step_n, step_n), step_n)
            grad[at, :, cols] = jnp.dot(lhs[0], tile_d[0, :, cols], preferred_element_type=F32)

            @pl.loop(1, p.dp)
            def _(q):
                grad[at, :, cols] += jnp.dot(lhs[q], tile_d[q, :, cols], preferred_element_type=F32)

            def body(i, acc):
                rows = pl.ds(pl.multiple_of(i * step_r, step_r), step_r)
                block = grad[at, rows, cols]
                sq = block * block + EPS_ONE
                r_lanes[rows, :] += lane_sum(sq)
                return acc + jnp.sum(sq, axis=0, keepdims=True)

            @pl.when(count)
            def _():
                c_sum[at, :, cols] = lax.fori_loop(0, p.mc // step_r, body, jnp.zeros((1, step_n), F32))

    def fold(v):
        v = jnp.reshape(v, (v.shape[0] // 8, 8, LANES))
        while v.shape[0] > 1:
            v = v[:v.shape[0] // 2] + v[v.shape[0] // 2:]
        return v[0]

    def to_row(block):
        return jnp.sum(block.T, axis=0, keepdims=True)

    def get_w(mat, i):
        src = down_rows(w_refs[mat], i) if mat == DOWN else cut(w_refs[mat], i, p.nc)
        return pltpu.make_async_copy(src, w_buf.at[lax.rem(i, 3)], wi_sem.at[lax.rem(i, 3)])

    def put_w(mat, i):
        dst = cut(o_gate if mat == GATE else o_up, i, p.nc)
        return pltpu.make_async_copy(w_buf.at[lax.rem(i, 3)], dst, wo_sem.at[lax.rem(i, 3)])

    def chunk(mat, i):
        count = mid if mat == DOWN else jnp.bool_(True)
        pl.when(count)(lambda: get_w(mat, i).start())
        product(i, count)

        @pl.when(count)
        def _():
            row = to_row(r_lanes[...])
            if mat == DOWN:
                r_row[i] = row
            else:
                r_row[0] = jnp.where(i == 0, row, r_row[0] + row)
            get_w(mat, i).wait()

            def body(n, acc):
                rows = pl.ds(pl.multiple_of(n * step_r, step_r), step_r)
                block = lane_sum(w_buf[lax.rem(i, 3), rows, :] * w_buf[lax.rem(i, 3), rows, :])
                return acc + fold(block)

            w_sq[mat] += lax.fori_loop(0, p.mc // step_r, body, jnp.zeros((8, LANES), F32))

    def first_copies(mat):
        copies = [pltpu.make_async_remote_copy(
            src_ref=rs[mat].at[y], dst_ref=rs[mat].at[y], send_sem=r1_send.at[mat, 0], recv_sem=r1_recv.at[mat, 0],
            device_id=(z, 1 - y, r), device_id_type=MESH)]
        for v in range(1, 4):
            copies.append(pltpu.make_async_remote_copy(
                src_ref=cs[mat].at[r], dst_ref=cs[mat].at[r], send_sem=r1_send.at[mat, v],
                recv_sem=r1_recv.at[mat, v], device_id=(z, y, flip_row(v)), device_id_type=MESH))
        return copies

    def second_copies(mat):
        me = y * 4 + r
        return [pltpu.make_async_remote_copy(
            src_ref=st_all.at[mat, me], dst_ref=st_all.at[mat, me], send_sem=r2_send.at[mat, f * 4 + v],
            recv_sem=r2_recv.at[mat, f * 4 + v], device_id=(z, 1 - y if f else y, flip_row(v)), device_id_type=MESH)
            for f, v in peers]

    def scale_rows(mat):
        return p.rows[mat] * p.row, p.cols[mat] * p.col

    blocks = p.mc // step_r

    def factors(mat, i, n):
        rows = pl.ds(pl.multiple_of(n * step_r, step_r), step_r)
        if mat == DOWN:
            return rows, a_cols[i, rows, :], b_rows[mat].at[:, :]
        return rows, a_cols[0, rows, :], b_rows[mat].at[:, pl.ds(pl.multiple_of(i * p.nc, p.nc), p.nc)]

    def finish_first(mat):
        parts = p.parts[mat]
        if mat != DOWN:
            for i in range(min(2, parts)):
                get_w(mat, jnp.int32(i)).start()
        if mat == DOWN:
            block = c_sum[0]
            for i in range(parts):
                rs[mat][y, :, i * p.mc:(i + 1) * p.mc] = r_row[i]
                if i:
                    block = block + c_sum[i]
            cs[mat][r] = block
        else:
            rs[mat][y] = r_row[0]
            for i in range(parts):
                cs[mat][r, :, i * p.nc:(i + 1) * p.nc] = c_sum[i]
        for c in first_copies(mat):
            c.start()

    def finish_second(mat):
        beta_two = hyper[0]
        m_total, n_total = scale_rows(mat)
        parts = p.parts[mat]
        for c in first_copies(mat):
            c.wait_recv()
        r_new = beta_two * old[mat][0][...] + (1.0 - beta_two) * ((rs[mat][0] + rs[mat][1]) / n_total)
        c_all = ((cs[mat][0] + cs[mat][1]) + cs[mat][2]) + cs[mat][3]
        c_new = beta_two * old[mat][1][...] + (1.0 - beta_two) * (c_all / m_total)
        new[mat][0][...] = r_new
        new[mat][1][...] = c_new
        t_own = jnp.sum(r_new, axis=1, keepdims=True)
        a_row = jnp.sqrt(t_own) / jnp.sqrt(r_new)
        b_rows[mat][...] = 1.0 / jnp.sqrt(c_new)
        if mat == DOWN:
            a_rows[...] = a_row
        for i in range(parts if mat == DOWN else 1):
            a_cols[i] = jnp.broadcast_to(a_row[:, i * p.mc:(i + 1) * p.mc], (LANES, p.mc)).T

        def add_up(j, acc):
            i, n = lax.div(j, blocks), lax.rem(j, blocks)
            rows, a_block, b_ref = factors(mat, i, n)
            for c in range(0, p.nc, LANES):
                upd = grad[i, rows, c:c + LANES] * a_block * b_ref[:, c:c + LANES]
                acc = acc + fold(upd * upd)
            return acc

        u_part = lax.fori_loop(0, parts * blocks, add_up, jnp.zeros((8, LANES), F32))

        def spot(v):
            return jnp.broadcast_to(jnp.sum(jnp.sum(v, axis=1, keepdims=True), axis=0, keepdims=True), (8, LANES))

        me = y * 4 + r
        st_all[mat, me, 0] = spot(u_part)
        st_all[mat, me, 1] = spot(w_sq[mat])
        st_all[mat, me, 2] = jnp.broadcast_to(t_own, (8, LANES))
        for c in second_copies(mat):
            c.start()

    def finish_third(mat):
        rho_step, clip_thr = hyper[1], hyper[2]
        m_total, n_total = scale_rows(mat)
        me = y * 4 + r
        for c in second_copies(mat):
            c.wait_recv()
        t_all = st_all[mat, 0, 2]
        for i in range(1, p.row):
            t_all = t_all + st_all[mat, i, 2]
        u_all = st_all[mat, 0, 0] * (t_all / st_all[mat, 0, 2])
        w_all = st_all[mat, 0, 1]
        for i in range(1, p.row * p.col):
            u_all = u_all + st_all[mat, i, 0] * (t_all / st_all[mat, i, 2])
            w_all = w_all + st_all[mat, i, 1]
        upd_rms = jnp.sqrt(u_all / (m_total * n_total))
        w_rms = jnp.sqrt(w_all / (m_total * n_total))
        scale = rho_step * jnp.maximum(EPS_TWO, w_rms) / jnp.maximum(1.0, upd_rms / clip_thr)
        scale = scale * jnp.sqrt(t_all / st_all[mat, me, 2])
        b_rows[mat][...] = b_rows[mat][...] * scale[0:1, 0:1]

    def renew(mat, low_i, high_i):
        parts = p.parts[mat]

        @pl.loop(low_i, high_i)
        def _(i):
            at = lax.rem(i, 3)
            get_w(mat, i).wait()

            @pl.loop(0, blocks)
            def _(n):
                rows, a_block, b_ref = factors(mat, i, n)
                for c in range(0, p.nc, LANES):
                    cols = slice(c, c + LANES)
                    fresh = w_buf[at, rows, cols] - grad[i, rows, cols] * a_block * b_ref[:, cols]
                    if mat == ATTN:
                        o_attn[rows, cols] = fresh
                    elif mat == UP and UP_KEPT:
                        o_up[i, rows, cols] = fresh
                    else:
                        w_buf[at, rows, cols] = fresh

            if mat == ATTN:
                put_rest().start()
                put_rest().wait()
            if mat == GATE or (mat == UP and not UP_KEPT):
                put_w(mat, i).start()
                pl.when(i >= 1)(lambda: put_w(mat, i - 1).wait())
            pl.when(i + 2 < parts)(lambda: get_w(mat, i + 2).start())

        if (mat == GATE or (mat == UP and not UP_KEPT)) and high_i == parts:
            put_w(mat, jnp.int32(parts - 1)).wait()

    def put_rest():
        return pltpu.make_async_copy(o_attn.at[pl.ds(p.first_rows, p.mc - p.first_rows), :], o_rest, wo_sem.at[0])

    def finish(mat, stage):
        parts = p.parts[mat]
        half = parts // 2 if parts > 1 else parts
        if stage == 1:
            finish_second(mat)
        elif stage == 2:
            finish_third(mat)
            if mat == DOWN:
                al_down[...] = a_rows[...]
                be_down[...] = b_rows[mat][...]
                for c in to_end_down():
                    c.start()
            else:
                renew(mat, 0, half)
        else:
            renew(mat, half, parts)

    def take_x(src, at, k, waits=True):
        copies = [(pltpu.make_async_copy(cut(src, at, p.mc), tile_x.at[z], l_sem.at[0]), z)]
        copies[0][0].start()
        for e in range(p.dp - 1):
            s = jnp.where(low, e, 2 - e)
            if src is h_mlp:
                in_parts(k, lambda part: spread(k, s, False, part).wait_recv())
            elif waits:
                spread(k, s, False, None).wait_recv()
            q = lax.rem(z + s + 1, p.dp)
            copies.append((pltpu.make_async_copy(buf_x.at[p.at(k), s], tile_x.at[q], l_sem.at[e + 1]), q))
            copies[-1][0].start()
            copies[-2][0].wait()
            turn(copies[-2][1])
        copies[-1][0].wait()
        turn(copies[-1][1])

    def got(name, i):
        k = look(i, [p.place[name, j] for j in range(sum(1 for n, _ in p.order if n == name))])
        partner(k, 0).wait_recv()
        partner(k, 1).wait_recv()
        return k

    def use_gate(i):
        pl.when(i == 0)(lambda: take_x(x_mlp, 0, jnp.int32(p.place['x_mlp', 0])))
        k = got('gate', i)
        load(dy_gate, i, p.nc, buf_d, p.at(k), tile_d)
        chunk(GATE, i)
        pl.when(i == p.parts[GATE] - 1)(lambda: finish_first(GATE))

    def use_attn(i):
        take_x(x_attn, 0, jnp.int32(p.place['x_attn', 0]))
        k = got('attn', i)
        load(dy_attn, 0, p.nc, buf_d, p.at(k), tile_d)
        chunk(ATTN, i)
        finish_first(ATTN)

    def use_up(i):
        pl.when(i == 0)(lambda: take_x(x_mlp, 0, jnp.int32(p.place['x_mlp', 0]), False))
        k = got('up', i)
        load(dy_up, i, p.nc, buf_d, p.at(k), tile_d)
        chunk(UP, i)
        pl.when(i == p.parts[UP] - 1)(lambda: finish_first(UP))

    def use_out():
        k = got('out', jnp.int32(0))
        load(dy_out, 0, p.nc, buf_d, p.at(k), tile_d)

    def use_h(i):
        pl.when(i == 0)(use_out)
        take_x(h_mlp, i, look(i, [p.place['h', j] for j in range(p.nh)]))
        chunk(DOWN, i)
        pl.when((i == p.parts[DOWN] - 1) & mid)(lambda: finish_first(DOWN))

    def work(t):
        for name, use in (('gate', use_gate), ('attn', use_attn), ('up', use_up), ('h', use_h)):
            at = jnp.int32(0)
            for i in range(sum(1 for n, _ in p.order if n == name)):
                when_mid = p.steps[True].get((name, i), -1)
                when_end = p.steps[False].get((name, i), -1)
                at = jnp.where(t == jnp.where(mid, when_mid, when_end), i + 1, at)
            pl.when(at > 0)(functools.partial(use, at - 1))
        for mat in MATS:
            for stage in (1, 2, 3):
                when_mid = p.steps[True].get(('finish', mat, stage), -1)
                when_end = p.steps[False].get(('finish', mat, stage), -1)
                if when_mid >= 0:
                    pl.when(t == jnp.where(mid, when_mid, when_end))(functools.partial(finish, mat, stage))

    def sent_to_end(refs, first):
        return [pltpu.make_async_remote_copy(
            src_ref=ref, dst_ref=ref, send_sem=e_send.at[first + i], recv_sem=e_recv.at[first + i],
            device_id=(end_z, y, r), device_id_type=MESH) for i, ref in enumerate(refs)]

    def to_end():
        return sent_to_end((nr_attn, nc_attn, o_attn.at[pl.ds(0, p.first_rows), :]), 0)

    def to_end_down():
        return sent_to_end((nr_down, nc_down, al_down, be_down), 3)

    w_sq[...] = jnp.zeros_like(w_sq)
    ahead = jnp.where(mid, AHEAD_MID, AHEAD_END)

    @pl.loop(0, AHEAD_END)
    def _(k):
        pl.when(k < ahead)(lambda: send_own(k))

    @pl.when(mid)
    def _():
        arrive(jnp.int32(0), jnp.int32(2), False)

    @pl.when(jnp.logical_not(mid))
    def _():
        for k in range(AHEAD_MID):
            arrive(jnp.int32(k), jnp.int32(0), False)

    @pl.loop(0, p.turns)
    def _(t):
        d, turn_no = lax.div(t, 3), lax.rem(t, 3)
        pl.when((turn_no == 0) & (d >= 1) & (d < p.count))(lambda: own_first_left(d - 1))
        early = jnp.where(mid, jnp.where(turn_no == 0, 1, 0), jnp.where(turn_no == 2, AHEAD_MID, 0))
        e = lax.rem(turn_no + jnp.where(mid, 2, 1), 3)
        k = d + early
        pl.when(k < p.count)(lambda: arrive(k, e, True))

        @pl.when(turn_no == 2)
        def _():
            pl.when(d + ahead < p.count)(lambda: send_own(d + ahead))

            @pl.when((d == p.count - 1) & mid)
            def _():
                for c in to_end():
                    c.start()

            k = d - jnp.where(mid, LATE_MID, LATE_END)

            @pl.when((k >= 0) & (k < p.count) & p.is_dy(k) & (mid | jnp.logical_not(p.is_attn(k))))
            def _():
                spread_done(k, True)
                partner(k, 1).start()

        work(t)

    @pl.loop(0, p.count)
    def _(k):
        def go(dy, part):
            some = slot(k, 0, dy, part)

            @pl.when(mid)
            def _():
                pass_on(k, dy, part, some, z, 0, 1).wait_send()
                pass_on(k, dy, part, some, z, 0, 4).wait_send()

                @pl.when(jnp.logical_not(p.is_attn(k)))
                def _():
                    pass_on(k, dy, part, some, z, 0, 2).wait_send()
                    pass_on(k, dy, part, some, z, 0, 3).wait_send()

            for s in range(p.dp - 1):
                spread(k, s, dy, part).wait_send()
            if dy:
                partner(k, 0).wait_send()
                partner(k, 1).wait_send()

        typed(k, go)

    own_first_left(jnp.int32(p.count - 1))
    for mat in (GATE, UP):
        for c in first_copies(mat) + second_copies(mat):
            c.wait_send()

    @pl.when(mid)
    def _():
        for mat in (ATTN, DOWN):
            for c in first_copies(mat) + second_copies(mat):
                c.wait_send()
        for c in to_end() + to_end_down():
            c.wait_send()

    @pl.when(jnp.logical_not(mid))
    def _():
        for c in to_end() + to_end_down():
            c.wait_recv()


def store_kernel(plan, o_attn, o_gate, o_up, grad, *refs):
    p = plan
    stats, al_down, be_down, w_old, (w_attn, w_gate, w_up, w_down), outs = (
        refs[:8], refs[8], refs[9], refs[10], refs[11:15], refs[15:23])
    bounce, w_buf, a_col, in_sem, out_sem, s_sem, wi_sem, wo_sem = refs[23:]
    depth, wide = bounce.shape[0], w_buf.shape[0]

    def cut(ref, i):
        return ref.at[:, i * p.nc:(i + 1) * p.nc]

    def rows(ref, i):
        return ref.at[i * p.mc:(i + 1) * p.mc, :]

    through = [(cut(o_gate, i), cut(w_gate, i)) for i in range(p.ng)]
    if not UP_KEPT:
        through += [(cut(o_up, i), cut(w_up, i)) for i in range(p.ng)]
    loads = [pltpu.make_async_copy(a, bounce.at[i % depth], in_sem.at[i]) for i, (a, _) in enumerate(through)]
    puts = [pltpu.make_async_copy(bounce.at[i % depth], b, out_sem.at[i]) for i, (_, b) in enumerate(through)]
    w_in = [pltpu.make_async_copy(rows(w_old, i), w_buf.at[i % wide], wi_sem.at[i]) for i in range(p.nh)]
    w_out = [pltpu.make_async_copy(w_buf.at[i % wide], rows(w_down, i), wo_sem.at[i]) for i in range(p.nh)]
    for i in range(wide // 2):
        w_in[i].start()
    for c in loads[:depth]:
        c.start()
    copies = [pltpu.make_async_copy(a, b, s_sem.at[i]) for i, (a, b) in enumerate(zip(stats, outs))]
    copies.append(pltpu.make_async_copy(o_attn, w_attn, s_sem.at[8]))
    if UP_KEPT:
        copies += [pltpu.make_async_copy(o_up.at[i], cut(w_up, i), s_sem.at[9 + i]) for i in range(p.ng)]
    for c in copies:
        c.start()
    step_r = min(64, p.mc)
    per = -(-len(through) // p.nh)
    done = 0
    for i in range(p.nh):
        a_col[...] = jnp.broadcast_to(al_down[:, i * p.mc:(i + 1) * p.mc], (LANES, p.mc)).T
        w_in[i].wait()

        @pl.loop(0, p.mc // step_r)
        def _(n):
            at = pl.ds(pl.multiple_of(n * step_r, step_r), step_r)
            a_block = a_col[at, :]
            for c in range(0, p.nc, LANES):
                cols = slice(c, c + LANES)
                w_buf[i % wide, at, cols] = w_buf[i % wide, at, cols] - grad[i, at, cols] * a_block * be_down[:, cols]

        w_out[i].start()
        again = i + wide // 2
        if again < p.nh:
            if again >= wide:
                w_out[again - wide].wait()
            w_in[again].start()
        for j in range(done, min(len(through), done + per)):
            loads[j].wait()
            puts[j].start()
            again = j + depth // 2
            if depth <= again < len(through):
                puts[again - depth].wait()
                loads[again].start()
        done += per
    for i in range(max(0, p.nh - wide), p.nh):
        if i + wide >= p.nh:
            w_out[i].wait()
    for i in range(max(0, len(through) - depth), len(through)):
        puts[i].wait()
    for c in copies:
        c.wait()


def solution(mesh):
    act_spec = P('dp', 'row')
    grad_spec = P('dp', 'col')
    w_spec = P('row', 'col')
    row_spec = P('row')
    col_spec = P('col')
    in_specs = (act_spec, grad_spec, act_spec, grad_spec, grad_spec, act_spec, grad_spec,
                w_spec, w_spec, w_spec, w_spec,
                row_spec, col_spec, row_spec, col_spec, row_spec, col_spec, row_spec, col_spec, P())
    out_specs = (w_spec, row_spec, col_spec) * 4

    def per_device(x_attn, dy_attn, x_mlp, dy_gate, dy_up, h_mlp, dy_out, w_attn, w_gate, w_up, w_down,
                   r_attn, c_attn, r_gate, c_gate, r_up, c_up, r_down, c_down, hyper_params):
        p = Plan(x_mlp, dy_gate, h_mlp, dy_out, mesh)
        stats = [v.reshape(1, -1) for v in (r_attn, c_attn, r_gate, c_gate, r_up, c_up, r_down, c_down)]
        any_spec = pl.BlockSpec(memory_space=pl.ANY)
        vmem_spec = pl.BlockSpec(memory_space=pltpu.VMEM)
        up_spec = vmem_spec if UP_KEPT else any_spec
        row_shapes = []
        for mat in MATS:
            row_shapes += [jax.ShapeDtypeStruct((1, p.rows[mat]), F32), jax.ShapeDtypeStruct((1, p.cols[mat]), F32)]
        w_shapes = [jax.ShapeDtypeStruct((p.rows[mat], p.cols[mat]), F32) for mat in MATS]
        o_shapes = [pltpu.VMEM((p.mc, p.nc), F32), w_shapes[GATE],
                    pltpu.VMEM((p.ng, p.mc, p.nc), F32) if UP_KEPT else w_shapes[UP],
                    pltpu.VMEM((p.pieces, p.mc, p.nc), F32)]
        bufs = [jax.ShapeDtypeStruct((p.n_dy, p.dp - 1, p.tok, p.nc), BF16),
                jax.ShapeDtypeStruct((p.n_x, p.dp - 1, p.tok, p.mc), BF16)]
        rest = jax.ShapeDtypeStruct((p.mc - p.first_rows, p.nc), F32)
        dma = pltpu.SemaphoreType.DMA
        lines = p.count + PARTS - 1
        scratch = [
            pltpu.VMEM((p.dp, p.mc, p.tok), BF16),
            pltpu.VMEM((p.dp, p.tok, p.mc), BF16),
            pltpu.VMEM((p.dp, p.tok, p.nc), BF16),
            pltpu.VMEM((3, p.mc, p.nc), F32),
            pltpu.VMEM((p.mc, LANES), F32),
            pltpu.VMEM((p.pieces, 1, p.mc), F32),
            pltpu.VMEM((p.pieces, 1, p.nc), F32),
            pltpu.VMEM((p.nh, p.mc, LANES), F32),
            pltpu.VMEM((1, p.rows[DOWN]), F32),
            pltpu.VMEM((4, 8, LANES), F32),
        ]
        scratch += [pltpu.VMEM((1, p.cols[mat]), F32) for mat in MATS]
        scratch += [pltpu.VMEM((2, 1, p.rows[mat]), F32) for mat in MATS]
        scratch += [pltpu.VMEM((4, 1, p.cols[mat]), F32) for mat in MATS]
        scratch += [
            pltpu.VMEM((4, 8, 3, 8, LANES), F32),
            dma((lines, 5)), dma((lines, p.dp - 1)),
            dma((lines, p.dp - 1)), dma((lines, p.dp - 1)),
            dma((p.n_dy, 2)), dma((p.n_dy, 2)),
            dma((4, 4)), dma((4, 4)), dma((4, 8)), dma((4, 8)),
            dma((7,)), dma((7,)),
            dma((p.dp,)), dma((3,)), dma((3,)),
        ]
        out = pl.pallas_call(
            functools.partial(gather_kernel, p),
            out_shape=o_shapes + [pltpu.VMEM(v.shape, F32) for v in row_shapes + row_shapes[-2:]] + [rest] + bufs,
            in_specs=[any_spec] * 11 + [vmem_spec] * 8 + [pl.BlockSpec(memory_space=pltpu.SMEM)],
            out_specs=[vmem_spec, any_spec, up_spec, vmem_spec] + [vmem_spec] * 10 + [any_spec] * 3,
            scratch_shapes=scratch,
            compiler_params=pltpu.CompilerParams(collective_id=0, has_side_effects=True, vmem_limit_bytes=VMEM_LIMIT),
        )(x_attn, dy_attn, x_mlp, dy_gate, dy_up, h_mlp, dy_out, w_attn, w_gate, w_up, w_down, *stats, hyper_params)
        res = pl.pallas_call(
            functools.partial(store_kernel, p),
            out_shape=w_shapes + row_shapes,
            in_specs=[vmem_spec, any_spec, up_spec, vmem_spec] + [vmem_spec] * 10 + [any_spec],
            out_specs=[any_spec] * 12,
            scratch_shapes=[pltpu.VMEM((DEPTH, p.mc, p.nc), F32), pltpu.VMEM((WIDE, p.mc, p.nc), F32),
                            pltpu.VMEM((p.mc, LANES), F32), dma((2 * p.ng,)), dma((2 * p.ng,)), dma((9 + p.ng,)),
                            dma((p.nh,)), dma((p.nh,))],
            compiler_params=pltpu.CompilerParams(vmem_limit_bytes=STORE_LIMIT),
            cost_estimate=pl.CostEstimate(flops=60_000_000_000, bytes_accessed=90_000_000, transcendentals=0),
        )(*[pltpu.with_memory_space_constraint(v, pltpu.VMEM) if i not in HBM_KEPT else v for i, v in enumerate(out[:14])],
          w_down)
        z = lax.axis_index('dp')
        got = lax.ppermute(out[14], 'dp', [(1, 0), (2, 3)])
        rows = jnp.where((z == 1) | (z == 2), out[14], got)
        res = [lax.dynamic_update_slice(res[0], rows, (p.first_rows, 0))] + list(res[1:])
        result = []
        for mat in MATS:
            result += [res[mat], res[4 + 2 * mat].reshape(-1), res[5 + 2 * mat].reshape(-1)]
        return tuple(result)

    return jax.shard_map(per_device, mesh=mesh, in_specs=in_specs, out_specs=out_specs, check_vma=False)
```

```python
import functools
import jax
import jax.numpy as jnp
from jax import lax
from jax.experimental import pallas as pl
from jax.experimental.pallas import tpu as pltpu
from jax.sharding import PartitionSpec as P

EPS_ONE = 1e-30
EPS_TWO = 1e-3
MESH = pl.DeviceIdType.MESH
LANES = 128
F32 = jnp.float32
BF16 = jnp.bfloat16
ATTN, GATE, UP, DOWN = range(4)
MATS = (ATTN, GATE, UP, DOWN)
FIRST = {'gate': ('x_mlp', 0), 'attn': ('x_attn', 0), 'up': ('x_mlp', 0), 'h': ('out', 0)}
AHEAD_MID, AHEAD_END = 2, 6
PARTS = 4
LATE_MID, LATE_END = 3, 2
VMEM_LIMIT = 29 * 1024 * 1024
STORE_LIMIT = 29 * 1024 * 1024
UP_KEPT = True
HBM_KEPT = (1,) if UP_KEPT else (1, 2)
DEPTH, WIDE = 4, 4


def look(k, table):
    out = jnp.int32(0)
    for i, v in enumerate(table):
        if v:
            out = jnp.where(k == i, v, out)
    return out


class Plan:
    def __init__(self, x_mlp, dy_gate, h_mlp, dy_out, mesh):
        self.dp, self.col, self.row = mesh.shape['dp'], mesh.shape['col'], mesh.shape['row']
        assert (self.dp, self.col, self.row) == (4, 2, 4)
        self.tok = x_mlp.shape[0]
        self.mc = x_mlp.shape[1]
        self.nc = dy_out.shape[1]
        self.ng = dy_gate.shape[1] // self.nc
        self.nh = h_mlp.shape[1] // self.mc
        self.tq = self.tok // self.row
        self.th = self.tok // self.col
        g = [('gate', i) for i in range(self.ng)]
        u = [('up', i) for i in range(self.ng)]
        h = [('h', i) for i in range(self.nh)]
        one, two = max(1, self.ng // 4), max(2, 3 * self.ng // 4)
        self.order = ([('x_mlp', 0)] + g[:one] + h[:1] + g[one:two] + h[1:2] + g[two:] + [('x_attn', 0), ('attn', 0)]
                      + u + [('out', 0)] + h[2:])
        self.count = len(self.order)
        self.place = {v: k for k, v in enumerate(self.order)}
        self.first_rows = self.mc * 5 // 16
        self.n_dy = 2 * self.ng + 2
        self.n_x = self.nh + 2
        self.pieces = max(self.ng, self.nh)
        self.rows = {ATTN: self.mc, GATE: self.mc, UP: self.mc, DOWN: self.mc * self.nh}
        self.cols = {ATTN: self.nc, GATE: self.nc * self.ng, UP: self.nc * self.ng, DOWN: self.nc}
        self.parts = {ATTN: 1, GATE: self.ng, UP: self.ng, DOWN: self.nh}
        base = {'gate': 0, 'up': self.ng, 'out': 2 * self.ng, 'attn': 2 * self.ng + 1, 'x_mlp': 0, 'x_attn': 1, 'h': 2}
        self.dy_table = [1 if n in ('gate', 'up', 'out', 'attn') else 0 for n, _ in self.order]
        self.at_table = [base[n] + i for n, i in self.order]
        self.attn_table = [1 if n in ('x_attn', 'attn') else 0 for n, _ in self.order]
        self.steps = {m: self.schedule(m) for m in (True, False)}
        self.turns = {m: max(max(v.values()) + 1, 3 * self.count) for m, v in self.steps.items()}

    def schedule(self, mid):
        late = LATE_MID if mid else LATE_END
        tasks = []
        for name, mat in (('gate', GATE), ('attn', ATTN), ('up', UP), ('h', DOWN)):
            if name == 'attn' and not mid:
                continue
            for i in range(self.parts[mat]):
                k = self.place[name, i]
                need = [3 * (k + late + 1)] if name != 'h' else [3 * (k + late) if mid else 3 * k + 5]
                if i == 0:
                    need.append(3 * (self.place[FIRST[name]] + late + (name == 'h')))
                tasks.append(((name, i), max(need)))
            stages = {ATTN: (1, 2), DOWN: (1, 2)}.get(mat, (1, 2, 3))
            if mid or mat != DOWN:
                tasks += [(('finish', mat, stage), 0) for stage in stages]
        out, t = {}, 0
        for task, first in tasks:
            t = max(t, first)
            out[task] = t
            t += 1
        return out

    def is_dy(self, k):
        return look(k, self.dy_table) == 1

    def is_attn(self, k):
        return look(k, self.attn_table) == 1

    def at(self, k):
        return look(k, self.at_table)


def gather_kernel(plan, x_attn, dy_attn, x_mlp, dy_gate, dy_up, h_mlp, dy_out, w_attn, w_gate, w_up, w_down,
                  r_attn, c_attn, r_gate, c_gate, r_up, c_up, r_down, c_down, hyper,
                  o_attn, o_gate, o_up, grad, nr_attn, nc_attn, nr_gate, nc_gate, nr_up, nc_up, nr_down, nc_down,
                  al_down, be_down, o_rest, buf_d, buf_x,
                  lhs, tile_x, tile_d, w_buf, r_lanes, r_row, c_sum, a_cols, a_rows, w_sq,
                  b_attn, b_gate, b_up, b_down, *more):
    p = plan
    old_refs = more[:8]
    (rs_attn, rs_gate, rs_up, rs_down, cs_attn, cs_gate, cs_up, cs_down, st_all,
     z_send, z_recv, f_send, f_recv, c_send, c_recv, r1_send, r1_recv, r2_send, r2_recv,
     e_send, e_recv, l_sem, wi_sem, wo_sem, o_sem) = more[8:]
    z, y, r = lax.axis_index('dp'), lax.axis_index('col'), lax.axis_index('row')
    low = z < 2
    mid = (z == 1) | (z == 2)
    end_z = jnp.where(low, 0, 3)
    mate_z = 3 - z
    w_refs = {ATTN: w_attn, GATE: w_gate, UP: w_up, DOWN: w_down}
    old_in = (r_attn, c_attn, r_gate, c_gate, r_up, c_up, r_down, c_down)
    old = {mat: (old_refs[2 * mat], old_refs[2 * mat + 1]) for mat in MATS}
    old_copies = [pltpu.make_async_copy(a, b, o_sem.at[i]) for i, (a, b) in enumerate(zip(old_in, old_refs))]
    new = {ATTN: (nr_attn, nc_attn), GATE: (nr_gate, nc_gate), UP: (nr_up, nc_up), DOWN: (nr_down, nc_down)}
    b_rows = {ATTN: b_attn, GATE: b_gate, UP: b_up, DOWN: b_down}
    rs = {ATTN: rs_attn, GATE: rs_gate, UP: rs_up, DOWN: rs_down}
    cs = {ATTN: cs_attn, GATE: cs_gate, UP: cs_up, DOWN: cs_down}

    def flip_row(v):
        bit0, bit1 = lax.rem(r, 2), lax.div(r, 2)
        if v & 1:
            bit0 = 1 - bit0
        if v & 2:
            bit1 = 1 - bit1
        return bit1 * 2 + bit0

    peers = [(f, v) for f in range(2) for v in range(4) if f or v]
    barrier = pltpu.get_barrier_semaphore()
    for f, v in peers:
        pl.semaphore_signal(barrier, inc=1, device_id=(z, 1 - y if f else y, flip_row(v)), device_id_type=MESH)

    @pl.when(mid)
    def _():
        pl.semaphore_signal(barrier, inc=1, device_id=(end_z, y, r), device_id_type=MESH)
        pl.semaphore_signal(barrier, inc=1, device_id=(mate_z, y, r), device_id_type=MESH)
        pl.semaphore_wait(barrier, len(peers) + 2)

    @pl.when(jnp.logical_not(mid))
    def _():
        pl.semaphore_signal(barrier, inc=1, device_id=(jnp.where(low, 1, 2), y, r), device_id_type=MESH)
        pl.semaphore_wait(barrier, len(peers) + 1)

    my_q = pl.ds(pl.multiple_of(r * p.tq, p.tq), p.tq)
    x_q = pl.ds(pl.multiple_of(flip_row(2) * p.tq, p.tq), p.tq)
    my_h = pl.ds(pl.multiple_of(y * p.th, p.th), p.th)

    def rows_of(dy, part):
        if dy:
            return my_q
        if part is None:
            return my_h
        size = p.th // PARTS
        return pl.ds(pl.multiple_of(y * p.th + part * size, size), size)

    def line_of(k, part):
        return k if part is None else k + part

    def slot(k, s, dy, part):
        return (buf_d if dy else buf_x).at[p.at(k), s, rows_of(dy, part), :]

    def pass_on(k, dy, part, src, to_z, to_slot, sem):
        line = line_of(k, part)
        return pltpu.make_async_remote_copy(
            src_ref=src, dst_ref=slot(k, to_slot, dy, part), send_sem=z_send.at[line, sem],
            recv_sem=z_recv.at[line, to_slot], device_id=(to_z, y, r), device_id_type=MESH)

    def spread(k, s, dy, part):
        to = (z, y, flip_row(2)) if dy else (z, 1 - y, r)
        line = line_of(k, part)
        return pltpu.make_async_remote_copy(
            src_ref=slot(k, s, dy, part), dst_ref=slot(k, s, dy, part), send_sem=f_send.at[line, s],
            recv_sem=f_recv.at[line, s], device_id=to, device_id_type=MESH)

    def partner(k, which):
        part = buf_d.at[p.at(k), :, x_q if which else my_q, :]
        return pltpu.make_async_remote_copy(
            src_ref=part, dst_ref=part, send_sem=c_send.at[p.at(k), which], recv_sem=c_recv.at[p.at(k), which],
            device_id=(z, y, flip_row(1)), device_id_type=MESH)

    def in_parts(k, go):
        pl.when(k != p.count - 1)(lambda: go(None))

        @pl.when(k == p.count - 1)
        def _():
            pl.loop(0, PARTS)(go)

    def typed(k, go):
        used = mid | jnp.logical_not(p.is_attn(k))
        pl.when(p.is_dy(k) & used)(lambda: go(True, None))
        pl.when(jnp.logical_not(p.is_dy(k)) & used)(lambda: in_parts(k, lambda part: go(False, part)))

    def cut(ref, at, size):
        return ref.at[:, pl.ds(pl.multiple_of(at * size, size), size)]

    def down_rows(ref, i):
        return ref.at[pl.ds(pl.multiple_of(i * p.mc, p.mc), p.mc), :]

    def own_to(k, dy, part, src):
        @pl.when(jnp.logical_not(mid))
        def _():
            pass_on(k, dy, part, src, jnp.where(low, 1, 2), jnp.where(low, 2, 0), 0).start()

        @pl.when(mid)
        def _():
            @pl.when(jnp.logical_not(p.is_attn(k)))
            def _():
                pass_on(k, dy, part, src, end_z, jnp.where(low, 0, 2), 0).start()
            pass_on(k, dy, part, src, mate_z, jnp.where(low, 2, 0), 1).start()

    def send_own(k):
        def go(ref, at, size, dy):
            def send(part):
                own_to(k, dy, part, ref.at[rows_of(dy, part), pl.ds(pl.multiple_of(at * size, size), size)])

            if ref is h_mlp:
                in_parts(k, send)
            else:
                send(None)

        for name, ref, dy in (('x_mlp', x_mlp, False), ('gate', dy_gate, True), ('x_attn', x_attn, False),
                              ('attn', dy_attn, True), ('up', dy_up, True), ('out', dy_out, True), ('h', h_mlp, False)):
            at = look(k, [i + 1 if n == name else 0 for n, i in p.order])
            size = p.nc if dy else p.mc
            pl.when(at > 0)(functools.partial(go, ref, at - 1, size, dy))

    def own_first_left(k):
        @pl.when(jnp.logical_not(mid & p.is_attn(k)))
        def _():
            def go(dy, part):
                pass_on(k, dy, part, slot(k, 0, dy, part), z, 0, 0).wait_send()

            pl.when(p.is_dy(k))(lambda: go(True, None))
            pl.when(jnp.logical_not(p.is_dy(k)))(lambda: in_parts(k, lambda part: go(False, part)))

    def arrive(k, e, whole):
        s = jnp.where(low, e, 2 - e)

        def go(dy, part):
            here = slot(k, s, dy, part)
            pass_on(k, dy, part, here, z, s, 0).wait_recv()

            @pl.when(mid & (e == 2))
            def _():
                pass_on(k, dy, part, here, mate_z, 1, 4).start()

            @pl.when(mid & (e < 2) & jnp.logical_not(p.is_attn(k)))
            def _():
                pass_on(k, dy, part, here, end_z, jnp.where(low, s + 1, s - 1), 2 + e).start()

            spread(k, s, dy, part).start()
            if dy and whole:
                pl.when(e == jnp.where(mid, 1, 2))(lambda: partner(k, 0).start())

        typed(k, go)

    def spread_done(k, dy):
        for s in range(p.dp - 1):
            spread(k, s, dy, None).wait_recv()

    def load(src, at, size, buf, index, dst):
        copies = [pltpu.make_async_copy(cut(src, at, size), dst.at[z], l_sem.at[0])]
        for d in range(1, p.dp):
            copies.append(pltpu.make_async_copy(buf.at[index, d - 1], dst.at[lax.rem(z + d, p.dp)], l_sem.at[d]))
        for c in copies:
            c.start()
        for c in copies:
            c.wait()

    step_t = min(256, p.tok)

    def turn(q):
        @pl.loop(0, p.tok // step_t)
        def _(t):
            at = pl.multiple_of(t * step_t, step_t)
            lhs[q, :, pl.ds(at, step_t)] = tile_x[q, pl.ds(at, step_t), :].T

    step_n = min(512, p.nc)
    step_r = min(64, p.mc)

    def lane_sum(v):
        out = v[:, 0:LANES]
        for i in range(1, v.shape[1] // LANES):
            out = out + v[:, i * LANES:(i + 1) * LANES]
        return out

    def product(at, count):
        r_lanes[...] = jnp.zeros_like(r_lanes)

        @pl.loop(0, p.nc // step_n)
        def _(n):
            cols = pl.ds(pl.multiple_of(n * step_n, step_n), step_n)
            grad[at, :, cols] = jnp.dot(lhs[0], tile_d[0, :, cols], preferred_element_type=F32)

            @pl.loop(1, p.dp)
            def _(q):
                grad[at, :, cols] += jnp.dot(lhs[q], tile_d[q, :, cols], preferred_element_type=F32)

            def body(i, acc):
                rows = pl.ds(pl.multiple_of(i * step_r, step_r), step_r)
                block = grad[at, rows, cols]
                sq = block * block + EPS_ONE
                r_lanes[rows, :] += lane_sum(sq)
                return acc + jnp.sum(sq, axis=0, keepdims=True)

            @pl.when(count)
            def _():
                c_sum[at, :, cols] = lax.fori_loop(0, p.mc // step_r, body, jnp.zeros((1, step_n), F32))

    def fold(v):
        v = jnp.reshape(v, (v.shape[0] // 8, 8, LANES))
        while v.shape[0] > 1:
            v = v[:v.shape[0] // 2] + v[v.shape[0] // 2:]
        return v[0]

    def to_row(block):
        return jnp.sum(block.T, axis=0, keepdims=True)

    def get_w(mat, i):
        src = down_rows(w_refs[mat], i) if mat == DOWN else cut(w_refs[mat], i, p.nc)
        return pltpu.make_async_copy(src, w_buf.at[lax.rem(i, 3)], wi_sem.at[lax.rem(i, 3)])

    def put_w(mat, i):
        dst = cut(o_gate if mat == GATE else o_up, i, p.nc)
        return pltpu.make_async_copy(w_buf.at[lax.rem(i, 3)], dst, wo_sem.at[lax.rem(i, 3)])

    def chunk(mat, i):
        count = mid if mat == DOWN else jnp.bool_(True)
        pl.when(count)(lambda: get_w(mat, i).start())
        product(i, count)

        @pl.when(count)
        def _():
            row = to_row(r_lanes[...])
            if mat == DOWN:
                r_row[i] = row
            else:
                r_row[0] = jnp.where(i == 0, row, r_row[0] + row)
            get_w(mat, i).wait()

            def body(n, acc):
                rows = pl.ds(pl.multiple_of(n * step_r, step_r), step_r)
                block = lane_sum(w_buf[lax.rem(i, 3), rows, :] * w_buf[lax.rem(i, 3), rows, :])
                return acc + fold(block)

            w_sq[mat] += lax.fori_loop(0, p.mc // step_r, body, jnp.zeros((8, LANES), F32))

    def first_copies(mat):
        copies = [pltpu.make_async_remote_copy(
            src_ref=rs[mat].at[y], dst_ref=rs[mat].at[y], send_sem=r1_send.at[mat, 0], recv_sem=r1_recv.at[mat, 0],
            device_id=(z, 1 - y, r), device_id_type=MESH)]
        for v in range(1, 4):
            copies.append(pltpu.make_async_remote_copy(
                src_ref=cs[mat].at[r], dst_ref=cs[mat].at[r], send_sem=r1_send.at[mat, v],
                recv_sem=r1_recv.at[mat, v], device_id=(z, y, flip_row(v)), device_id_type=MESH))
        return copies

    def second_copies(mat):
        me = y * 4 + r
        return [pltpu.make_async_remote_copy(
            src_ref=st_all.at[mat, me], dst_ref=st_all.at[mat, me], send_sem=r2_send.at[mat, f * 4 + v],
            recv_sem=r2_recv.at[mat, f * 4 + v], device_id=(z, 1 - y if f else y, flip_row(v)), device_id_type=MESH)
            for f, v in peers]

    def scale_rows(mat):
        return p.rows[mat] * p.row, p.cols[mat] * p.col

    blocks = p.mc // step_r

    def factors(mat, i, n):
        rows = pl.ds(pl.multiple_of(n * step_r, step_r), step_r)
        if mat == DOWN:
            return rows, a_cols[i, rows, :], b_rows[mat].at[:, :]
        return rows, a_cols[0, rows, :], b_rows[mat].at[:, pl.ds(pl.multiple_of(i * p.nc, p.nc), p.nc)]

    def finish_first(mat):
        parts = p.parts[mat]
        if mat != DOWN:
            for i in range(min(2, parts)):
                get_w(mat, jnp.int32(i)).start()
        if mat == DOWN:
            block = c_sum[0]
            for i in range(parts):
                rs[mat][y, :, i * p.mc:(i + 1) * p.mc] = r_row[i]
                if i:
                    block = block + c_sum[i]
            cs[mat][r] = block
        else:
            rs[mat][y] = r_row[0]
            for i in range(parts):
                cs[mat][r, :, i * p.nc:(i + 1) * p.nc] = c_sum[i]
        for c in first_copies(mat):
            c.start()

    def finish_second(mat):
        beta_two = hyper[0]
        m_total, n_total = scale_rows(mat)
        parts = p.parts[mat]
        for c in first_copies(mat):
            c.wait_recv()
        r_new = beta_two * old[mat][0][...] + (1.0 - beta_two) * ((rs[mat][0] + rs[mat][1]) / n_total)
        c_all = ((cs[mat][0] + cs[mat][1]) + cs[mat][2]) + cs[mat][3]
        c_new = beta_two * old[mat][1][...] + (1.0 - beta_two) * (c_all / m_total)
        new[mat][0][...] = r_new
        new[mat][1][...] = c_new
        t_own = jnp.sum(r_new, axis=1, keepdims=True)
        a_row = jnp.sqrt(t_own) / jnp.sqrt(r_new)
        b_rows[mat][...] = 1.0 / jnp.sqrt(c_new)
        if mat == DOWN:
            a_rows[...] = a_row
        for i in range(parts if mat == DOWN else 1):
            a_cols[i] = jnp.broadcast_to(a_row[:, i * p.mc:(i + 1) * p.mc], (LANES, p.mc)).T

        def add_up(j, acc):
            i, n = lax.div(j, blocks), lax.rem(j, blocks)
            rows, a_block, b_ref = factors(mat, i, n)
            for c in range(0, p.nc, LANES):
                upd = grad[i, rows, c:c + LANES] * a_block * b_ref[:, c:c + LANES]
                acc = acc + fold(upd * upd)
            return acc

        u_part = lax.fori_loop(0, parts * blocks, add_up, jnp.zeros((8, LANES), F32))

        def spot(v):
            return jnp.broadcast_to(jnp.sum(jnp.sum(v, axis=1, keepdims=True), axis=0, keepdims=True), (8, LANES))

        me = y * 4 + r
        st_all[mat, me, 0] = spot(u_part)
        st_all[mat, me, 1] = spot(w_sq[mat])
        st_all[mat, me, 2] = jnp.broadcast_to(t_own, (8, LANES))
        for c in second_copies(mat):
            c.start()

    def finish_third(mat):
        rho_step, clip_thr = hyper[1], hyper[2]
        m_total, n_total = scale_rows(mat)
        me = y * 4 + r
        for c in second_copies(mat):
            c.wait_recv()
        t_all = st_all[mat, 0, 2]
        for i in range(1, p.row):
            t_all = t_all + st_all[mat, i, 2]
        u_all = st_all[mat, 0, 0] * (t_all / st_all[mat, 0, 2])
        w_all = st_all[mat, 0, 1]
        for i in range(1, p.row * p.col):
            u_all = u_all + st_all[mat, i, 0] * (t_all / st_all[mat, i, 2])
            w_all = w_all + st_all[mat, i, 1]
        upd_rms = jnp.sqrt(u_all / (m_total * n_total))
        w_rms = jnp.sqrt(w_all / (m_total * n_total))
        scale = rho_step * jnp.maximum(EPS_TWO, w_rms) / jnp.maximum(1.0, upd_rms / clip_thr)
        scale = scale * jnp.sqrt(t_all / st_all[mat, me, 2])
        b_rows[mat][...] = b_rows[mat][...] * scale[0:1, 0:1]

    def renew(mat, low_i, high_i):
        parts = p.parts[mat]

        @pl.loop(low_i, high_i)
        def _(i):
            at = lax.rem(i, 3)
            get_w(mat, i).wait()

            @pl.loop(0, blocks)
            def _(n):
                rows, a_block, b_ref = factors(mat, i, n)
                for c in range(0, p.nc, LANES):
                    cols = slice(c, c + LANES)
                    fresh = w_buf[at, rows, cols] - grad[i, rows, cols] * a_block * b_ref[:, cols]
                    if mat == ATTN:
                        o_attn[rows, cols] = fresh
                    elif mat == UP and UP_KEPT:
                        o_up[i, rows, cols] = fresh
                    else:
                        w_buf[at, rows, cols] = fresh

            if mat == ATTN:
                put_rest().start()
                put_rest().wait()
            if mat == GATE or (mat == UP and not UP_KEPT):
                put_w(mat, i).start()
                pl.when(i >= 1)(lambda: put_w(mat, i - 1).wait())
            pl.when(i + 2 < parts)(lambda: get_w(mat, i + 2).start())

        if (mat == GATE or (mat == UP and not UP_KEPT)) and high_i == parts:
            put_w(mat, jnp.int32(parts - 1)).wait()

    def put_rest():
        return pltpu.make_async_copy(o_attn.at[pl.ds(p.first_rows, p.mc - p.first_rows), :], o_rest, wo_sem.at[0])

    def finish(mat, stage):
        parts = p.parts[mat]
        half = parts // 2 if parts > 1 else parts
        if stage == 1:
            finish_second(mat)
        elif stage == 2:
            finish_third(mat)
            if mat == DOWN:
                al_down[...] = a_rows[...]
                be_down[...] = b_rows[mat][...]
                for c in to_end_down():
                    c.start()
            else:
                renew(mat, 0, half)
        else:
            renew(mat, half, parts)

    def take_x(src, at, k, waits=True):
        copies = [(pltpu.make_async_copy(cut(src, at, p.mc), tile_x.at[z], l_sem.at[0]), z)]
        copies[0][0].start()
        for e in range(p.dp - 1):
            s = jnp.where(low, e, 2 - e)
            if src is h_mlp:
                in_parts(k, lambda part: spread(k, s, False, part).wait_recv())
            elif waits:
                spread(k, s, False, None).wait_recv()
            q = lax.rem(z + s + 1, p.dp)
            copies.append((pltpu.make_async_copy(buf_x.at[p.at(k), s], tile_x.at[q], l_sem.at[e + 1]), q))
            copies[-1][0].start()
            copies[-2][0].wait()
            turn(copies[-2][1])
        copies[-1][0].wait()
        turn(copies[-1][1])

    def got(name, i):
        k = look(i, [p.place[name, j] for j in range(sum(1 for n, _ in p.order if n == name))])
        partner(k, 0).wait_recv()
        partner(k, 1).wait_recv()
        return k

    def use_gate(i):
        pl.when(i == 0)(lambda: take_x(x_mlp, 0, jnp.int32(p.place['x_mlp', 0])))
        k = got('gate', i)
        load(dy_gate, i, p.nc, buf_d, p.at(k), tile_d)
        chunk(GATE, i)
        pl.when(i == p.parts[GATE] - 1)(lambda: finish_first(GATE))

    def use_attn(i):
        take_x(x_attn, 0, jnp.int32(p.place['x_attn', 0]))
        k = got('attn', i)
        load(dy_attn, 0, p.nc, buf_d, p.at(k), tile_d)
        chunk(ATTN, i)
        finish_first(ATTN)

    def use_up(i):
        pl.when(i == 0)(lambda: take_x(x_mlp, 0, jnp.int32(p.place['x_mlp', 0]), False))
        k = got('up', i)
        load(dy_up, i, p.nc, buf_d, p.at(k), tile_d)
        chunk(UP, i)
        pl.when(i == p.parts[UP] - 1)(lambda: finish_first(UP))

    def use_out():
        k = got('out', jnp.int32(0))
        load(dy_out, 0, p.nc, buf_d, p.at(k), tile_d)

    def use_h(i):
        pl.when(i == 0)(use_out)
        take_x(h_mlp, i, look(i, [p.place['h', j] for j in range(p.nh)]))
        chunk(DOWN, i)
        pl.when((i == p.parts[DOWN] - 1) & mid)(lambda: finish_first(DOWN))

    def work(t):
        for name, use in (('gate', use_gate), ('attn', use_attn), ('up', use_up), ('h', use_h)):
            at = jnp.int32(0)
            for i in range(sum(1 for n, _ in p.order if n == name)):
                when_mid = p.steps[True].get((name, i), -1)
                when_end = p.steps[False].get((name, i), -1)
                at = jnp.where(t == jnp.where(mid, when_mid, when_end), i + 1, at)
            pl.when(at > 0)(functools.partial(use, at - 1))
        for mat in MATS:
            for stage in (1, 2, 3):
                when_mid = p.steps[True].get(('finish', mat, stage), -1)
                when_end = p.steps[False].get(('finish', mat, stage), -1)
                if when_mid >= 0:
                    pl.when(t == jnp.where(mid, when_mid, when_end))(functools.partial(finish, mat, stage))

    def sent_to_end(refs, first):
        return [pltpu.make_async_remote_copy(
            src_ref=ref, dst_ref=ref, send_sem=e_send.at[first + i], recv_sem=e_recv.at[first + i],
            device_id=(end_z, y, r), device_id_type=MESH) for i, ref in enumerate(refs)]

    def to_end():
        return sent_to_end((nr_attn, nc_attn, o_attn.at[pl.ds(0, p.first_rows), :]), 0)

    def to_end_down():
        return sent_to_end((nr_down, nc_down, al_down, be_down), 3)

    def sends_left(k):
        def go(dy, part):
            some = slot(k, 0, dy, part)

            @pl.when(mid)
            def _():
                pass_on(k, dy, part, some, z, 0, 1).wait_send()
                pass_on(k, dy, part, some, z, 0, 4).wait_send()

                @pl.when(jnp.logical_not(p.is_attn(k)))
                def _():
                    pass_on(k, dy, part, some, z, 0, 2).wait_send()
                    pass_on(k, dy, part, some, z, 0, 3).wait_send()

            for s in range(p.dp - 1):
                spread(k, s, dy, part).wait_send()
            if dy:
                partner(k, 0).wait_send()
                partner(k, 1).wait_send()

        typed(k, go)

    w_sq[...] = jnp.zeros_like(w_sq)
    ahead = jnp.where(mid, AHEAD_MID, AHEAD_END)

    @pl.loop(0, AHEAD_END)
    def _(k):
        pl.when(k < ahead)(lambda: send_own(k))

    @pl.when(mid)
    def _():
        arrive(jnp.int32(0), jnp.int32(2), False)

    for c in old_copies:
        c.start()
    for c in old_copies:
        c.wait()

    @pl.when(jnp.logical_not(mid))
    def _():
        for k in range(AHEAD_MID):
            arrive(jnp.int32(k), jnp.int32(0), False)

    last_mid, last_end = p.turns[True], p.turns[False] - 2
    assert last_end >= 3 * p.count and last_end not in p.steps[False].values()

    def one_turn(t):
        d, turn_no = lax.div(t, 3), lax.rem(t, 3)
        pl.when((turn_no == 0) & (d >= 1) & (d < p.count))(lambda: own_first_left(d - 1))
        early = jnp.where(mid, jnp.where(turn_no == 0, 1, 0), jnp.where(turn_no == 2, AHEAD_MID, 0))
        e = lax.rem(turn_no + jnp.where(mid, 2, 1), 3)
        k = d + early
        pl.when(k < p.count)(lambda: arrive(k, e, True))

        @pl.when(turn_no == 2)
        def _():
            pl.when(d + ahead < p.count)(lambda: send_own(d + ahead))

            @pl.when((d == p.count - 1) & mid)
            def _():
                for c in to_end():
                    c.start()

            k = d - jnp.where(mid, LATE_MID, LATE_END)

            @pl.when((k >= 0) & (k < p.count) & p.is_dy(k) & (mid | jnp.logical_not(p.is_attn(k))))
            def _():
                spread_done(k, True)
                partner(k, 1).start()

        pl.when(t == jnp.where(mid, last_mid, last_end))(lambda: pl.loop(0, p.count)(sends_left))
        work(t)

    @pl.loop(0, last_mid + 1)
    def _(t):
        pl.when(mid | (t < p.turns[False]))(lambda: one_turn(t))

    own_first_left(jnp.int32(p.count - 1))
    for mat in (GATE, UP):
        for c in first_copies(mat) + second_copies(mat):
            c.wait_send()

    @pl.when(mid)
    def _():
        for mat in (ATTN, DOWN):
            for c in first_copies(mat) + second_copies(mat):
                c.wait_send()
        for c in to_end() + to_end_down():
            c.wait_send()

    @pl.when(jnp.logical_not(mid))
    def _():
        for c in to_end() + to_end_down():
            c.wait_recv()


def store_kernel(plan, o_attn, o_gate, o_up, grad, *refs):
    p = plan
    stats, al_down, be_down, w_old, (w_attn, w_gate, w_up, w_down), outs = (
        refs[:8], refs[8], refs[9], refs[10], refs[11:15], refs[15:23])
    bounce, w_buf, a_col, in_sem, out_sem, s_sem, wi_sem, wo_sem = refs[23:]
    depth, wide = bounce.shape[0], w_buf.shape[0]

    def cut(ref, i):
        return ref.at[:, i * p.nc:(i + 1) * p.nc]

    def rows(ref, i):
        return ref.at[i * p.mc:(i + 1) * p.mc, :]

    through = [(cut(o_gate, i), cut(w_gate, i)) for i in range(p.ng)]
    if not UP_KEPT:
        through += [(cut(o_up, i), cut(w_up, i)) for i in range(p.ng)]
    loads = [pltpu.make_async_copy(a, bounce.at[i % depth], in_sem.at[i]) for i, (a, _) in enumerate(through)]
    puts = [pltpu.make_async_copy(bounce.at[i % depth], b, out_sem.at[i]) for i, (_, b) in enumerate(through)]
    w_in = [pltpu.make_async_copy(rows(w_old, i), w_buf.at[i % wide], wi_sem.at[i]) for i in range(p.nh)]
    w_out = [pltpu.make_async_copy(w_buf.at[i % wide], rows(w_down, i), wo_sem.at[i]) for i in range(p.nh)]
    for i in range(wide // 2):
        w_in[i].start()
    for c in loads[:depth]:
        c.start()
    copies = [pltpu.make_async_copy(a, b, s_sem.at[i]) for i, (a, b) in enumerate(zip(stats, outs))]
    copies.append(pltpu.make_async_copy(o_attn, w_attn, s_sem.at[8]))
    if UP_KEPT:
        copies += [pltpu.make_async_copy(o_up.at[i], cut(w_up, i), s_sem.at[9 + i]) for i in range(p.ng)]
    for c in copies:
        c.start()
    step_r = min(64, p.mc)
    per = -(-len(through) // p.nh)
    done = 0
    for i in range(p.nh):
        a_col[...] = jnp.broadcast_to(al_down[:, i * p.mc:(i + 1) * p.mc], (LANES, p.mc)).T
        w_in[i].wait()

        @pl.loop(0, p.mc // step_r)
        def _(n):
            at = pl.ds(pl.multiple_of(n * step_r, step_r), step_r)
            a_block = a_col[at, :]
            for c in range(0, p.nc, LANES):
                cols = slice(c, c + LANES)
                w_buf[i % wide, at, cols] = w_buf[i % wide, at, cols] - grad[i, at, cols] * a_block * be_down[:, cols]

        w_out[i].start()
        again = i + wide // 2
        if again < p.nh:
            if again >= wide:
                w_out[again - wide].wait()
            w_in[again].start()
        for j in range(done, min(len(through), done + per)):
            loads[j].wait()
            puts[j].start()
            again = j + depth // 2
            if depth <= again < len(through):
                puts[again - depth].wait()
                loads[again].start()
        done += per
    for i in range(max(0, p.nh - wide), p.nh):
        if i + wide >= p.nh:
            w_out[i].wait()
    for i in range(max(0, len(through) - depth), len(through)):
        puts[i].wait()
    for c in copies:
        c.wait()


def solution(mesh):
    act_spec = P('dp', 'row')
    grad_spec = P('dp', 'col')
    w_spec = P('row', 'col')
    row_spec = P('row')
    col_spec = P('col')
    in_specs = (act_spec, grad_spec, act_spec, grad_spec, grad_spec, act_spec, grad_spec,
                w_spec, w_spec, w_spec, w_spec,
                row_spec, col_spec, row_spec, col_spec, row_spec, col_spec, row_spec, col_spec, P())
    out_specs = (w_spec, row_spec, col_spec) * 4

    def per_device(x_attn, dy_attn, x_mlp, dy_gate, dy_up, h_mlp, dy_out, w_attn, w_gate, w_up, w_down,
                   r_attn, c_attn, r_gate, c_gate, r_up, c_up, r_down, c_down, hyper_params):
        p = Plan(x_mlp, dy_gate, h_mlp, dy_out, mesh)
        stats = [v.reshape(1, -1) for v in (r_attn, c_attn, r_gate, c_gate, r_up, c_up, r_down, c_down)]
        any_spec = pl.BlockSpec(memory_space=pl.ANY)
        vmem_spec = pl.BlockSpec(memory_space=pltpu.VMEM)
        up_spec = vmem_spec if UP_KEPT else any_spec
        row_shapes = []
        for mat in MATS:
            row_shapes += [jax.ShapeDtypeStruct((1, p.rows[mat]), F32), jax.ShapeDtypeStruct((1, p.cols[mat]), F32)]
        w_shapes = [jax.ShapeDtypeStruct((p.rows[mat], p.cols[mat]), F32) for mat in MATS]
        o_shapes = [pltpu.VMEM((p.mc, p.nc), F32), w_shapes[GATE],
                    pltpu.VMEM((p.ng, p.mc, p.nc), F32) if UP_KEPT else w_shapes[UP],
                    pltpu.VMEM((p.pieces, p.mc, p.nc), F32)]
        bufs = [jax.ShapeDtypeStruct((p.n_dy, p.dp - 1, p.tok, p.nc), BF16),
                jax.ShapeDtypeStruct((p.n_x, p.dp - 1, p.tok, p.mc), BF16)]
        rest = jax.ShapeDtypeStruct((p.mc - p.first_rows, p.nc), F32)
        dma = pltpu.SemaphoreType.DMA
        lines = p.count + PARTS - 1
        scratch = [
            pltpu.VMEM((p.dp, p.mc, p.tok), BF16),
            pltpu.VMEM((p.dp, p.tok, p.mc), BF16),
            pltpu.VMEM((p.dp, p.tok, p.nc), BF16),
            pltpu.VMEM((3, p.mc, p.nc), F32),
            pltpu.VMEM((p.mc, LANES), F32),
            pltpu.VMEM((p.pieces, 1, p.mc), F32),
            pltpu.VMEM((p.pieces, 1, p.nc), F32),
            pltpu.VMEM((p.nh, p.mc, LANES), F32),
            pltpu.VMEM((1, p.rows[DOWN]), F32),
            pltpu.VMEM((4, 8, LANES), F32),
        ]
        scratch += [pltpu.VMEM((1, p.cols[mat]), F32) for mat in MATS]
        scratch += [pltpu.VMEM(v.shape, F32) for v in row_shapes]
        scratch += [pltpu.VMEM((2, 1, p.rows[mat]), F32) for mat in MATS]
        scratch += [pltpu.VMEM((4, 1, p.cols[mat]), F32) for mat in MATS]
        scratch += [
            pltpu.VMEM((4, 8, 3, 8, LANES), F32),
            dma((lines, 5)), dma((lines, p.dp - 1)),
            dma((lines, p.dp - 1)), dma((lines, p.dp - 1)),
            dma((p.n_dy, 2)), dma((p.n_dy, 2)),
            dma((4, 4)), dma((4, 4)), dma((4, 8)), dma((4, 8)),
            dma((7,)), dma((7,)),
            dma((p.dp,)), dma((3,)), dma((3,)), dma((8,)),
        ]
        out = pl.pallas_call(
            functools.partial(gather_kernel, p),
            out_shape=o_shapes + [pltpu.VMEM(v.shape, F32) for v in row_shapes + row_shapes[-2:]] + [rest] + bufs,
            in_specs=[any_spec] * 19 + [pl.BlockSpec(memory_space=pltpu.SMEM)],
            out_specs=[vmem_spec, any_spec, up_spec, vmem_spec] + [vmem_spec] * 10 + [any_spec] * 3,
            scratch_shapes=scratch,
            compiler_params=pltpu.CompilerParams(collective_id=0, has_side_effects=True, vmem_limit_bytes=VMEM_LIMIT),
        )(x_attn, dy_attn, x_mlp, dy_gate, dy_up, h_mlp, dy_out, w_attn, w_gate, w_up, w_down, *stats, hyper_params)
        res = pl.pallas_call(
            functools.partial(store_kernel, p),
            out_shape=w_shapes + row_shapes,
            in_specs=[vmem_spec, any_spec, up_spec, vmem_spec] + [vmem_spec] * 10 + [any_spec],
            out_specs=[any_spec] * 12,
            scratch_shapes=[pltpu.VMEM((DEPTH, p.mc, p.nc), F32), pltpu.VMEM((WIDE, p.mc, p.nc), F32),
                            pltpu.VMEM((p.mc, LANES), F32), dma((2 * p.ng,)), dma((2 * p.ng,)), dma((9 + p.ng,)),
                            dma((p.nh,)), dma((p.nh,))],
            compiler_params=pltpu.CompilerParams(vmem_limit_bytes=STORE_LIMIT),
            cost_estimate=pl.CostEstimate(flops=60_000_000_000, bytes_accessed=90_000_000, transcendentals=0),
        )(*[pltpu.with_memory_space_constraint(v, pltpu.VMEM) if i not in HBM_KEPT else v for i, v in enumerate(out[:14])],
          w_down)
        z = lax.axis_index('dp')
        got = lax.ppermute(out[14], 'dp', [(1, 0), (2, 3)])
        rows = jnp.where((z == 1) | (z == 2), out[14], got)
        res = [lax.dynamic_update_slice(res[0], rows, (p.first_rows, 0))] + list(res[1:])
        result = []
        for mat in MATS:
            result += [res[mat], res[4 + 2 * mat].reshape(-1), res[5 + 2 * mat].reshape(-1)]
        return tuple(result)

    return jax.shard_map(per_device, mesh=mesh, in_specs=in_specs, out_specs=out_specs, check_vma=False)
```

```python
import functools
import jax
import jax.numpy as jnp
from jax import lax
from jax.experimental import pallas as pl
from jax.experimental.pallas import tpu as pltpu
from jax.sharding import PartitionSpec as P

EPS_ONE = 1e-30
EPS_TWO = 1e-3
MESH = pl.DeviceIdType.MESH
LANES = 128
F32 = jnp.float32
BF16 = jnp.bfloat16
ATTN, GATE, UP, DOWN = range(4)
MATS = (ATTN, GATE, UP, DOWN)
FIRST = {'gate': ('x_mlp', 0), 'attn': ('x_attn', 0), 'up': ('x_mlp', 0), 'h': ('out', 0)}
AHEAD_MID, AHEAD_END = 2, 6
PARTS = 4
LATE_MID, LATE_END = 3, 2
VMEM_LIMIT = 29 * 1024 * 1024
STORE_LIMIT = 29 * 1024 * 1024
UP_KEPT = True
HBM_KEPT = (1,) if UP_KEPT else (1, 2)
DEPTH, WIDE = 4, 4


def look(k, table):
    out = jnp.int32(0)
    for i, v in enumerate(table):
        if v:
            out = jnp.where(k == i, v, out)
    return out


class Plan:
    def __init__(self, x_mlp, dy_gate, h_mlp, dy_out, mesh):
        self.dp, self.col, self.row = mesh.shape['dp'], mesh.shape['col'], mesh.shape['row']
        assert (self.dp, self.col, self.row) == (4, 2, 4)
        self.tok = x_mlp.shape[0]
        self.mc = x_mlp.shape[1]
        self.nc = dy_out.shape[1]
        self.ng = dy_gate.shape[1] // self.nc
        self.nh = h_mlp.shape[1] // self.mc
        self.tq = self.tok // self.row
        self.th = self.tok // self.col
        g = [('gate', i) for i in range(self.ng)]
        u = [('up', i) for i in range(self.ng)]
        h = [('h', i) for i in range(self.nh)]
        one, two = max(1, self.ng // 4), max(2, 3 * self.ng // 4)
        self.order = ([('x_mlp', 0)] + g[:one] + h[:1] + g[one:two] + h[1:2] + g[two:] + [('x_attn', 0), ('attn', 0)]
                      + u + [('out', 0)] + h[2:])
        self.count = len(self.order)
        self.place = {v: k for k, v in enumerate(self.order)}
        self.first_rows = self.mc * 5 // 16
        self.n_dy = 2 * self.ng + 2
        self.n_x = self.nh + 2
        self.pieces = max(self.ng, self.nh)
        self.rows = {ATTN: self.mc, GATE: self.mc, UP: self.mc, DOWN: self.mc * self.nh}
        self.cols = {ATTN: self.nc, GATE: self.nc * self.ng, UP: self.nc * self.ng, DOWN: self.nc}
        self.parts = {ATTN: 1, GATE: self.ng, UP: self.ng, DOWN: self.nh}
        base = {'gate': 0, 'up': self.ng, 'out': 2 * self.ng, 'attn': 2 * self.ng + 1, 'x_mlp': 0, 'x_attn': 1, 'h': 2}
        self.dy_table = [1 if n in ('gate', 'up', 'out', 'attn') else 0 for n, _ in self.order]
        self.at_table = [base[n] + i for n, i in self.order]
        self.attn_table = [1 if n in ('x_attn', 'attn') else 0 for n, _ in self.order]
        self.steps = {m: self.schedule(m) for m in (True, False)}
        self.turns = {m: max(max(v.values()) + 1, 3 * self.count) for m, v in self.steps.items()}

    def schedule(self, mid):
        late = LATE_MID if mid else LATE_END
        tasks = []
        for name, mat in (('gate', GATE), ('attn', ATTN), ('up', UP), ('h', DOWN)):
            if name == 'attn' and not mid:
                continue
            for i in range(self.parts[mat]):
                k = self.place[name, i]
                need = [3 * (k + late + 1)] if name != 'h' else [3 * (k + late) if mid else 3 * k + 5]
                if i == 0:
                    need.append(3 * (self.place[FIRST[name]] + late + (name == 'h')))
                tasks.append(((name, i), max(need)))
            stages = {ATTN: (1, 2), DOWN: (1, 2)}.get(mat, (1, 2, 3))
            if mid or mat != DOWN:
                tasks += [(('finish', mat, stage), 0) for stage in stages]
        out, t = {}, 0
        for task, first in tasks:
            t = max(t, first)
            out[task] = t
            t += 1
        return out

    def is_dy(self, k):
        return look(k, self.dy_table) == 1

    def is_attn(self, k):
        return look(k, self.attn_table) == 1

    def at(self, k):
        return look(k, self.at_table)


def gather_kernel(plan, x_attn, dy_attn, x_mlp, dy_gate, dy_up, h_mlp, dy_out, w_attn, w_gate, w_up, w_down,
                  r_attn, c_attn, r_gate, c_gate, r_up, c_up, r_down, c_down, hyper,
                  o_attn, o_gate, o_up, grad, nr_attn, nc_attn, nr_gate, nc_gate, nr_up, nc_up, nr_down, nc_down,
                  al_down, be_down, o_rest, buf_d, buf_x,
                  lhs, tile_x, tile_d, w_buf, r_lanes, r_row, c_sum, a_cols, a_rows, w_sq,
                  b_attn, b_gate, b_up, b_down, *more):
    p = plan
    old_refs = more[:8]
    (rs_attn, rs_gate, rs_up, rs_down, cs_attn, cs_gate, cs_up, cs_down, st_all,
     z_send, z_recv, f_send, f_recv, c_send, c_recv, r1_send, r1_recv, r2_send, r2_recv,
     e_send, e_recv, l_sem, wi_sem, wo_sem, o_sem) = more[8:]
    z, y, r = lax.axis_index('dp'), lax.axis_index('col'), lax.axis_index('row')
    low = z < 2
    mid = (z == 1) | (z == 2)
    end_z = jnp.where(low, 0, 3)
    mate_z = 3 - z
    w_refs = {ATTN: w_attn, GATE: w_gate, UP: w_up, DOWN: w_down}
    old_in = (r_attn, c_attn, r_gate, c_gate, r_up, c_up, r_down, c_down)
    old = {mat: (old_refs[2 * mat], old_refs[2 * mat + 1]) for mat in MATS}
    old_copies = [pltpu.make_async_copy(a, b, o_sem.at[i]) for i, (a, b) in enumerate(zip(old_in, old_refs))]
    new = {ATTN: (nr_attn, nc_attn), GATE: (nr_gate, nc_gate), UP: (nr_up, nc_up), DOWN: (nr_down, nc_down)}
    b_rows = {ATTN: b_attn, GATE: b_gate, UP: b_up, DOWN: b_down}
    rs = {ATTN: rs_attn, GATE: rs_gate, UP: rs_up, DOWN: rs_down}
    cs = {ATTN: cs_attn, GATE: cs_gate, UP: cs_up, DOWN: cs_down}

    def flip_row(v):
        bit0, bit1 = lax.rem(r, 2), lax.div(r, 2)
        if v & 1:
            bit0 = 1 - bit0
        if v & 2:
            bit1 = 1 - bit1
        return bit1 * 2 + bit0

    peers = [(f, v) for f in range(2) for v in range(4) if f or v]
    barrier = pltpu.get_barrier_semaphore()
    for f, v in peers:
        pl.semaphore_signal(barrier, inc=1, device_id=(z, 1 - y if f else y, flip_row(v)), device_id_type=MESH)

    @pl.when(mid)
    def _():
        pl.semaphore_signal(barrier, inc=1, device_id=(end_z, y, r), device_id_type=MESH)
        pl.semaphore_signal(barrier, inc=1, device_id=(mate_z, y, r), device_id_type=MESH)
        pl.semaphore_wait(barrier, len(peers) + 2)

    @pl.when(jnp.logical_not(mid))
    def _():
        pl.semaphore_signal(barrier, inc=1, device_id=(jnp.where(low, 1, 2), y, r), device_id_type=MESH)
        pl.semaphore_wait(barrier, len(peers) + 1)

    my_q = pl.ds(pl.multiple_of(r * p.tq, p.tq), p.tq)
    x_q = pl.ds(pl.multiple_of(flip_row(2) * p.tq, p.tq), p.tq)
    my_h = pl.ds(pl.multiple_of(y * p.th, p.th), p.th)

    def rows_of(dy, part):
        if dy:
            return my_q
        if part is None:
            return my_h
        size = p.th // PARTS
        return pl.ds(pl.multiple_of(y * p.th + part * size, size), size)

    def line_of(k, part):
        return k if part is None else k + part

    def slot(k, s, dy, part):
        return (buf_d if dy else buf_x).at[p.at(k), s, rows_of(dy, part), :]

    def pass_on(k, dy, part, src, to_z, to_slot, sem):
        line = line_of(k, part)
        return pltpu.make_async_remote_copy(
            src_ref=src, dst_ref=slot(k, to_slot, dy, part), send_sem=z_send.at[line, sem],
            recv_sem=z_recv.at[line, to_slot], device_id=(to_z, y, r), device_id_type=MESH)

    def spread(k, s, dy, part):
        to = (z, y, flip_row(2)) if dy else (z, 1 - y, r)
        line = line_of(k, part)
        return pltpu.make_async_remote_copy(
            src_ref=slot(k, s, dy, part), dst_ref=slot(k, s, dy, part), send_sem=f_send.at[line, s],
            recv_sem=f_recv.at[line, s], device_id=to, device_id_type=MESH)

    def partner(k, which):
        part = buf_d.at[p.at(k), :, x_q if which else my_q, :]
        return pltpu.make_async_remote_copy(
            src_ref=part, dst_ref=part, send_sem=c_send.at[p.at(k), which], recv_sem=c_recv.at[p.at(k), which],
            device_id=(z, y, flip_row(1)), device_id_type=MESH)

    def in_parts(k, go):
        pl.when(k != p.count - 1)(lambda: go(None))

        @pl.when(k == p.count - 1)
        def _():
            pl.loop(0, PARTS)(go)

    def typed(k, go):
        used = mid | jnp.logical_not(p.is_attn(k))
        pl.when(p.is_dy(k) & used)(lambda: go(True, None))
        pl.when(jnp.logical_not(p.is_dy(k)) & used)(lambda: in_parts(k, lambda part: go(False, part)))

    def cut(ref, at, size):
        return ref.at[:, pl.ds(pl.multiple_of(at * size, size), size)]

    def down_rows(ref, i):
        return ref.at[pl.ds(pl.multiple_of(i * p.mc, p.mc), p.mc), :]

    def own_to(k, dy, part, src):
        @pl.when(jnp.logical_not(mid))
        def _():
            pass_on(k, dy, part, src, jnp.where(low, 1, 2), jnp.where(low, 2, 0), 0).start()

        @pl.when(mid)
        def _():
            @pl.when(jnp.logical_not(p.is_attn(k)))
            def _():
                pass_on(k, dy, part, src, end_z, jnp.where(low, 0, 2), 0).start()
            pass_on(k, dy, part, src, mate_z, jnp.where(low, 2, 0), 1).start()

    def send_own(k):
        def go(ref, at, size, dy):
            def send(part):
                own_to(k, dy, part, ref.at[rows_of(dy, part), pl.ds(pl.multiple_of(at * size, size), size)])

            if ref is h_mlp:
                in_parts(k, send)
            else:
                send(None)

        for name, ref, dy in (('x_mlp', x_mlp, False), ('gate', dy_gate, True), ('x_attn', x_attn, False),
                              ('attn', dy_attn, True), ('up', dy_up, True), ('out', dy_out, True), ('h', h_mlp, False)):
            at = look(k, [i + 1 if n == name else 0 for n, i in p.order])
            size = p.nc if dy else p.mc
            pl.when(at > 0)(functools.partial(go, ref, at - 1, size, dy))

    def own_first_left(k):
        @pl.when(jnp.logical_not(mid & p.is_attn(k)))
        def _():
            def go(dy, part):
                pass_on(k, dy, part, slot(k, 0, dy, part), z, 0, 0).wait_send()

            pl.when(p.is_dy(k))(lambda: go(True, None))
            pl.when(jnp.logical_not(p.is_dy(k)))(lambda: in_parts(k, lambda part: go(False, part)))

    def arrive(k, e, whole):
        s = jnp.where(low, e, 2 - e)

        def go(dy, part):
            here = slot(k, s, dy, part)
            pass_on(k, dy, part, here, z, s, 0).wait_recv()

            @pl.when(mid & (e == 2))
            def _():
                pass_on(k, dy, part, here, mate_z, 1, 4).start()

            @pl.when(mid & (e < 2) & jnp.logical_not(p.is_attn(k)))
            def _():
                pass_on(k, dy, part, here, end_z, jnp.where(low, s + 1, s - 1), 2 + e).start()

            spread(k, s, dy, part).start()
            if dy and whole:
                pl.when(e == jnp.where(mid, 1, 2))(lambda: partner(k, 0).start())

        typed(k, go)

    def spread_done(k, dy):
        for s in range(p.dp - 1):
            spread(k, s, dy, None).wait_recv()

    def load(src, at, size, buf, index, dst):
        copies = [pltpu.make_async_copy(cut(src, at, size), dst.at[z], l_sem.at[0])]
        for d in range(1, p.dp):
            copies.append(pltpu.make_async_copy(buf.at[index, d - 1], dst.at[lax.rem(z + d, p.dp)], l_sem.at[d]))
        for c in copies:
            c.start()
        for c in copies:
            c.wait()

    step_t = min(256, p.tok)

    def turn(q):
        @pl.loop(0, p.tok // step_t)
        def _(t):
            at = pl.multiple_of(t * step_t, step_t)
            lhs[q, :, pl.ds(at, step_t)] = tile_x[q, pl.ds(at, step_t), :].T

    step_n = min(512, p.nc)
    step_r = min(64, p.mc)

    def lane_sum(v):
        out = v[:, 0:LANES]
        for i in range(1, v.shape[1] // LANES):
            out = out + v[:, i * LANES:(i + 1) * LANES]
        return out

    def product(at, count):
        r_lanes[...] = jnp.zeros_like(r_lanes)

        @pl.loop(0, p.nc // step_n)
        def _(n):
            cols = pl.ds(pl.multiple_of(n * step_n, step_n), step_n)
            grad[at, :, cols] = jnp.dot(lhs[0], tile_d[0, :, cols], preferred_element_type=F32)

            @pl.loop(1, p.dp)
            def _(q):
                grad[at, :, cols] += jnp.dot(lhs[q], tile_d[q, :, cols], preferred_element_type=F32)

            def body(i, acc):
                rows = pl.ds(pl.multiple_of(i * step_r, step_r), step_r)
                block = grad[at, rows, cols]
                sq = block * block + EPS_ONE
                r_lanes[rows, :] += lane_sum(sq)
                return acc + jnp.sum(sq, axis=0, keepdims=True)

            @pl.when(count)
            def _():
                c_sum[at, :, cols] = lax.fori_loop(0, p.mc // step_r, body, jnp.zeros((1, step_n), F32))

    def fold(v):
        v = jnp.reshape(v, (v.shape[0] // 8, 8, LANES))
        while v.shape[0] > 1:
            v = v[:v.shape[0] // 2] + v[v.shape[0] // 2:]
        return v[0]

    def to_row(block):
        return jnp.sum(block.T, axis=0, keepdims=True)

    def get_w(mat, i):
        src = down_rows(w_refs[mat], i) if mat == DOWN else cut(w_refs[mat], i, p.nc)
        return pltpu.make_async_copy(src, w_buf.at[lax.rem(i, 3)], wi_sem.at[lax.rem(i, 3)])

    def put_w(mat, i):
        dst = cut(o_gate if mat == GATE else o_up, i, p.nc)
        return pltpu.make_async_copy(w_buf.at[lax.rem(i, 3)], dst, wo_sem.at[lax.rem(i, 3)])

    def chunk(mat, i):
        count = mid if mat == DOWN else jnp.bool_(True)
        pl.when(count)(lambda: get_w(mat, i).start())
        product(i, count)

        @pl.when(count)
        def _():
            row = to_row(r_lanes[...])
            if mat == DOWN:
                r_row[i] = row
            else:
                r_row[0] = jnp.where(i == 0, row, r_row[0] + row)
            get_w(mat, i).wait()

            def body(n, acc):
                rows = pl.ds(pl.multiple_of(n * step_r, step_r), step_r)
                block = lane_sum(w_buf[lax.rem(i, 3), rows, :] * w_buf[lax.rem(i, 3), rows, :])
                return acc + fold(block)

            w_sq[mat] += lax.fori_loop(0, p.mc // step_r, body, jnp.zeros((8, LANES), F32))

    def first_copies(mat):
        copies = [pltpu.make_async_remote_copy(
            src_ref=rs[mat].at[y], dst_ref=rs[mat].at[y], send_sem=r1_send.at[mat, 0], recv_sem=r1_recv.at[mat, 0],
            device_id=(z, 1 - y, r), device_id_type=MESH)]
        for v in range(1, 4):
            copies.append(pltpu.make_async_remote_copy(
                src_ref=cs[mat].at[r], dst_ref=cs[mat].at[r], send_sem=r1_send.at[mat, v],
                recv_sem=r1_recv.at[mat, v], device_id=(z, y, flip_row(v)), device_id_type=MESH))
        return copies

    def second_copies(mat):
        me = y * 4 + r
        return [pltpu.make_async_remote_copy(
            src_ref=st_all.at[mat, me], dst_ref=st_all.at[mat, me], send_sem=r2_send.at[mat, f * 4 + v],
            recv_sem=r2_recv.at[mat, f * 4 + v], device_id=(z, 1 - y if f else y, flip_row(v)), device_id_type=MESH)
            for f, v in peers]

    def scale_rows(mat):
        return p.rows[mat] * p.row, p.cols[mat] * p.col

    blocks = p.mc // step_r

    def factors(mat, i, n):
        rows = pl.ds(pl.multiple_of(n * step_r, step_r), step_r)
        if mat == DOWN:
            return rows, a_cols[i, rows, :], b_rows[mat].at[:, :]
        return rows, a_cols[0, rows, :], b_rows[mat].at[:, pl.ds(pl.multiple_of(i * p.nc, p.nc), p.nc)]

    def finish_first(mat):
        parts = p.parts[mat]
        if mat != DOWN:
            for i in range(min(2, parts)):
                get_w(mat, jnp.int32(i)).start()
        if mat == DOWN:
            block = c_sum[0]
            for i in range(parts):
                rs[mat][y, :, i * p.mc:(i + 1) * p.mc] = r_row[i]
                if i:
                    block = block + c_sum[i]
            cs[mat][r] = block
        else:
            rs[mat][y] = r_row[0]
            for i in range(parts):
                cs[mat][r, :, i * p.nc:(i + 1) * p.nc] = c_sum[i]
        for c in first_copies(mat):
            c.start()

    def finish_second(mat):
        beta_two = hyper[0]
        m_total, n_total = scale_rows(mat)
        parts = p.parts[mat]
        for c in first_copies(mat):
            c.wait_recv()
        r_new = beta_two * old[mat][0][...] + (1.0 - beta_two) * ((rs[mat][0] + rs[mat][1]) / n_total)
        c_all = ((cs[mat][0] + cs[mat][1]) + cs[mat][2]) + cs[mat][3]
        c_new = beta_two * old[mat][1][...] + (1.0 - beta_two) * (c_all / m_total)
        new[mat][0][...] = r_new
        new[mat][1][...] = c_new
        t_own = jnp.sum(r_new, axis=1, keepdims=True)
        a_row = jnp.sqrt(t_own) / jnp.sqrt(r_new)
        b_rows[mat][...] = 1.0 / jnp.sqrt(c_new)
        if mat == DOWN:
            a_rows[...] = a_row
        for i in range(parts if mat == DOWN else 1):
            a_cols[i] = jnp.broadcast_to(a_row[:, i * p.mc:(i + 1) * p.mc], (LANES, p.mc)).T

        def add_up(j, acc):
            i, n = lax.div(j, blocks), lax.rem(j, blocks)
            rows, a_block, b_ref = factors(mat, i, n)
            for c in range(0, p.nc, LANES):
                upd = grad[i, rows, c:c + LANES] * a_block * b_ref[:, c:c + LANES]
                acc = acc + fold(upd * upd)
            return acc

        u_part = lax.fori_loop(0, parts * blocks, add_up, jnp.zeros((8, LANES), F32))

        def spot(v):
            return jnp.broadcast_to(jnp.sum(jnp.sum(v, axis=1, keepdims=True), axis=0, keepdims=True), (8, LANES))

        me = y * 4 + r
        st_all[mat, me, 0] = spot(u_part)
        st_all[mat, me, 1] = spot(w_sq[mat])
        st_all[mat, me, 2] = jnp.broadcast_to(t_own, (8, LANES))
        for c in second_copies(mat):
            c.start()

    def finish_third(mat):
        rho_step, clip_thr = hyper[1], hyper[2]
        m_total, n_total = scale_rows(mat)
        me = y * 4 + r
        for c in second_copies(mat):
            c.wait_recv()
        t_all = st_all[mat, 0, 2]
        for i in range(1, p.row):
            t_all = t_all + st_all[mat, i, 2]
        u_all = st_all[mat, 0, 0] * (t_all / st_all[mat, 0, 2])
        w_all = st_all[mat, 0, 1]
        for i in range(1, p.row * p.col):
            u_all = u_all + st_all[mat, i, 0] * (t_all / st_all[mat, i, 2])
            w_all = w_all + st_all[mat, i, 1]
        upd_rms = jnp.sqrt(u_all / (m_total * n_total))
        w_rms = jnp.sqrt(w_all / (m_total * n_total))
        scale = rho_step * jnp.maximum(EPS_TWO, w_rms) / jnp.maximum(1.0, upd_rms / clip_thr)
        scale = scale * jnp.sqrt(t_all / st_all[mat, me, 2])
        b_rows[mat][...] = b_rows[mat][...] * scale[0:1, 0:1]

    def renew(mat, low_i, high_i):
        parts = p.parts[mat]

        @pl.loop(low_i, high_i)
        def _(i):
            at = lax.rem(i, 3)
            get_w(mat, i).wait()

            @pl.loop(0, blocks)
            def _(n):
                rows, a_block, b_ref = factors(mat, i, n)
                for c in range(0, p.nc, LANES):
                    cols = slice(c, c + LANES)
                    fresh = w_buf[at, rows, cols] - grad[i, rows, cols] * a_block * b_ref[:, cols]
                    if mat == ATTN:
                        o_attn[rows, cols] = fresh
                    elif mat == UP and UP_KEPT:
                        o_up[i, rows, cols] = fresh
                    else:
                        w_buf[at, rows, cols] = fresh

            if mat == ATTN:
                put_rest().start()
                put_rest().wait()
            if mat == GATE or (mat == UP and not UP_KEPT):
                put_w(mat, i).start()
                pl.when(i >= 1)(lambda: put_w(mat, i - 1).wait())
            pl.when(i + 2 < parts)(lambda: get_w(mat, i + 2).start())

        if (mat == GATE or (mat == UP and not UP_KEPT)) and high_i == parts:
            put_w(mat, jnp.int32(parts - 1)).wait()

    def put_rest():
        return pltpu.make_async_copy(o_attn.at[pl.ds(p.first_rows, p.mc - p.first_rows), :], o_rest, wo_sem.at[0])

    def finish(mat, stage):
        parts = p.parts[mat]
        half = parts // 2 if parts > 1 else parts
        if stage == 1:
            finish_second(mat)
        elif stage == 2:
            finish_third(mat)
            if mat == DOWN:
                al_down[...] = a_rows[...]
                be_down[...] = b_rows[mat][...]
                for c in to_end_down():
                    c.start()
            else:
                renew(mat, 0, half)
        else:
            renew(mat, half, parts)

    def take_x(src, at, k, waits=True):
        copies = [(pltpu.make_async_copy(cut(src, at, p.mc), tile_x.at[z], l_sem.at[0]), z)]
        copies[0][0].start()
        for e in range(p.dp - 1):
            s = jnp.where(low, e, 2 - e)
            if src is h_mlp:
                in_parts(k, lambda part: spread(k, s, False, part).wait_recv())
            elif waits:
                spread(k, s, False, None).wait_recv()
            q = lax.rem(z + s + 1, p.dp)
            copies.append((pltpu.make_async_copy(buf_x.at[p.at(k), s], tile_x.at[q], l_sem.at[e + 1]), q))
            copies[-1][0].start()
            copies[-2][0].wait()
            turn(copies[-2][1])
        copies[-1][0].wait()
        turn(copies[-1][1])

    def got(name, i):
        k = look(i, [p.place[name, j] for j in range(sum(1 for n, _ in p.order if n == name))])
        partner(k, 0).wait_recv()
        partner(k, 1).wait_recv()
        return k

    def use_gate(i):
        pl.when(i == 0)(lambda: take_x(x_mlp, 0, jnp.int32(p.place['x_mlp', 0])))
        k = got('gate', i)
        load(dy_gate, i, p.nc, buf_d, p.at(k), tile_d)
        chunk(GATE, i)
        pl.when(i == p.parts[GATE] - 1)(lambda: finish_first(GATE))

    def use_attn(i):
        take_x(x_attn, 0, jnp.int32(p.place['x_attn', 0]))
        k = got('attn', i)
        load(dy_attn, 0, p.nc, buf_d, p.at(k), tile_d)
        chunk(ATTN, i)
        finish_first(ATTN)

    def use_up(i):
        pl.when(i == 0)(lambda: take_x(x_mlp, 0, jnp.int32(p.place['x_mlp', 0]), False))
        k = got('up', i)
        load(dy_up, i, p.nc, buf_d, p.at(k), tile_d)
        chunk(UP, i)
        pl.when(i == p.parts[UP] - 1)(lambda: finish_first(UP))

    def use_out():
        k = got('out', jnp.int32(0))
        load(dy_out, 0, p.nc, buf_d, p.at(k), tile_d)

    def use_h(i):
        pl.when(i == 0)(use_out)
        take_x(h_mlp, i, look(i, [p.place['h', j] for j in range(p.nh)]))
        chunk(DOWN, i)
        pl.when((i == p.parts[DOWN] - 1) & mid)(lambda: finish_first(DOWN))

    def work(t):
        for name, use in (('gate', use_gate), ('attn', use_attn), ('up', use_up), ('h', use_h)):
            at = jnp.int32(0)
            for i in range(sum(1 for n, _ in p.order if n == name)):
                when_mid = p.steps[True].get((name, i), -1)
                when_end = p.steps[False].get((name, i), -1)
                at = jnp.where(t == jnp.where(mid, when_mid, when_end), i + 1, at)
            pl.when(at > 0)(functools.partial(use, at - 1))
        for mat in MATS:
            for stage in (1, 2, 3):
                when_mid = p.steps[True].get(('finish', mat, stage), -1)
                when_end = p.steps[False].get(('finish', mat, stage), -1)
                if when_mid >= 0:
                    pl.when(t == jnp.where(mid, when_mid, when_end))(functools.partial(finish, mat, stage))

    def sent_to_end(refs, first):
        return [pltpu.make_async_remote_copy(
            src_ref=ref, dst_ref=ref, send_sem=e_send.at[first + i], recv_sem=e_recv.at[first + i],
            device_id=(end_z, y, r), device_id_type=MESH) for i, ref in enumerate(refs)]

    def to_end():
        return sent_to_end((nr_attn, nc_attn, o_attn.at[pl.ds(0, p.first_rows), :]), 0)

    def to_end_down():
        return sent_to_end((nr_down, nc_down, al_down, be_down), 3)

    def sends_left(k):
        def go(dy, part):
            some = slot(k, 0, dy, part)

            @pl.when(mid)
            def _():
                pass_on(k, dy, part, some, z, 0, 1).wait_send()
                pass_on(k, dy, part, some, z, 0, 4).wait_send()

                @pl.when(jnp.logical_not(p.is_attn(k)))
                def _():
                    pass_on(k, dy, part, some, z, 0, 2).wait_send()
                    pass_on(k, dy, part, some, z, 0, 3).wait_send()

            for s in range(p.dp - 1):
                spread(k, s, dy, part).wait_send()
            if dy:
                partner(k, 0).wait_send()
                partner(k, 1).wait_send()

        typed(k, go)

    w_sq[...] = jnp.zeros_like(w_sq)
    ahead = jnp.where(mid, AHEAD_MID, AHEAD_END)

    @pl.loop(0, AHEAD_END)
    def _(k):
        pl.when(k < ahead)(lambda: send_own(k))

    @pl.when(mid)
    def _():
        arrive(jnp.int32(0), jnp.int32(2), False)

    for c in old_copies:
        c.start()
    for c in old_copies:
        c.wait()

    @pl.when(jnp.logical_not(mid))
    def _():
        for k in range(AHEAD_MID):
            arrive(jnp.int32(k), jnp.int32(0), False)

    last_mid, last_end = p.turns[True], p.turns[False] - 1

    def one_turn(t):
        d, turn_no = lax.div(t, 3), lax.rem(t, 3)
        pl.when((turn_no == 0) & (d >= 1) & (d < p.count))(lambda: own_first_left(d - 1))
        early = jnp.where(mid, jnp.where(turn_no == 0, 1, 0), jnp.where(turn_no == 2, AHEAD_MID, 0))
        e = lax.rem(turn_no + jnp.where(mid, 2, 1), 3)
        k = d + early
        pl.when(k < p.count)(lambda: arrive(k, e, True))

        @pl.when(turn_no == 2)
        def _():
            pl.when(d + ahead < p.count)(lambda: send_own(d + ahead))

            @pl.when((d == p.count - 1) & mid)
            def _():
                for c in to_end():
                    c.start()

            k = d - jnp.where(mid, LATE_MID, LATE_END)

            @pl.when((k >= 0) & (k < p.count) & p.is_dy(k) & (mid | jnp.logical_not(p.is_attn(k))))
            def _():
                spread_done(k, True)
                partner(k, 1).start()

        work(t)
        first_end = 3 * p.count - 3
        assert first_end not in p.steps[False].values()

        @pl.when((mid & (t == last_mid)) | (jnp.logical_not(mid) & ((t == first_end) | (t == last_end))))
        def _():
            @pl.loop(0, p.count)
            def _(k):
                pl.when(mid | ((t == first_end) == (k < p.count - 2)))(lambda: sends_left(k))

    @pl.loop(0, last_mid + 1)
    def _(t):
        pl.when(mid | (t < p.turns[False]))(lambda: one_turn(t))

    own_first_left(jnp.int32(p.count - 1))
    for mat in (GATE, UP):
        for c in first_copies(mat) + second_copies(mat):
            c.wait_send()

    @pl.when(mid)
    def _():
        for mat in (ATTN, DOWN):
            for c in first_copies(mat) + second_copies(mat):
                c.wait_send()
        for c in to_end() + to_end_down():
            c.wait_send()

    @pl.when(jnp.logical_not(mid))
    def _():
        for c in to_end() + to_end_down():
            c.wait_recv()


def store_kernel(plan, o_attn, o_gate, o_up, grad, *refs):
    p = plan
    stats, al_down, be_down, w_old, (w_attn, w_gate, w_up, w_down), outs = (
        refs[:8], refs[8], refs[9], refs[10], refs[11:15], refs[15:23])
    bounce, w_buf, a_col, in_sem, out_sem, s_sem, wi_sem, wo_sem = refs[23:]
    depth, wide = bounce.shape[0], w_buf.shape[0]

    def cut(ref, i):
        return ref.at[:, i * p.nc:(i + 1) * p.nc]

    def rows(ref, i):
        return ref.at[i * p.mc:(i + 1) * p.mc, :]

    through = [(cut(o_gate, i), cut(w_gate, i)) for i in range(p.ng)]
    if not UP_KEPT:
        through += [(cut(o_up, i), cut(w_up, i)) for i in range(p.ng)]
    loads = [pltpu.make_async_copy(a, bounce.at[i % depth], in_sem.at[i]) for i, (a, _) in enumerate(through)]
    puts = [pltpu.make_async_copy(bounce.at[i % depth], b, out_sem.at[i]) for i, (_, b) in enumerate(through)]
    w_in = [pltpu.make_async_copy(rows(w_old, i), w_buf.at[i % wide], wi_sem.at[i]) for i in range(p.nh)]
    w_out = [pltpu.make_async_copy(w_buf.at[i % wide], rows(w_down, i), wo_sem.at[i]) for i in range(p.nh)]
    for i in range(wide // 2):
        w_in[i].start()
    for c in loads[:depth]:
        c.start()
    copies = [pltpu.make_async_copy(a, b, s_sem.at[i]) for i, (a, b) in enumerate(zip(stats, outs))]
    copies.append(pltpu.make_async_copy(o_attn, w_attn, s_sem.at[8]))
    if UP_KEPT:
        copies += [pltpu.make_async_copy(o_up.at[i], cut(w_up, i), s_sem.at[9 + i]) for i in range(p.ng)]
    for c in copies:
        c.start()
    step_r = min(64, p.mc)
    per = -(-len(through) // p.nh)
    done = 0
    for i in range(p.nh):
        a_col[...] = jnp.broadcast_to(al_down[:, i * p.mc:(i + 1) * p.mc], (LANES, p.mc)).T
        w_in[i].wait()

        @pl.loop(0, p.mc // step_r)
        def _(n):
            at = pl.ds(pl.multiple_of(n * step_r, step_r), step_r)
            a_block = a_col[at, :]
            for c in range(0, p.nc, LANES):
                cols = slice(c, c + LANES)
                w_buf[i % wide, at, cols] = w_buf[i % wide, at, cols] - grad[i, at, cols] * a_block * be_down[:, cols]

        w_out[i].start()
        again = i + wide // 2
        if again < p.nh:
            if again >= wide:
                w_out[again - wide].wait()
            w_in[again].start()
        for j in range(done, min(len(through), done + per)):
            loads[j].wait()
            puts[j].start()
            again = j + depth // 2
            if depth <= again < len(through):
                puts[again - depth].wait()
                loads[again].start()
        done += per
    for i in range(max(0, p.nh - wide), p.nh):
        if i + wide >= p.nh:
            w_out[i].wait()
    for i in range(max(0, len(through) - depth), len(through)):
        puts[i].wait()
    for c in copies:
        c.wait()


def solution(mesh):
    act_spec = P('dp', 'row')
    grad_spec = P('dp', 'col')
    w_spec = P('row', 'col')
    row_spec = P('row')
    col_spec = P('col')
    in_specs = (act_spec, grad_spec, act_spec, grad_spec, grad_spec, act_spec, grad_spec,
                w_spec, w_spec, w_spec, w_spec,
                row_spec, col_spec, row_spec, col_spec, row_spec, col_spec, row_spec, col_spec, P())
    out_specs = (w_spec, row_spec, col_spec) * 4

    def per_device(x_attn, dy_attn, x_mlp, dy_gate, dy_up, h_mlp, dy_out, w_attn, w_gate, w_up, w_down,
                   r_attn, c_attn, r_gate, c_gate, r_up, c_up, r_down, c_down, hyper_params):
        p = Plan(x_mlp, dy_gate, h_mlp, dy_out, mesh)
        stats = [v.reshape(1, -1) for v in (r_attn, c_attn, r_gate, c_gate, r_up, c_up, r_down, c_down)]
        any_spec = pl.BlockSpec(memory_space=pl.ANY)
        vmem_spec = pl.BlockSpec(memory_space=pltpu.VMEM)
        up_spec = vmem_spec if UP_KEPT else any_spec
        row_shapes = []
        for mat in MATS:
            row_shapes += [jax.ShapeDtypeStruct((1, p.rows[mat]), F32), jax.ShapeDtypeStruct((1, p.cols[mat]), F32)]
        w_shapes = [jax.ShapeDtypeStruct((p.rows[mat], p.cols[mat]), F32) for mat in MATS]
        o_shapes = [pltpu.VMEM((p.mc, p.nc), F32), w_shapes[GATE],
                    pltpu.VMEM((p.ng, p.mc, p.nc), F32) if UP_KEPT else w_shapes[UP],
                    pltpu.VMEM((p.pieces, p.mc, p.nc), F32)]
        bufs = [jax.ShapeDtypeStruct((p.n_dy, p.dp - 1, p.tok, p.nc), BF16),
                jax.ShapeDtypeStruct((p.n_x, p.dp - 1, p.tok, p.mc), BF16)]
        rest = jax.ShapeDtypeStruct((p.mc - p.first_rows, p.nc), F32)
        dma = pltpu.SemaphoreType.DMA
        lines = p.count + PARTS - 1
        scratch = [
            pltpu.VMEM((p.dp, p.mc, p.tok), BF16),
            pltpu.VMEM((p.dp, p.tok, p.mc), BF16),
            pltpu.VMEM((p.dp, p.tok, p.nc), BF16),
            pltpu.VMEM((3, p.mc, p.nc), F32),
            pltpu.VMEM((p.mc, LANES), F32),
            pltpu.VMEM((p.pieces, 1, p.mc), F32),
            pltpu.VMEM((p.pieces, 1, p.nc), F32),
            pltpu.VMEM((p.nh, p.mc, LANES), F32),
            pltpu.VMEM((1, p.rows[DOWN]), F32),
            pltpu.VMEM((4, 8, LANES), F32),
        ]
        scratch += [pltpu.VMEM((1, p.cols[mat]), F32) for mat in MATS]
        scratch += [pltpu.VMEM(v.shape, F32) for v in row_shapes]
        scratch += [pltpu.VMEM((2, 1, p.rows[mat]), F32) for mat in MATS]
        scratch += [pltpu.VMEM((4, 1, p.cols[mat]), F32) for mat in MATS]
        scratch += [
            pltpu.VMEM((4, 8, 3, 8, LANES), F32),
            dma((lines, 5)), dma((lines, p.dp - 1)),
            dma((lines, p.dp - 1)), dma((lines, p.dp - 1)),
            dma((p.n_dy, 2)), dma((p.n_dy, 2)),
            dma((4, 4)), dma((4, 4)), dma((4, 8)), dma((4, 8)),
            dma((7,)), dma((7,)),
            dma((p.dp,)), dma((3,)), dma((3,)), dma((8,)),
        ]
        out = pl.pallas_call(
            functools.partial(gather_kernel, p),
            out_shape=o_shapes + [pltpu.VMEM(v.shape, F32) for v in row_shapes + row_shapes[-2:]] + [rest] + bufs,
            in_specs=[any_spec] * 19 + [pl.BlockSpec(memory_space=pltpu.SMEM)],
            out_specs=[vmem_spec, any_spec, up_spec, vmem_spec] + [vmem_spec] * 10 + [any_spec] * 3,
            scratch_shapes=scratch,
            compiler_params=pltpu.CompilerParams(collective_id=0, has_side_effects=True, vmem_limit_bytes=VMEM_LIMIT),
        )(x_attn, dy_attn, x_mlp, dy_gate, dy_up, h_mlp, dy_out, w_attn, w_gate, w_up, w_down, *stats, hyper_params)
        res = pl.pallas_call(
            functools.partial(store_kernel, p),
            out_shape=w_shapes + row_shapes,
            in_specs=[vmem_spec, any_spec, up_spec, vmem_spec] + [vmem_spec] * 10 + [any_spec],
            out_specs=[any_spec] * 12,
            scratch_shapes=[pltpu.VMEM((DEPTH, p.mc, p.nc), F32), pltpu.VMEM((WIDE, p.mc, p.nc), F32),
                            pltpu.VMEM((p.mc, LANES), F32), dma((2 * p.ng,)), dma((2 * p.ng,)), dma((9 + p.ng,)),
                            dma((p.nh,)), dma((p.nh,))],
            compiler_params=pltpu.CompilerParams(vmem_limit_bytes=STORE_LIMIT),
            cost_estimate=pl.CostEstimate(flops=60_000_000_000, bytes_accessed=90_000_000, transcendentals=0),
        )(*[pltpu.with_memory_space_constraint(v, pltpu.VMEM) if i not in HBM_KEPT else v for i, v in enumerate(out[:14])],
          w_down)
        z = lax.axis_index('dp')
        got = lax.ppermute(out[14], 'dp', [(1, 0), (2, 3)])
        rows = jnp.where((z == 1) | (z == 2), out[14], got)
        res = [lax.dynamic_update_slice(res[0], rows, (p.first_rows, 0))] + list(res[1:])
        result = []
        for mat in MATS:
            result += [res[mat], res[4 + 2 * mat].reshape(-1), res[5 + 2 * mat].reshape(-1)]
        return tuple(result)

    return jax.shard_map(per_device, mesh=mesh, in_specs=in_specs, out_specs=out_specs, check_vma=False)
```

```python
import functools
import jax
import jax.numpy as jnp
from jax import lax
from jax.experimental import pallas as pl
from jax.experimental.pallas import tpu as pltpu
from jax.sharding import PartitionSpec as P

EPS_ONE = 1e-30
EPS_TWO = 1e-3
MESH = pl.DeviceIdType.MESH
LANES = 128
F32 = jnp.float32
BF16 = jnp.bfloat16
ATTN, GATE, UP, DOWN = range(4)
MATS = (ATTN, GATE, UP, DOWN)
FIRST = {'gate': ('x_mlp', 0), 'attn': ('x_attn', 0), 'up': ('x_mlp', 0), 'h': ('out', 0)}
AHEAD_MID, AHEAD_END = 2, 6
PARTS = 4
LATE_MID, LATE_END = 3, 2
VMEM_LIMIT = 29 * 1024 * 1024
STORE_LIMIT = 29 * 1024 * 1024
UP_KEPT = True
HBM_KEPT = (1,) if UP_KEPT else (1, 2)
DEPTH, WIDE = 4, 4


def look(k, table):
    out = jnp.int32(0)
    for i, v in enumerate(table):
        if v:
            out = jnp.where(k == i, v, out)
    return out


class Plan:
    def __init__(self, x_mlp, dy_gate, h_mlp, dy_out, mesh):
        self.dp, self.col, self.row = mesh.shape['dp'], mesh.shape['col'], mesh.shape['row']
        assert (self.dp, self.col, self.row) == (4, 2, 4)
        self.tok = x_mlp.shape[0]
        self.mc = x_mlp.shape[1]
        self.nc = dy_out.shape[1]
        self.ng = dy_gate.shape[1] // self.nc
        self.nh = h_mlp.shape[1] // self.mc
        self.tq = self.tok // self.row
        self.th = self.tok // self.col
        g = [('gate', i) for i in range(self.ng)]
        u = [('up', i) for i in range(self.ng)]
        h = [('h', i) for i in range(self.nh)]
        one, two = max(1, self.ng // 4), max(2, 3 * self.ng // 4)
        self.order = ([('x_mlp', 0)] + g[:one] + h[:1] + g[one:two] + h[1:2] + g[two:] + [('x_attn', 0), ('attn', 0)]
                      + u + [('out', 0)] + h[2:])
        self.count = len(self.order)
        self.place = {v: k for k, v in enumerate(self.order)}
        self.first_rows = self.mc * 5 // 16
        self.n_dy = 2 * self.ng + 2
        self.n_x = self.nh + 2
        self.pieces = max(self.ng, self.nh)
        self.rows = {ATTN: self.mc, GATE: self.mc, UP: self.mc, DOWN: self.mc * self.nh}
        self.cols = {ATTN: self.nc, GATE: self.nc * self.ng, UP: self.nc * self.ng, DOWN: self.nc}
        self.parts = {ATTN: 1, GATE: self.ng, UP: self.ng, DOWN: self.nh}
        base = {'gate': 0, 'up': self.ng, 'out': 2 * self.ng, 'attn': 2 * self.ng + 1, 'x_mlp': 0, 'x_attn': 1, 'h': 2}
        self.dy_table = [1 if n in ('gate', 'up', 'out', 'attn') else 0 for n, _ in self.order]
        self.at_table = [base[n] + i for n, i in self.order]
        self.attn_table = [1 if n in ('x_attn', 'attn') else 0 for n, _ in self.order]
        self.steps = {m: self.schedule(m) for m in (True, False)}
        self.turns = {m: max(max(v.values()) + 1, 3 * self.count) for m, v in self.steps.items()}

    def schedule(self, mid):
        late = LATE_MID if mid else LATE_END
        tasks = []
        for name, mat in (('gate', GATE), ('attn', ATTN), ('up', UP), ('h', DOWN)):
            if name == 'attn' and not mid:
                continue
            for i in range(self.parts[mat]):
                k = self.place[name, i]
                need = [3 * (k + late + 1)] if name != 'h' else [3 * (k + late) if mid else 3 * k + 5]
                if i == 0:
                    need.append(3 * (self.place[FIRST[name]] + late + (name == 'h')))
                tasks.append(((name, i), max(need)))
            stages = {ATTN: (1, 2), DOWN: (1, 2)}.get(mat, (1, 2, 3))
            if mid or mat != DOWN:
                tasks += [(('finish', mat, stage), 0) for stage in stages]
        out, t = {}, 0
        for task, first in tasks:
            t = max(t, first)
            out[task] = t
            t += 1
        return out

    def is_dy(self, k):
        return look(k, self.dy_table) == 1

    def is_attn(self, k):
        return look(k, self.attn_table) == 1

    def at(self, k):
        return look(k, self.at_table)


def gather_kernel(plan, x_attn, dy_attn, x_mlp, dy_gate, dy_up, h_mlp, dy_out, w_attn, w_gate, w_up, w_down,
                  r_attn, c_attn, r_gate, c_gate, r_up, c_up, r_down, c_down, hyper,
                  o_attn, o_gate, o_up, grad, nr_attn, nc_attn, nr_gate, nc_gate, nr_up, nc_up, nr_down, nc_down,
                  al_down, be_down, o_rest, buf_d, buf_x,
                  lhs, tile_x, tile_d, w_buf, r_lanes, r_row, c_sum, a_cols, a_rows, w_sq,
                  b_attn, b_gate, b_up, b_down, *more):
    p = plan
    old_refs = more[:8]
    (rs_attn, rs_gate, rs_up, rs_down, cs_attn, cs_gate, cs_up, cs_down, st_all,
     z_send, z_recv, f_send, f_recv, c_send, c_recv, r1_send, r1_recv, r2_send, r2_recv,
     e_send, e_recv, l_sem, wi_sem, wo_sem, o_sem) = more[8:]
    z, y, r = lax.axis_index('dp'), lax.axis_index('col'), lax.axis_index('row')
    low = z < 2
    mid = (z == 1) | (z == 2)
    end_z = jnp.where(low, 0, 3)
    mate_z = 3 - z
    w_refs = {ATTN: w_attn, GATE: w_gate, UP: w_up, DOWN: w_down}
    old_in = (r_attn, c_attn, r_gate, c_gate, r_up, c_up, r_down, c_down)
    old = {mat: (old_refs[2 * mat], old_refs[2 * mat + 1]) for mat in MATS}
    old_copies = [pltpu.make_async_copy(a, b, o_sem.at[i]) for i, (a, b) in enumerate(zip(old_in, old_refs))]
    new = {ATTN: (nr_attn, nc_attn), GATE: (nr_gate, nc_gate), UP: (nr_up, nc_up), DOWN: (nr_down, nc_down)}
    b_rows = {ATTN: b_attn, GATE: b_gate, UP: b_up, DOWN: b_down}
    rs = {ATTN: rs_attn, GATE: rs_gate, UP: rs_up, DOWN: rs_down}
    cs = {ATTN: cs_attn, GATE: cs_gate, UP: cs_up, DOWN: cs_down}

    def flip_row(v):
        bit0, bit1 = lax.rem(r, 2), lax.div(r, 2)
        if v & 1:
            bit0 = 1 - bit0
        if v & 2:
            bit1 = 1 - bit1
        return bit1 * 2 + bit0

    peers = [(f, v) for f in range(2) for v in range(4) if f or v]
    barrier = pltpu.get_barrier_semaphore()
    for f, v in peers:
        pl.semaphore_signal(barrier, inc=1, device_id=(z, 1 - y if f else y, flip_row(v)), device_id_type=MESH)

    @pl.when(mid)
    def _():
        pl.semaphore_signal(barrier, inc=1, device_id=(end_z, y, r), device_id_type=MESH)
        pl.semaphore_signal(barrier, inc=1, device_id=(mate_z, y, r), device_id_type=MESH)
        pl.semaphore_wait(barrier, len(peers) + 2)

    @pl.when(jnp.logical_not(mid))
    def _():
        pl.semaphore_signal(barrier, inc=1, device_id=(jnp.where(low, 1, 2), y, r), device_id_type=MESH)
        pl.semaphore_wait(barrier, len(peers) + 1)

    my_q = pl.ds(pl.multiple_of(r * p.tq, p.tq), p.tq)
    x_q = pl.ds(pl.multiple_of(flip_row(2) * p.tq, p.tq), p.tq)
    my_h = pl.ds(pl.multiple_of(y * p.th, p.th), p.th)

    def rows_of(dy, part):
        if dy:
            return my_q
        if part is None:
            return my_h
        size = p.th // PARTS
        return pl.ds(pl.multiple_of(y * p.th + part * size, size), size)

    def line_of(k, part):
        return k if part is None else k + part

    def slot(k, s, dy, part):
        return (buf_d if dy else buf_x).at[p.at(k), s, rows_of(dy, part), :]

    def pass_on(k, dy, part, src, to_z, to_slot, sem):
        line = line_of(k, part)
        return pltpu.make_async_remote_copy(
            src_ref=src, dst_ref=slot(k, to_slot, dy, part), send_sem=z_send.at[line, sem],
            recv_sem=z_recv.at[line, to_slot], device_id=(to_z, y, r), device_id_type=MESH)

    def spread(k, s, dy, part):
        to = (z, y, flip_row(2)) if dy else (z, 1 - y, r)
        line = line_of(k, part)
        return pltpu.make_async_remote_copy(
            src_ref=slot(k, s, dy, part), dst_ref=slot(k, s, dy, part), send_sem=f_send.at[line, s],
            recv_sem=f_recv.at[line, s], device_id=to, device_id_type=MESH)

    def partner(k, which):
        part = buf_d.at[p.at(k), :, x_q if which else my_q, :]
        return pltpu.make_async_remote_copy(
            src_ref=part, dst_ref=part, send_sem=c_send.at[p.at(k), which], recv_sem=c_recv.at[p.at(k), which],
            device_id=(z, y, flip_row(1)), device_id_type=MESH)

    def in_parts(k, go):
        pl.when(k != p.count - 1)(lambda: go(None))

        @pl.when(k == p.count - 1)
        def _():
            pl.loop(0, PARTS)(go)

    def typed(k, go):
        used = mid | jnp.logical_not(p.is_attn(k))
        pl.when(p.is_dy(k) & used)(lambda: go(True, None))
        pl.when(jnp.logical_not(p.is_dy(k)) & used)(lambda: in_parts(k, lambda part: go(False, part)))

    def cut(ref, at, size):
        return ref.at[:, pl.ds(pl.multiple_of(at * size, size), size)]

    def down_rows(ref, i):
        return ref.at[pl.ds(pl.multiple_of(i * p.mc, p.mc), p.mc), :]

    def own_to(k, dy, part, src, end_too, mate_too):
        @pl.when(jnp.logical_not(mid))
        def _():
            pass_on(k, dy, part, src, jnp.where(low, 1, 2), jnp.where(low, 2, 0), 0).start()

        @pl.when(mid)
        def _():
            @pl.when(jnp.logical_not(p.is_attn(k)) & end_too)
            def _():
                pass_on(k, dy, part, src, end_z, jnp.where(low, 0, 2), 0).start()

            @pl.when(mate_too)
            def _():
                pass_on(k, dy, part, src, mate_z, jnp.where(low, 2, 0), 1).start()

    def send_own(k, end_too, mate_too):
        def go(ref, at, size, dy):
            def send(part):
                src = ref.at[rows_of(dy, part), pl.ds(pl.multiple_of(at * size, size), size)]
                own_to(k, dy, part, src, end_too, mate_too)

            if ref is h_mlp:
                in_parts(k, send)
            else:
                send(None)

        for name, ref, dy in (('x_mlp', x_mlp, False), ('gate', dy_gate, True), ('x_attn', x_attn, False),
                              ('attn', dy_attn, True), ('up', dy_up, True), ('out', dy_out, True), ('h', h_mlp, False)):
            at = look(k, [i + 1 if n == name else 0 for n, i in p.order])
            size = p.nc if dy else p.mc
            pl.when(at > 0)(functools.partial(go, ref, at - 1, size, dy))

    def own_first_left(k):
        @pl.when(jnp.logical_not(mid & p.is_attn(k)))
        def _():
            def go(dy, part):
                pass_on(k, dy, part, slot(k, 0, dy, part), z, 0, 0).wait_send()

            pl.when(p.is_dy(k))(lambda: go(True, None))
            pl.when(jnp.logical_not(p.is_dy(k)))(lambda: in_parts(k, lambda part: go(False, part)))

    def arrive(k, e, whole):
        s = jnp.where(low, e, 2 - e)

        def go(dy, part):
            here = slot(k, s, dy, part)
            pass_on(k, dy, part, here, z, s, 0).wait_recv()

            @pl.when(mid & (e == 2))
            def _():
                pass_on(k, dy, part, here, mate_z, 1, 4).start()

            @pl.when(mid & (e < 2) & jnp.logical_not(p.is_attn(k)))
            def _():
                pass_on(k, dy, part, here, end_z, jnp.where(low, s + 1, s - 1), 2 + e).start()

            spread(k, s, dy, part).start()
            if dy and whole:
                pl.when(e == jnp.where(mid, 1, 2))(lambda: partner(k, 0).start())

        typed(k, go)

    def spread_done(k, dy):
        for s in range(p.dp - 1):
            spread(k, s, dy, None).wait_recv()

    def load(src, at, size, buf, index, dst):
        copies = [pltpu.make_async_copy(cut(src, at, size), dst.at[z], l_sem.at[0])]
        for d in range(1, p.dp):
            copies.append(pltpu.make_async_copy(buf.at[index, d - 1], dst.at[lax.rem(z + d, p.dp)], l_sem.at[d]))
        for c in copies:
            c.start()
        for c in copies:
            c.wait()

    step_t = min(256, p.tok)

    def turn(q):
        @pl.loop(0, p.tok // step_t)
        def _(t):
            at = pl.multiple_of(t * step_t, step_t)
            lhs[q, :, pl.ds(at, step_t)] = tile_x[q, pl.ds(at, step_t), :].T

    step_n = min(512, p.nc)
    step_r = min(64, p.mc)

    def lane_sum(v):
        out = v[:, 0:LANES]
        for i in range(1, v.shape[1] // LANES):
            out = out + v[:, i * LANES:(i + 1) * LANES]
        return out

    def product(at, count):
        r_lanes[...] = jnp.zeros_like(r_lanes)

        @pl.loop(0, p.nc // step_n)
        def _(n):
            cols = pl.ds(pl.multiple_of(n * step_n, step_n), step_n)
            grad[at, :, cols] = jnp.dot(lhs[0], tile_d[0, :, cols], preferred_element_type=F32)

            @pl.loop(1, p.dp)
            def _(q):
                grad[at, :, cols] += jnp.dot(lhs[q], tile_d[q, :, cols], preferred_element_type=F32)

            def body(i, acc):
                rows = pl.ds(pl.multiple_of(i * step_r, step_r), step_r)
                block = grad[at, rows, cols]
                sq = block * block + EPS_ONE
                r_lanes[rows, :] += lane_sum(sq)
                return acc + jnp.sum(sq, axis=0, keepdims=True)

            @pl.when(count)
            def _():
                c_sum[at, :, cols] = lax.fori_loop(0, p.mc // step_r, body, jnp.zeros((1, step_n), F32))

    def fold(v):
        v = jnp.reshape(v, (v.shape[0] // 8, 8, LANES))
        while v.shape[0] > 1:
            v = v[:v.shape[0] // 2] + v[v.shape[0] // 2:]
        return v[0]

    def to_row(block):
        return jnp.sum(block.T, axis=0, keepdims=True)

    def get_w(mat, i):
        src = down_rows(w_refs[mat], i) if mat == DOWN else cut(w_refs[mat], i, p.nc)
        return pltpu.make_async_copy(src, w_buf.at[lax.rem(i, 3)], wi_sem.at[lax.rem(i, 3)])

    def put_w(mat, i):
        dst = cut(o_gate if mat == GATE else o_up, i, p.nc)
        return pltpu.make_async_copy(w_buf.at[lax.rem(i, 3)], dst, wo_sem.at[lax.rem(i, 3)])

    def chunk(mat, i):
        count = mid if mat == DOWN else jnp.bool_(True)
        pl.when(count)(lambda: get_w(mat, i).start())
        product(i, count)

        @pl.when(count)
        def _():
            row = to_row(r_lanes[...])
            if mat == DOWN:
                r_row[i] = row
            else:
                r_row[0] = jnp.where(i == 0, row, r_row[0] + row)
            get_w(mat, i).wait()

            def body(n, acc):
                rows = pl.ds(pl.multiple_of(n * step_r, step_r), step_r)
                block = lane_sum(w_buf[lax.rem(i, 3), rows, :] * w_buf[lax.rem(i, 3), rows, :])
                return acc + fold(block)

            w_sq[mat] += lax.fori_loop(0, p.mc // step_r, body, jnp.zeros((8, LANES), F32))

    def first_copies(mat):
        copies = [pltpu.make_async_remote_copy(
            src_ref=rs[mat].at[y], dst_ref=rs[mat].at[y], send_sem=r1_send.at[mat, 0], recv_sem=r1_recv.at[mat, 0],
            device_id=(z, 1 - y, r), device_id_type=MESH)]
        for v in range(1, 4):
            copies.append(pltpu.make_async_remote_copy(
                src_ref=cs[mat].at[r], dst_ref=cs[mat].at[r], send_sem=r1_send.at[mat, v],
                recv_sem=r1_recv.at[mat, v], device_id=(z, y, flip_row(v)), device_id_type=MESH))
        return copies

    def second_copies(mat):
        me = y * 4 + r
        return [pltpu.make_async_remote_copy(
            src_ref=st_all.at[mat, me], dst_ref=st_all.at[mat, me], send_sem=r2_send.at[mat, f * 4 + v],
            recv_sem=r2_recv.at[mat, f * 4 + v], device_id=(z, 1 - y if f else y, flip_row(v)), device_id_type=MESH)
            for f, v in peers]

    def scale_rows(mat):
        return p.rows[mat] * p.row, p.cols[mat] * p.col

    blocks = p.mc // step_r

    def factors(mat, i, n):
        rows = pl.ds(pl.multiple_of(n * step_r, step_r), step_r)
        if mat == DOWN:
            return rows, a_cols[i, rows, :], b_rows[mat].at[:, :]
        return rows, a_cols[0, rows, :], b_rows[mat].at[:, pl.ds(pl.multiple_of(i * p.nc, p.nc), p.nc)]

    def finish_first(mat):
        parts = p.parts[mat]
        if mat != DOWN:
            for i in range(min(2, parts)):
                get_w(mat, jnp.int32(i)).start()
        if mat == DOWN:
            block = c_sum[0]
            for i in range(parts):
                rs[mat][y, :, i * p.mc:(i + 1) * p.mc] = r_row[i]
                if i:
                    block = block + c_sum[i]
            cs[mat][r] = block
        else:
            rs[mat][y] = r_row[0]
            for i in range(parts):
                cs[mat][r, :, i * p.nc:(i + 1) * p.nc] = c_sum[i]
        for c in first_copies(mat):
            c.start()

    def finish_second(mat):
        beta_two = hyper[0]
        m_total, n_total = scale_rows(mat)
        parts = p.parts[mat]
        for c in first_copies(mat):
            c.wait_recv()
        r_new = beta_two * old[mat][0][...] + (1.0 - beta_two) * ((rs[mat][0] + rs[mat][1]) / n_total)
        c_all = ((cs[mat][0] + cs[mat][1]) + cs[mat][2]) + cs[mat][3]
        c_new = beta_two * old[mat][1][...] + (1.0 - beta_two) * (c_all / m_total)
        new[mat][0][...] = r_new
        new[mat][1][...] = c_new
        t_own = jnp.sum(r_new, axis=1, keepdims=True)
        a_row = jnp.sqrt(t_own) / jnp.sqrt(r_new)
        b_rows[mat][...] = 1.0 / jnp.sqrt(c_new)
        if mat == DOWN:
            a_rows[...] = a_row
        for i in range(parts if mat == DOWN else 1):
            a_cols[i] = jnp.broadcast_to(a_row[:, i * p.mc:(i + 1) * p.mc], (LANES, p.mc)).T

        def add_up(j, acc):
            i, n = lax.div(j, blocks), lax.rem(j, blocks)
            rows, a_block, b_ref = factors(mat, i, n)
            for c in range(0, p.nc, LANES):
                upd = grad[i, rows, c:c + LANES] * a_block * b_ref[:, c:c + LANES]
                acc = acc + fold(upd * upd)
            return acc

        u_part = lax.fori_loop(0, parts * blocks, add_up, jnp.zeros((8, LANES), F32))

        def spot(v):
            return jnp.broadcast_to(jnp.sum(jnp.sum(v, axis=1, keepdims=True), axis=0, keepdims=True), (8, LANES))

        me = y * 4 + r
        st_all[mat, me, 0] = spot(u_part)
        st_all[mat, me, 1] = spot(w_sq[mat])
        st_all[mat, me, 2] = jnp.broadcast_to(t_own, (8, LANES))
        for c in second_copies(mat):
            c.start()

    def finish_third(mat):
        rho_step, clip_thr = hyper[1], hyper[2]
        m_total, n_total = scale_rows(mat)
        me = y * 4 + r
        for c in second_copies(mat):
            c.wait_recv()
        t_all = st_all[mat, 0, 2]
        for i in range(1, p.row):
            t_all = t_all + st_all[mat, i, 2]
        u_all = st_all[mat, 0, 0] * (t_all / st_all[mat, 0, 2])
        w_all = st_all[mat, 0, 1]
        for i in range(1, p.row * p.col):
            u_all = u_all + st_all[mat, i, 0] * (t_all / st_all[mat, i, 2])
            w_all = w_all + st_all[mat, i, 1]
        upd_rms = jnp.sqrt(u_all / (m_total * n_total))
        w_rms = jnp.sqrt(w_all / (m_total * n_total))
        scale = rho_step * jnp.maximum(EPS_TWO, w_rms) / jnp.maximum(1.0, upd_rms / clip_thr)
        scale = scale * jnp.sqrt(t_all / st_all[mat, me, 2])
        b_rows[mat][...] = b_rows[mat][...] * scale[0:1, 0:1]

    def renew(mat, low_i, high_i):
        parts = p.parts[mat]

        @pl.loop(low_i, high_i)
        def _(i):
            at = lax.rem(i, 3)
            get_w(mat, i).wait()

            @pl.loop(0, blocks)
            def _(n):
                rows, a_block, b_ref = factors(mat, i, n)
                for c in range(0, p.nc, LANES):
                    cols = slice(c, c + LANES)
                    fresh = w_buf[at, rows, cols] - grad[i, rows, cols] * a_block * b_ref[:, cols]
                    if mat == ATTN:
                        o_attn[rows, cols] = fresh
                    elif mat == UP and UP_KEPT:
                        o_up[i, rows, cols] = fresh
                    else:
                        w_buf[at, rows, cols] = fresh

            if mat == ATTN:
                put_rest().start()
                put_rest().wait()
            if mat == GATE or (mat == UP and not UP_KEPT):
                put_w(mat, i).start()
                pl.when(i >= 1)(lambda: put_w(mat, i - 1).wait())
            pl.when(i + 2 < parts)(lambda: get_w(mat, i + 2).start())

        if (mat == GATE or (mat == UP and not UP_KEPT)) and high_i == parts:
            put_w(mat, jnp.int32(parts - 1)).wait()

    def put_rest():
        return pltpu.make_async_copy(o_attn.at[pl.ds(p.first_rows, p.mc - p.first_rows), :], o_rest, wo_sem.at[0])

    def finish(mat, stage):
        parts = p.parts[mat]
        half = parts // 2 if parts > 1 else parts
        if stage == 1:
            finish_second(mat)
        elif stage == 2:
            finish_third(mat)
            if mat == DOWN:
                al_down[...] = a_rows[...]
                be_down[...] = b_rows[mat][...]
                for c in to_end_down():
                    c.start()
            else:
                renew(mat, 0, half)
        else:
            renew(mat, half, parts)

    def take_x(src, at, k, waits=True):
        copies = [(pltpu.make_async_copy(cut(src, at, p.mc), tile_x.at[z], l_sem.at[0]), z)]
        copies[0][0].start()
        for e in range(p.dp - 1):
            s = jnp.where(low, e, 2 - e)
            if src is h_mlp:
                in_parts(k, lambda part: spread(k, s, False, part).wait_recv())
            elif waits:
                spread(k, s, False, None).wait_recv()
            q = lax.rem(z + s + 1, p.dp)
            copies.append((pltpu.make_async_copy(buf_x.at[p.at(k), s], tile_x.at[q], l_sem.at[e + 1]), q))
            copies[-1][0].start()
            copies[-2][0].wait()
            turn(copies[-2][1])
        copies[-1][0].wait()
        turn(copies[-1][1])

    def got(name, i):
        k = look(i, [p.place[name, j] for j in range(sum(1 for n, _ in p.order if n == name))])
        partner(k, 0).wait_recv()
        partner(k, 1).wait_recv()
        return k

    def use_gate(i):
        pl.when(i == 0)(lambda: take_x(x_mlp, 0, jnp.int32(p.place['x_mlp', 0])))
        k = got('gate', i)
        load(dy_gate, i, p.nc, buf_d, p.at(k), tile_d)
        chunk(GATE, i)
        pl.when(i == p.parts[GATE] - 1)(lambda: finish_first(GATE))

    def use_attn(i):
        take_x(x_attn, 0, jnp.int32(p.place['x_attn', 0]))
        k = got('attn', i)
        load(dy_attn, 0, p.nc, buf_d, p.at(k), tile_d)
        chunk(ATTN, i)
        finish_first(ATTN)

    def use_up(i):
        pl.when(i == 0)(lambda: take_x(x_mlp, 0, jnp.int32(p.place['x_mlp', 0]), False))
        k = got('up', i)
        load(dy_up, i, p.nc, buf_d, p.at(k), tile_d)
        chunk(UP, i)
        pl.when(i == p.parts[UP] - 1)(lambda: finish_first(UP))

    def use_out():
        k = got('out', jnp.int32(0))
        load(dy_out, 0, p.nc, buf_d, p.at(k), tile_d)

    def use_h(i):
        pl.when(i == 0)(use_out)
        take_x(h_mlp, i, look(i, [p.place['h', j] for j in range(p.nh)]))
        chunk(DOWN, i)
        pl.when((i == p.parts[DOWN] - 1) & mid)(lambda: finish_first(DOWN))

    def work(t):
        for name, use in (('gate', use_gate), ('attn', use_attn), ('up', use_up), ('h', use_h)):
            at = jnp.int32(0)
            for i in range(sum(1 for n, _ in p.order if n == name)):
                when_mid = p.steps[True].get((name, i), -1)
                when_end = p.steps[False].get((name, i), -1)
                at = jnp.where(t == jnp.where(mid, when_mid, when_end), i + 1, at)
            pl.when(at > 0)(functools.partial(use, at - 1))
        for mat in MATS:
            for stage in (1, 2, 3):
                when_mid = p.steps[True].get(('finish', mat, stage), -1)
                when_end = p.steps[False].get(('finish', mat, stage), -1)
                if when_mid >= 0:
                    pl.when(t == jnp.where(mid, when_mid, when_end))(functools.partial(finish, mat, stage))

    def sent_to_end(refs, first):
        return [pltpu.make_async_remote_copy(
            src_ref=ref, dst_ref=ref, send_sem=e_send.at[first + i], recv_sem=e_recv.at[first + i],
            device_id=(end_z, y, r), device_id_type=MESH) for i, ref in enumerate(refs)]

    def to_end():
        return sent_to_end((nr_attn, nc_attn, o_attn.at[pl.ds(0, p.first_rows), :]), 0)

    def to_end_down():
        return sent_to_end((nr_down, nc_down, al_down, be_down), 3)

    def sends_left(k):
        def go(dy, part):
            some = slot(k, 0, dy, part)

            @pl.when(mid)
            def _():
                pass_on(k, dy, part, some, z, 0, 1).wait_send()
                pass_on(k, dy, part, some, z, 0, 4).wait_send()

                @pl.when(jnp.logical_not(p.is_attn(k)))
                def _():
                    pass_on(k, dy, part, some, z, 0, 2).wait_send()
                    pass_on(k, dy, part, some, z, 0, 3).wait_send()

            for s in range(p.dp - 1):
                spread(k, s, dy, part).wait_send()
            if dy:
                partner(k, 0).wait_send()
                partner(k, 1).wait_send()

        typed(k, go)

    w_sq[...] = jnp.zeros_like(w_sq)
    ahead = jnp.where(mid, AHEAD_MID, AHEAD_END)

    @pl.loop(0, AHEAD_END)
    def _(k):
        pl.when(k < jnp.where(mid, AHEAD_MID + 1, AHEAD_END))(lambda: send_own(k, True, k < AHEAD_MID))

    @pl.when(mid)
    def _():
        arrive(jnp.int32(0), jnp.int32(2), False)

    for c in old_copies:
        c.start()
    for c in old_copies:
        c.wait()

    @pl.when(jnp.logical_not(mid))
    def _():
        for k in range(AHEAD_MID):
            arrive(jnp.int32(k), jnp.int32(0), False)

    last_mid, last_end = p.turns[True], p.turns[False] - 1

    def one_turn(t):
        d, turn_no = lax.div(t, 3), lax.rem(t, 3)
        pl.when((turn_no == 0) & (d >= 1) & (d < p.count))(lambda: own_first_left(d - 1))
        early = jnp.where(mid, jnp.where(turn_no == 0, 1, 0), jnp.where(turn_no == 2, AHEAD_MID, 0))
        e = lax.rem(turn_no + jnp.where(mid, 2, 1), 3)
        k = d + early
        pl.when(k < p.count)(lambda: arrive(k, e, True))

        @pl.when(turn_no == 2)
        def _():
            pl.when(d + ahead < p.count)(lambda: send_own(d + ahead, d > 0, True))

            @pl.when((d == p.count - 1) & mid)
            def _():
                for c in to_end():
                    c.start()

            k = d - jnp.where(mid, LATE_MID, LATE_END)

            @pl.when((k >= 0) & (k < p.count) & p.is_dy(k) & (mid | jnp.logical_not(p.is_attn(k))))
            def _():
                spread_done(k, True)
                partner(k, 1).start()

        work(t)
        first_end = 3 * p.count - 3
        assert first_end not in p.steps[False].values()

        @pl.when((mid & (t == last_mid)) | (jnp.logical_not(mid) & ((t == first_end) | (t == last_end))))
        def _():
            @pl.loop(0, p.count)
            def _(k):
                pl.when(mid | ((t == first_end) == (k < p.count - 2)))(lambda: sends_left(k))

    @pl.loop(0, last_mid + 1)
    def _(t):
        pl.when(mid | (t < p.turns[False]))(lambda: one_turn(t))

    own_first_left(jnp.int32(p.count - 1))
    for mat in (GATE, UP):
        for c in first_copies(mat) + second_copies(mat):
            c.wait_send()

    @pl.when(mid)
    def _():
        for mat in (ATTN, DOWN):
            for c in first_copies(mat) + second_copies(mat):
                c.wait_send()
        for c in to_end() + to_end_down():
            c.wait_send()

    @pl.when(jnp.logical_not(mid))
    def _():
        for c in to_end() + to_end_down():
            c.wait_recv()


def store_kernel(plan, o_attn, o_gate, o_up, grad, *refs):
    p = plan
    stats, al_down, be_down, w_old, (w_attn, w_gate, w_up, w_down), outs = (
        refs[:8], refs[8], refs[9], refs[10], refs[11:15], refs[15:23])
    bounce, w_buf, a_col, in_sem, out_sem, s_sem, wi_sem, wo_sem = refs[23:]
    depth, wide = bounce.shape[0], w_buf.shape[0]

    def cut(ref, i):
        return ref.at[:, i * p.nc:(i + 1) * p.nc]

    def rows(ref, i):
        return ref.at[i * p.mc:(i + 1) * p.mc, :]

    through = [(cut(o_gate, i), cut(w_gate, i)) for i in range(p.ng)]
    if not UP_KEPT:
        through += [(cut(o_up, i), cut(w_up, i)) for i in range(p.ng)]
    loads = [pltpu.make_async_copy(a, bounce.at[i % depth], in_sem.at[i]) for i, (a, _) in enumerate(through)]
    puts = [pltpu.make_async_copy(bounce.at[i % depth], b, out_sem.at[i]) for i, (_, b) in enumerate(through)]
    w_in = [pltpu.make_async_copy(rows(w_old, i), w_buf.at[i % wide], wi_sem.at[i]) for i in range(p.nh)]
    w_out = [pltpu.make_async_copy(w_buf.at[i % wide], rows(w_down, i), wo_sem.at[i]) for i in range(p.nh)]
    for i in range(wide // 2):
        w_in[i].start()
    for c in loads[:depth]:
        c.start()
    copies = [pltpu.make_async_copy(a, b, s_sem.at[i]) for i, (a, b) in enumerate(zip(stats, outs))]
    copies.append(pltpu.make_async_copy(o_attn, w_attn, s_sem.at[8]))
    if UP_KEPT:
        copies += [pltpu.make_async_copy(o_up.at[i], cut(w_up, i), s_sem.at[9 + i]) for i in range(p.ng)]
    for c in copies:
        c.start()
    step_r = min(64, p.mc)
    per = -(-len(through) // p.nh)
    done = 0
    for i in range(p.nh):
        a_col[...] = jnp.broadcast_to(al_down[:, i * p.mc:(i + 1) * p.mc], (LANES, p.mc)).T
        w_in[i].wait()

        @pl.loop(0, p.mc // step_r)
        def _(n):
            at = pl.ds(pl.multiple_of(n * step_r, step_r), step_r)
            a_block = a_col[at, :]
            for c in range(0, p.nc, LANES):
                cols = slice(c, c + LANES)
                w_buf[i % wide, at, cols] = w_buf[i % wide, at, cols] - grad[i, at, cols] * a_block * be_down[:, cols]

        w_out[i].start()
        again = i + wide // 2
        if again < p.nh:
            if again >= wide:
                w_out[again - wide].wait()
            w_in[again].start()
        for j in range(done, min(len(through), done + per)):
            loads[j].wait()
            puts[j].start()
            again = j + depth // 2
            if depth <= again < len(through):
                puts[again - depth].wait()
                loads[again].start()
        done += per
    for i in range(max(0, p.nh - wide), p.nh):
        if i + wide >= p.nh:
            w_out[i].wait()
    for i in range(max(0, len(through) - depth), len(through)):
        puts[i].wait()
    for c in copies:
        c.wait()


def solution(mesh):
    act_spec = P('dp', 'row')
    grad_spec = P('dp', 'col')
    w_spec = P('row', 'col')
    row_spec = P('row')
    col_spec = P('col')
    in_specs = (act_spec, grad_spec, act_spec, grad_spec, grad_spec, act_spec, grad_spec,
                w_spec, w_spec, w_spec, w_spec,
                row_spec, col_spec, row_spec, col_spec, row_spec, col_spec, row_spec, col_spec, P())
    out_specs = (w_spec, row_spec, col_spec) * 4

    def per_device(x_attn, dy_attn, x_mlp, dy_gate, dy_up, h_mlp, dy_out, w_attn, w_gate, w_up, w_down,
                   r_attn, c_attn, r_gate, c_gate, r_up, c_up, r_down, c_down, hyper_params):
        p = Plan(x_mlp, dy_gate, h_mlp, dy_out, mesh)
        stats = [v.reshape(1, -1) for v in (r_attn, c_attn, r_gate, c_gate, r_up, c_up, r_down, c_down)]
        any_spec = pl.BlockSpec(memory_space=pl.ANY)
        vmem_spec = pl.BlockSpec(memory_space=pltpu.VMEM)
        up_spec = vmem_spec if UP_KEPT else any_spec
        row_shapes = []
        for mat in MATS:
            row_shapes += [jax.ShapeDtypeStruct((1, p.rows[mat]), F32), jax.ShapeDtypeStruct((1, p.cols[mat]), F32)]
        w_shapes = [jax.ShapeDtypeStruct((p.rows[mat], p.cols[mat]), F32) for mat in MATS]
        o_shapes = [pltpu.VMEM((p.mc, p.nc), F32), w_shapes[GATE],
                    pltpu.VMEM((p.ng, p.mc, p.nc), F32) if UP_KEPT else w_shapes[UP],
                    pltpu.VMEM((p.pieces, p.mc, p.nc), F32)]
        bufs = [jax.ShapeDtypeStruct((p.n_dy, p.dp - 1, p.tok, p.nc), BF16),
                jax.ShapeDtypeStruct((p.n_x, p.dp - 1, p.tok, p.mc), BF16)]
        rest = jax.ShapeDtypeStruct((p.mc - p.first_rows, p.nc), F32)
        dma = pltpu.SemaphoreType.DMA
        lines = p.count + PARTS - 1
        scratch = [
            pltpu.VMEM((p.dp, p.mc, p.tok), BF16),
            pltpu.VMEM((p.dp, p.tok, p.mc), BF16),
            pltpu.VMEM((p.dp, p.tok, p.nc), BF16),
            pltpu.VMEM((3, p.mc, p.nc), F32),
            pltpu.VMEM((p.mc, LANES), F32),
            pltpu.VMEM((p.pieces, 1, p.mc), F32),
            pltpu.VMEM((p.pieces, 1, p.nc), F32),
            pltpu.VMEM((p.nh, p.mc, LANES), F32),
            pltpu.VMEM((1, p.rows[DOWN]), F32),
            pltpu.VMEM((4, 8, LANES), F32),
        ]
        scratch += [pltpu.VMEM((1, p.cols[mat]), F32) for mat in MATS]
        scratch += [pltpu.VMEM(v.shape, F32) for v in row_shapes]
        scratch += [pltpu.VMEM((2, 1, p.rows[mat]), F32) for mat in MATS]
        scratch += [pltpu.VMEM((4, 1, p.cols[mat]), F32) for mat in MATS]
        scratch += [
            pltpu.VMEM((4, 8, 3, 8, LANES), F32),
            dma((lines, 5)), dma((lines, p.dp - 1)),
            dma((lines, p.dp - 1)), dma((lines, p.dp - 1)),
            dma((p.n_dy, 2)), dma((p.n_dy, 2)),
            dma((4, 4)), dma((4, 4)), dma((4, 8)), dma((4, 8)),
            dma((7,)), dma((7,)),
            dma((p.dp,)), dma((3,)), dma((3,)), dma((8,)),
        ]
        out = pl.pallas_call(
            functools.partial(gather_kernel, p),
            out_shape=o_shapes + [pltpu.VMEM(v.shape, F32) for v in row_shapes + row_shapes[-2:]] + [rest] + bufs,
            in_specs=[any_spec] * 19 + [pl.BlockSpec(memory_space=pltpu.SMEM)],
            out_specs=[vmem_spec, any_spec, up_spec, vmem_spec] + [vmem_spec] * 10 + [any_spec] * 3,
            scratch_shapes=scratch,
            compiler_params=pltpu.CompilerParams(collective_id=0, has_side_effects=True, vmem_limit_bytes=VMEM_LIMIT),
        )(x_attn, dy_attn, x_mlp, dy_gate, dy_up, h_mlp, dy_out, w_attn, w_gate, w_up, w_down, *stats, hyper_params)
        res = pl.pallas_call(
            functools.partial(store_kernel, p),
            out_shape=w_shapes + row_shapes,
            in_specs=[vmem_spec, any_spec, up_spec, vmem_spec] + [vmem_spec] * 10 + [any_spec],
            out_specs=[any_spec] * 12,
            scratch_shapes=[pltpu.VMEM((DEPTH, p.mc, p.nc), F32), pltpu.VMEM((WIDE, p.mc, p.nc), F32),
                            pltpu.VMEM((p.mc, LANES), F32), dma((2 * p.ng,)), dma((2 * p.ng,)), dma((9 + p.ng,)),
                            dma((p.nh,)), dma((p.nh,))],
            compiler_params=pltpu.CompilerParams(vmem_limit_bytes=STORE_LIMIT),
            cost_estimate=pl.CostEstimate(flops=60_000_000_000, bytes_accessed=90_000_000, transcendentals=0),
        )(*[pltpu.with_memory_space_constraint(v, pltpu.VMEM) if i not in HBM_KEPT else v for i, v in enumerate(out[:14])],
          w_down)
        z = lax.axis_index('dp')
        got = lax.ppermute(out[14], 'dp', [(1, 0), (2, 3)])
        rows = jnp.where((z == 1) | (z == 2), out[14], got)
        res = [lax.dynamic_update_slice(res[0], rows, (p.first_rows, 0))] + list(res[1:])
        result = []
        for mat in MATS:
            result += [res[mat], res[4 + 2 * mat].reshape(-1), res[5 + 2 * mat].reshape(-1)]
        return tuple(result)

    return jax.shard_map(per_device, mesh=mesh, in_specs=in_specs, out_specs=out_specs, check_vma=False)
```

```python
import functools
import jax
import jax.numpy as jnp
from jax import lax
from jax.experimental import pallas as pl
from jax.experimental.pallas import tpu as pltpu
from jax.sharding import PartitionSpec as P

EPS_ONE = 1e-30
EPS_TWO = 1e-3
MESH = pl.DeviceIdType.MESH
LANES = 128
F32 = jnp.float32
BF16 = jnp.bfloat16
ATTN, GATE, UP, DOWN = range(4)
MATS = (ATTN, GATE, UP, DOWN)
FIRST = {'gate': ('x_mlp', 0), 'attn': ('x_attn', 0), 'up': ('x_mlp', 0), 'h': ('out', 0)}
AHEAD_MID, AHEAD_END = 2, 6
PARTS = 4
LATE_MID, LATE_END = 3, 2
VMEM_LIMIT = 29 * 1024 * 1024
STORE_LIMIT = 29 * 1024 * 1024
UP_KEPT = True
HBM_KEPT = (1,) if UP_KEPT else (1, 2)
DEPTH, WIDE = 6, 6


def look(k, table):
    out = jnp.int32(0)
    for i, v in enumerate(table):
        if v:
            out = jnp.where(k == i, v, out)
    return out


class Plan:
    def __init__(self, x_mlp, dy_gate, h_mlp, dy_out, mesh):
        self.dp, self.col, self.row = mesh.shape['dp'], mesh.shape['col'], mesh.shape['row']
        assert (self.dp, self.col, self.row) == (4, 2, 4)
        self.tok = x_mlp.shape[0]
        self.mc = x_mlp.shape[1]
        self.nc = dy_out.shape[1]
        self.ng = dy_gate.shape[1] // self.nc
        self.nh = h_mlp.shape[1] // self.mc
        self.tq = self.tok // self.row
        self.th = self.tok // self.col
        g = [('gate', i) for i in range(self.ng)]
        u = [('up', i) for i in range(self.ng)]
        h = [('h', i) for i in range(self.nh)]
        one, two = max(1, self.ng // 4), max(2, 3 * self.ng // 4)
        self.order = ([('x_mlp', 0)] + g[:one] + h[:1] + g[one:two] + h[1:2] + g[two:] + [('x_attn', 0), ('attn', 0)]
                      + u + [('out', 0)] + h[2:])
        self.count = len(self.order)
        self.place = {v: k for k, v in enumerate(self.order)}
        self.first_rows = self.mc * 13 // 32 // 8 * 8
        self.n_dy = 2 * self.ng + 2
        self.n_x = self.nh + 2
        self.pieces = max(self.ng, self.nh)
        self.rows = {ATTN: self.mc, GATE: self.mc, UP: self.mc, DOWN: self.mc * self.nh}
        self.cols = {ATTN: self.nc, GATE: self.nc * self.ng, UP: self.nc * self.ng, DOWN: self.nc}
        self.parts = {ATTN: 1, GATE: self.ng, UP: self.ng, DOWN: self.nh}
        base = {'gate': 0, 'up': self.ng, 'out': 2 * self.ng, 'attn': 2 * self.ng + 1, 'x_mlp': 0, 'x_attn': 1, 'h': 2}
        self.dy_table = [1 if n in ('gate', 'up', 'out', 'attn') else 0 for n, _ in self.order]
        self.at_table = [base[n] + i for n, i in self.order]
        self.attn_table = [1 if n in ('x_attn', 'attn') else 0 for n, _ in self.order]
        self.steps = {m: self.schedule(m) for m in (True, False)}
        self.turns = {m: max(max(v.values()) + 1, 3 * self.count) for m, v in self.steps.items()}

    def schedule(self, mid):
        late = LATE_MID if mid else LATE_END
        tasks = []
        for name, mat in (('gate', GATE), ('attn', ATTN), ('up', UP), ('h', DOWN)):
            if name == 'attn' and not mid:
                continue
            for i in range(self.parts[mat]):
                k = self.place[name, i]
                need = [3 * (k + late + 1)] if name != 'h' else [3 * (k + late) if mid else 3 * k + 5]
                if i == 0:
                    need.append(3 * (self.place[FIRST[name]] + late + (name == 'h')))
                tasks.append(((name, i), max(need)))
            stages = {ATTN: (1, 2), DOWN: (1, 2)}.get(mat, (1, 2, 3))
            if mid or mat != DOWN:
                tasks += [(('finish', mat, stage), 0) for stage in stages]
        out, t = {}, 0
        for task, first in tasks:
            t = max(t, first)
            out[task] = t
            t += 1
        return out

    def is_dy(self, k):
        return look(k, self.dy_table) == 1

    def is_attn(self, k):
        return look(k, self.attn_table) == 1

    def at(self, k):
        return look(k, self.at_table)


def gather_kernel(plan, x_attn, dy_attn, x_mlp, dy_gate, dy_up, h_mlp, dy_out, w_attn, w_gate, w_up, w_down,
                  r_attn, c_attn, r_gate, c_gate, r_up, c_up, r_down, c_down, hyper,
                  o_attn, o_gate, o_up, grad, nr_attn, nc_attn, nr_gate, nc_gate, nr_up, nc_up, nr_down, nc_down,
                  al_down, be_down, o_rest, buf_d, buf_x,
                  lhs, tile_x, tile_d, w_buf, r_lanes, r_row, c_sum, a_cols, a_rows, w_sq,
                  b_attn, b_gate, b_up, b_down, *more):
    p = plan
    old_refs = more[:8]
    (rs_attn, rs_gate, rs_up, rs_down, cs_attn, cs_gate, cs_up, cs_down, st_all,
     z_send, z_recv, f_send, f_recv, c_send, c_recv, r1_send, r1_recv, r2_send, r2_recv,
     e_send, e_recv, l_sem, wi_sem, wo_sem, o_sem) = more[8:]
    z, y, r = lax.axis_index('dp'), lax.axis_index('col'), lax.axis_index('row')
    low = z < 2
    mid = (z == 1) | (z == 2)
    end_z = jnp.where(low, 0, 3)
    mate_z = 3 - z
    w_refs = {ATTN: w_attn, GATE: w_gate, UP: w_up, DOWN: w_down}
    old_in = (r_attn, c_attn, r_gate, c_gate, r_up, c_up, r_down, c_down)
    old = {mat: (old_refs[2 * mat], old_refs[2 * mat + 1]) for mat in MATS}
    old_copies = [pltpu.make_async_copy(a, b, o_sem.at[i]) for i, (a, b) in enumerate(zip(old_in, old_refs))]
    new = {ATTN: (nr_attn, nc_attn), GATE: (nr_gate, nc_gate), UP: (nr_up, nc_up), DOWN: (nr_down, nc_down)}
    b_rows = {ATTN: b_attn, GATE: b_gate, UP: b_up, DOWN: b_down}
    rs = {ATTN: rs_attn, GATE: rs_gate, UP: rs_up, DOWN: rs_down}
    cs = {ATTN: cs_attn, GATE: cs_gate, UP: cs_up, DOWN: cs_down}

    def flip_row(v):
        bit0, bit1 = lax.rem(r, 2), lax.div(r, 2)
        if v & 1:
            bit0 = 1 - bit0
        if v & 2:
            bit1 = 1 - bit1
        return bit1 * 2 + bit0

    peers = [(f, v) for f in range(2) for v in range(4) if f or v]
    barrier = pltpu.get_barrier_semaphore()
    for f, v in peers:
        pl.semaphore_signal(barrier, inc=1, device_id=(z, 1 - y if f else y, flip_row(v)), device_id_type=MESH)

    @pl.when(mid)
    def _():
        pl.semaphore_signal(barrier, inc=1, device_id=(end_z, y, r), device_id_type=MESH)
        pl.semaphore_signal(barrier, inc=1, device_id=(mate_z, y, r), device_id_type=MESH)
        pl.semaphore_wait(barrier, len(peers) + 2)

    @pl.when(jnp.logical_not(mid))
    def _():
        pl.semaphore_signal(barrier, inc=1, device_id=(jnp.where(low, 1, 2), y, r), device_id_type=MESH)
        pl.semaphore_wait(barrier, len(peers) + 1)

    my_q = pl.ds(pl.multiple_of(r * p.tq, p.tq), p.tq)
    x_q = pl.ds(pl.multiple_of(flip_row(2) * p.tq, p.tq), p.tq)
    my_h = pl.ds(pl.multiple_of(y * p.th, p.th), p.th)

    def rows_of(dy, part):
        if dy:
            return my_q
        if part is None:
            return my_h
        size = p.th // PARTS
        return pl.ds(pl.multiple_of(y * p.th + part * size, size), size)

    def line_of(k, part):
        return k if part is None else k + part

    def slot(k, s, dy, part):
        return (buf_d if dy else buf_x).at[p.at(k), s, rows_of(dy, part), :]

    def pass_on(k, dy, part, src, to_z, to_slot, sem):
        line = line_of(k, part)
        return pltpu.make_async_remote_copy(
            src_ref=src, dst_ref=slot(k, to_slot, dy, part), send_sem=z_send.at[line, sem],
            recv_sem=z_recv.at[line, to_slot], device_id=(to_z, y, r), device_id_type=MESH)

    def spread(k, s, dy, part):
        to = (z, y, flip_row(2)) if dy else (z, 1 - y, r)
        line = line_of(k, part)
        return pltpu.make_async_remote_copy(
            src_ref=slot(k, s, dy, part), dst_ref=slot(k, s, dy, part), send_sem=f_send.at[line, s],
            recv_sem=f_recv.at[line, s], device_id=to, device_id_type=MESH)

    def partner(k, which):
        part = buf_d.at[p.at(k), :, x_q if which else my_q, :]
        return pltpu.make_async_remote_copy(
            src_ref=part, dst_ref=part, send_sem=c_send.at[p.at(k), which], recv_sem=c_recv.at[p.at(k), which],
            device_id=(z, y, flip_row(1)), device_id_type=MESH)

    def in_parts(k, go):
        pl.when(k != p.count - 1)(lambda: go(None))

        @pl.when(k == p.count - 1)
        def _():
            pl.loop(0, PARTS)(go)

    def typed(k, go):
        used = mid | jnp.logical_not(p.is_attn(k))
        pl.when(p.is_dy(k) & used)(lambda: go(True, None))
        pl.when(jnp.logical_not(p.is_dy(k)) & used)(lambda: in_parts(k, lambda part: go(False, part)))

    def cut(ref, at, size):
        return ref.at[:, pl.ds(pl.multiple_of(at * size, size), size)]

    def down_rows(ref, i):
        return ref.at[pl.ds(pl.multiple_of(i * p.mc, p.mc), p.mc), :]

    def own_to(k, dy, part, src, end_too, mate_too):
        @pl.when(jnp.logical_not(mid))
        def _():
            pass_on(k, dy, part, src, jnp.where(low, 1, 2), jnp.where(low, 2, 0), 0).start()

        @pl.when(mid)
        def _():
            @pl.when(jnp.logical_not(p.is_attn(k)) & end_too)
            def _():
                pass_on(k, dy, part, src, end_z, jnp.where(low, 0, 2), 0).start()

            @pl.when(mate_too)
            def _():
                pass_on(k, dy, part, src, mate_z, jnp.where(low, 2, 0), 1).start()

    def send_own(k, end_too, mate_too):
        def go(ref, at, size, dy):
            def send(part):
                src = ref.at[rows_of(dy, part), pl.ds(pl.multiple_of(at * size, size), size)]
                own_to(k, dy, part, src, end_too, mate_too)

            if ref is h_mlp:
                in_parts(k, send)
            else:
                send(None)

        for name, ref, dy in (('x_mlp', x_mlp, False), ('gate', dy_gate, True), ('x_attn', x_attn, False),
                              ('attn', dy_attn, True), ('up', dy_up, True), ('out', dy_out, True), ('h', h_mlp, False)):
            at = look(k, [i + 1 if n == name else 0 for n, i in p.order])
            size = p.nc if dy else p.mc
            pl.when(at > 0)(functools.partial(go, ref, at - 1, size, dy))

    def own_first_left(k):
        @pl.when(jnp.logical_not(mid & p.is_attn(k)))
        def _():
            def go(dy, part):
                pass_on(k, dy, part, slot(k, 0, dy, part), z, 0, 0).wait_send()

            pl.when(p.is_dy(k))(lambda: go(True, None))
            pl.when(jnp.logical_not(p.is_dy(k)))(lambda: in_parts(k, lambda part: go(False, part)))

    def arrive(k, e, whole):
        s = jnp.where(low, e, 2 - e)

        def go(dy, part):
            here = slot(k, s, dy, part)
            pass_on(k, dy, part, here, z, s, 0).wait_recv()

            @pl.when(mid & (e == 2))
            def _():
                pass_on(k, dy, part, here, mate_z, 1, 4).start()

            @pl.when(mid & (e < 2) & jnp.logical_not(p.is_attn(k)))
            def _():
                pass_on(k, dy, part, here, end_z, jnp.where(low, s + 1, s - 1), 2 + e).start()

            spread(k, s, dy, part).start()
            if dy and whole:
                pl.when(e == jnp.where(mid, 1, 2))(lambda: partner(k, 0).start())

        typed(k, go)

    def spread_done(k, dy):
        for s in range(p.dp - 1):
            spread(k, s, dy, None).wait_recv()

    def load(src, at, size, buf, index, dst):
        copies = [pltpu.make_async_copy(cut(src, at, size), dst.at[z], l_sem.at[0])]
        for d in range(1, p.dp):
            copies.append(pltpu.make_async_copy(buf.at[index, d - 1], dst.at[lax.rem(z + d, p.dp)], l_sem.at[d]))
        for c in copies:
            c.start()
        for c in copies:
            c.wait()

    step_t = min(256, p.tok)

    def turn(q):
        @pl.loop(0, p.tok // step_t)
        def _(t):
            at = pl.multiple_of(t * step_t, step_t)
            lhs[q, :, pl.ds(at, step_t)] = tile_x[q, pl.ds(at, step_t), :].T

    step_n = min(512, p.nc)
    step_r = min(64, p.mc)

    def lane_sum(v):
        out = v[:, 0:LANES]
        for i in range(1, v.shape[1] // LANES):
            out = out + v[:, i * LANES:(i + 1) * LANES]
        return out

    def product(at, count):
        r_lanes[...] = jnp.zeros_like(r_lanes)

        @pl.loop(0, p.nc // step_n)
        def _(n):
            cols = pl.ds(pl.multiple_of(n * step_n, step_n), step_n)
            grad[at, :, cols] = jnp.dot(lhs[0], tile_d[0, :, cols], preferred_element_type=F32)

            @pl.loop(1, p.dp)
            def _(q):
                grad[at, :, cols] += jnp.dot(lhs[q], tile_d[q, :, cols], preferred_element_type=F32)

            def body(i, acc):
                rows = pl.ds(pl.multiple_of(i * step_r, step_r), step_r)
                block = grad[at, rows, cols]
                sq = block * block + EPS_ONE
                r_lanes[rows, :] += lane_sum(sq)
                return acc + jnp.sum(sq, axis=0, keepdims=True)

            @pl.when(count)
            def _():
                c_sum[at, :, cols] = lax.fori_loop(0, p.mc // step_r, body, jnp.zeros((1, step_n), F32))

    def fold(v):
        v = jnp.reshape(v, (v.shape[0] // 8, 8, LANES))
        while v.shape[0] > 1:
            v = v[:v.shape[0] // 2] + v[v.shape[0] // 2:]
        return v[0]

    def to_row(block):
        return jnp.sum(block.T, axis=0, keepdims=True)

    def get_w(mat, i):
        src = down_rows(w_refs[mat], i) if mat == DOWN else cut(w_refs[mat], i, p.nc)
        return pltpu.make_async_copy(src, w_buf.at[lax.rem(i, 3)], wi_sem.at[lax.rem(i, 3)])

    def put_w(mat, i):
        dst = cut(o_gate if mat == GATE else o_up, i, p.nc)
        return pltpu.make_async_copy(w_buf.at[lax.rem(i, 3)], dst, wo_sem.at[lax.rem(i, 3)])

    def chunk(mat, i):
        count = mid if mat == DOWN else jnp.bool_(True)
        pl.when(count)(lambda: get_w(mat, i).start())
        product(i, count)

        @pl.when(count)
        def _():
            row = to_row(r_lanes[...])
            if mat == DOWN:
                r_row[i] = row
            else:
                r_row[0] = jnp.where(i == 0, row, r_row[0] + row)
            get_w(mat, i).wait()

            def body(n, acc):
                rows = pl.ds(pl.multiple_of(n * step_r, step_r), step_r)
                block = lane_sum(w_buf[lax.rem(i, 3), rows, :] * w_buf[lax.rem(i, 3), rows, :])
                return acc + fold(block)

            w_sq[mat] += lax.fori_loop(0, p.mc // step_r, body, jnp.zeros((8, LANES), F32))

    def first_copies(mat):
        copies = [pltpu.make_async_remote_copy(
            src_ref=rs[mat].at[y], dst_ref=rs[mat].at[y], send_sem=r1_send.at[mat, 0], recv_sem=r1_recv.at[mat, 0],
            device_id=(z, 1 - y, r), device_id_type=MESH)]
        for v in range(1, 4):
            copies.append(pltpu.make_async_remote_copy(
                src_ref=cs[mat].at[r], dst_ref=cs[mat].at[r], send_sem=r1_send.at[mat, v],
                recv_sem=r1_recv.at[mat, v], device_id=(z, y, flip_row(v)), device_id_type=MESH))
        return copies

    def second_copies(mat):
        me = y * 4 + r
        return [pltpu.make_async_remote_copy(
            src_ref=st_all.at[mat, me], dst_ref=st_all.at[mat, me], send_sem=r2_send.at[mat, f * 4 + v],
            recv_sem=r2_recv.at[mat, f * 4 + v], device_id=(z, 1 - y if f else y, flip_row(v)), device_id_type=MESH)
            for f, v in peers]

    def scale_rows(mat):
        return p.rows[mat] * p.row, p.cols[mat] * p.col

    blocks = p.mc // step_r

    def factors(mat, i, n):
        rows = pl.ds(pl.multiple_of(n * step_r, step_r), step_r)
        if mat == DOWN:
            return rows, a_cols[i, rows, :], b_rows[mat].at[:, :]
        return rows, a_cols[0, rows, :], b_rows[mat].at[:, pl.ds(pl.multiple_of(i * p.nc, p.nc), p.nc)]

    def finish_first(mat):
        parts = p.parts[mat]
        if mat != DOWN:
            for i in range(min(2, parts)):
                get_w(mat, jnp.int32(i)).start()
        if mat == DOWN:
            block = c_sum[0]
            for i in range(parts):
                rs[mat][y, :, i * p.mc:(i + 1) * p.mc] = r_row[i]
                if i:
                    block = block + c_sum[i]
            cs[mat][r] = block
        else:
            rs[mat][y] = r_row[0]
            for i in range(parts):
                cs[mat][r, :, i * p.nc:(i + 1) * p.nc] = c_sum[i]
        for c in first_copies(mat):
            c.start()

    def finish_second(mat):
        beta_two = hyper[0]
        m_total, n_total = scale_rows(mat)
        parts = p.parts[mat]
        for c in first_copies(mat):
            c.wait_recv()
        r_new = beta_two * old[mat][0][...] + (1.0 - beta_two) * ((rs[mat][0] + rs[mat][1]) / n_total)
        c_all = ((cs[mat][0] + cs[mat][1]) + cs[mat][2]) + cs[mat][3]
        c_new = beta_two * old[mat][1][...] + (1.0 - beta_two) * (c_all / m_total)
        new[mat][0][...] = r_new
        new[mat][1][...] = c_new
        t_own = jnp.sum(r_new, axis=1, keepdims=True)
        a_row = jnp.sqrt(t_own) / jnp.sqrt(r_new)
        b_rows[mat][...] = 1.0 / jnp.sqrt(c_new)
        if mat == DOWN:
            a_rows[...] = a_row
        for i in range(parts if mat == DOWN else 1):
            a_cols[i] = jnp.broadcast_to(a_row[:, i * p.mc:(i + 1) * p.mc], (LANES, p.mc)).T

        def add_up(j, acc):
            i, n = lax.div(j, blocks), lax.rem(j, blocks)
            rows, a_block, b_ref = factors(mat, i, n)
            for c in range(0, p.nc, LANES):
                upd = grad[i, rows, c:c + LANES] * a_block * b_ref[:, c:c + LANES]
                acc = acc + fold(upd * upd)
            return acc

        u_part = lax.fori_loop(0, parts * blocks, add_up, jnp.zeros((8, LANES), F32))

        def spot(v):
            return jnp.broadcast_to(jnp.sum(jnp.sum(v, axis=1, keepdims=True), axis=0, keepdims=True), (8, LANES))

        me = y * 4 + r
        st_all[mat, me, 0] = spot(u_part)
        st_all[mat, me, 1] = spot(w_sq[mat])
        st_all[mat, me, 2] = jnp.broadcast_to(t_own, (8, LANES))
        for c in second_copies(mat):
            c.start()

    def finish_third(mat):
        rho_step, clip_thr = hyper[1], hyper[2]
        m_total, n_total = scale_rows(mat)
        me = y * 4 + r
        for c in second_copies(mat):
            c.wait_recv()
        t_all = st_all[mat, 0, 2]
        for i in range(1, p.row):
            t_all = t_all + st_all[mat, i, 2]
        u_all = st_all[mat, 0, 0] * (t_all / st_all[mat, 0, 2])
        w_all = st_all[mat, 0, 1]
        for i in range(1, p.row * p.col):
            u_all = u_all + st_all[mat, i, 0] * (t_all / st_all[mat, i, 2])
            w_all = w_all + st_all[mat, i, 1]
        upd_rms = jnp.sqrt(u_all / (m_total * n_total))
        w_rms = jnp.sqrt(w_all / (m_total * n_total))
        scale = rho_step * jnp.maximum(EPS_TWO, w_rms) / jnp.maximum(1.0, upd_rms / clip_thr)
        scale = scale * jnp.sqrt(t_all / st_all[mat, me, 2])
        b_rows[mat][...] = b_rows[mat][...] * scale[0:1, 0:1]

    def renew(mat, low_i, high_i):
        parts = p.parts[mat]

        @pl.loop(low_i, high_i)
        def _(i):
            at = lax.rem(i, 3)
            get_w(mat, i).wait()

            @pl.loop(0, blocks)
            def _(n):
                rows, a_block, b_ref = factors(mat, i, n)
                for c in range(0, p.nc, LANES):
                    cols = slice(c, c + LANES)
                    fresh = w_buf[at, rows, cols] - grad[i, rows, cols] * a_block * b_ref[:, cols]
                    if mat == ATTN:
                        o_attn[rows, cols] = fresh
                    elif mat == UP and UP_KEPT:
                        o_up[i, rows, cols] = fresh
                    else:
                        w_buf[at, rows, cols] = fresh

            if mat == ATTN:
                put_rest().start()
                put_rest().wait()
            if mat == GATE or (mat == UP and not UP_KEPT):
                put_w(mat, i).start()
                pl.when(i >= 1)(lambda: put_w(mat, i - 1).wait())
            pl.when(i + 2 < parts)(lambda: get_w(mat, i + 2).start())

        if (mat == GATE or (mat == UP and not UP_KEPT)) and high_i == parts:
            put_w(mat, jnp.int32(parts - 1)).wait()

    def put_rest():
        return pltpu.make_async_copy(o_attn.at[pl.ds(p.first_rows, p.mc - p.first_rows), :], o_rest, wo_sem.at[0])

    def finish(mat, stage):
        parts = p.parts[mat]
        half = parts // 2 if parts > 1 else parts
        if stage == 1:
            finish_second(mat)
        elif stage == 2:
            finish_third(mat)
            if mat == DOWN:
                al_down[...] = a_rows[...]
                be_down[...] = b_rows[mat][...]
                for c in to_end_down():
                    c.start()
            else:
                renew(mat, 0, half)
        else:
            renew(mat, half, parts)

    def take_x(src, at, k, waits=True):
        copies = [(pltpu.make_async_copy(cut(src, at, p.mc), tile_x.at[z], l_sem.at[0]), z)]
        copies[0][0].start()
        for e in range(p.dp - 1):
            s = jnp.where(low, e, 2 - e)
            if src is h_mlp:
                in_parts(k, lambda part: spread(k, s, False, part).wait_recv())
            elif waits:
                spread(k, s, False, None).wait_recv()
            q = lax.rem(z + s + 1, p.dp)
            copies.append((pltpu.make_async_copy(buf_x.at[p.at(k), s], tile_x.at[q], l_sem.at[e + 1]), q))
            copies[-1][0].start()
            copies[-2][0].wait()
            turn(copies[-2][1])
        copies[-1][0].wait()
        turn(copies[-1][1])

    def got(name, i):
        k = look(i, [p.place[name, j] for j in range(sum(1 for n, _ in p.order if n == name))])
        partner(k, 0).wait_recv()
        partner(k, 1).wait_recv()
        return k

    def use_gate(i):
        pl.when(i == 0)(lambda: take_x(x_mlp, 0, jnp.int32(p.place['x_mlp', 0])))
        k = got('gate', i)
        load(dy_gate, i, p.nc, buf_d, p.at(k), tile_d)
        chunk(GATE, i)
        pl.when(i == p.parts[GATE] - 1)(lambda: finish_first(GATE))

    def use_attn(i):
        take_x(x_attn, 0, jnp.int32(p.place['x_attn', 0]))
        k = got('attn', i)
        load(dy_attn, 0, p.nc, buf_d, p.at(k), tile_d)
        chunk(ATTN, i)
        finish_first(ATTN)

    def use_up(i):
        pl.when(i == 0)(lambda: take_x(x_mlp, 0, jnp.int32(p.place['x_mlp', 0]), False))
        k = got('up', i)
        load(dy_up, i, p.nc, buf_d, p.at(k), tile_d)
        chunk(UP, i)
        pl.when(i == p.parts[UP] - 1)(lambda: finish_first(UP))

    def use_out():
        k = got('out', jnp.int32(0))
        load(dy_out, 0, p.nc, buf_d, p.at(k), tile_d)

    def use_h(i):
        pl.when(i == 0)(use_out)
        take_x(h_mlp, i, look(i, [p.place['h', j] for j in range(p.nh)]))
        chunk(DOWN, i)
        pl.when((i == p.parts[DOWN] - 1) & mid)(lambda: finish_first(DOWN))

    def work(t):
        for name, use in (('gate', use_gate), ('attn', use_attn), ('up', use_up), ('h', use_h)):
            at = jnp.int32(0)
            for i in range(sum(1 for n, _ in p.order if n == name)):
                when_mid = p.steps[True].get((name, i), -1)
                when_end = p.steps[False].get((name, i), -1)
                at = jnp.where(t == jnp.where(mid, when_mid, when_end), i + 1, at)
            pl.when(at > 0)(functools.partial(use, at - 1))
        for mat in MATS:
            for stage in (1, 2, 3):
                when_mid = p.steps[True].get(('finish', mat, stage), -1)
                when_end = p.steps[False].get(('finish', mat, stage), -1)
                if when_mid >= 0:
                    pl.when(t == jnp.where(mid, when_mid, when_end))(functools.partial(finish, mat, stage))

    def sent_to_end(refs, first):
        return [pltpu.make_async_remote_copy(
            src_ref=ref, dst_ref=ref, send_sem=e_send.at[first + i], recv_sem=e_recv.at[first + i],
            device_id=(end_z, y, r), device_id_type=MESH) for i, ref in enumerate(refs)]

    def to_end():
        return sent_to_end((nr_attn, nc_attn, o_attn.at[pl.ds(0, p.first_rows), :]), 0)

    def to_end_down():
        return sent_to_end((nr_down, nc_down, al_down, be_down), 3)

    def sends_left(k):
        def go(dy, part):
            some = slot(k, 0, dy, part)

            @pl.when(mid)
            def _():
                pass_on(k, dy, part, some, z, 0, 1).wait_send()
                pass_on(k, dy, part, some, z, 0, 4).wait_send()

                @pl.when(jnp.logical_not(p.is_attn(k)))
                def _():
                    pass_on(k, dy, part, some, z, 0, 2).wait_send()
                    pass_on(k, dy, part, some, z, 0, 3).wait_send()

            for s in range(p.dp - 1):
                spread(k, s, dy, part).wait_send()
            if dy:
                partner(k, 0).wait_send()
                partner(k, 1).wait_send()

        typed(k, go)

    w_sq[...] = jnp.zeros_like(w_sq)
    ahead = jnp.where(mid, AHEAD_MID, AHEAD_END)

    @pl.loop(0, AHEAD_END)
    def _(k):
        pl.when(k < jnp.where(mid, AHEAD_MID + 1, AHEAD_END))(lambda: send_own(k, True, k < AHEAD_MID))

    @pl.when(mid)
    def _():
        arrive(jnp.int32(0), jnp.int32(2), False)

    for c in old_copies:
        c.start()
    for c in old_copies:
        c.wait()

    @pl.when(jnp.logical_not(mid))
    def _():
        for k in range(AHEAD_MID):
            arrive(jnp.int32(k), jnp.int32(0), False)

    last_mid, last_end = p.turns[True], p.turns[False] - 1

    def one_turn(t):
        d, turn_no = lax.div(t, 3), lax.rem(t, 3)
        pl.when((turn_no == 0) & (d >= 1) & (d < p.count))(lambda: own_first_left(d - 1))
        early = jnp.where(mid, jnp.where(turn_no == 0, 1, 0), jnp.where(turn_no == 2, AHEAD_MID, 0))
        e = lax.rem(turn_no + jnp.where(mid, 2, 1), 3)
        k = d + early
        pl.when(k < p.count)(lambda: arrive(k, e, True))

        @pl.when(turn_no == 2)
        def _():
            pl.when(d + ahead < p.count)(lambda: send_own(d + ahead, d > 0, True))

            @pl.when((d == p.count - 1) & mid)
            def _():
                for c in to_end():
                    c.start()

            k = d - jnp.where(mid, LATE_MID, LATE_END)

            @pl.when((k >= 0) & (k < p.count) & p.is_dy(k) & (mid | jnp.logical_not(p.is_attn(k))))
            def _():
                spread_done(k, True)
                partner(k, 1).start()

        work(t)
        first_end = 3 * p.count - 3
        assert first_end not in p.steps[False].values()

        @pl.when((mid & (t == last_mid)) | (jnp.logical_not(mid) & ((t == first_end) | (t == last_end))))
        def _():
            @pl.loop(0, p.count)
            def _(k):
                pl.when(mid | ((t == first_end) == (k < p.count - 2)))(lambda: sends_left(k))

    @pl.loop(0, last_mid + 1)
    def _(t):
        pl.when(mid | (t < p.turns[False]))(lambda: one_turn(t))

    own_first_left(jnp.int32(p.count - 1))
    for mat in (GATE, UP):
        for c in first_copies(mat) + second_copies(mat):
            c.wait_send()

    @pl.when(mid)
    def _():
        for mat in (ATTN, DOWN):
            for c in first_copies(mat) + second_copies(mat):
                c.wait_send()
        for c in to_end() + to_end_down():
            c.wait_send()

    @pl.when(jnp.logical_not(mid))
    def _():
        for c in to_end() + to_end_down():
            c.wait_recv()


def store_kernel(plan, o_attn, o_gate, o_up, grad, *refs):
    p = plan
    stats, al_down, be_down, w_old, (w_attn, w_gate, w_up, w_down), outs = (
        refs[:8], refs[8], refs[9], refs[10], refs[11:15], refs[15:23])
    bounce, w_buf, a_col, in_sem, out_sem, s_sem, wi_sem, wo_sem = refs[23:]
    depth, wide = bounce.shape[0], w_buf.shape[0]

    def cut(ref, i):
        return ref.at[:, i * p.nc:(i + 1) * p.nc]

    def rows(ref, i):
        return ref.at[i * p.mc:(i + 1) * p.mc, :]

    through = [(cut(o_gate, i), cut(w_gate, i)) for i in range(p.ng)]
    if not UP_KEPT:
        through += [(cut(o_up, i), cut(w_up, i)) for i in range(p.ng)]
    loads = [pltpu.make_async_copy(a, bounce.at[i % depth], in_sem.at[i]) for i, (a, _) in enumerate(through)]
    puts = [pltpu.make_async_copy(bounce.at[i % depth], b, out_sem.at[i]) for i, (_, b) in enumerate(through)]
    w_in = [pltpu.make_async_copy(rows(w_old, i), w_buf.at[i % wide], wi_sem.at[i]) for i in range(p.nh)]
    w_out = [pltpu.make_async_copy(w_buf.at[i % wide], rows(w_down, i), wo_sem.at[i]) for i in range(p.nh)]
    for i in range(wide // 2):
        w_in[i].start()
    for c in loads[:depth]:
        c.start()
    copies = [pltpu.make_async_copy(a, b, s_sem.at[i]) for i, (a, b) in enumerate(zip(stats, outs))]
    copies.append(pltpu.make_async_copy(o_attn, w_attn, s_sem.at[8]))
    if UP_KEPT:
        copies += [pltpu.make_async_copy(o_up.at[i], cut(w_up, i), s_sem.at[9 + i]) for i in range(p.ng)]
    for c in copies:
        c.start()
    step_r = min(64, p.mc)
    per = -(-len(through) // p.nh)
    done = 0
    for i in range(p.nh):
        a_col[...] = jnp.broadcast_to(al_down[:, i * p.mc:(i + 1) * p.mc], (LANES, p.mc)).T
        w_in[i].wait()

        @pl.loop(0, p.mc // step_r)
        def _(n):
            at = pl.ds(pl.multiple_of(n * step_r, step_r), step_r)
            a_block = a_col[at, :]
            for c in range(0, p.nc, LANES):
                cols = slice(c, c + LANES)
                w_buf[i % wide, at, cols] = w_buf[i % wide, at, cols] - grad[i, at, cols] * a_block * be_down[:, cols]

        w_out[i].start()
        again = i + wide // 2
        if again < p.nh:
            if again >= wide:
                w_out[again - wide].wait()
            w_in[again].start()
        for j in range(done, min(len(through), done + per)):
            loads[j].wait()
            puts[j].start()
            again = j + depth // 2
            if depth <= again < len(through):
                puts[again - depth].wait()
                loads[again].start()
        done += per
    for i in range(max(0, p.nh - wide), p.nh):
        if i + wide >= p.nh:
            w_out[i].wait()
    for i in range(max(0, len(through) - depth), len(through)):
        puts[i].wait()
    for c in copies:
        c.wait()


def solution(mesh):
    act_spec = P('dp', 'row')
    grad_spec = P('dp', 'col')
    w_spec = P('row', 'col')
    row_spec = P('row')
    col_spec = P('col')
    in_specs = (act_spec, grad_spec, act_spec, grad_spec, grad_spec, act_spec, grad_spec,
                w_spec, w_spec, w_spec, w_spec,
                row_spec, col_spec, row_spec, col_spec, row_spec, col_spec, row_spec, col_spec, P())
    out_specs = (w_spec, row_spec, col_spec) * 4

    def per_device(x_attn, dy_attn, x_mlp, dy_gate, dy_up, h_mlp, dy_out, w_attn, w_gate, w_up, w_down,
                   r_attn, c_attn, r_gate, c_gate, r_up, c_up, r_down, c_down, hyper_params):
        p = Plan(x_mlp, dy_gate, h_mlp, dy_out, mesh)
        stats = [v.reshape(1, -1) for v in (r_attn, c_attn, r_gate, c_gate, r_up, c_up, r_down, c_down)]
        any_spec = pl.BlockSpec(memory_space=pl.ANY)
        vmem_spec = pl.BlockSpec(memory_space=pltpu.VMEM)
        up_spec = vmem_spec if UP_KEPT else any_spec
        row_shapes = []
        for mat in MATS:
            row_shapes += [jax.ShapeDtypeStruct((1, p.rows[mat]), F32), jax.ShapeDtypeStruct((1, p.cols[mat]), F32)]
        w_shapes = [jax.ShapeDtypeStruct((p.rows[mat], p.cols[mat]), F32) for mat in MATS]
        o_shapes = [pltpu.VMEM((p.mc, p.nc), F32), w_shapes[GATE],
                    pltpu.VMEM((p.ng, p.mc, p.nc), F32) if UP_KEPT else w_shapes[UP],
                    pltpu.VMEM((p.pieces, p.mc, p.nc), F32)]
        bufs = [jax.ShapeDtypeStruct((p.n_dy, p.dp - 1, p.tok, p.nc), BF16),
                jax.ShapeDtypeStruct((p.n_x, p.dp - 1, p.tok, p.mc), BF16)]
        rest = jax.ShapeDtypeStruct((p.mc - p.first_rows, p.nc), F32)
        dma = pltpu.SemaphoreType.DMA
        lines = p.count + PARTS - 1
        scratch = [
            pltpu.VMEM((p.dp, p.mc, p.tok), BF16),
            pltpu.VMEM((p.dp, p.tok, p.mc), BF16),
            pltpu.VMEM((p.dp, p.tok, p.nc), BF16),
            pltpu.VMEM((3, p.mc, p.nc), F32),
            pltpu.VMEM((p.mc, LANES), F32),
            pltpu.VMEM((p.pieces, 1, p.mc), F32),
            pltpu.VMEM((p.pieces, 1, p.nc), F32),
            pltpu.VMEM((p.nh, p.mc, LANES), F32),
            pltpu.VMEM((1, p.rows[DOWN]), F32),
            pltpu.VMEM((4, 8, LANES), F32),
        ]
        scratch += [pltpu.VMEM((1, p.cols[mat]), F32) for mat in MATS]
        scratch += [pltpu.VMEM(v.shape, F32) for v in row_shapes]
        scratch += [pltpu.VMEM((2, 1, p.rows[mat]), F32) for mat in MATS]
        scratch += [pltpu.VMEM((4, 1, p.cols[mat]), F32) for mat in MATS]
        scratch += [
            pltpu.VMEM((4, 8, 3, 8, LANES), F32),
            dma((lines, 5)), dma((lines, p.dp - 1)),
            dma((lines, p.dp - 1)), dma((lines, p.dp - 1)),
            dma((p.n_dy, 2)), dma((p.n_dy, 2)),
            dma((4, 4)), dma((4, 4)), dma((4, 8)), dma((4, 8)),
            dma((7,)), dma((7,)),
            dma((p.dp,)), dma((3,)), dma((3,)), dma((8,)),
        ]
        out = pl.pallas_call(
            functools.partial(gather_kernel, p),
            out_shape=o_shapes + [pltpu.VMEM(v.shape, F32) for v in row_shapes + row_shapes[-2:]] + [rest] + bufs,
            in_specs=[any_spec] * 19 + [pl.BlockSpec(memory_space=pltpu.SMEM)],
            out_specs=[vmem_spec, any_spec, up_spec, vmem_spec] + [vmem_spec] * 10 + [any_spec] * 3,
            scratch_shapes=scratch,
            compiler_params=pltpu.CompilerParams(collective_id=0, has_side_effects=True, vmem_limit_bytes=VMEM_LIMIT),
        )(x_attn, dy_attn, x_mlp, dy_gate, dy_up, h_mlp, dy_out, w_attn, w_gate, w_up, w_down, *stats, hyper_params)
        res = pl.pallas_call(
            functools.partial(store_kernel, p),
            out_shape=w_shapes + row_shapes,
            in_specs=[vmem_spec, any_spec, up_spec, vmem_spec] + [vmem_spec] * 10 + [any_spec],
            out_specs=[any_spec] * 12,
            scratch_shapes=[pltpu.VMEM((DEPTH, p.mc, p.nc), F32), pltpu.VMEM((WIDE, p.mc, p.nc), F32),
                            pltpu.VMEM((p.mc, LANES), F32), dma((2 * p.ng,)), dma((2 * p.ng,)), dma((9 + p.ng,)),
                            dma((p.nh,)), dma((p.nh,))],
            compiler_params=pltpu.CompilerParams(vmem_limit_bytes=STORE_LIMIT),
            cost_estimate=pl.CostEstimate(flops=60_000_000_000, bytes_accessed=90_000_000, transcendentals=0),
        )(*[pltpu.with_memory_space_constraint(v, pltpu.VMEM) if i not in HBM_KEPT else v for i, v in enumerate(out[:14])],
          w_down)
        z = lax.axis_index('dp')
        got = lax.ppermute(out[14], 'dp', [(1, 0), (2, 3)])
        rows = jnp.where((z == 1) | (z == 2), out[14], got)
        res = [lax.dynamic_update_slice(res[0], rows, (p.first_rows, 0))] + list(res[1:])
        result = []
        for mat in MATS:
            result += [res[mat], res[4 + 2 * mat].reshape(-1), res[5 + 2 * mat].reshape(-1)]
        return tuple(result)

    return jax.shard_map(per_device, mesh=mesh, in_specs=in_specs, out_specs=out_specs, check_vma=False)
```

```python
import functools
import jax
import jax.numpy as jnp
from jax import lax
from jax.experimental import pallas as pl
from jax.experimental.pallas import tpu as pltpu
from jax.sharding import PartitionSpec as P

EPS_ONE = 1e-30
EPS_TWO = 1e-3
MESH = pl.DeviceIdType.MESH
LANES = 128
F32 = jnp.float32
BF16 = jnp.bfloat16
ATTN, GATE, UP, DOWN = range(4)
MATS = (ATTN, GATE, UP, DOWN)
FIRST = {'gate': ('x_mlp', 0), 'attn': ('x_attn', 0), 'up': ('x_mlp', 0), 'h': ('out', 0)}
AHEAD_MID, AHEAD_END = 2, 6
PARTS = 4
LATE_MID, LATE_END = 3, 2
VMEM_LIMIT = 29 * 1024 * 1024
STORE_LIMIT = 29 * 1024 * 1024
UP_KEPT = True
HBM_KEPT = (1,) if UP_KEPT else (1, 2)
DEPTH, WIDE = 6, 6
END_H = {1: 2, 2: 3}


def look(k, table):
    out = jnp.int32(0)
    for i, v in enumerate(table):
        if v:
            out = jnp.where(k == i, v, out)
    return out


class Plan:
    def __init__(self, x_mlp, dy_gate, h_mlp, dy_out, mesh):
        self.dp, self.col, self.row = mesh.shape['dp'], mesh.shape['col'], mesh.shape['row']
        assert (self.dp, self.col, self.row) == (4, 2, 4)
        self.tok = x_mlp.shape[0]
        self.mc = x_mlp.shape[1]
        self.nc = dy_out.shape[1]
        self.ng = dy_gate.shape[1] // self.nc
        self.nh = h_mlp.shape[1] // self.mc
        self.tq = self.tok // self.row
        self.th = self.tok // self.col
        g = [('gate', i) for i in range(self.ng)]
        u = [('up', i) for i in range(self.ng)]
        h = [('h', i) for i in range(self.nh)]
        one, two = max(1, self.ng // 4), max(2, 3 * self.ng // 4)
        self.order = ([('x_mlp', 0)] + g[:one] + h[:1] + g[one:two] + h[1:2] + g[two:] + [('x_attn', 0), ('attn', 0)]
                      + u + [('out', 0)] + h[2:])
        self.count = len(self.order)
        self.place = {v: k for k, v in enumerate(self.order)}
        self.first_rows = self.mc * 11 // 32 // 8 * 8
        self.n_dy = 2 * self.ng + 2
        self.n_x = self.nh + 2
        self.pieces = max(self.ng, self.nh)
        self.rows = {ATTN: self.mc, GATE: self.mc, UP: self.mc, DOWN: self.mc * self.nh}
        self.cols = {ATTN: self.nc, GATE: self.nc * self.ng, UP: self.nc * self.ng, DOWN: self.nc}
        self.parts = {ATTN: 1, GATE: self.ng, UP: self.ng, DOWN: self.nh}
        base = {'gate': 0, 'up': self.ng, 'out': 2 * self.ng, 'attn': 2 * self.ng + 1, 'x_mlp': 0, 'x_attn': 1, 'h': 2}
        self.dy_table = [1 if n in ('gate', 'up', 'out', 'attn') else 0 for n, _ in self.order]
        self.at_table = [base[n] + i for n, i in self.order]
        self.attn_table = [1 if n in ('x_attn', 'attn') else 0 for n, _ in self.order]
        self.steps = {m: self.schedule(m) for m in (True, False)}
        self.turns = {m: max(max(v.values()) + 1, 3 * self.count) for m, v in self.steps.items()}

    def schedule(self, mid):
        late = LATE_MID if mid else LATE_END
        tasks = []
        for name, mat in (('gate', GATE), ('attn', ATTN), ('up', UP), ('h', DOWN)):
            if name == 'attn' and not mid:
                continue
            for i in range(self.parts[mat]):
                k = self.place[name, i]
                need = [3 * (k + late + 1)] if name != 'h' else [3 * (k + late) if mid else 3 * k + END_H.get(self.count - k, 5)]
                if i == 0:
                    need.append(3 * (self.place[FIRST[name]] + late + (name == 'h')))
                tasks.append(((name, i), max(need)))
            stages = {ATTN: (1, 2), DOWN: (1, 2)}.get(mat, (1, 2, 3))
            if mid or mat != DOWN:
                tasks += [(('finish', mat, stage), 0) for stage in stages]
        out, t = {}, 0
        for task, first in tasks:
            t = max(t, first)
            out[task] = t
            t += 1
        return out

    def is_dy(self, k):
        return look(k, self.dy_table) == 1

    def is_attn(self, k):
        return look(k, self.attn_table) == 1

    def at(self, k):
        return look(k, self.at_table)


def gather_kernel(plan, x_attn, dy_attn, x_mlp, dy_gate, dy_up, h_mlp, dy_out, w_attn, w_gate, w_up, w_down,
                  r_attn, c_attn, r_gate, c_gate, r_up, c_up, r_down, c_down, hyper,
                  o_attn, o_gate, o_up, grad, nr_attn, nc_attn, nr_gate, nc_gate, nr_up, nc_up, nr_down, nc_down,
                  al_down, be_down, o_rest, buf_d, buf_x,
                  lhs, tile_x, tile_d, w_buf, r_lanes, r_row, c_sum, a_cols, a_rows, w_sq,
                  b_attn, b_gate, b_up, b_down, *more):
    p = plan
    old_refs = more[:8]
    (rs_attn, rs_gate, rs_up, rs_down, cs_attn, cs_gate, cs_up, cs_down, st_all,
     z_send, z_recv, f_send, f_recv, c_send, c_recv, r1_send, r1_recv, r2_send, r2_recv,
     e_send, e_recv, l_sem, wi_sem, wo_sem, o_sem) = more[8:]
    z, y, r = lax.axis_index('dp'), lax.axis_index('col'), lax.axis_index('row')
    low = z < 2
    mid = (z == 1) | (z == 2)
    end_z = jnp.where(low, 0, 3)
    mate_z = 3 - z
    w_refs = {ATTN: w_attn, GATE: w_gate, UP: w_up, DOWN: w_down}
    old_in = (r_attn, c_attn, r_gate, c_gate, r_up, c_up, r_down, c_down)
    old = {mat: (old_refs[2 * mat], old_refs[2 * mat + 1]) for mat in MATS}
    old_copies = [pltpu.make_async_copy(a, b, o_sem.at[i]) for i, (a, b) in enumerate(zip(old_in, old_refs))]
    new = {ATTN: (nr_attn, nc_attn), GATE: (nr_gate, nc_gate), UP: (nr_up, nc_up), DOWN: (nr_down, nc_down)}
    b_rows = {ATTN: b_attn, GATE: b_gate, UP: b_up, DOWN: b_down}
    rs = {ATTN: rs_attn, GATE: rs_gate, UP: rs_up, DOWN: rs_down}
    cs = {ATTN: cs_attn, GATE: cs_gate, UP: cs_up, DOWN: cs_down}

    def flip_row(v):
        bit0, bit1 = lax.rem(r, 2), lax.div(r, 2)
        if v & 1:
            bit0 = 1 - bit0
        if v & 2:
            bit1 = 1 - bit1
        return bit1 * 2 + bit0

    peers = [(f, v) for f in range(2) for v in range(4) if f or v]
    barrier = pltpu.get_barrier_semaphore()
    for f, v in peers:
        pl.semaphore_signal(barrier, inc=1, device_id=(z, 1 - y if f else y, flip_row(v)), device_id_type=MESH)

    @pl.when(mid)
    def _():
        pl.semaphore_signal(barrier, inc=1, device_id=(end_z, y, r), device_id_type=MESH)
        pl.semaphore_signal(barrier, inc=1, device_id=(mate_z, y, r), device_id_type=MESH)
        pl.semaphore_wait(barrier, len(peers) + 2)

    @pl.when(jnp.logical_not(mid))
    def _():
        pl.semaphore_signal(barrier, inc=1, device_id=(jnp.where(low, 1, 2), y, r), device_id_type=MESH)
        pl.semaphore_wait(barrier, len(peers) + 1)

    my_q = pl.ds(pl.multiple_of(r * p.tq, p.tq), p.tq)
    x_q = pl.ds(pl.multiple_of(flip_row(2) * p.tq, p.tq), p.tq)
    my_h = pl.ds(pl.multiple_of(y * p.th, p.th), p.th)

    def rows_of(dy, part):
        if dy:
            return my_q
        if part is None:
            return my_h
        size = p.th // PARTS
        return pl.ds(pl.multiple_of(y * p.th + part * size, size), size)

    def line_of(k, part):
        return k if part is None else k + part

    def slot(k, s, dy, part):
        return (buf_d if dy else buf_x).at[p.at(k), s, rows_of(dy, part), :]

    def pass_on(k, dy, part, src, to_z, to_slot, sem):
        line = line_of(k, part)
        return pltpu.make_async_remote_copy(
            src_ref=src, dst_ref=slot(k, to_slot, dy, part), send_sem=z_send.at[line, sem],
            recv_sem=z_recv.at[line, to_slot], device_id=(to_z, y, r), device_id_type=MESH)

    def spread(k, s, dy, part):
        to = (z, y, flip_row(2)) if dy else (z, 1 - y, r)
        line = line_of(k, part)
        return pltpu.make_async_remote_copy(
            src_ref=slot(k, s, dy, part), dst_ref=slot(k, s, dy, part), send_sem=f_send.at[line, s],
            recv_sem=f_recv.at[line, s], device_id=to, device_id_type=MESH)

    def partner(k, which):
        part = buf_d.at[p.at(k), :, x_q if which else my_q, :]
        return pltpu.make_async_remote_copy(
            src_ref=part, dst_ref=part, send_sem=c_send.at[p.at(k), which], recv_sem=c_recv.at[p.at(k), which],
            device_id=(z, y, flip_row(1)), device_id_type=MESH)

    def in_parts(k, go):
        pl.when(k != p.count - 1)(lambda: go(None))

        @pl.when(k == p.count - 1)
        def _():
            pl.loop(0, PARTS)(go)

    def typed(k, go):
        used = mid | jnp.logical_not(p.is_attn(k))
        pl.when(p.is_dy(k) & used)(lambda: go(True, None))
        pl.when(jnp.logical_not(p.is_dy(k)) & used)(lambda: in_parts(k, lambda part: go(False, part)))

    def cut(ref, at, size):
        return ref.at[:, pl.ds(pl.multiple_of(at * size, size), size)]

    def down_rows(ref, i):
        return ref.at[pl.ds(pl.multiple_of(i * p.mc, p.mc), p.mc), :]

    def own_to(k, dy, part, src, end_too, mate_too):
        @pl.when(jnp.logical_not(mid))
        def _():
            pass_on(k, dy, part, src, jnp.where(low, 1, 2), jnp.where(low, 2, 0), 0).start()

        @pl.when(mid)
        def _():
            @pl.when(jnp.logical_not(p.is_attn(k)) & end_too)
            def _():
                pass_on(k, dy, part, src, end_z, jnp.where(low, 0, 2), 0).start()

            @pl.when(mate_too)
            def _():
                pass_on(k, dy, part, src, mate_z, jnp.where(low, 2, 0), 1).start()

    def send_own(k, end_too, mate_too):
        def go(ref, at, size, dy):
            def send(part):
                src = ref.at[rows_of(dy, part), pl.ds(pl.multiple_of(at * size, size), size)]
                own_to(k, dy, part, src, end_too, mate_too)

            if ref is h_mlp:
                in_parts(k, send)
            else:
                send(None)

        for name, ref, dy in (('x_mlp', x_mlp, False), ('gate', dy_gate, True), ('x_attn', x_attn, False),
                              ('attn', dy_attn, True), ('up', dy_up, True), ('out', dy_out, True), ('h', h_mlp, False)):
            at = look(k, [i + 1 if n == name else 0 for n, i in p.order])
            size = p.nc if dy else p.mc
            pl.when(at > 0)(functools.partial(go, ref, at - 1, size, dy))

    def own_first_left(k):
        @pl.when(jnp.logical_not(mid & p.is_attn(k)))
        def _():
            def go(dy, part):
                pass_on(k, dy, part, slot(k, 0, dy, part), z, 0, 0).wait_send()

            pl.when(p.is_dy(k))(lambda: go(True, None))
            pl.when(jnp.logical_not(p.is_dy(k)))(lambda: in_parts(k, lambda part: go(False, part)))

    def arrive(k, e, whole):
        s = jnp.where(low, e, 2 - e)

        def go(dy, part):
            here = slot(k, s, dy, part)
            pass_on(k, dy, part, here, z, s, 0).wait_recv()

            @pl.when(mid & (e == 2))
            def _():
                pass_on(k, dy, part, here, mate_z, 1, 4).start()

            @pl.when(mid & (e < 2) & jnp.logical_not(p.is_attn(k)))
            def _():
                pass_on(k, dy, part, here, end_z, jnp.where(low, s + 1, s - 1), 2 + e).start()

            spread(k, s, dy, part).start()
            if dy and whole:
                pl.when(e == jnp.where(mid, 1, 2))(lambda: partner(k, 0).start())

        typed(k, go)

    def spread_done(k, dy):
        for s in range(p.dp - 1):
            spread(k, s, dy, None).wait_recv()

    def load(src, at, size, buf, index, dst):
        copies = [pltpu.make_async_copy(cut(src, at, size), dst.at[z], l_sem.at[0])]
        for d in range(1, p.dp):
            copies.append(pltpu.make_async_copy(buf.at[index, d - 1], dst.at[lax.rem(z + d, p.dp)], l_sem.at[d]))
        for c in copies:
            c.start()
        for c in copies:
            c.wait()

    step_t = min(256, p.tok)

    def turn(q):
        @pl.loop(0, p.tok // step_t)
        def _(t):
            at = pl.multiple_of(t * step_t, step_t)
            lhs[q, :, pl.ds(at, step_t)] = tile_x[q, pl.ds(at, step_t), :].T

    step_n = min(512, p.nc)
    step_r = min(64, p.mc)

    def lane_sum(v):
        out = v[:, 0:LANES]
        for i in range(1, v.shape[1] // LANES):
            out = out + v[:, i * LANES:(i + 1) * LANES]
        return out

    def product(at, count):
        r_lanes[...] = jnp.zeros_like(r_lanes)

        @pl.loop(0, p.nc // step_n)
        def _(n):
            cols = pl.ds(pl.multiple_of(n * step_n, step_n), step_n)
            grad[at, :, cols] = jnp.dot(lhs[0], tile_d[0, :, cols], preferred_element_type=F32)

            @pl.loop(1, p.dp)
            def _(q):
                grad[at, :, cols] += jnp.dot(lhs[q], tile_d[q, :, cols], preferred_element_type=F32)

            def body(i, acc):
                rows = pl.ds(pl.multiple_of(i * step_r, step_r), step_r)
                block = grad[at, rows, cols]
                sq = block * block + EPS_ONE
                r_lanes[rows, :] += lane_sum(sq)
                return acc + jnp.sum(sq, axis=0, keepdims=True)

            @pl.when(count)
            def _():
                c_sum[at, :, cols] = lax.fori_loop(0, p.mc // step_r, body, jnp.zeros((1, step_n), F32))

    def fold(v):
        v = jnp.reshape(v, (v.shape[0] // 8, 8, LANES))
        while v.shape[0] > 1:
            v = v[:v.shape[0] // 2] + v[v.shape[0] // 2:]
        return v[0]

    def to_row(block):
        return jnp.sum(block.T, axis=0, keepdims=True)

    def get_w(mat, i):
        src = down_rows(w_refs[mat], i) if mat == DOWN else cut(w_refs[mat], i, p.nc)
        return pltpu.make_async_copy(src, w_buf.at[lax.rem(i, 3)], wi_sem.at[lax.rem(i, 3)])

    def put_w(mat, i):
        dst = cut(o_gate if mat == GATE else o_up, i, p.nc)
        return pltpu.make_async_copy(w_buf.at[lax.rem(i, 3)], dst, wo_sem.at[lax.rem(i, 3)])

    def chunk(mat, i):
        count = mid if mat == DOWN else jnp.bool_(True)
        pl.when(count)(lambda: get_w(mat, i).start())
        product(i, count)

        @pl.when(count)
        def _():
            row = to_row(r_lanes[...])
            if mat == DOWN:
                r_row[i] = row
            else:
                r_row[0] = jnp.where(i == 0, row, r_row[0] + row)
            get_w(mat, i).wait()

            def body(n, acc):
                rows = pl.ds(pl.multiple_of(n * step_r, step_r), step_r)
                block = lane_sum(w_buf[lax.rem(i, 3), rows, :] * w_buf[lax.rem(i, 3), rows, :])
                return acc + fold(block)

            w_sq[mat] += lax.fori_loop(0, p.mc // step_r, body, jnp.zeros((8, LANES), F32))

    def first_copies(mat):
        copies = [pltpu.make_async_remote_copy(
            src_ref=rs[mat].at[y], dst_ref=rs[mat].at[y], send_sem=r1_send.at[mat, 0], recv_sem=r1_recv.at[mat, 0],
            device_id=(z, 1 - y, r), device_id_type=MESH)]
        for v in range(1, 4):
            copies.append(pltpu.make_async_remote_copy(
                src_ref=cs[mat].at[r], dst_ref=cs[mat].at[r], send_sem=r1_send.at[mat, v],
                recv_sem=r1_recv.at[mat, v], device_id=(z, y, flip_row(v)), device_id_type=MESH))
        return copies

    def second_copies(mat):
        me = y * 4 + r
        return [pltpu.make_async_remote_copy(
            src_ref=st_all.at[mat, me], dst_ref=st_all.at[mat, me], send_sem=r2_send.at[mat, f * 4 + v],
            recv_sem=r2_recv.at[mat, f * 4 + v], device_id=(z, 1 - y if f else y, flip_row(v)), device_id_type=MESH)
            for f, v in peers]

    def scale_rows(mat):
        return p.rows[mat] * p.row, p.cols[mat] * p.col

    blocks = p.mc // step_r

    def factors(mat, i, n):
        rows = pl.ds(pl.multiple_of(n * step_r, step_r), step_r)
        if mat == DOWN:
            return rows, a_cols[i, rows, :], b_rows[mat].at[:, :]
        return rows, a_cols[0, rows, :], b_rows[mat].at[:, pl.ds(pl.multiple_of(i * p.nc, p.nc), p.nc)]

    def finish_first(mat):
        parts = p.parts[mat]
        if mat != DOWN:
            for i in range(min(2, parts)):
                get_w(mat, jnp.int32(i)).start()
        if mat == DOWN:
            block = c_sum[0]
            for i in range(parts):
                rs[mat][y, :, i * p.mc:(i + 1) * p.mc] = r_row[i]
                if i:
                    block = block + c_sum[i]
            cs[mat][r] = block
        else:
            rs[mat][y] = r_row[0]
            for i in range(parts):
                cs[mat][r, :, i * p.nc:(i + 1) * p.nc] = c_sum[i]
        for c in first_copies(mat):
            c.start()

    def finish_second(mat):
        beta_two = hyper[0]
        m_total, n_total = scale_rows(mat)
        parts = p.parts[mat]
        for c in first_copies(mat):
            c.wait_recv()
        r_new = beta_two * old[mat][0][...] + (1.0 - beta_two) * ((rs[mat][0] + rs[mat][1]) / n_total)
        c_all = ((cs[mat][0] + cs[mat][1]) + cs[mat][2]) + cs[mat][3]
        c_new = beta_two * old[mat][1][...] + (1.0 - beta_two) * (c_all / m_total)
        new[mat][0][...] = r_new
        new[mat][1][...] = c_new
        t_own = jnp.sum(r_new, axis=1, keepdims=True)
        a_row = jnp.sqrt(t_own) / jnp.sqrt(r_new)
        b_rows[mat][...] = 1.0 / jnp.sqrt(c_new)
        if mat == DOWN:
            a_rows[...] = a_row
        for i in range(parts if mat == DOWN else 1):
            a_cols[i] = jnp.broadcast_to(a_row[:, i * p.mc:(i + 1) * p.mc], (LANES, p.mc)).T

        def add_up(j, acc):
            i, n = lax.div(j, blocks), lax.rem(j, blocks)
            rows, a_block, b_ref = factors(mat, i, n)
            for c in range(0, p.nc, LANES):
                upd = grad[i, rows, c:c + LANES] * a_block * b_ref[:, c:c + LANES]
                acc = acc + fold(upd * upd)
            return acc

        u_part = lax.fori_loop(0, parts * blocks, add_up, jnp.zeros((8, LANES), F32))

        def spot(v):
            return jnp.broadcast_to(jnp.sum(jnp.sum(v, axis=1, keepdims=True), axis=0, keepdims=True), (8, LANES))

        me = y * 4 + r
        st_all[mat, me, 0] = spot(u_part)
        st_all[mat, me, 1] = spot(w_sq[mat])
        st_all[mat, me, 2] = jnp.broadcast_to(t_own, (8, LANES))
        for c in second_copies(mat):
            c.start()

    def finish_third(mat):
        rho_step, clip_thr = hyper[1], hyper[2]
        m_total, n_total = scale_rows(mat)
        me = y * 4 + r
        for c in second_copies(mat):
            c.wait_recv()
        t_all = st_all[mat, 0, 2]
        for i in range(1, p.row):
            t_all = t_all + st_all[mat, i, 2]
        u_all = st_all[mat, 0, 0] * (t_all / st_all[mat, 0, 2])
        w_all = st_all[mat, 0, 1]
        for i in range(1, p.row * p.col):
            u_all = u_all + st_all[mat, i, 0] * (t_all / st_all[mat, i, 2])
            w_all = w_all + st_all[mat, i, 1]
        upd_rms = jnp.sqrt(u_all / (m_total * n_total))
        w_rms = jnp.sqrt(w_all / (m_total * n_total))
        scale = rho_step * jnp.maximum(EPS_TWO, w_rms) / jnp.maximum(1.0, upd_rms / clip_thr)
        scale = scale * jnp.sqrt(t_all / st_all[mat, me, 2])
        b_rows[mat][...] = b_rows[mat][...] * scale[0:1, 0:1]

    def renew(mat, low_i, high_i):
        parts = p.parts[mat]

        @pl.loop(low_i, high_i)
        def _(i):
            at = lax.rem(i, 3)
            get_w(mat, i).wait()

            @pl.loop(0, blocks)
            def _(n):
                rows, a_block, b_ref = factors(mat, i, n)
                for c in range(0, p.nc, LANES):
                    cols = slice(c, c + LANES)
                    fresh = w_buf[at, rows, cols] - grad[i, rows, cols] * a_block * b_ref[:, cols]
                    if mat == ATTN:
                        o_attn[rows, cols] = fresh
                    elif mat == UP and UP_KEPT:
                        o_up[i, rows, cols] = fresh
                    else:
                        w_buf[at, rows, cols] = fresh

            if mat == ATTN:
                put_rest().start()
                put_rest().wait()
            if mat == GATE or (mat == UP and not UP_KEPT):
                put_w(mat, i).start()
                pl.when(i >= 1)(lambda: put_w(mat, i - 1).wait())
            pl.when(i + 2 < parts)(lambda: get_w(mat, i + 2).start())

        if (mat == GATE or (mat == UP and not UP_KEPT)) and high_i == parts:
            put_w(mat, jnp.int32(parts - 1)).wait()

    def put_rest():
        return pltpu.make_async_copy(o_attn.at[pl.ds(p.first_rows, p.mc - p.first_rows), :], o_rest, wo_sem.at[0])

    def finish(mat, stage):
        parts = p.parts[mat]
        half = parts // 2 if parts > 1 else parts
        if stage == 1:
            finish_second(mat)
        elif stage == 2:
            finish_third(mat)
            if mat == DOWN:
                al_down[...] = a_rows[...]
                be_down[...] = b_rows[mat][...]
                for c in to_end_down():
                    c.start()
            else:
                renew(mat, 0, half)
        else:
            renew(mat, half, parts)

    def take_x(src, at, k, waits=True):
        copies = [(pltpu.make_async_copy(cut(src, at, p.mc), tile_x.at[z], l_sem.at[0]), z)]
        copies[0][0].start()
        for e in range(p.dp - 1):
            s = jnp.where(low, e, 2 - e)
            if src is h_mlp:
                in_parts(k, lambda part: spread(k, s, False, part).wait_recv())
            elif waits:
                spread(k, s, False, None).wait_recv()
            q = lax.rem(z + s + 1, p.dp)
            copies.append((pltpu.make_async_copy(buf_x.at[p.at(k), s], tile_x.at[q], l_sem.at[e + 1]), q))
            copies[-1][0].start()
            copies[-2][0].wait()
            turn(copies[-2][1])
        copies[-1][0].wait()
        turn(copies[-1][1])

    def got(name, i):
        k = look(i, [p.place[name, j] for j in range(sum(1 for n, _ in p.order if n == name))])
        partner(k, 0).wait_recv()
        partner(k, 1).wait_recv()
        return k

    def use_gate(i):
        pl.when(i == 0)(lambda: take_x(x_mlp, 0, jnp.int32(p.place['x_mlp', 0])))
        k = got('gate', i)
        load(dy_gate, i, p.nc, buf_d, p.at(k), tile_d)
        chunk(GATE, i)
        pl.when(i == p.parts[GATE] - 1)(lambda: finish_first(GATE))

    def use_attn(i):
        take_x(x_attn, 0, jnp.int32(p.place['x_attn', 0]))
        k = got('attn', i)
        load(dy_attn, 0, p.nc, buf_d, p.at(k), tile_d)
        chunk(ATTN, i)
        finish_first(ATTN)

    def use_up(i):
        pl.when(i == 0)(lambda: take_x(x_mlp, 0, jnp.int32(p.place['x_mlp', 0]), False))
        k = got('up', i)
        load(dy_up, i, p.nc, buf_d, p.at(k), tile_d)
        chunk(UP, i)
        pl.when(i == p.parts[UP] - 1)(lambda: finish_first(UP))

    def use_out():
        k = got('out', jnp.int32(0))
        load(dy_out, 0, p.nc, buf_d, p.at(k), tile_d)

    def use_h(i):
        pl.when(i == 0)(use_out)
        take_x(h_mlp, i, look(i, [p.place['h', j] for j in range(p.nh)]))
        chunk(DOWN, i)
        pl.when((i == p.parts[DOWN] - 1) & mid)(lambda: finish_first(DOWN))

    def work(t):
        for name, use in (('gate', use_gate), ('attn', use_attn), ('up', use_up), ('h', use_h)):
            at = jnp.int32(0)
            for i in range(sum(1 for n, _ in p.order if n == name)):
                when_mid = p.steps[True].get((name, i), -1)
                when_end = p.steps[False].get((name, i), -1)
                at = jnp.where(t == jnp.where(mid, when_mid, when_end), i + 1, at)
            pl.when(at > 0)(functools.partial(use, at - 1))
        for mat in MATS:
            for stage in (1, 2, 3):
                when_mid = p.steps[True].get(('finish', mat, stage), -1)
                when_end = p.steps[False].get(('finish', mat, stage), -1)
                if when_mid >= 0:
                    pl.when(t == jnp.where(mid, when_mid, when_end))(functools.partial(finish, mat, stage))

    def sent_to_end(refs, first):
        return [pltpu.make_async_remote_copy(
            src_ref=ref, dst_ref=ref, send_sem=e_send.at[first + i], recv_sem=e_recv.at[first + i],
            device_id=(end_z, y, r), device_id_type=MESH) for i, ref in enumerate(refs)]

    def to_end():
        return sent_to_end((nr_attn, nc_attn, o_attn.at[pl.ds(0, p.first_rows), :]), 0)

    def to_end_down():
        return sent_to_end((nr_down, nc_down, al_down, be_down), 3)

    def sends_left(k):
        def go(dy, part):
            some = slot(k, 0, dy, part)

            @pl.when(mid)
            def _():
                pass_on(k, dy, part, some, z, 0, 1).wait_send()
                pass_on(k, dy, part, some, z, 0, 4).wait_send()

                @pl.when(jnp.logical_not(p.is_attn(k)))
                def _():
                    pass_on(k, dy, part, some, z, 0, 2).wait_send()
                    pass_on(k, dy, part, some, z, 0, 3).wait_send()

            for s in range(p.dp - 1):
                spread(k, s, dy, part).wait_send()
            if dy:
                partner(k, 0).wait_send()
                partner(k, 1).wait_send()

        typed(k, go)

    w_sq[...] = jnp.zeros_like(w_sq)
    ahead = jnp.where(mid, AHEAD_MID, AHEAD_END)

    @pl.loop(0, AHEAD_END)
    def _(k):
        pl.when(k < jnp.where(mid, AHEAD_MID + 1, AHEAD_END))(lambda: send_own(k, True, k < AHEAD_MID))

    @pl.when(mid)
    def _():
        arrive(jnp.int32(0), jnp.int32(2), False)

    for c in old_copies:
        c.start()
    for c in old_copies:
        c.wait()

    @pl.when(jnp.logical_not(mid))
    def _():
        for k in range(AHEAD_MID):
            arrive(jnp.int32(k), jnp.int32(0), False)

    last_mid, last_end = p.turns[True], p.turns[False] - 1

    def one_turn(t):
        d, turn_no = lax.div(t, 3), lax.rem(t, 3)
        pl.when((turn_no == 0) & (d >= 1) & (d < p.count))(lambda: own_first_left(d - 1))
        late_own = d == p.count - 2
        near = jnp.where(late_own, 1, jnp.where(d == p.count - 3, p.count, AHEAD_MID))
        early = jnp.where(mid, jnp.where(turn_no == 0, 1, 0), jnp.where(turn_no == 2, near, 0))
        e = lax.rem(turn_no + jnp.where(mid, 2, 1), 3)
        k = d + early
        pl.when(k < p.count)(lambda: arrive(k, e, True))

        @pl.when(turn_no == 2)
        def _():
            own = d + jnp.where(mid, near, AHEAD_END)
            pl.when(own < p.count)(lambda: send_own(own, d > 0, True))

            @pl.when((d == p.count - 1) & mid)
            def _():
                for c in to_end():
                    c.start()

            k = d - jnp.where(mid, LATE_MID, LATE_END)

            @pl.when((k >= 0) & (k < p.count) & p.is_dy(k) & (mid | jnp.logical_not(p.is_attn(k))))
            def _():
                spread_done(k, True)
                partner(k, 1).start()

        work(t)
        first_end = max(set(range(3 * p.count - 4)) - set(p.steps[False].values()))

        @pl.when((mid & (t == last_mid)) | (jnp.logical_not(mid) & ((t == first_end) | (t == last_end))))
        def _():
            @pl.loop(0, p.count)
            def _(k):
                pl.when(mid | ((t == first_end) == (k < p.count - 2)))(lambda: sends_left(k))

    @pl.loop(0, last_mid + 1)
    def _(t):
        pl.when(mid | (t < p.turns[False]))(lambda: one_turn(t))

    own_first_left(jnp.int32(p.count - 1))
    for mat in (GATE, UP):
        for c in first_copies(mat) + second_copies(mat):
            c.wait_send()

    @pl.when(mid)
    def _():
        for mat in (ATTN, DOWN):
            for c in first_copies(mat) + second_copies(mat):
                c.wait_send()
        for c in to_end() + to_end_down():
            c.wait_send()

    @pl.when(jnp.logical_not(mid))
    def _():
        for c in to_end() + to_end_down():
            c.wait_recv()


def store_kernel(plan, o_attn, o_gate, o_up, grad, *refs):
    p = plan
    stats, al_down, be_down, w_old, (w_attn, w_gate, w_up, w_down), outs = (
        refs[:8], refs[8], refs[9], refs[10], refs[11:15], refs[15:23])
    bounce, w_buf, a_col, in_sem, out_sem, s_sem, wi_sem, wo_sem = refs[23:]
    depth, wide = bounce.shape[0], w_buf.shape[0]

    def cut(ref, i):
        return ref.at[:, i * p.nc:(i + 1) * p.nc]

    def rows(ref, i):
        return ref.at[i * p.mc:(i + 1) * p.mc, :]

    through = [(cut(o_gate, i), cut(w_gate, i)) for i in range(p.ng)]
    if not UP_KEPT:
        through += [(cut(o_up, i), cut(w_up, i)) for i in range(p.ng)]
    loads = [pltpu.make_async_copy(a, bounce.at[i % depth], in_sem.at[i]) for i, (a, _) in enumerate(through)]
    puts = [pltpu.make_async_copy(bounce.at[i % depth], b, out_sem.at[i]) for i, (_, b) in enumerate(through)]
    w_in = [pltpu.make_async_copy(rows(w_old, i), w_buf.at[i % wide], wi_sem.at[i]) for i in range(p.nh)]
    w_out = [pltpu.make_async_copy(w_buf.at[i % wide], rows(w_down, i), wo_sem.at[i]) for i in range(p.nh)]
    for i in range(wide // 2):
        w_in[i].start()
    for c in loads[:depth]:
        c.start()
    copies = [pltpu.make_async_copy(a, b, s_sem.at[i]) for i, (a, b) in enumerate(zip(stats, outs))]
    copies.append(pltpu.make_async_copy(o_attn, w_attn, s_sem.at[8]))
    if UP_KEPT:
        copies += [pltpu.make_async_copy(o_up.at[i], cut(w_up, i), s_sem.at[9 + i]) for i in range(p.ng)]
    for c in copies:
        c.start()
    step_r = min(64, p.mc)
    per = -(-len(through) // p.nh)
    done = 0
    for i in range(p.nh):
        a_col[...] = jnp.broadcast_to(al_down[:, i * p.mc:(i + 1) * p.mc], (LANES, p.mc)).T
        w_in[i].wait()

        @pl.loop(0, p.mc // step_r)
        def _(n):
            at = pl.ds(pl.multiple_of(n * step_r, step_r), step_r)
            a_block = a_col[at, :]
            for c in range(0, p.nc, LANES):
                cols = slice(c, c + LANES)
                w_buf[i % wide, at, cols] = w_buf[i % wide, at, cols] - grad[i, at, cols] * a_block * be_down[:, cols]

        w_out[i].start()
        again = i + wide // 2
        if again < p.nh:
            if again >= wide:
                w_out[again - wide].wait()
            w_in[again].start()
        for j in range(done, min(len(through), done + per)):
            loads[j].wait()
            puts[j].start()
            again = j + depth // 2
            if depth <= again < len(through):
                puts[again - depth].wait()
                loads[again].start()
        done += per
    for i in range(max(0, p.nh - wide), p.nh):
        if i + wide >= p.nh:
            w_out[i].wait()
    for i in range(max(0, len(through) - depth), len(through)):
        puts[i].wait()
    for c in copies:
        c.wait()


def solution(mesh):
    act_spec = P('dp', 'row')
    grad_spec = P('dp', 'col')
    w_spec = P('row', 'col')
    row_spec = P('row')
    col_spec = P('col')
    in_specs = (act_spec, grad_spec, act_spec, grad_spec, grad_spec, act_spec, grad_spec,
                w_spec, w_spec, w_spec, w_spec,
                row_spec, col_spec, row_spec, col_spec, row_spec, col_spec, row_spec, col_spec, P())
    out_specs = (w_spec, row_spec, col_spec) * 4

    def per_device(x_attn, dy_attn, x_mlp, dy_gate, dy_up, h_mlp, dy_out, w_attn, w_gate, w_up, w_down,
                   r_attn, c_attn, r_gate, c_gate, r_up, c_up, r_down, c_down, hyper_params):
        p = Plan(x_mlp, dy_gate, h_mlp, dy_out, mesh)
        stats = [v.reshape(1, -1) for v in (r_attn, c_attn, r_gate, c_gate, r_up, c_up, r_down, c_down)]
        any_spec = pl.BlockSpec(memory_space=pl.ANY)
        vmem_spec = pl.BlockSpec(memory_space=pltpu.VMEM)
        up_spec = vmem_spec if UP_KEPT else any_spec
        row_shapes = []
        for mat in MATS:
            row_shapes += [jax.ShapeDtypeStruct((1, p.rows[mat]), F32), jax.ShapeDtypeStruct((1, p.cols[mat]), F32)]
        w_shapes = [jax.ShapeDtypeStruct((p.rows[mat], p.cols[mat]), F32) for mat in MATS]
        o_shapes = [pltpu.VMEM((p.mc, p.nc), F32), w_shapes[GATE],
                    pltpu.VMEM((p.ng, p.mc, p.nc), F32) if UP_KEPT else w_shapes[UP],
                    pltpu.VMEM((p.pieces, p.mc, p.nc), F32)]
        bufs = [jax.ShapeDtypeStruct((p.n_dy, p.dp - 1, p.tok, p.nc), BF16),
                jax.ShapeDtypeStruct((p.n_x, p.dp - 1, p.tok, p.mc), BF16)]
        rest = jax.ShapeDtypeStruct((p.mc - p.first_rows, p.nc), F32)
        dma = pltpu.SemaphoreType.DMA
        lines = p.count + PARTS - 1
        scratch = [
            pltpu.VMEM((p.dp, p.mc, p.tok), BF16),
            pltpu.VMEM((p.dp, p.tok, p.mc), BF16),
            pltpu.VMEM((p.dp, p.tok, p.nc), BF16),
            pltpu.VMEM((3, p.mc, p.nc), F32),
            pltpu.VMEM((p.mc, LANES), F32),
            pltpu.VMEM((p.pieces, 1, p.mc), F32),
            pltpu.VMEM((p.pieces, 1, p.nc), F32),
            pltpu.VMEM((p.nh, p.mc, LANES), F32),
            pltpu.VMEM((1, p.rows[DOWN]), F32),
            pltpu.VMEM((4, 8, LANES), F32),
        ]
        scratch += [pltpu.VMEM((1, p.cols[mat]), F32) for mat in MATS]
        scratch += [pltpu.VMEM(v.shape, F32) for v in row_shapes]
        scratch += [pltpu.VMEM((2, 1, p.rows[mat]), F32) for mat in MATS]
        scratch += [pltpu.VMEM((4, 1, p.cols[mat]), F32) for mat in MATS]
        scratch += [
            pltpu.VMEM((4, 8, 3, 8, LANES), F32),
            dma((lines, 5)), dma((lines, p.dp - 1)),
            dma((lines, p.dp - 1)), dma((lines, p.dp - 1)),
            dma((p.n_dy, 2)), dma((p.n_dy, 2)),
            dma((4, 4)), dma((4, 4)), dma((4, 8)), dma((4, 8)),
            dma((7,)), dma((7,)),
            dma((p.dp,)), dma((3,)), dma((3,)), dma((8,)),
        ]
        out = pl.pallas_call(
            functools.partial(gather_kernel, p),
            out_shape=o_shapes + [pltpu.VMEM(v.shape, F32) for v in row_shapes + row_shapes[-2:]] + [rest] + bufs,
            in_specs=[any_spec] * 19 + [pl.BlockSpec(memory_space=pltpu.SMEM)],
            out_specs=[vmem_spec, any_spec, up_spec, vmem_spec] + [vmem_spec] * 10 + [any_spec] * 3,
            scratch_shapes=scratch,
            compiler_params=pltpu.CompilerParams(collective_id=0, has_side_effects=True, vmem_limit_bytes=VMEM_LIMIT),
        )(x_attn, dy_attn, x_mlp, dy_gate, dy_up, h_mlp, dy_out, w_attn, w_gate, w_up, w_down, *stats, hyper_params)
        res = pl.pallas_call(
            functools.partial(store_kernel, p),
            out_shape=w_shapes + row_shapes,
            in_specs=[vmem_spec, any_spec, up_spec, vmem_spec] + [vmem_spec] * 10 + [any_spec],
            out_specs=[any_spec] * 12,
            scratch_shapes=[pltpu.VMEM((DEPTH, p.mc, p.nc), F32), pltpu.VMEM((WIDE, p.mc, p.nc), F32),
                            pltpu.VMEM((p.mc, LANES), F32), dma((2 * p.ng,)), dma((2 * p.ng,)), dma((9 + p.ng,)),
                            dma((p.nh,)), dma((p.nh,))],
            compiler_params=pltpu.CompilerParams(vmem_limit_bytes=STORE_LIMIT),
            cost_estimate=pl.CostEstimate(flops=60_000_000_000, bytes_accessed=90_000_000, transcendentals=0),
        )(*[pltpu.with_memory_space_constraint(v, pltpu.VMEM) if i not in HBM_KEPT else v for i, v in enumerate(out[:14])],
          w_down)
        z = lax.axis_index('dp')
        got = lax.ppermute(out[14], 'dp', [(1, 0), (2, 3)])
        rows = jnp.where((z == 1) | (z == 2), out[14], got)
        res = [lax.dynamic_update_slice(res[0], rows, (p.first_rows, 0))] + list(res[1:])
        result = []
        for mat in MATS:
            result += [res[mat], res[4 + 2 * mat].reshape(-1), res[5 + 2 * mat].reshape(-1)]
        return tuple(result)

    return jax.shard_map(per_device, mesh=mesh, in_specs=in_specs, out_specs=out_specs, check_vma=False)
```

```python
import functools
import jax
import jax.numpy as jnp
from jax import lax
from jax.experimental import pallas as pl
from jax.experimental.pallas import tpu as pltpu
from jax.sharding import PartitionSpec as P

EPS_ONE = 1e-30
EPS_TWO = 1e-3
MESH = pl.DeviceIdType.MESH
LANES = 128
F32 = jnp.float32
BF16 = jnp.bfloat16
ATTN, GATE, UP, DOWN = range(4)
MATS = (ATTN, GATE, UP, DOWN)
FIRST = {'gate': ('x_mlp', 0), 'attn': ('x_attn', 0), 'up': ('x_mlp', 0), 'h': ('out', 0)}
AHEAD_MID, AHEAD_END = 2, 6
PARTS = 4
LATE_MID, LATE_END = 3, 2
VMEM_LIMIT = 29 * 1024 * 1024
STORE_LIMIT = 29 * 1024 * 1024
UP_KEPT = True
HBM_KEPT = (1,) if UP_KEPT else (1, 2)
DEPTH, WIDE = 6, 6


def look(k, table):
    out = jnp.int32(0)
    for i, v in enumerate(table):
        if v:
            out = jnp.where(k == i, v, out)
    return out


class Plan:
    def __init__(self, x_mlp, dy_gate, h_mlp, dy_out, mesh):
        self.dp, self.col, self.row = mesh.shape['dp'], mesh.shape['col'], mesh.shape['row']
        assert (self.dp, self.col, self.row) == (4, 2, 4)
        self.tok = x_mlp.shape[0]
        self.mc = x_mlp.shape[1]
        self.nc = dy_out.shape[1]
        self.ng = dy_gate.shape[1] // self.nc
        self.nh = h_mlp.shape[1] // self.mc
        self.tq = self.tok // self.row
        self.th = self.tok // self.col
        g = [('gate', i) for i in range(self.ng)]
        u = [('up', i) for i in range(self.ng)]
        h = [('h', i) for i in range(self.nh)]
        one, two = max(1, self.ng // 4), max(2, 3 * self.ng // 4)
        self.order = ([('x_mlp', 0)] + g[:one] + h[:1] + g[one:two] + h[1:2] + g[two:] + [('x_attn', 0), ('attn', 0)]
                      + u + [('out', 0)] + h[2:])
        self.count = len(self.order)
        self.place = {v: k for k, v in enumerate(self.order)}
        self.first_rows = self.mc * 13 // 32 // 8 * 8
        self.n_dy = 2 * self.ng + 2
        self.n_x = self.nh + 2
        self.pieces = max(self.ng, self.nh)
        self.rows = {ATTN: self.mc, GATE: self.mc, UP: self.mc, DOWN: self.mc * self.nh}
        self.cols = {ATTN: self.nc, GATE: self.nc * self.ng, UP: self.nc * self.ng, DOWN: self.nc}
        self.parts = {ATTN: 1, GATE: self.ng, UP: self.ng, DOWN: self.nh}
        base = {'gate': 0, 'up': self.ng, 'out': 2 * self.ng, 'attn': 2 * self.ng + 1, 'x_mlp': 0, 'x_attn': 1, 'h': 2}
        self.dy_table = [1 if n in ('gate', 'up', 'out', 'attn') else 0 for n, _ in self.order]
        self.at_table = [base[n] + i for n, i in self.order]
        self.attn_table = [1 if n in ('x_attn', 'attn') else 0 for n, _ in self.order]
        self.steps = {m: self.schedule(m) for m in (True, False)}
        self.turns = {m: max(max(v.values()) + 1, 3 * self.count) for m, v in self.steps.items()}

    def schedule(self, mid):
        late = LATE_MID if mid else LATE_END
        tasks = []
        for name, mat in (('gate', GATE), ('attn', ATTN), ('up', UP), ('h', DOWN)):
            if name == 'attn' and not mid:
                continue
            for i in range(self.parts[mat]):
                k = self.place[name, i]
                need = [3 * (k + late + 1)] if name != 'h' else [3 * (k + late) if mid else 3 * k + (3 if k == self.count - 1 else 5)]
                if i == 0:
                    need.append(3 * (self.place[FIRST[name]] + late + (name == 'h')))
                tasks.append(((name, i), max(need)))
            stages = {ATTN: (1, 2), DOWN: (1, 2)}.get(mat, (1, 2, 3))
            if mid or mat != DOWN:
                tasks += [(('finish', mat, stage), 0) for stage in stages]
        out, t = {}, 0
        for task, first in tasks:
            t = max(t, first)
            out[task] = t
            t += 1
        return out

    def is_dy(self, k):
        return look(k, self.dy_table) == 1

    def is_attn(self, k):
        return look(k, self.attn_table) == 1

    def at(self, k):
        return look(k, self.at_table)


def gather_kernel(plan, x_attn, dy_attn, x_mlp, dy_gate, dy_up, h_mlp, dy_out, w_attn, w_gate, w_up, w_down,
                  r_attn, c_attn, r_gate, c_gate, r_up, c_up, r_down, c_down, hyper,
                  o_attn, o_gate, o_up, grad, nr_attn, nc_attn, nr_gate, nc_gate, nr_up, nc_up, nr_down, nc_down,
                  al_down, be_down, o_rest, buf_d, buf_x,
                  lhs, tile_x, tile_d, w_buf, r_lanes, r_row, c_sum, a_cols, a_rows, w_sq,
                  b_attn, b_gate, b_up, b_down, *more):
    p = plan
    old_refs = more[:8]
    (rs_attn, rs_gate, rs_up, rs_down, cs_attn, cs_gate, cs_up, cs_down, st_all,
     z_send, z_recv, f_send, f_recv, c_send, c_recv, r1_send, r1_recv, r2_send, r2_recv,
     e_send, e_recv, l_sem, wi_sem, wo_sem, o_sem) = more[8:]
    z, y, r = lax.axis_index('dp'), lax.axis_index('col'), lax.axis_index('row')
    low = z < 2
    mid = (z == 1) | (z == 2)
    end_z = jnp.where(low, 0, 3)
    mate_z = 3 - z
    w_refs = {ATTN: w_attn, GATE: w_gate, UP: w_up, DOWN: w_down}
    old_in = (r_attn, c_attn, r_gate, c_gate, r_up, c_up, r_down, c_down)
    old = {mat: (old_refs[2 * mat], old_refs[2 * mat + 1]) for mat in MATS}
    old_copies = [pltpu.make_async_copy(a, b, o_sem.at[i]) for i, (a, b) in enumerate(zip(old_in, old_refs))]
    new = {ATTN: (nr_attn, nc_attn), GATE: (nr_gate, nc_gate), UP: (nr_up, nc_up), DOWN: (nr_down, nc_down)}
    b_rows = {ATTN: b_attn, GATE: b_gate, UP: b_up, DOWN: b_down}
    rs = {ATTN: rs_attn, GATE: rs_gate, UP: rs_up, DOWN: rs_down}
    cs = {ATTN: cs_attn, GATE: cs_gate, UP: cs_up, DOWN: cs_down}

    def flip_row(v):
        bit0, bit1 = lax.rem(r, 2), lax.div(r, 2)
        if v & 1:
            bit0 = 1 - bit0
        if v & 2:
            bit1 = 1 - bit1
        return bit1 * 2 + bit0

    peers = [(f, v) for f in range(2) for v in range(4) if f or v]
    barrier = pltpu.get_barrier_semaphore()
    for f, v in peers:
        pl.semaphore_signal(barrier, inc=1, device_id=(z, 1 - y if f else y, flip_row(v)), device_id_type=MESH)

    @pl.when(mid)
    def _():
        pl.semaphore_signal(barrier, inc=1, device_id=(end_z, y, r), device_id_type=MESH)
        pl.semaphore_signal(barrier, inc=1, device_id=(mate_z, y, r), device_id_type=MESH)
        pl.semaphore_wait(barrier, len(peers) + 2)

    @pl.when(jnp.logical_not(mid))
    def _():
        pl.semaphore_signal(barrier, inc=1, device_id=(jnp.where(low, 1, 2), y, r), device_id_type=MESH)
        pl.semaphore_wait(barrier, len(peers) + 1)

    my_q = pl.ds(pl.multiple_of(r * p.tq, p.tq), p.tq)
    x_q = pl.ds(pl.multiple_of(flip_row(2) * p.tq, p.tq), p.tq)
    my_h = pl.ds(pl.multiple_of(y * p.th, p.th), p.th)

    def rows_of(dy, part):
        if dy:
            return my_q
        if part is None:
            return my_h
        size = p.th // PARTS
        return pl.ds(pl.multiple_of(y * p.th + part * size, size), size)

    def line_of(k, part):
        return k if part is None else k + part

    def slot(k, s, dy, part):
        return (buf_d if dy else buf_x).at[p.at(k), s, rows_of(dy, part), :]

    def pass_on(k, dy, part, src, to_z, to_slot, sem):
        line = line_of(k, part)
        return pltpu.make_async_remote_copy(
            src_ref=src, dst_ref=slot(k, to_slot, dy, part), send_sem=z_send.at[line, sem],
            recv_sem=z_recv.at[line, to_slot], device_id=(to_z, y, r), device_id_type=MESH)

    def spread(k, s, dy, part):
        to = (z, y, flip_row(2)) if dy else (z, 1 - y, r)
        line = line_of(k, part)
        return pltpu.make_async_remote_copy(
            src_ref=slot(k, s, dy, part), dst_ref=slot(k, s, dy, part), send_sem=f_send.at[line, s],
            recv_sem=f_recv.at[line, s], device_id=to, device_id_type=MESH)

    def partner(k, which):
        part = buf_d.at[p.at(k), :, x_q if which else my_q, :]
        return pltpu.make_async_remote_copy(
            src_ref=part, dst_ref=part, send_sem=c_send.at[p.at(k), which], recv_sem=c_recv.at[p.at(k), which],
            device_id=(z, y, flip_row(1)), device_id_type=MESH)

    def in_parts(k, go):
        pl.when(k != p.count - 1)(lambda: go(None))

        @pl.when(k == p.count - 1)
        def _():
            pl.loop(0, PARTS)(go)

    def typed(k, go):
        used = mid | jnp.logical_not(p.is_attn(k))
        pl.when(p.is_dy(k) & used)(lambda: go(True, None))
        pl.when(jnp.logical_not(p.is_dy(k)) & used)(lambda: in_parts(k, lambda part: go(False, part)))

    def cut(ref, at, size):
        return ref.at[:, pl.ds(pl.multiple_of(at * size, size), size)]

    def down_rows(ref, i):
        return ref.at[pl.ds(pl.multiple_of(i * p.mc, p.mc), p.mc), :]

    def own_to(k, dy, part, src, end_too, mate_too):
        @pl.when(jnp.logical_not(mid))
        def _():
            pass_on(k, dy, part, src, jnp.where(low, 1, 2), jnp.where(low, 2, 0), 0).start()

        @pl.when(mid)
        def _():
            @pl.when(jnp.logical_not(p.is_attn(k)) & end_too)
            def _():
                pass_on(k, dy, part, src, end_z, jnp.where(low, 0, 2), 0).start()

            @pl.when(mate_too)
            def _():
                pass_on(k, dy, part, src, mate_z, jnp.where(low, 2, 0), 1).start()

    def send_own(k, end_too, mate_too):
        def go(ref, at, size, dy):
            def send(part):
                src = ref.at[rows_of(dy, part), pl.ds(pl.multiple_of(at * size, size), size)]
                own_to(k, dy, part, src, end_too, mate_too)

            if ref is h_mlp:
                in_parts(k, send)
            else:
                send(None)

        for name, ref, dy in (('x_mlp', x_mlp, False), ('gate', dy_gate, True), ('x_attn', x_attn, False),
                              ('attn', dy_attn, True), ('up', dy_up, True), ('out', dy_out, True), ('h', h_mlp, False)):
            at = look(k, [i + 1 if n == name else 0 for n, i in p.order])
            size = p.nc if dy else p.mc
            pl.when(at > 0)(functools.partial(go, ref, at - 1, size, dy))

    def own_first_left(k):
        @pl.when(jnp.logical_not(mid & p.is_attn(k)))
        def _():
            def go(dy, part):
                pass_on(k, dy, part, slot(k, 0, dy, part), z, 0, 0).wait_send()

            pl.when(p.is_dy(k))(lambda: go(True, None))
            pl.when(jnp.logical_not(p.is_dy(k)))(lambda: in_parts(k, lambda part: go(False, part)))

    def arrive(k, e, whole):
        s = jnp.where(low, e, 2 - e)

        def go(dy, part):
            here = slot(k, s, dy, part)
            pass_on(k, dy, part, here, z, s, 0).wait_recv()

            @pl.when(mid & (e == 2))
            def _():
                pass_on(k, dy, part, here, mate_z, 1, 4).start()

            @pl.when(mid & (e < 2) & jnp.logical_not(p.is_attn(k)))
            def _():
                pass_on(k, dy, part, here, end_z, jnp.where(low, s + 1, s - 1), 2 + e).start()

            spread(k, s, dy, part).start()
            if dy and whole:
                pl.when(e == jnp.where(mid, 1, 2))(lambda: partner(k, 0).start())

        typed(k, go)

    def spread_done(k, dy):
        for s in range(p.dp - 1):
            spread(k, s, dy, None).wait_recv()

    def load(src, at, size, buf, index, dst):
        copies = [pltpu.make_async_copy(cut(src, at, size), dst.at[z], l_sem.at[0])]
        for d in range(1, p.dp):
            copies.append(pltpu.make_async_copy(buf.at[index, d - 1], dst.at[lax.rem(z + d, p.dp)], l_sem.at[d]))
        for c in copies:
            c.start()
        for c in copies:
            c.wait()

    step_t = min(256, p.tok)

    def turn(q):
        @pl.loop(0, p.tok // step_t)
        def _(t):
            at = pl.multiple_of(t * step_t, step_t)
            lhs[q, :, pl.ds(at, step_t)] = tile_x[q, pl.ds(at, step_t), :].T

    step_n = min(512, p.nc)
    step_r = min(64, p.mc)

    def lane_sum(v):
        out = v[:, 0:LANES]
        for i in range(1, v.shape[1] // LANES):
            out = out + v[:, i * LANES:(i + 1) * LANES]
        return out

    def product(at, count):
        r_lanes[...] = jnp.zeros_like(r_lanes)

        @pl.loop(0, p.nc // step_n)
        def _(n):
            cols = pl.ds(pl.multiple_of(n * step_n, step_n), step_n)
            grad[at, :, cols] = jnp.dot(lhs[0], tile_d[0, :, cols], preferred_element_type=F32)

            @pl.loop(1, p.dp)
            def _(q):
                grad[at, :, cols] += jnp.dot(lhs[q], tile_d[q, :, cols], preferred_element_type=F32)

            def body(i, acc):
                rows = pl.ds(pl.multiple_of(i * step_r, step_r), step_r)
                block = grad[at, rows, cols]
                sq = block * block + EPS_ONE
                r_lanes[rows, :] += lane_sum(sq)
                return acc + jnp.sum(sq, axis=0, keepdims=True)

            @pl.when(count)
            def _():
                c_sum[at, :, cols] = lax.fori_loop(0, p.mc // step_r, body, jnp.zeros((1, step_n), F32))

    def fold(v):
        v = jnp.reshape(v, (v.shape[0] // 8, 8, LANES))
        while v.shape[0] > 1:
            v = v[:v.shape[0] // 2] + v[v.shape[0] // 2:]
        return v[0]

    def to_row(block):
        return jnp.sum(block.T, axis=0, keepdims=True)

    def get_w(mat, i):
        src = down_rows(w_refs[mat], i) if mat == DOWN else cut(w_refs[mat], i, p.nc)
        return pltpu.make_async_copy(src, w_buf.at[lax.rem(i, 3)], wi_sem.at[lax.rem(i, 3)])

    def put_w(mat, i):
        dst = cut(o_gate if mat == GATE else o_up, i, p.nc)
        return pltpu.make_async_copy(w_buf.at[lax.rem(i, 3)], dst, wo_sem.at[lax.rem(i, 3)])

    def chunk(mat, i):
        count = mid if mat == DOWN else jnp.bool_(True)
        pl.when(count)(lambda: get_w(mat, i).start())
        product(i, count)

        @pl.when(count)
        def _():
            row = to_row(r_lanes[...])
            if mat == DOWN:
                r_row[i] = row
            else:
                r_row[0] = jnp.where(i == 0, row, r_row[0] + row)
            get_w(mat, i).wait()

            def body(n, acc):
                rows = pl.ds(pl.multiple_of(n * step_r, step_r), step_r)
                block = lane_sum(w_buf[lax.rem(i, 3), rows, :] * w_buf[lax.rem(i, 3), rows, :])
                return acc + fold(block)

            w_sq[mat] += lax.fori_loop(0, p.mc // step_r, body, jnp.zeros((8, LANES), F32))

    def first_copies(mat):
        copies = [pltpu.make_async_remote_copy(
            src_ref=rs[mat].at[y], dst_ref=rs[mat].at[y], send_sem=r1_send.at[mat, 0], recv_sem=r1_recv.at[mat, 0],
            device_id=(z, 1 - y, r), device_id_type=MESH)]
        for v in range(1, 4):
            copies.append(pltpu.make_async_remote_copy(
                src_ref=cs[mat].at[r], dst_ref=cs[mat].at[r], send_sem=r1_send.at[mat, v],
                recv_sem=r1_recv.at[mat, v], device_id=(z, y, flip_row(v)), device_id_type=MESH))
        return copies

    def second_copies(mat):
        me = y * 4 + r
        return [pltpu.make_async_remote_copy(
            src_ref=st_all.at[mat, me], dst_ref=st_all.at[mat, me], send_sem=r2_send.at[mat, f * 4 + v],
            recv_sem=r2_recv.at[mat, f * 4 + v], device_id=(z, 1 - y if f else y, flip_row(v)), device_id_type=MESH)
            for f, v in peers]

    def scale_rows(mat):
        return p.rows[mat] * p.row, p.cols[mat] * p.col

    blocks = p.mc // step_r

    def factors(mat, i, n):
        rows = pl.ds(pl.multiple_of(n * step_r, step_r), step_r)
        if mat == DOWN:
            return rows, a_cols[i, rows, :], b_rows[mat].at[:, :]
        return rows, a_cols[0, rows, :], b_rows[mat].at[:, pl.ds(pl.multiple_of(i * p.nc, p.nc), p.nc)]

    def finish_first(mat):
        parts = p.parts[mat]
        if mat != DOWN:
            for i in range(min(2, parts)):
                get_w(mat, jnp.int32(i)).start()
        if mat == DOWN:
            block = c_sum[0]
            for i in range(parts):
                rs[mat][y, :, i * p.mc:(i + 1) * p.mc] = r_row[i]
                if i:
                    block = block + c_sum[i]
            cs[mat][r] = block
        else:
            rs[mat][y] = r_row[0]
            for i in range(parts):
                cs[mat][r, :, i * p.nc:(i + 1) * p.nc] = c_sum[i]
        for c in first_copies(mat):
            c.start()

    def finish_second(mat):
        beta_two = hyper[0]
        m_total, n_total = scale_rows(mat)
        parts = p.parts[mat]
        for c in first_copies(mat):
            c.wait_recv()
        r_new = beta_two * old[mat][0][...] + (1.0 - beta_two) * ((rs[mat][0] + rs[mat][1]) / n_total)
        c_all = ((cs[mat][0] + cs[mat][1]) + cs[mat][2]) + cs[mat][3]
        c_new = beta_two * old[mat][1][...] + (1.0 - beta_two) * (c_all / m_total)
        new[mat][0][...] = r_new
        new[mat][1][...] = c_new
        t_own = jnp.sum(r_new, axis=1, keepdims=True)
        a_row = jnp.sqrt(t_own) / jnp.sqrt(r_new)
        b_rows[mat][...] = 1.0 / jnp.sqrt(c_new)
        if mat == DOWN:
            a_rows[...] = a_row
        for i in range(parts if mat == DOWN else 1):
            a_cols[i] = jnp.broadcast_to(a_row[:, i * p.mc:(i + 1) * p.mc], (LANES, p.mc)).T

        def add_up(j, acc):
            i, n = lax.div(j, blocks), lax.rem(j, blocks)
            rows, a_block, b_ref = factors(mat, i, n)
            for c in range(0, p.nc, LANES):
                upd = grad[i, rows, c:c + LANES] * a_block * b_ref[:, c:c + LANES]
                acc = acc + fold(upd * upd)
            return acc

        u_part = lax.fori_loop(0, parts * blocks, add_up, jnp.zeros((8, LANES), F32))

        def spot(v):
            return jnp.broadcast_to(jnp.sum(jnp.sum(v, axis=1, keepdims=True), axis=0, keepdims=True), (8, LANES))

        me = y * 4 + r
        st_all[mat, me, 0] = spot(u_part)
        st_all[mat, me, 1] = spot(w_sq[mat])
        st_all[mat, me, 2] = jnp.broadcast_to(t_own, (8, LANES))
        for c in second_copies(mat):
            c.start()

    def finish_third(mat):
        rho_step, clip_thr = hyper[1], hyper[2]
        m_total, n_total = scale_rows(mat)
        me = y * 4 + r
        for c in second_copies(mat):
            c.wait_recv()
        t_all = st_all[mat, 0, 2]
        for i in range(1, p.row):
            t_all = t_all + st_all[mat, i, 2]
        u_all = st_all[mat, 0, 0] * (t_all / st_all[mat, 0, 2])
        w_all = st_all[mat, 0, 1]
        for i in range(1, p.row * p.col):
            u_all = u_all + st_all[mat, i, 0] * (t_all / st_all[mat, i, 2])
            w_all = w_all + st_all[mat, i, 1]
        upd_rms = jnp.sqrt(u_all / (m_total * n_total))
        w_rms = jnp.sqrt(w_all / (m_total * n_total))
        scale = rho_step * jnp.maximum(EPS_TWO, w_rms) / jnp.maximum(1.0, upd_rms / clip_thr)
        scale = scale * jnp.sqrt(t_all / st_all[mat, me, 2])
        b_rows[mat][...] = b_rows[mat][...] * scale[0:1, 0:1]

    def renew(mat, low_i, high_i):
        parts = p.parts[mat]

        @pl.loop(low_i, high_i)
        def _(i):
            at = lax.rem(i, 3)
            get_w(mat, i).wait()

            @pl.loop(0, blocks)
            def _(n):
                rows, a_block, b_ref = factors(mat, i, n)
                for c in range(0, p.nc, LANES):
                    cols = slice(c, c + LANES)
                    fresh = w_buf[at, rows, cols] - grad[i, rows, cols] * a_block * b_ref[:, cols]
                    if mat == ATTN:
                        o_attn[rows, cols] = fresh
                    elif mat == UP and UP_KEPT:
                        o_up[i, rows, cols] = fresh
                    else:
                        w_buf[at, rows, cols] = fresh

            if mat == ATTN:
                put_rest().start()
                put_rest().wait()
            if mat == GATE or (mat == UP and not UP_KEPT):
                put_w(mat, i).start()
                pl.when(i >= 1)(lambda: put_w(mat, i - 1).wait())
            pl.when(i + 2 < parts)(lambda: get_w(mat, i + 2).start())

        if (mat == GATE or (mat == UP and not UP_KEPT)) and high_i == parts:
            put_w(mat, jnp.int32(parts - 1)).wait()

    def put_rest():
        return pltpu.make_async_copy(o_attn.at[pl.ds(p.first_rows, p.mc - p.first_rows), :], o_rest, wo_sem.at[0])

    def finish(mat, stage):
        parts = p.parts[mat]
        half = parts // 2 if parts > 1 else parts
        if stage == 1:
            finish_second(mat)
        elif stage == 2:
            finish_third(mat)
            if mat == DOWN:
                al_down[...] = a_rows[...]
                be_down[...] = b_rows[mat][...]
                for c in to_end_down():
                    c.start()
            else:
                renew(mat, 0, half)
        else:
            renew(mat, half, parts)

    def take_x(src, at, k, waits=True):
        copies = [(pltpu.make_async_copy(cut(src, at, p.mc), tile_x.at[z], l_sem.at[0]), z)]
        copies[0][0].start()
        for e in range(p.dp - 1):
            s = jnp.where(low, e, 2 - e)
            if src is h_mlp:
                in_parts(k, lambda part: spread(k, s, False, part).wait_recv())
            elif waits:
                spread(k, s, False, None).wait_recv()
            q = lax.rem(z + s + 1, p.dp)
            copies.append((pltpu.make_async_copy(buf_x.at[p.at(k), s], tile_x.at[q], l_sem.at[e + 1]), q))
            copies[-1][0].start()
            copies[-2][0].wait()
            turn(copies[-2][1])
        copies[-1][0].wait()
        turn(copies[-1][1])

    def got(name, i):
        k = look(i, [p.place[name, j] for j in range(sum(1 for n, _ in p.order if n == name))])
        partner(k, 0).wait_recv()
        partner(k, 1).wait_recv()
        return k

    def use_gate(i):
        pl.when(i == 0)(lambda: take_x(x_mlp, 0, jnp.int32(p.place['x_mlp', 0])))
        k = got('gate', i)
        load(dy_gate, i, p.nc, buf_d, p.at(k), tile_d)
        chunk(GATE, i)
        pl.when(i == p.parts[GATE] - 1)(lambda: finish_first(GATE))

    def use_attn(i):
        take_x(x_attn, 0, jnp.int32(p.place['x_attn', 0]))
        k = got('attn', i)
        load(dy_attn, 0, p.nc, buf_d, p.at(k), tile_d)
        chunk(ATTN, i)
        finish_first(ATTN)

    def use_up(i):
        pl.when(i == 0)(lambda: take_x(x_mlp, 0, jnp.int32(p.place['x_mlp', 0]), False))
        k = got('up', i)
        load(dy_up, i, p.nc, buf_d, p.at(k), tile_d)
        chunk(UP, i)
        pl.when(i == p.parts[UP] - 1)(lambda: finish_first(UP))

    def use_out():
        k = got('out', jnp.int32(0))
        load(dy_out, 0, p.nc, buf_d, p.at(k), tile_d)

    def use_h(i):
        pl.when(i == 0)(use_out)
        take_x(h_mlp, i, look(i, [p.place['h', j] for j in range(p.nh)]))
        chunk(DOWN, i)
        pl.when((i == p.parts[DOWN] - 1) & mid)(lambda: finish_first(DOWN))

    def work(t):
        for name, use in (('gate', use_gate), ('attn', use_attn), ('up', use_up), ('h', use_h)):
            at = jnp.int32(0)
            for i in range(sum(1 for n, _ in p.order if n == name)):
                when_mid = p.steps[True].get((name, i), -1)
                when_end = p.steps[False].get((name, i), -1)
                at = jnp.where(t == jnp.where(mid, when_mid, when_end), i + 1, at)
            pl.when(at > 0)(functools.partial(use, at - 1))
        for mat in MATS:
            for stage in (1, 2, 3):
                when_mid = p.steps[True].get(('finish', mat, stage), -1)
                when_end = p.steps[False].get(('finish', mat, stage), -1)
                if when_mid >= 0:
                    pl.when(t == jnp.where(mid, when_mid, when_end))(functools.partial(finish, mat, stage))

    def sent_to_end(refs, first):
        return [pltpu.make_async_remote_copy(
            src_ref=ref, dst_ref=ref, send_sem=e_send.at[first + i], recv_sem=e_recv.at[first + i],
            device_id=(end_z, y, r), device_id_type=MESH) for i, ref in enumerate(refs)]

    def to_end():
        return sent_to_end((nr_attn, nc_attn, o_attn.at[pl.ds(0, p.first_rows), :]), 0)

    def to_end_down():
        return sent_to_end((nr_down, nc_down, al_down, be_down), 3)

    def sends_left(k):
        def go(dy, part):
            some = slot(k, 0, dy, part)

            @pl.when(mid)
            def _():
                pass_on(k, dy, part, some, z, 0, 1).wait_send()
                pass_on(k, dy, part, some, z, 0, 4).wait_send()

                @pl.when(jnp.logical_not(p.is_attn(k)))
                def _():
                    pass_on(k, dy, part, some, z, 0, 2).wait_send()
                    pass_on(k, dy, part, some, z, 0, 3).wait_send()

            for s in range(p.dp - 1):
                spread(k, s, dy, part).wait_send()
            if dy:
                partner(k, 0).wait_send()
                partner(k, 1).wait_send()

        typed(k, go)

    w_sq[...] = jnp.zeros_like(w_sq)
    ahead = jnp.where(mid, AHEAD_MID, AHEAD_END)

    @pl.loop(0, AHEAD_END)
    def _(k):
        pl.when(k < jnp.where(mid, AHEAD_MID + 1, AHEAD_END))(lambda: send_own(k, True, k < AHEAD_MID))

    @pl.when(mid)
    def _():
        arrive(jnp.int32(0), jnp.int32(2), False)

    for c in old_copies:
        c.start()
    for c in old_copies:
        c.wait()

    @pl.when(jnp.logical_not(mid))
    def _():
        for k in range(AHEAD_MID):
            arrive(jnp.int32(k), jnp.int32(0), False)

    last_mid, last_end = p.turns[True], p.turns[False] - 1

    def one_turn(t):
        d, turn_no = lax.div(t, 3), lax.rem(t, 3)
        pl.when((turn_no == 0) & (d >= 1) & (d < p.count))(lambda: own_first_left(d - 1))
        early = jnp.where(mid, jnp.where(turn_no == 0, 1, 0), jnp.where(turn_no == 2, AHEAD_MID, 0))
        e = lax.rem(turn_no + jnp.where(mid, 2, 1), 3)
        k = d + early
        pl.when(k < p.count)(lambda: arrive(k, e, True))

        @pl.when(turn_no == 2)
        def _():
            pl.when(d + ahead < p.count)(lambda: send_own(d + ahead, d > 0, True))

            @pl.when((d == p.count - 1) & mid)
            def _():
                for c in to_end():
                    c.start()

            k = d - jnp.where(mid, LATE_MID, LATE_END)

            @pl.when((k >= 0) & (k < p.count) & p.is_dy(k) & (mid | jnp.logical_not(p.is_attn(k))))
            def _():
                spread_done(k, True)
                partner(k, 1).start()

        work(t)
        first_end = 3 * p.count - 3
        assert first_end not in p.steps[False].values()

        @pl.when((mid & (t == last_mid)) | (jnp.logical_not(mid) & ((t == first_end) | (t == last_end))))
        def _():
            @pl.loop(0, p.count)
            def _(k):
                pl.when(mid | ((t == first_end) == (k < p.count - 2)))(lambda: sends_left(k))

    @pl.loop(0, last_mid + 1)
    def _(t):
        pl.when(mid | (t < p.turns[False]))(lambda: one_turn(t))

    own_first_left(jnp.int32(p.count - 1))
    for mat in (GATE, UP):
        for c in first_copies(mat) + second_copies(mat):
            c.wait_send()

    @pl.when(mid)
    def _():
        for mat in (ATTN, DOWN):
            for c in first_copies(mat) + second_copies(mat):
                c.wait_send()
        for c in to_end() + to_end_down():
            c.wait_send()

    @pl.when(jnp.logical_not(mid))
    def _():
        for c in to_end() + to_end_down():
            c.wait_recv()


def store_kernel(plan, o_attn, o_gate, o_up, grad, *refs):
    p = plan
    stats, al_down, be_down, w_old, (w_attn, w_gate, w_up, w_down), outs = (
        refs[:8], refs[8], refs[9], refs[10], refs[11:15], refs[15:23])
    bounce, w_buf, a_col, in_sem, out_sem, s_sem, wi_sem, wo_sem = refs[23:]
    depth, wide = bounce.shape[0], w_buf.shape[0]

    def cut(ref, i):
        return ref.at[:, i * p.nc:(i + 1) * p.nc]

    def rows(ref, i):
        return ref.at[i * p.mc:(i + 1) * p.mc, :]

    through = [(cut(o_gate, i), cut(w_gate, i)) for i in range(p.ng)]
    if not UP_KEPT:
        through += [(cut(o_up, i), cut(w_up, i)) for i in range(p.ng)]
    loads = [pltpu.make_async_copy(a, bounce.at[i % depth], in_sem.at[i]) for i, (a, _) in enumerate(through)]
    puts = [pltpu.make_async_copy(bounce.at[i % depth], b, out_sem.at[i]) for i, (_, b) in enumerate(through)]
    w_in = [pltpu.make_async_copy(rows(w_old, i), w_buf.at[i % wide], wi_sem.at[i]) for i in range(p.nh)]
    w_out = [pltpu.make_async_copy(w_buf.at[i % wide], rows(w_down, i), wo_sem.at[i]) for i in range(p.nh)]
    for i in range(wide // 2):
        w_in[i].start()
    for c in loads[:depth]:
        c.start()
    copies = [pltpu.make_async_copy(a, b, s_sem.at[i]) for i, (a, b) in enumerate(zip(stats, outs))]
    copies.append(pltpu.make_async_copy(o_attn, w_attn, s_sem.at[8]))
    if UP_KEPT:
        copies += [pltpu.make_async_copy(o_up.at[i], cut(w_up, i), s_sem.at[9 + i]) for i in range(p.ng)]
    for c in copies:
        c.start()
    step_r = min(64, p.mc)
    per = -(-len(through) // p.nh)
    done = 0
    for i in range(p.nh):
        a_col[...] = jnp.broadcast_to(al_down[:, i * p.mc:(i + 1) * p.mc], (LANES, p.mc)).T
        w_in[i].wait()

        @pl.loop(0, p.mc // step_r)
        def _(n):
            at = pl.ds(pl.multiple_of(n * step_r, step_r), step_r)
            a_block = a_col[at, :]
            for c in range(0, p.nc, LANES):
                cols = slice(c, c + LANES)
                w_buf[i % wide, at, cols] = w_buf[i % wide, at, cols] - grad[i, at, cols] * a_block * be_down[:, cols]

        w_out[i].start()
        again = i + wide // 2
        if again < p.nh:
            if again >= wide:
                w_out[again - wide].wait()
            w_in[again].start()
        for j in range(done, min(len(through), done + per)):
            loads[j].wait()
            puts[j].start()
            again = j + depth // 2
            if depth <= again < len(through):
                puts[again - depth].wait()
                loads[again].start()
        done += per
    for i in range(max(0, p.nh - wide), p.nh):
        if i + wide >= p.nh:
            w_out[i].wait()
    for i in range(max(0, len(through) - depth), len(through)):
        puts[i].wait()
    for c in copies:
        c.wait()


def solution(mesh):
    act_spec = P('dp', 'row')
    grad_spec = P('dp', 'col')
    w_spec = P('row', 'col')
    row_spec = P('row')
    col_spec = P('col')
    in_specs = (act_spec, grad_spec, act_spec, grad_spec, grad_spec, act_spec, grad_spec,
                w_spec, w_spec, w_spec, w_spec,
                row_spec, col_spec, row_spec, col_spec, row_spec, col_spec, row_spec, col_spec, P())
    out_specs = (w_spec, row_spec, col_spec) * 4

    def per_device(x_attn, dy_attn, x_mlp, dy_gate, dy_up, h_mlp, dy_out, w_attn, w_gate, w_up, w_down,
                   r_attn, c_attn, r_gate, c_gate, r_up, c_up, r_down, c_down, hyper_params):
        p = Plan(x_mlp, dy_gate, h_mlp, dy_out, mesh)
        stats = [v.reshape(1, -1) for v in (r_attn, c_attn, r_gate, c_gate, r_up, c_up, r_down, c_down)]
        any_spec = pl.BlockSpec(memory_space=pl.ANY)
        vmem_spec = pl.BlockSpec(memory_space=pltpu.VMEM)
        up_spec = vmem_spec if UP_KEPT else any_spec
        row_shapes = []
        for mat in MATS:
            row_shapes += [jax.ShapeDtypeStruct((1, p.rows[mat]), F32), jax.ShapeDtypeStruct((1, p.cols[mat]), F32)]
        w_shapes = [jax.ShapeDtypeStruct((p.rows[mat], p.cols[mat]), F32) for mat in MATS]
        o_shapes = [pltpu.VMEM((p.mc, p.nc), F32), w_shapes[GATE],
                    pltpu.VMEM((p.ng, p.mc, p.nc), F32) if UP_KEPT else w_shapes[UP],
                    pltpu.VMEM((p.pieces, p.mc, p.nc), F32)]
        bufs = [jax.ShapeDtypeStruct((p.n_dy, p.dp - 1, p.tok, p.nc), BF16),
                jax.ShapeDtypeStruct((p.n_x, p.dp - 1, p.tok, p.mc), BF16)]
        rest = jax.ShapeDtypeStruct((p.mc - p.first_rows, p.nc), F32)
        dma = pltpu.SemaphoreType.DMA
        lines = p.count + PARTS - 1
        scratch = [
            pltpu.VMEM((p.dp, p.mc, p.tok), BF16),
            pltpu.VMEM((p.dp, p.tok, p.mc), BF16),
            pltpu.VMEM((p.dp, p.tok, p.nc), BF16),
            pltpu.VMEM((3, p.mc, p.nc), F32),
            pltpu.VMEM((p.mc, LANES), F32),
            pltpu.VMEM((p.pieces, 1, p.mc), F32),
            pltpu.VMEM((p.pieces, 1, p.nc), F32),
            pltpu.VMEM((p.nh, p.mc, LANES), F32),
            pltpu.VMEM((1, p.rows[DOWN]), F32),
            pltpu.VMEM((4, 8, LANES), F32),
        ]
        scratch += [pltpu.VMEM((1, p.cols[mat]), F32) for mat in MATS]
        scratch += [pltpu.VMEM(v.shape, F32) for v in row_shapes]
        scratch += [pltpu.VMEM((2, 1, p.rows[mat]), F32) for mat in MATS]
        scratch += [pltpu.VMEM((4, 1, p.cols[mat]), F32) for mat in MATS]
        scratch += [
            pltpu.VMEM((4, 8, 3, 8, LANES), F32),
            dma((lines, 5)), dma((lines, p.dp - 1)),
            dma((lines, p.dp - 1)), dma((lines, p.dp - 1)),
            dma((p.n_dy, 2)), dma((p.n_dy, 2)),
            dma((4, 4)), dma((4, 4)), dma((4, 8)), dma((4, 8)),
            dma((7,)), dma((7,)),
            dma((p.dp,)), dma((3,)), dma((3,)), dma((8,)),
        ]
        out = pl.pallas_call(
            functools.partial(gather_kernel, p),
            out_shape=o_shapes + [pltpu.VMEM(v.shape, F32) for v in row_shapes + row_shapes[-2:]] + [rest] + bufs,
            in_specs=[any_spec] * 19 + [pl.BlockSpec(memory_space=pltpu.SMEM)],
            out_specs=[vmem_spec, any_spec, up_spec, vmem_spec] + [vmem_spec] * 10 + [any_spec] * 3,
            scratch_shapes=scratch,
            compiler_params=pltpu.CompilerParams(collective_id=0, has_side_effects=True, vmem_limit_bytes=VMEM_LIMIT),
        )(x_attn, dy_attn, x_mlp, dy_gate, dy_up, h_mlp, dy_out, w_attn, w_gate, w_up, w_down, *stats, hyper_params)
        res = pl.pallas_call(
            functools.partial(store_kernel, p),
            out_shape=w_shapes + row_shapes,
            in_specs=[vmem_spec, any_spec, up_spec, vmem_spec] + [vmem_spec] * 10 + [any_spec],
            out_specs=[any_spec] * 12,
            scratch_shapes=[pltpu.VMEM((DEPTH, p.mc, p.nc), F32), pltpu.VMEM((WIDE, p.mc, p.nc), F32),
                            pltpu.VMEM((p.mc, LANES), F32), dma((2 * p.ng,)), dma((2 * p.ng,)), dma((9 + p.ng,)),
                            dma((p.nh,)), dma((p.nh,))],
            compiler_params=pltpu.CompilerParams(vmem_limit_bytes=STORE_LIMIT),
            cost_estimate=pl.CostEstimate(flops=60_000_000_000, bytes_accessed=90_000_000, transcendentals=0),
        )(*[pltpu.with_memory_space_constraint(v, pltpu.VMEM) if i not in HBM_KEPT else v for i, v in enumerate(out[:14])],
          w_down)
        z = lax.axis_index('dp')
        got = lax.ppermute(out[14], 'dp', [(1, 0), (2, 3)])
        rows = jnp.where((z == 1) | (z == 2), out[14], got)
        res = [lax.dynamic_update_slice(res[0], rows, (p.first_rows, 0))] + list(res[1:])
        result = []
        for mat in MATS:
            result += [res[mat], res[4 + 2 * mat].reshape(-1), res[5 + 2 * mat].reshape(-1)]
        return tuple(result)

    return jax.shard_map(per_device, mesh=mesh, in_specs=in_specs, out_specs=out_specs, check_vma=False)
```

```python
import functools
import jax
import jax.numpy as jnp
from jax import lax
from jax.experimental import pallas as pl
from jax.experimental.pallas import tpu as pltpu
from jax.sharding import PartitionSpec as P

EPS_ONE = 1e-30
EPS_TWO = 1e-3
MESH = pl.DeviceIdType.MESH
LANES = 128
F32 = jnp.float32
BF16 = jnp.bfloat16
ATTN, GATE, UP, DOWN = range(4)
MATS = (ATTN, GATE, UP, DOWN)
FIRST = {'gate': ('x_mlp', 0), 'attn': ('x_attn', 0), 'up': ('x_mlp', 0), 'h': ('out', 0)}
AHEAD_MID, AHEAD_END = 2, 6
PARTS = 4
LATE_MID, LATE_END = 3, 2
VMEM_LIMIT = 29 * 1024 * 1024
STORE_LIMIT = 29 * 1024 * 1024
UP_KEPT = True
HBM_KEPT = (1,) if UP_KEPT else (1, 2)
DEPTH, WIDE = 6, 6


def look(k, table):
    out = jnp.int32(0)
    for i, v in enumerate(table):
        if v:
            out = jnp.where(k == i, v, out)
    return out


class Plan:
    def __init__(self, x_mlp, dy_gate, h_mlp, dy_out, mesh):
        self.dp, self.col, self.row = mesh.shape['dp'], mesh.shape['col'], mesh.shape['row']
        assert (self.dp, self.col, self.row) == (4, 2, 4)
        self.tok = x_mlp.shape[0]
        self.mc = x_mlp.shape[1]
        self.nc = dy_out.shape[1]
        self.ng = dy_gate.shape[1] // self.nc
        self.nh = h_mlp.shape[1] // self.mc
        self.tq = self.tok // self.row
        self.th = self.tok // self.col
        g = [('gate', i) for i in range(self.ng)]
        u = [('up', i) for i in range(self.ng)]
        h = [('h', i) for i in range(self.nh)]
        one, two = max(1, self.ng // 4), max(2, 3 * self.ng // 4)
        self.order = ([('x_mlp', 0)] + g[:one] + h[:1] + g[one:two] + h[1:2] + g[two:] + [('x_attn', 0), ('attn', 0)]
                      + u + [('out', 0)] + h[2:])
        self.count = len(self.order)
        self.place = {v: k for k, v in enumerate(self.order)}
        self.first_rows = self.mc * 12 // 32 // 8 * 8
        self.n_dy = 2 * self.ng + 2
        self.n_x = self.nh + 2
        self.pieces = max(self.ng, self.nh)
        self.rows = {ATTN: self.mc, GATE: self.mc, UP: self.mc, DOWN: self.mc * self.nh}
        self.cols = {ATTN: self.nc, GATE: self.nc * self.ng, UP: self.nc * self.ng, DOWN: self.nc}
        self.parts = {ATTN: 1, GATE: self.ng, UP: self.ng, DOWN: self.nh}
        base = {'gate': 0, 'up': self.ng, 'out': 2 * self.ng, 'attn': 2 * self.ng + 1, 'x_mlp': 0, 'x_attn': 1, 'h': 2}
        self.dy_table = [1 if n in ('gate', 'up', 'out', 'attn') else 0 for n, _ in self.order]
        self.at_table = [base[n] + i for n, i in self.order]
        self.attn_table = [1 if n in ('x_attn', 'attn') else 0 for n, _ in self.order]
        self.steps = {m: self.schedule(m) for m in (True, False)}
        self.turns = {m: max(max(v.values()) + 1, 3 * self.count) for m, v in self.steps.items()}

    def schedule(self, mid):
        late = LATE_MID if mid else LATE_END
        tasks = []
        for name, mat in (('gate', GATE), ('attn', ATTN), ('up', UP), ('h', DOWN)):
            if name == 'attn' and not mid:
                continue
            for i in range(self.parts[mat]):
                k = self.place[name, i]
                need = [3 * (k + late + 1)] if name != 'h' else [3 * (k + late) if mid else 3 * k + (3 if k == self.count - 1 else 5)]
                if i == 0:
                    need.append(3 * (self.place[FIRST[name]] + late + (name == 'h')))
                tasks.append(((name, i), max(need)))
            stages = {ATTN: (1, 2), DOWN: (1, 2)}.get(mat, (1, 2, 3))
            if mid or mat != DOWN:
                tasks += [(('finish', mat, stage), 0) for stage in stages]
        out, t = {}, 0
        for task, first in tasks:
            t = max(t, first)
            out[task] = t
            t += 1
        return out

    def is_dy(self, k):
        return look(k, self.dy_table) == 1

    def is_attn(self, k):
        return look(k, self.attn_table) == 1

    def at(self, k):
        return look(k, self.at_table)


def gather_kernel(plan, x_attn, dy_attn, x_mlp, dy_gate, dy_up, h_mlp, dy_out, w_attn, w_gate, w_up, w_down,
                  r_attn, c_attn, r_gate, c_gate, r_up, c_up, r_down, c_down, hyper,
                  o_attn, o_gate, o_up, grad, nr_attn, nc_attn, nr_gate, nc_gate, nr_up, nc_up, nr_down, nc_down,
                  al_down, be_down, o_rest, buf_d, buf_x,
                  lhs, tile_x, tile_d, w_buf, r_lanes, r_row, c_sum, a_cols, a_rows, w_sq,
                  b_attn, b_gate, b_up, b_down, *more):
    p = plan
    old_refs = more[:8]
    (rs_attn, rs_gate, rs_up, rs_down, cs_attn, cs_gate, cs_up, cs_down, st_all,
     z_send, z_recv, f_send, f_recv, c_send, c_recv, r1_send, r1_recv, r2_send, r2_recv,
     e_send, e_recv, l_sem, wi_sem, wo_sem, o_sem) = more[8:]
    z, y, r = lax.axis_index('dp'), lax.axis_index('col'), lax.axis_index('row')
    low = z < 2
    mid = (z == 1) | (z == 2)
    end_z = jnp.where(low, 0, 3)
    mate_z = 3 - z
    w_refs = {ATTN: w_attn, GATE: w_gate, UP: w_up, DOWN: w_down}
    old_in = (r_attn, c_attn, r_gate, c_gate, r_up, c_up, r_down, c_down)
    old = {mat: (old_refs[2 * mat], old_refs[2 * mat + 1]) for mat in MATS}
    old_copies = [pltpu.make_async_copy(a, b, o_sem.at[i]) for i, (a, b) in enumerate(zip(old_in, old_refs))]
    new = {ATTN: (nr_attn, nc_attn), GATE: (nr_gate, nc_gate), UP: (nr_up, nc_up), DOWN: (nr_down, nc_down)}
    b_rows = {ATTN: b_attn, GATE: b_gate, UP: b_up, DOWN: b_down}
    rs = {ATTN: rs_attn, GATE: rs_gate, UP: rs_up, DOWN: rs_down}
    cs = {ATTN: cs_attn, GATE: cs_gate, UP: cs_up, DOWN: cs_down}

    def flip_row(v):
        bit0, bit1 = lax.rem(r, 2), lax.div(r, 2)
        if v & 1:
            bit0 = 1 - bit0
        if v & 2:
            bit1 = 1 - bit1
        return bit1 * 2 + bit0

    peers = [(f, v) for f in range(2) for v in range(4) if f or v]
    barrier = pltpu.get_barrier_semaphore()
    for f, v in peers:
        pl.semaphore_signal(barrier, inc=1, device_id=(z, 1 - y if f else y, flip_row(v)), device_id_type=MESH)

    @pl.when(mid)
    def _():
        pl.semaphore_signal(barrier, inc=1, device_id=(end_z, y, r), device_id_type=MESH)
        pl.semaphore_signal(barrier, inc=1, device_id=(mate_z, y, r), device_id_type=MESH)
        pl.semaphore_wait(barrier, len(peers) + 2)

    @pl.when(jnp.logical_not(mid))
    def _():
        pl.semaphore_signal(barrier, inc=1, device_id=(jnp.where(low, 1, 2), y, r), device_id_type=MESH)
        pl.semaphore_wait(barrier, len(peers) + 1)

    my_q = pl.ds(pl.multiple_of(r * p.tq, p.tq), p.tq)
    x_q = pl.ds(pl.multiple_of(flip_row(2) * p.tq, p.tq), p.tq)
    my_h = pl.ds(pl.multiple_of(y * p.th, p.th), p.th)

    def rows_of(dy, part):
        if dy:
            return my_q
        if part is None:
            return my_h
        size = p.th // PARTS
        return pl.ds(pl.multiple_of(y * p.th + part * size, size), size)

    def line_of(k, part):
        return k if part is None else k + part

    def slot(k, s, dy, part):
        return (buf_d if dy else buf_x).at[p.at(k), s, rows_of(dy, part), :]

    def pass_on(k, dy, part, src, to_z, to_slot, sem):
        line = line_of(k, part)
        return pltpu.make_async_remote_copy(
            src_ref=src, dst_ref=slot(k, to_slot, dy, part), send_sem=z_send.at[line, sem],
            recv_sem=z_recv.at[line, to_slot], device_id=(to_z, y, r), device_id_type=MESH)

    def spread(k, s, dy, part):
        to = (z, y, flip_row(2)) if dy else (z, 1 - y, r)
        line = line_of(k, part)
        return pltpu.make_async_remote_copy(
            src_ref=slot(k, s, dy, part), dst_ref=slot(k, s, dy, part), send_sem=f_send.at[line, s],
            recv_sem=f_recv.at[line, s], device_id=to, device_id_type=MESH)

    def partner(k, which):
        part = buf_d.at[p.at(k), :, x_q if which else my_q, :]
        return pltpu.make_async_remote_copy(
            src_ref=part, dst_ref=part, send_sem=c_send.at[p.at(k), which], recv_sem=c_recv.at[p.at(k), which],
            device_id=(z, y, flip_row(1)), device_id_type=MESH)

    def in_parts(k, go):
        pl.when(k != p.count - 1)(lambda: go(None))

        @pl.when(k == p.count - 1)
        def _():
            pl.loop(0, PARTS)(go)

    def typed(k, go):
        used = mid | jnp.logical_not(p.is_attn(k))
        pl.when(p.is_dy(k) & used)(lambda: go(True, None))
        pl.when(jnp.logical_not(p.is_dy(k)) & used)(lambda: in_parts(k, lambda part: go(False, part)))

    def cut(ref, at, size):
        return ref.at[:, pl.ds(pl.multiple_of(at * size, size), size)]

    def down_rows(ref, i):
        return ref.at[pl.ds(pl.multiple_of(i * p.mc, p.mc), p.mc), :]

    def own_to(k, dy, part, src, end_too, mate_too):
        @pl.when(jnp.logical_not(mid))
        def _():
            pass_on(k, dy, part, src, jnp.where(low, 1, 2), jnp.where(low, 2, 0), 0).start()

        @pl.when(mid)
        def _():
            @pl.when(jnp.logical_not(p.is_attn(k)) & end_too)
            def _():
                pass_on(k, dy, part, src, end_z, jnp.where(low, 0, 2), 0).start()

            @pl.when(mate_too)
            def _():
                pass_on(k, dy, part, src, mate_z, jnp.where(low, 2, 0), 1).start()

    def send_own(k, end_too, mate_too):
        def go(ref, at, size, dy):
            def send(part):
                src = ref.at[rows_of(dy, part), pl.ds(pl.multiple_of(at * size, size), size)]
                own_to(k, dy, part, src, end_too, mate_too)

            if ref is h_mlp:
                in_parts(k, send)
            else:
                send(None)

        for name, ref, dy in (('x_mlp', x_mlp, False), ('gate', dy_gate, True), ('x_attn', x_attn, False),
                              ('attn', dy_attn, True), ('up', dy_up, True), ('out', dy_out, True), ('h', h_mlp, False)):
            at = look(k, [i + 1 if n == name else 0 for n, i in p.order])
            size = p.nc if dy else p.mc
            pl.when(at > 0)(functools.partial(go, ref, at - 1, size, dy))

    def own_first_left(k):
        @pl.when(jnp.logical_not(mid & p.is_attn(k)))
        def _():
            def go(dy, part):
                pass_on(k, dy, part, slot(k, 0, dy, part), z, 0, 0).wait_send()

            pl.when(p.is_dy(k))(lambda: go(True, None))
            pl.when(jnp.logical_not(p.is_dy(k)))(lambda: in_parts(k, lambda part: go(False, part)))

    def arrive(k, e, whole):
        s = jnp.where(low, e, 2 - e)

        def go(dy, part):
            here = slot(k, s, dy, part)
            pass_on(k, dy, part, here, z, s, 0).wait_recv()

            @pl.when(mid & (e == 2))
            def _():
                pass_on(k, dy, part, here, mate_z, 1, 4).start()

            @pl.when(mid & (e < 2) & jnp.logical_not(p.is_attn(k)))
            def _():
                pass_on(k, dy, part, here, end_z, jnp.where(low, s + 1, s - 1), 2 + e).start()

            spread(k, s, dy, part).start()
            if dy and whole:
                pl.when(e == jnp.where(mid, 1, 2))(lambda: partner(k, 0).start())

        typed(k, go)

    def spread_done(k, dy):
        for s in range(p.dp - 1):
            spread(k, s, dy, None).wait_recv()

    def load(src, at, size, buf, index, dst):
        copies = [pltpu.make_async_copy(cut(src, at, size), dst.at[z], l_sem.at[0])]
        for d in range(1, p.dp):
            copies.append(pltpu.make_async_copy(buf.at[index, d - 1], dst.at[lax.rem(z + d, p.dp)], l_sem.at[d]))
        for c in copies:
            c.start()
        for c in copies:
            c.wait()

    step_t = min(256, p.tok)

    def turn(q):
        @pl.loop(0, p.tok // step_t)
        def _(t):
            at = pl.multiple_of(t * step_t, step_t)
            lhs[q, :, pl.ds(at, step_t)] = tile_x[q, pl.ds(at, step_t), :].T

    step_n = min(512, p.nc)
    step_r = min(64, p.mc)

    def lane_sum(v):
        out = v[:, 0:LANES]
        for i in range(1, v.shape[1] // LANES):
            out = out + v[:, i * LANES:(i + 1) * LANES]
        return out

    def product(at, count):
        r_lanes[...] = jnp.zeros_like(r_lanes)

        @pl.loop(0, p.nc // step_n)
        def _(n):
            cols = pl.ds(pl.multiple_of(n * step_n, step_n), step_n)
            grad[at, :, cols] = jnp.dot(lhs[0], tile_d[0, :, cols], preferred_element_type=F32)

            @pl.loop(1, p.dp)
            def _(q):
                grad[at, :, cols] += jnp.dot(lhs[q], tile_d[q, :, cols], preferred_element_type=F32)

            def body(i, acc):
                rows = pl.ds(pl.multiple_of(i * step_r, step_r), step_r)
                block = grad[at, rows, cols]
                sq = block * block + EPS_ONE
                r_lanes[rows, :] += lane_sum(sq)
                return acc + jnp.sum(sq, axis=0, keepdims=True)

            @pl.when(count)
            def _():
                c_sum[at, :, cols] = lax.fori_loop(0, p.mc // step_r, body, jnp.zeros((1, step_n), F32))

    def fold(v):
        v = jnp.reshape(v, (v.shape[0] // 8, 8, LANES))
        while v.shape[0] > 1:
            v = v[:v.shape[0] // 2] + v[v.shape[0] // 2:]
        return v[0]

    def to_row(block):
        return jnp.sum(block.T, axis=0, keepdims=True)

    def get_w(mat, i):
        src = down_rows(w_refs[mat], i) if mat == DOWN else cut(w_refs[mat], i, p.nc)
        return pltpu.make_async_copy(src, w_buf.at[lax.rem(i, 3)], wi_sem.at[lax.rem(i, 3)])

    def put_w(mat, i):
        dst = cut(o_gate if mat == GATE else o_up, i, p.nc)
        return pltpu.make_async_copy(w_buf.at[lax.rem(i, 3)], dst, wo_sem.at[lax.rem(i, 3)])

    def chunk(mat, i):
        count = mid if mat == DOWN else jnp.bool_(True)
        pl.when(count)(lambda: get_w(mat, i).start())
        product(i, count)

        @pl.when(count)
        def _():
            row = to_row(r_lanes[...])
            if mat == DOWN:
                r_row[i] = row
            else:
                r_row[0] = jnp.where(i == 0, row, r_row[0] + row)
            get_w(mat, i).wait()

            def body(n, acc):
                rows = pl.ds(pl.multiple_of(n * step_r, step_r), step_r)
                block = lane_sum(w_buf[lax.rem(i, 3), rows, :] * w_buf[lax.rem(i, 3), rows, :])
                return acc + fold(block)

            w_sq[mat] += lax.fori_loop(0, p.mc // step_r, body, jnp.zeros((8, LANES), F32))

    def first_copies(mat):
        copies = [pltpu.make_async_remote_copy(
            src_ref=rs[mat].at[y], dst_ref=rs[mat].at[y], send_sem=r1_send.at[mat, 0], recv_sem=r1_recv.at[mat, 0],
            device_id=(z, 1 - y, r), device_id_type=MESH)]
        for v in range(1, 4):
            copies.append(pltpu.make_async_remote_copy(
                src_ref=cs[mat].at[r], dst_ref=cs[mat].at[r], send_sem=r1_send.at[mat, v],
                recv_sem=r1_recv.at[mat, v], device_id=(z, y, flip_row(v)), device_id_type=MESH))
        return copies

    def second_copies(mat):
        me = y * 4 + r
        return [pltpu.make_async_remote_copy(
            src_ref=st_all.at[mat, me], dst_ref=st_all.at[mat, me], send_sem=r2_send.at[mat, f * 4 + v],
            recv_sem=r2_recv.at[mat, f * 4 + v], device_id=(z, 1 - y if f else y, flip_row(v)), device_id_type=MESH)
            for f, v in peers]

    def scale_rows(mat):
        return p.rows[mat] * p.row, p.cols[mat] * p.col

    blocks = p.mc // step_r

    def factors(mat, i, n):
        rows = pl.ds(pl.multiple_of(n * step_r, step_r), step_r)
        if mat == DOWN:
            return rows, a_cols[i, rows, :], b_rows[mat].at[:, :]
        return rows, a_cols[0, rows, :], b_rows[mat].at[:, pl.ds(pl.multiple_of(i * p.nc, p.nc), p.nc)]

    def finish_first(mat):
        parts = p.parts[mat]
        if mat != DOWN:
            for i in range(min(2, parts)):
                get_w(mat, jnp.int32(i)).start()
        if mat == DOWN:
            block = c_sum[0]
            for i in range(parts):
                rs[mat][y, :, i * p.mc:(i + 1) * p.mc] = r_row[i]
                if i:
                    block = block + c_sum[i]
            cs[mat][r] = block
        else:
            rs[mat][y] = r_row[0]
            for i in range(parts):
                cs[mat][r, :, i * p.nc:(i + 1) * p.nc] = c_sum[i]
        for c in first_copies(mat):
            c.start()

    def finish_second(mat):
        beta_two = hyper[0]
        m_total, n_total = scale_rows(mat)
        parts = p.parts[mat]
        for c in first_copies(mat):
            c.wait_recv()
        r_new = beta_two * old[mat][0][...] + (1.0 - beta_two) * ((rs[mat][0] + rs[mat][1]) / n_total)
        c_all = ((cs[mat][0] + cs[mat][1]) + cs[mat][2]) + cs[mat][3]
        c_new = beta_two * old[mat][1][...] + (1.0 - beta_two) * (c_all / m_total)
        new[mat][0][...] = r_new
        new[mat][1][...] = c_new
        t_own = jnp.sum(r_new, axis=1, keepdims=True)
        a_row = jnp.sqrt(t_own) / jnp.sqrt(r_new)
        b_rows[mat][...] = 1.0 / jnp.sqrt(c_new)
        if mat == DOWN:
            a_rows[...] = a_row
        for i in range(parts if mat == DOWN else 1):
            a_cols[i] = jnp.broadcast_to(a_row[:, i * p.mc:(i + 1) * p.mc], (LANES, p.mc)).T

        def add_up(j, acc):
            i, n = lax.div(j, blocks), lax.rem(j, blocks)
            rows, a_block, b_ref = factors(mat, i, n)
            for c in range(0, p.nc, LANES):
                upd = grad[i, rows, c:c + LANES] * a_block * b_ref[:, c:c + LANES]
                acc = acc + fold(upd * upd)
            return acc

        u_part = lax.fori_loop(0, parts * blocks, add_up, jnp.zeros((8, LANES), F32))

        def spot(v):
            return jnp.broadcast_to(jnp.sum(jnp.sum(v, axis=1, keepdims=True), axis=0, keepdims=True), (8, LANES))

        me = y * 4 + r
        st_all[mat, me, 0] = spot(u_part)
        st_all[mat, me, 1] = spot(w_sq[mat])
        st_all[mat, me, 2] = jnp.broadcast_to(t_own, (8, LANES))
        for c in second_copies(mat):
            c.start()

    def finish_third(mat):
        rho_step, clip_thr = hyper[1], hyper[2]
        m_total, n_total = scale_rows(mat)
        me = y * 4 + r
        for c in second_copies(mat):
            c.wait_recv()
        t_all = st_all[mat, 0, 2]
        for i in range(1, p.row):
            t_all = t_all + st_all[mat, i, 2]
        u_all = st_all[mat, 0, 0] * (t_all / st_all[mat, 0, 2])
        w_all = st_all[mat, 0, 1]
        for i in range(1, p.row * p.col):
            u_all = u_all + st_all[mat, i, 0] * (t_all / st_all[mat, i, 2])
            w_all = w_all + st_all[mat, i, 1]
        upd_rms = jnp.sqrt(u_all / (m_total * n_total))
        w_rms = jnp.sqrt(w_all / (m_total * n_total))
        scale = rho_step * jnp.maximum(EPS_TWO, w_rms) / jnp.maximum(1.0, upd_rms / clip_thr)
        scale = scale * jnp.sqrt(t_all / st_all[mat, me, 2])
        b_rows[mat][...] = b_rows[mat][...] * scale[0:1, 0:1]

    def renew(mat, low_i, high_i):
        parts = p.parts[mat]

        @pl.loop(low_i, high_i)
        def _(i):
            at = lax.rem(i, 3)
            get_w(mat, i).wait()

            @pl.loop(0, blocks)
            def _(n):
                rows, a_block, b_ref = factors(mat, i, n)
                for c in range(0, p.nc, LANES):
                    cols = slice(c, c + LANES)
                    fresh = w_buf[at, rows, cols] - grad[i, rows, cols] * a_block * b_ref[:, cols]
                    if mat == ATTN:
                        o_attn[rows, cols] = fresh
                    elif mat == UP and UP_KEPT:
                        o_up[i, rows, cols] = fresh
                    else:
                        w_buf[at, rows, cols] = fresh

            if mat == ATTN:
                put_rest().start()
                put_rest().wait()
            if mat == GATE or (mat == UP and not UP_KEPT):
                put_w(mat, i).start()
                pl.when(i >= 1)(lambda: put_w(mat, i - 1).wait())
            pl.when(i + 2 < parts)(lambda: get_w(mat, i + 2).start())

        if (mat == GATE or (mat == UP and not UP_KEPT)) and high_i == parts:
            put_w(mat, jnp.int32(parts - 1)).wait()

    def put_rest():
        return pltpu.make_async_copy(o_attn.at[pl.ds(p.first_rows, p.mc - p.first_rows), :], o_rest, wo_sem.at[0])

    def finish(mat, stage):
        parts = p.parts[mat]
        half = parts // 2 if parts > 1 else parts
        if stage == 1:
            finish_second(mat)
        elif stage == 2:
            finish_third(mat)
            if mat == DOWN:
                al_down[...] = a_rows[...]
                be_down[...] = b_rows[mat][...]
                for c in to_end_down():
                    c.start()
            else:
                renew(mat, 0, half)
        else:
            renew(mat, half, parts)

    def take_x(src, at, k, waits=True):
        copies = [(pltpu.make_async_copy(cut(src, at, p.mc), tile_x.at[z], l_sem.at[0]), z)]
        copies[0][0].start()
        for e in range(p.dp - 1):
            s = jnp.where(low, e, 2 - e)
            if src is h_mlp:
                in_parts(k, lambda part: spread(k, s, False, part).wait_recv())
            elif waits:
                spread(k, s, False, None).wait_recv()
            q = lax.rem(z + s + 1, p.dp)
            copies.append((pltpu.make_async_copy(buf_x.at[p.at(k), s], tile_x.at[q], l_sem.at[e + 1]), q))
            copies[-1][0].start()
            copies[-2][0].wait()
            turn(copies[-2][1])
        copies[-1][0].wait()
        turn(copies[-1][1])

    def got(name, i):
        k = look(i, [p.place[name, j] for j in range(sum(1 for n, _ in p.order if n == name))])
        partner(k, 0).wait_recv()
        partner(k, 1).wait_recv()
        return k

    def use_gate(i):
        pl.when(i == 0)(lambda: take_x(x_mlp, 0, jnp.int32(p.place['x_mlp', 0])))
        k = got('gate', i)
        load(dy_gate, i, p.nc, buf_d, p.at(k), tile_d)
        chunk(GATE, i)
        pl.when(i == p.parts[GATE] - 1)(lambda: finish_first(GATE))

    def use_attn(i):
        take_x(x_attn, 0, jnp.int32(p.place['x_attn', 0]))
        k = got('attn', i)
        load(dy_attn, 0, p.nc, buf_d, p.at(k), tile_d)
        chunk(ATTN, i)
        finish_first(ATTN)

    def use_up(i):
        pl.when(i == 0)(lambda: take_x(x_mlp, 0, jnp.int32(p.place['x_mlp', 0]), False))
        k = got('up', i)
        load(dy_up, i, p.nc, buf_d, p.at(k), tile_d)
        chunk(UP, i)
        pl.when(i == p.parts[UP] - 1)(lambda: finish_first(UP))

    def use_out():
        k = got('out', jnp.int32(0))
        load(dy_out, 0, p.nc, buf_d, p.at(k), tile_d)

    def use_h(i):
        pl.when(i == 0)(use_out)
        take_x(h_mlp, i, look(i, [p.place['h', j] for j in range(p.nh)]))
        chunk(DOWN, i)
        pl.when((i == p.parts[DOWN] - 1) & mid)(lambda: finish_first(DOWN))

    def work(t):
        for name, use in (('gate', use_gate), ('attn', use_attn), ('up', use_up), ('h', use_h)):
            at = jnp.int32(0)
            for i in range(sum(1 for n, _ in p.order if n == name)):
                when_mid = p.steps[True].get((name, i), -1)
                when_end = p.steps[False].get((name, i), -1)
                at = jnp.where(t == jnp.where(mid, when_mid, when_end), i + 1, at)
            pl.when(at > 0)(functools.partial(use, at - 1))
        for mat in MATS:
            for stage in (1, 2, 3):
                when_mid = p.steps[True].get(('finish', mat, stage), -1)
                when_end = p.steps[False].get(('finish', mat, stage), -1)
                if when_mid >= 0:
                    pl.when(t == jnp.where(mid, when_mid, when_end))(functools.partial(finish, mat, stage))

    def sent_to_end(refs, first):
        return [pltpu.make_async_remote_copy(
            src_ref=ref, dst_ref=ref, send_sem=e_send.at[first + i], recv_sem=e_recv.at[first + i],
            device_id=(end_z, y, r), device_id_type=MESH) for i, ref in enumerate(refs)]

    def to_end():
        return sent_to_end((nr_attn, nc_attn, o_attn.at[pl.ds(0, p.first_rows), :]), 0)

    def to_end_down():
        return sent_to_end((nr_down, nc_down, al_down, be_down), 3)

    def sends_left(k):
        def go(dy, part):
            some = slot(k, 0, dy, part)

            @pl.when(mid)
            def _():
                pass_on(k, dy, part, some, z, 0, 1).wait_send()
                pass_on(k, dy, part, some, z, 0, 4).wait_send()

                @pl.when(jnp.logical_not(p.is_attn(k)))
                def _():
                    pass_on(k, dy, part, some, z, 0, 2).wait_send()
                    pass_on(k, dy, part, some, z, 0, 3).wait_send()

            for s in range(p.dp - 1):
                spread(k, s, dy, part).wait_send()
            if dy:
                partner(k, 0).wait_send()
                partner(k, 1).wait_send()

        typed(k, go)

    w_sq[...] = jnp.zeros_like(w_sq)
    ahead = jnp.where(mid, AHEAD_MID, AHEAD_END)

    @pl.loop(0, AHEAD_END)
    def _(k):
        pl.when(k < jnp.where(mid, AHEAD_MID + 1, AHEAD_END))(lambda: send_own(k, True, k < AHEAD_MID))

    @pl.when(mid)
    def _():
        arrive(jnp.int32(0), jnp.int32(2), False)

    for c in old_copies:
        c.start()
    for c in old_copies:
        c.wait()

    @pl.when(jnp.logical_not(mid))
    def _():
        for k in range(AHEAD_MID):
            arrive(jnp.int32(k), jnp.int32(0), False)

    last_mid, last_end = p.turns[True], p.turns[False] - 1

    def one_turn(t):
        d, turn_no = lax.div(t, 3), lax.rem(t, 3)
        pl.when((turn_no == 0) & (d >= 1) & (d < p.count))(lambda: own_first_left(d - 1))
        early = jnp.where(mid, jnp.where(turn_no == 0, 1, 0), jnp.where(turn_no == 2, AHEAD_MID, 0))
        e = lax.rem(turn_no + jnp.where(mid, 2, 1), 3)
        k = d + early
        pl.when(k < p.count)(lambda: arrive(k, e, True))

        @pl.when(turn_no == 2)
        def _():
            pl.when(d + ahead < p.count)(lambda: send_own(d + ahead, d > 0, True))

            @pl.when((d == p.count - 1) & mid)
            def _():
                for c in to_end():
                    c.start()

            k = d - jnp.where(mid, LATE_MID, LATE_END)

            @pl.when((k >= 0) & (k < p.count) & p.is_dy(k) & (mid | jnp.logical_not(p.is_attn(k))))
            def _():
                spread_done(k, True)
                partner(k, 1).start()

        work(t)
        first_end = 3 * p.count - 3
        assert first_end not in p.steps[False].values()

        @pl.when((mid & (t == last_mid)) | (jnp.logical_not(mid) & ((t == first_end) | (t == last_end))))
        def _():
            @pl.loop(0, p.count)
            def _(k):
                pl.when(mid | ((t == first_end) == (k < p.count - 2)))(lambda: sends_left(k))

    @pl.loop(0, last_mid + 1)
    def _(t):
        pl.when(mid | (t < p.turns[False]))(lambda: one_turn(t))

    own_first_left(jnp.int32(p.count - 1))
    for mat in (GATE, UP):
        for c in first_copies(mat) + second_copies(mat):
            c.wait_send()

    @pl.when(mid)
    def _():
        for mat in (ATTN, DOWN):
            for c in first_copies(mat) + second_copies(mat):
                c.wait_send()
        for c in to_end() + to_end_down():
            c.wait_send()

    @pl.when(jnp.logical_not(mid))
    def _():
        for c in to_end() + to_end_down():
            c.wait_recv()


def store_kernel(plan, o_attn, o_gate, o_up, grad, *refs):
    p = plan
    stats, al_down, be_down, w_old, (w_attn, w_gate, w_up, w_down), outs = (
        refs[:8], refs[8], refs[9], refs[10], refs[11:15], refs[15:23])
    bounce, w_buf, a_col, in_sem, out_sem, s_sem, wi_sem, wo_sem = refs[23:]
    depth, wide = bounce.shape[0], w_buf.shape[0]

    def cut(ref, i):
        return ref.at[:, i * p.nc:(i + 1) * p.nc]

    def rows(ref, i):
        return ref.at[i * p.mc:(i + 1) * p.mc, :]

    through = [(cut(o_gate, i), cut(w_gate, i)) for i in range(p.ng)]
    if not UP_KEPT:
        through += [(cut(o_up, i), cut(w_up, i)) for i in range(p.ng)]
    loads = [pltpu.make_async_copy(a, bounce.at[i % depth], in_sem.at[i]) for i, (a, _) in enumerate(through)]
    puts = [pltpu.make_async_copy(bounce.at[i % depth], b, out_sem.at[i]) for i, (_, b) in enumerate(through)]
    w_in = [pltpu.make_async_copy(rows(w_old, i), w_buf.at[i % wide], wi_sem.at[i]) for i in range(p.nh)]
    w_out = [pltpu.make_async_copy(w_buf.at[i % wide], rows(w_down, i), wo_sem.at[i]) for i in range(p.nh)]
    for i in range(wide // 2):
        w_in[i].start()
    for c in loads[:depth]:
        c.start()
    copies = [pltpu.make_async_copy(a, b, s_sem.at[i]) for i, (a, b) in enumerate(zip(stats, outs))]
    copies.append(pltpu.make_async_copy(o_attn, w_attn, s_sem.at[8]))
    if UP_KEPT:
        copies += [pltpu.make_async_copy(o_up.at[i], cut(w_up, i), s_sem.at[9 + i]) for i in range(p.ng)]
    for c in copies:
        c.start()
    step_r = min(64, p.mc)
    per = -(-len(through) // p.nh)
    done = 0
    for i in range(p.nh):
        a_col[...] = jnp.broadcast_to(al_down[:, i * p.mc:(i + 1) * p.mc], (LANES, p.mc)).T
        w_in[i].wait()

        @pl.loop(0, p.mc // step_r)
        def _(n):
            at = pl.ds(pl.multiple_of(n * step_r, step_r), step_r)
            a_block = a_col[at, :]
            for c in range(0, p.nc, LANES):
                cols = slice(c, c + LANES)
                w_buf[i % wide, at, cols] = w_buf[i % wide, at, cols] - grad[i, at, cols] * a_block * be_down[:, cols]

        w_out[i].start()
        again = i + wide // 2
        if again < p.nh:
            if again >= wide:
                w_out[again - wide].wait()
            w_in[again].start()
        for j in range(done, min(len(through), done + per)):
            loads[j].wait()
            puts[j].start()
            again = j + depth // 2
            if depth <= again < len(through):
                puts[again - depth].wait()
                loads[again].start()
        done += per
    for i in range(max(0, p.nh - wide), p.nh):
        if i + wide >= p.nh:
            w_out[i].wait()
    for i in range(max(0, len(through) - depth), len(through)):
        puts[i].wait()
    for c in copies:
        c.wait()


def solution(mesh):
    act_spec = P('dp', 'row')
    grad_spec = P('dp', 'col')
    w_spec = P('row', 'col')
    row_spec = P('row')
    col_spec = P('col')
    in_specs = (act_spec, grad_spec, act_spec, grad_spec, grad_spec, act_spec, grad_spec,
                w_spec, w_spec, w_spec, w_spec,
                row_spec, col_spec, row_spec, col_spec, row_spec, col_spec, row_spec, col_spec, P())
    out_specs = (w_spec, row_spec, col_spec) * 4

    def per_device(x_attn, dy_attn, x_mlp, dy_gate, dy_up, h_mlp, dy_out, w_attn, w_gate, w_up, w_down,
                   r_attn, c_attn, r_gate, c_gate, r_up, c_up, r_down, c_down, hyper_params):
        p = Plan(x_mlp, dy_gate, h_mlp, dy_out, mesh)
        stats = [v.reshape(1, -1) for v in (r_attn, c_attn, r_gate, c_gate, r_up, c_up, r_down, c_down)]
        any_spec = pl.BlockSpec(memory_space=pl.ANY)
        vmem_spec = pl.BlockSpec(memory_space=pltpu.VMEM)
        up_spec = vmem_spec if UP_KEPT else any_spec
        row_shapes = []
        for mat in MATS:
            row_shapes += [jax.ShapeDtypeStruct((1, p.rows[mat]), F32), jax.ShapeDtypeStruct((1, p.cols[mat]), F32)]
        w_shapes = [jax.ShapeDtypeStruct((p.rows[mat], p.cols[mat]), F32) for mat in MATS]
        o_shapes = [pltpu.VMEM((p.mc, p.nc), F32), w_shapes[GATE],
                    pltpu.VMEM((p.ng, p.mc, p.nc), F32) if UP_KEPT else w_shapes[UP],
                    pltpu.VMEM((p.pieces, p.mc, p.nc), F32)]
        bufs = [jax.ShapeDtypeStruct((p.n_dy, p.dp - 1, p.tok, p.nc), BF16),
                jax.ShapeDtypeStruct((p.n_x, p.dp - 1, p.tok, p.mc), BF16)]
        rest = jax.ShapeDtypeStruct((p.mc - p.first_rows, p.nc), F32)
        dma = pltpu.SemaphoreType.DMA
        lines = p.count + PARTS - 1
        scratch = [
            pltpu.VMEM((p.dp, p.mc, p.tok), BF16),
            pltpu.VMEM((p.dp, p.tok, p.mc), BF16),
            pltpu.VMEM((p.dp, p.tok, p.nc), BF16),
            pltpu.VMEM((3, p.mc, p.nc), F32),
            pltpu.VMEM((p.mc, LANES), F32),
            pltpu.VMEM((p.pieces, 1, p.mc), F32),
            pltpu.VMEM((p.pieces, 1, p.nc), F32),
            pltpu.VMEM((p.nh, p.mc, LANES), F32),
            pltpu.VMEM((1, p.rows[DOWN]), F32),
            pltpu.VMEM((4, 8, LANES), F32),
        ]
        scratch += [pltpu.VMEM((1, p.cols[mat]), F32) for mat in MATS]
        scratch += [pltpu.VMEM(v.shape, F32) for v in row_shapes]
        scratch += [pltpu.VMEM((2, 1, p.rows[mat]), F32) for mat in MATS]
        scratch += [pltpu.VMEM((4, 1, p.cols[mat]), F32) for mat in MATS]
        scratch += [
            pltpu.VMEM((4, 8, 3, 8, LANES), F32),
            dma((lines, 5)), dma((lines, p.dp - 1)),
            dma((lines, p.dp - 1)), dma((lines, p.dp - 1)),
            dma((p.n_dy, 2)), dma((p.n_dy, 2)),
            dma((4, 4)), dma((4, 4)), dma((4, 8)), dma((4, 8)),
            dma((7,)), dma((7,)),
            dma((p.dp,)), dma((3,)), dma((3,)), dma((8,)),
        ]
        out = pl.pallas_call(
            functools.partial(gather_kernel, p),
            out_shape=o_shapes + [pltpu.VMEM(v.shape, F32) for v in row_shapes + row_shapes[-2:]] + [rest] + bufs,
            in_specs=[any_spec] * 19 + [pl.BlockSpec(memory_space=pltpu.SMEM)],
            out_specs=[vmem_spec, any_spec, up_spec, vmem_spec] + [vmem_spec] * 10 + [any_spec] * 3,
            scratch_shapes=scratch,
            compiler_params=pltpu.CompilerParams(collective_id=0, has_side_effects=True, vmem_limit_bytes=VMEM_LIMIT),
        )(x_attn, dy_attn, x_mlp, dy_gate, dy_up, h_mlp, dy_out, w_attn, w_gate, w_up, w_down, *stats, hyper_params)
        res = pl.pallas_call(
            functools.partial(store_kernel, p),
            out_shape=w_shapes + row_shapes,
            in_specs=[vmem_spec, any_spec, up_spec, vmem_spec] + [vmem_spec] * 10 + [any_spec],
            out_specs=[any_spec] * 12,
            scratch_shapes=[pltpu.VMEM((DEPTH, p.mc, p.nc), F32), pltpu.VMEM((WIDE, p.mc, p.nc), F32),
                            pltpu.VMEM((p.mc, LANES), F32), dma((2 * p.ng,)), dma((2 * p.ng,)), dma((9 + p.ng,)),
                            dma((p.nh,)), dma((p.nh,))],
            compiler_params=pltpu.CompilerParams(vmem_limit_bytes=STORE_LIMIT),
            cost_estimate=pl.CostEstimate(flops=60_000_000_000, bytes_accessed=90_000_000, transcendentals=0),
        )(*[pltpu.with_memory_space_constraint(v, pltpu.VMEM) if i not in HBM_KEPT else v for i, v in enumerate(out[:14])],
          w_down)
        z = lax.axis_index('dp')
        got = lax.ppermute(out[14], 'dp', [(1, 0), (2, 3)])
        rows = jnp.where((z == 1) | (z == 2), out[14], got)
        res = [lax.dynamic_update_slice(res[0], rows, (p.first_rows, 0))] + list(res[1:])
        result = []
        for mat in MATS:
            result += [res[mat], res[4 + 2 * mat].reshape(-1), res[5 + 2 * mat].reshape(-1)]
        return tuple(result)

    return jax.shard_map(per_device, mesh=mesh, in_specs=in_specs, out_specs=out_specs, check_vma=False)
```
